16 devices in a mesh: dp: 2 (over z), tp: 8 (over y, x, core).
Axes of the slice: x: 2, y: 2, z: 2, core: 2. Of those that a mesh axis runs over, the one named last changes fastest.
Arguments:
- hidden: bfloat16 [6, 1536, 2048], P('dp', 'tp'), parts along dimension 0
- grad_out: bfloat16 [6, 1536, 2048], P('dp', 'tp'), parts along dimension 0
- prefix_len: int32 [6], P('dp'), parts along dimension 0
- valid_len: int32 [6], P('dp'), parts along dimension 0
- attn_norm: bfloat16 [2048], replicated
- w_query: bfloat16 [2048, 2048], P(None, 'tp')
- w_key: bfloat16 [2048, 256], replicated
- w_value: bfloat16 [2048, 256], replicated
- w_out: bfloat16 [2048, 2048], P('tp')
- mlp_norm: bfloat16 [2048], replicated
- w_gate: bfloat16 [2048, 16384], P(None, 'tp')
- w_up: bfloat16 [2048, 16384], P(None, 'tp')
- w_down: bfloat16 [16384, 2048], P('tp')
Outputs:
- output 1: bfloat16 [6, 1536, 2048], P('dp', 'tp'), parts along dimension 0
- output 2: bfloat16 [6, 1536, 2048], P('dp', 'tp'), parts along dimension 0
- output 3: float32 [4096], P('dp'), parts along dimension 0
- output 4: float32 [4096, 2048], P('dp', 'tp'), parts along dimension 0
- output 5: float32 [4096, 256], P('dp'), parts along dimension 0
- output 6: float32 [4096, 256], P('dp'), parts along dimension 0
- output 7: float32 [4096, 2048], P(('dp', 'tp')), parts along dimension 0
- output 8: float32 [4096], P('dp'), parts along dimension 0
- output 9: float32 [4096, 16384], P('dp', 'tp'), parts along dimension 0
- output 10: float32 [4096, 16384], P('dp', 'tp'), parts along dimension 0
- output 11: float32 [32768, 2048], P(('dp', 'tp')), parts along dimension 0
There are 2 independent parts. The reference program is written for one: setup_inputs(seed, part) draws one part's arguments, and reference() takes and returns one part's arrays. A program takes and returns all parts, laid end to end along the dimension named above; an argument that names none is the same for every part.
All inputs are finite; a program needn't handle non-finite values.
Results may differ from the reference program's by a relative error of at most 0.02.
Values are sent between devices in bfloat16 or wider.
A program may use at most 1 GiB of HBM per device.

```python
import math
import jax
import jax.numpy as jnp
from jax import lax

BATCH_SIZE = 3
SEQ_LEN = 1536
MODEL_DIM = 2048
NUM_HEADS = 8
HEAD_DIM = 256
FFN_DIM = 16384


def rms_norm(x_in, gain):
    x_f = x_in.astype(jnp.float32)
    inv_rms = lax.rsqrt(jnp.mean(x_f * x_f, axis=-1, keepdims=True) + 1e-6)
    return (x_f * inv_rms * (1.0 + gain.astype(jnp.float32))).astype(jnp.bfloat16)


def rope_tables(positions, head_dim):
    half_dim = head_dim // 2
    exponent = jnp.arange(half_dim, dtype=jnp.float32) * (2.0 / head_dim)
    inv_freq = jnp.exp(exponent * (-math.log(10000.0)))
    angles = positions.astype(jnp.float32)[:, None] * inv_freq[None, :]
    return jnp.cos(angles), jnp.sin(angles)


def apply_rope(x_f, cos_t, sin_t):
    half_dim = x_f.shape[-1] // 2
    first = x_f[..., :half_dim]
    second = x_f[..., half_dim:]
    return jnp.concatenate([first * cos_t - second * sin_t, second * cos_t + first * sin_t], axis=-1)


def attend_one(operands):
    query, keys, values, prefix_count, valid_count = operands
    seq_len = query.shape[0]
    scale = query.shape[-1] ** -0.5
    scores = jnp.einsum("qhd,kd->hqk", query.astype(jnp.float32), keys.astype(jnp.float32)) * scale
    q_pos = jnp.arange(seq_len)[:, None]
    k_pos = jnp.arange(seq_len)[None, :]
    visible = (k_pos < valid_count) & ((k_pos < prefix_count) | (k_pos <= q_pos))
    scores = jnp.where(visible[None], scores, -1e30)
    probs = jax.nn.softmax(scores, axis=-1).astype(jnp.bfloat16)
    mixed = jnp.einsum("hqk,kd->qhd", probs.astype(jnp.float32), values.astype(jnp.float32))
    return mixed.astype(jnp.bfloat16)


def layer_forward(hidden, prefix_len, valid_len, weights):
    attn_norm, w_query, w_key, w_value, w_out, mlp_norm, w_gate, w_up, w_down = weights
    batch, seq_len, model_dim = hidden.shape
    head_dim = w_key.shape[1]
    num_heads = w_query.shape[1] // head_dim
    num_rows = batch * seq_len
    normed = rms_norm(hidden, attn_norm).reshape(num_rows, model_dim)
    cos_t, sin_t = rope_tables(jnp.arange(seq_len), head_dim)
    q_raw = jnp.dot(normed, w_query, preferred_element_type=jnp.float32).reshape(batch, seq_len, num_heads, head_dim)
    query = apply_rope(q_raw, cos_t[:, None, :], sin_t[:, None, :]).astype(jnp.bfloat16)
    k_raw = jnp.dot(normed, w_key, preferred_element_type=jnp.float32).reshape(batch, seq_len, head_dim)
    keys = apply_rope(k_raw, cos_t, sin_t).astype(jnp.bfloat16)
    values = jnp.dot(normed, w_value, preferred_element_type=jnp.float32).astype(jnp.bfloat16).reshape(batch, seq_len, head_dim)
    mixed = lax.map(jax.checkpoint(attend_one), (query, keys, values, prefix_len, valid_len))
    attn_out = jnp.dot(mixed.reshape(num_rows, num_heads * head_dim), w_out, preferred_element_type=jnp.float32)
    resid = (hidden.astype(jnp.float32) + attn_out.reshape(batch, seq_len, model_dim)).astype(jnp.bfloat16)
    gated_in = rms_norm(resid, mlp_norm).reshape(num_rows, model_dim)
    gate = jnp.dot(gated_in, w_gate, preferred_element_type=jnp.float32)
    upper = jnp.dot(gated_in, w_up, preferred_element_type=jnp.float32)
    act = (jax.nn.gelu(gate, approximate=True) * upper).astype(jnp.bfloat16)
    mlp_out = jnp.dot(act, w_down, preferred_element_type=jnp.float32)
    return (resid.astype(jnp.float32) + mlp_out.reshape(batch, seq_len, model_dim)).astype(jnp.bfloat16)


def setup_inputs(seed: int = 0, part: int = 0) -> dict:
    base_key = jax.random.key(seed)
    part_keys = jax.random.split(jax.random.fold_in(base_key, part), 4)
    shared_keys = jax.random.split(base_key, 9)
    q_dim = NUM_HEADS * HEAD_DIM
    act_shape = (BATCH_SIZE, SEQ_LEN, MODEL_DIM)
    hidden = (0.25 * jax.random.normal(part_keys[0], act_shape, jnp.float32)).astype(jnp.bfloat16)
    grad_out = jax.random.normal(part_keys[1], act_shape, jnp.float32).astype(jnp.bfloat16)
    valid_len = jax.random.randint(part_keys[2], (BATCH_SIZE,), (3 * SEQ_LEN) // 4, SEQ_LEN + 1, dtype=jnp.int32)
    valid_len = valid_len.at[0].set(SEQ_LEN)
    prefix_len = jax.random.randint(part_keys[3], (BATCH_SIZE,), SEQ_LEN // 8, (3 * SEQ_LEN) // 4 + 1, dtype=jnp.int32)
    in_scale = 1.0 / math.sqrt(MODEL_DIM)
    out_scale = math.sqrt(SEQ_LEN / (64.0 * q_dim))
    down_scale = 1.0 / math.sqrt(FFN_DIM)
    attn_norm = (0.3 * jax.random.normal(shared_keys[0], (MODEL_DIM,), jnp.float32)).astype(jnp.bfloat16)
    w_query = (in_scale * jax.random.normal(shared_keys[1], (MODEL_DIM, q_dim), jnp.float32)).astype(jnp.bfloat16)
    w_key = (in_scale * jax.random.normal(shared_keys[2], (MODEL_DIM, HEAD_DIM), jnp.float32)).astype(jnp.bfloat16)
    w_value = (in_scale * jax.random.normal(shared_keys[3], (MODEL_DIM, HEAD_DIM), jnp.float32)).astype(jnp.bfloat16)
    w_out = (out_scale * jax.random.normal(shared_keys[4], (q_dim, MODEL_DIM), jnp.float32)).astype(jnp.bfloat16)
    mlp_norm = (0.3 * jax.random.normal(shared_keys[5], (MODEL_DIM,), jnp.float32)).astype(jnp.bfloat16)
    w_gate = (in_scale * jax.random.normal(shared_keys[6], (MODEL_DIM, FFN_DIM), jnp.float32)).astype(jnp.bfloat16)
    w_up = (in_scale * jax.random.normal(shared_keys[7], (MODEL_DIM, FFN_DIM), jnp.float32)).astype(jnp.bfloat16)
    w_down = (down_scale * jax.random.normal(shared_keys[8], (FFN_DIM, MODEL_DIM), jnp.float32)).astype(jnp.bfloat16)
    return {"hidden": hidden, "grad_out": grad_out, "prefix_len": prefix_len, "valid_len": valid_len, "attn_norm": attn_norm, "w_query": w_query, "w_key": w_key, "w_value": w_value, "w_out": w_out, "mlp_norm": mlp_norm, "w_gate": w_gate, "w_up": w_up, "w_down": w_down}


def reference(hidden, grad_out, prefix_len, valid_len, attn_norm, w_query, w_key, w_value, w_out, mlp_norm, w_gate, w_up, w_down):
    weights = (attn_norm, w_query, w_key, w_value, w_out, mlp_norm, w_gate, w_up, w_down)

    def forward(hidden_in, weights_in):
        return layer_forward(hidden_in, prefix_len, valid_len, weights_in)

    hidden_out, pullback = jax.vjp(forward, hidden, weights)
    grad_hidden, grad_weights = pullback(grad_out)
    g_attn_norm, g_query, g_key, g_value, g_out, g_mlp_norm, g_gate, g_up, g_down = grad_weights
    return (hidden_out, grad_hidden, g_attn_norm.astype(jnp.float32), g_query.astype(jnp.float32), g_key.astype(jnp.float32), g_value.astype(jnp.float32), g_out.astype(jnp.float32), g_mlp_norm.astype(jnp.float32), g_gate.astype(jnp.float32), g_up.astype(jnp.float32), g_down.astype(jnp.float32))
```

```python
import functools
import math
import jax
import jax.numpy as jnp
from jax import lax
from jax.experimental import pallas as pl
from jax.experimental.pallas import tpu as pltpu
from jax.sharding import PartitionSpec as P

NORM_EPS = 1e-6
BF16 = jnp.bfloat16
F32 = jnp.float32
GELU_C = math.sqrt(2.0 / math.pi)
GELU_K = 0.044715
MASKED = -1e30
NT = (((1,), (1,)), ((), ()))
TN = (((0,), (0,)), ((), ()))


def rms_norm(x_in, gain):
    x_f = x_in.astype(F32)
    inv_rms = lax.rsqrt(jnp.mean(x_f * x_f, axis=-1, keepdims=True) + NORM_EPS)
    return (x_f * inv_rms * (1.0 + gain)).astype(BF16)


def rope_tables(positions, head_dim):
    half_dim = head_dim // 2
    exponent = jnp.arange(half_dim, dtype=F32) * (2.0 / head_dim)
    inv_freq = jnp.exp(exponent * (-math.log(10000.0)))
    angles = positions.astype(F32)[:, None] * inv_freq[None, :]
    return jnp.cos(angles), jnp.sin(angles)


def apply_rope(x_f, cos_t, sin_t):
    half_dim = x_f.shape[-1] // 2
    first = x_f[..., :half_dim]
    second = x_f[..., half_dim:]
    return jnp.concatenate([first * cos_t - second * sin_t, second * cos_t + first * sin_t], axis=-1)


def dot_nn(a, b):
    return jnp.dot(a, b, preferred_element_type=F32)


def dot_nt(a, b):
    return lax.dot_general(a, b, NT, preferred_element_type=F32)


def dot_tn(a, b):
    return lax.dot_general(a, b, TN, preferred_element_type=F32)


def swap(x, bit):
    return lax.ppermute(x, "tp", [(t, t ^ bit) for t in range(8)])


def gather_relative(own):
    half = own.shape[0] // 2
    part = swap(own, 1)
    side = swap(own, 2)
    back = swap(own, 4)
    diag = jnp.concatenate([swap(side[:half], 4), swap(back[half:], 2)], axis=0)
    return [own, part, side, swap(side, 1), back, swap(back, 1), diag, swap(diag, 1)]


def scatter_relative(parts):
    def join(kept, came):
        return kept.astype(F32) + came.astype(F32)

    near = [join(parts[s], swap(parts[s + 1], 1)) for s in (0, 2, 4, 6)]
    own, side, back, diag = near
    half = diag.shape[0] // 2
    diag = diag.astype(parts[0].dtype)
    came_side = swap(diag[:half], 2)
    came_back = swap(diag[half:], 4)
    back = jnp.concatenate([join(back[:half], came_side), back[half:]], axis=0).astype(parts[0].dtype)
    side = jnp.concatenate([side[:half], join(side[half:], came_back)], axis=0).astype(parts[0].dtype)
    return own + swap(side, 2).astype(F32) + swap(back, 4).astype(F32)


def all_sum_small(x):
    for bit in (1, 2, 4):
        x = x + swap(x, bit)
    return x


def attn_fwd_kernel(lens_ref, kpos_ref, q_ref, k_ref, v_ref, o_ref, p_ref):
    heads, shard, head_dim = q_ref.shape
    tp = k_ref.shape[0]
    total = tp * shard
    s_id = pl.program_id(0)
    prefix = lens_ref[0, s_id]
    valid = lens_ref[1, s_id]
    first = lens_ref[2, 0] * shard
    keys = k_ref[...].reshape(total, head_dim)
    values = v_ref[...].reshape(total, head_dim)
    q_pos = first + lax.broadcasted_iota(jnp.int32, (shard, 1), 0)
    visible = kpos_ref[...] < jnp.minimum(valid, jnp.maximum(prefix, q_pos + 1))
    scale = head_dim ** -0.5
    query = q_ref[...].reshape(heads * shard, head_dim)
    scores = dot_nt(query, keys)
    for h in range(heads):
        rows = slice(h * shard, (h + 1) * shard)
        s = jnp.where(visible, scores[rows] * scale, MASKED)
        e = jnp.exp(s - jnp.max(s, axis=-1, keepdims=True))
        p_ref[rows, :] = (e / jnp.sum(e, axis=-1, keepdims=True)).astype(BF16)
    mixed = dot_nn(p_ref[...], values).astype(BF16)
    for h in range(heads):
        o_ref[:, h * head_dim:(h + 1) * head_dim] = mixed[h * shard:(h + 1) * shard]


def attn_bwd_kernel(lens_ref, q_ref, k_ref, v_ref, do_ref, dq_ref, dk_ref, dv_ref, dkv_acc):
    heads, shard, head_dim = q_ref.shape
    tp = k_ref.shape[0]
    total = tp * shard
    rows = heads * shard
    s_id = pl.program_id(0)
    g_id = pl.program_id(1)
    prefix = lens_ref[0, s_id]
    valid = lens_ref[1, s_id]
    first = lens_ref[2, 0] * shard
    keys = k_ref[...].reshape(total, head_dim)
    values = v_ref[...].reshape(total, head_dim)
    query = q_ref[...].reshape(rows, head_dim)
    d_out = jnp.concatenate([do_ref[:, h * head_dim:(h + 1) * head_dim] for h in range(heads)], axis=0)
    scale = head_dim ** -0.5
    step = lax.broadcasted_iota(jnp.int32, (shard, 1), 0)
    k_pos = jnp.concatenate([step + lens_ref[3 + r, 0] for r in range(tp)], axis=0)
    q_pos = first + lax.rem(lax.broadcasted_iota(jnp.int32, (1, rows), 1), shard)
    limit = jnp.minimum(valid, jnp.maximum(prefix, q_pos + 1))
    s = jnp.where(k_pos < limit, dot_nt(keys, query) * scale, MASKED)
    e = jnp.exp(s - jnp.max(s, axis=0, keepdims=True))
    p = e * (1.0 / jnp.sum(e, axis=0, keepdims=True))
    d_p = dot_nt(values, d_out)
    delta = jnp.sum(p * d_p, axis=0, keepdims=True)
    d_s = (p * (d_p - delta) * scale).astype(BF16)
    d_v = dot_nn(p.astype(BF16), d_out)
    d_k = dot_nn(d_s, query)
    dq_ref[...] = dot_tn(d_s, keys).astype(BF16).reshape(heads, shard, head_dim)

    @pl.when(g_id == 0)
    def _():
        dkv_acc[0] = d_k
        dkv_acc[1] = d_v

    @pl.when(g_id > 0)
    def _():
        dkv_acc[0] += d_k
        dkv_acc[1] += d_v

    @pl.when(g_id == pl.num_programs(1) - 1)
    def _():
        dk_ref[...] = dkv_acc[0].astype(BF16).reshape(tp, shard, head_dim)
        dv_ref[...] = dkv_acc[1].astype(BF16).reshape(tp, shard, head_dim)


def attention_forward(lens, k_pos, query, kv_all, batch, group=4):
    heads, rows, head_dim = query.shape
    tp = kv_all.shape[0]
    shard = rows // batch
    total = tp * shard
    q_spec = pl.BlockSpec((group, shard, head_dim), lambda s, g, *_: (g, s, 0))
    return pl.pallas_call(
        attn_fwd_kernel,
        out_shape=jax.ShapeDtypeStruct((rows, heads * head_dim), BF16),
        grid_spec=pltpu.PrefetchScalarGridSpec(
            num_scalar_prefetch=1, grid=(batch, heads // group),
            in_specs=[pl.BlockSpec((1, total), lambda s, g, *_: (0, 0)), q_spec,
                      pl.BlockSpec((tp, shard, head_dim), lambda s, g, *_: (0, s, 0)),
                      pl.BlockSpec((tp, shard, head_dim), lambda s, g, *_: (0, s, 1))],
            out_specs=pl.BlockSpec((shard, group * head_dim), lambda s, g, *_: (s, g)),
            scratch_shapes=[pltpu.VMEM((group * shard, total), BF16)]),
        compiler_params=pltpu.CompilerParams(dimension_semantics=("arbitrary", "arbitrary"), vmem_limit_bytes=48 << 20),
        cost_estimate=pl.CostEstimate(flops=4 * heads * rows * total * head_dim, bytes_accessed=12 << 20, transcendentals=heads * rows * total),
        name="attn_fwd",
    )(lens, k_pos, query, kv_all, kv_all)


def attention_backward(lens, query, kv_all, d_mixed, batch, group=4):
    heads, rows, head_dim = query.shape
    tp = kv_all.shape[0]
    shard = rows // batch
    total = tp * shard
    q_spec = pl.BlockSpec((group, shard, head_dim), lambda s, g, *_: (g, s, 0))
    kv_specs = [pl.BlockSpec((tp, shard, head_dim), lambda s, g, *_: (0, s, 0)),
                pl.BlockSpec((tp, shard, head_dim), lambda s, g, *_: (0, s, 1))]
    kv_out = pl.BlockSpec((tp, shard, head_dim), lambda s, g, *_: (0, s, 0))
    return pl.pallas_call(
        attn_bwd_kernel,
        out_shape=(jax.ShapeDtypeStruct((heads, rows, head_dim), BF16),
                   jax.ShapeDtypeStruct((tp, rows, head_dim), BF16),
                   jax.ShapeDtypeStruct((tp, rows, head_dim), BF16)),
        grid_spec=pltpu.PrefetchScalarGridSpec(
            num_scalar_prefetch=1, grid=(batch, heads // group),
            in_specs=[q_spec] + kv_specs + [pl.BlockSpec((shard, group * head_dim), lambda s, g, *_: (s, g))],
            out_specs=(q_spec, kv_out, kv_out),
            scratch_shapes=[pltpu.VMEM((2, total, head_dim), F32)]),
        compiler_params=pltpu.CompilerParams(dimension_semantics=("arbitrary", "arbitrary"), vmem_limit_bytes=56 << 20),
        cost_estimate=pl.CostEstimate(flops=10 * heads * rows * total * head_dim, bytes_accessed=20 << 20, transcendentals=heads * rows * total),
        name="attn_bwd",
    )(lens, query, kv_all, kv_all, d_mixed)


def gated_kernel(z_ref, g_ref, wg_ref, wu_ref, wd_ref, act_ref, dg_ref, du_ref, *, sub):
    for lo in range(0, z_ref.shape[0], sub):
        rows = slice(lo, lo + sub)
        gate = dot_nn(z_ref[rows], wg_ref[...])
        upper = dot_nn(z_ref[rows], wu_ref[...])
        d_act = dot_nt(g_ref[rows], wd_ref[...]).astype(BF16).astype(F32)
        sq = gate * gate
        th = jnp.tanh(gate * (GELU_C + (GELU_C * GELU_K) * sq))
        half = 0.5 + 0.5 * th
        gelu = gate * half
        slope = half + gate * (0.5 - 0.5 * (th * th)) * (GELU_C + (3.0 * GELU_C * GELU_K) * sq)
        act_ref[rows, :] = (gelu * upper).astype(BF16)
        du_ref[rows, :] = (d_act * gelu).astype(BF16)
        dg_ref[rows, :] = (d_act * upper * slope).astype(BF16)


def gated_layer(z_all, grad_all, w_gate, w_up, w_down, bm=1152, bn=512, sub=576):
    rows, dim = z_all.shape
    width = w_gate.shape[1]
    lhs = pl.BlockSpec((bm, dim), lambda i, j: (i, 0))
    col = pl.BlockSpec((dim, bn), lambda i, j: (0, j))
    out = pl.BlockSpec((bm, bn), lambda i, j: (i, j))
    shape = jax.ShapeDtypeStruct((rows, width), BF16)
    return pl.pallas_call(
        functools.partial(gated_kernel, sub=sub),
        out_shape=(shape, shape, shape),
        grid=(rows // bm, width // bn),
        in_specs=[lhs, lhs, col, col, pl.BlockSpec((bn, dim), lambda i, j: (j, 0))],
        out_specs=(out, out, out),
        compiler_params=pltpu.CompilerParams(dimension_semantics=("arbitrary", "arbitrary"), vmem_limit_bytes=58 << 20),
        cost_estimate=pl.CostEstimate(flops=6 * rows * dim * width, bytes_accessed=200 << 20, transcendentals=rows * width),
        name="gated",
    )(z_all, grad_all, w_gate, w_up, w_down)


def pair_kernel(a_ref, b_ref, wa_ref, wb_ref, o_ref):
    o_ref[...] = (dot_nt(a_ref[...], wa_ref[...]) + dot_nt(b_ref[...], wb_ref[...])).astype(BF16)


def pair_back(a, b, w_a, w_b, bm=1152, bn=512):
    rows, width = a.shape
    dim = w_a.shape[0]
    lhs = pl.BlockSpec((bm, width), lambda i, j: (i, 0))
    row = pl.BlockSpec((bn, width), lambda i, j: (j, 0))
    return pl.pallas_call(
        pair_kernel,
        out_shape=jax.ShapeDtypeStruct((rows, dim), BF16),
        grid=(rows // bm, dim // bn),
        in_specs=[lhs, lhs, row, row],
        out_specs=pl.BlockSpec((bm, bn), lambda i, j: (i, j)),
        compiler_params=pltpu.CompilerParams(dimension_semantics=("arbitrary", "arbitrary"), vmem_limit_bytes=56 << 20),
        cost_estimate=pl.CostEstimate(flops=4 * rows * dim * width, bytes_accessed=140 << 20, transcendentals=0),
        name="pair_back",
    )(a, b, w_a, w_b)


def solution(mesh):
    tp_size = mesh.shape["tp"]
    act_spec = P("dp", "tp", None)
    in_specs = (act_spec, act_spec, P("dp"), P("dp"), P(None), P(None, "tp"), P(None, None), P(None, None), P("tp", None), P(None), P(None, "tp"), P(None, "tp"), P("tp", None))
    out_specs = (act_spec, act_spec, P("dp"), P("dp", "tp"), P("dp", None), P("dp", None), P(("dp", "tp"), None), P("dp"), P("dp", "tp"), P("dp", "tp"), P(("dp", "tp"), None))

    def local_layer(hidden, grad_out, prefix_len, valid_len, attn_norm, w_query, w_key, w_value, w_out, mlp_norm, w_gate, w_up, w_down):
        batch, shard, dim = hidden.shape
        head_dim = w_key.shape[1]
        rows = batch * shard
        me = lax.axis_index("tp")
        starts = (me ^ jnp.arange(tp_size, dtype=jnp.int32)) * shard
        k_pos = (starts[:, None] + jnp.arange(shard, dtype=jnp.int32)).reshape(1, tp_size * shard)
        lens = jnp.concatenate([jnp.stack([prefix_len, valid_len, jnp.full((batch,), me, jnp.int32)]),
                                jnp.broadcast_to(starts[:, None], (tp_size, batch))])
        cos_t, sin_t = rope_tables(me * shard + jnp.arange(shard), head_dim)
        cos_t, sin_t = jnp.tile(cos_t, (batch, 1)), jnp.tile(sin_t, (batch, 1))

        def rope(raw_proj):
            return apply_rope(raw_proj, cos_t, sin_t).astype(BF16)

        wq_all = lax.all_gather(w_query, "tp", axis=0)
        hidden = hidden.reshape(rows, dim)
        grad_out = grad_out.reshape(rows, dim)
        normed, norm1_pull = jax.vjp(rms_norm, hidden, attn_norm.astype(F32))
        keys, key_pull = jax.vjp(rope, dot_nn(normed, w_key))
        values = dot_nn(normed, w_value).astype(BF16)
        kv_all = jnp.stack(gather_relative(jnp.concatenate([keys, values], axis=1)))
        wo_all = lax.all_gather(w_out, "tp", axis=0, tiled=True)
        grad_all = lax.all_gather(grad_out, "tp", axis=0, tiled=True)

        q_raw = jnp.einsum("td,hde->hte", normed, wq_all, preferred_element_type=F32)
        query, query_pull = jax.vjp(rope, q_raw)
        mixed = attention_forward(lens, k_pos, query, kv_all, batch)
        attn_out = dot_nn(mixed, wo_all)
        resid = (hidden.astype(F32) + attn_out).astype(BF16)
        gated_in, norm2_pull = jax.vjp(rms_norm, resid, mlp_norm.astype(F32))
        gated_all = lax.all_gather(gated_in, "tp", axis=0, tiled=True)

        act, d_gate, d_upper = gated_layer(gated_all, grad_all, w_gate, w_up, w_down)
        d_gated_part = pair_back(d_gate, d_upper, w_gate, w_up)
        d_gated = lax.psum_scatter(d_gated_part, "tp", scatter_dimension=0, tiled=True)
        mlp_part = dot_nn(act, w_down).astype(BF16)
        mlp_sum = lax.psum_scatter(mlp_part, "tp", scatter_dimension=0, tiled=True)
        hidden_out = (resid.astype(F32) + mlp_sum.astype(F32)).astype(BF16)
        g_down = dot_tn(act, grad_all)
        g_gate = dot_tn(gated_all, d_gate)
        g_up = dot_tn(gated_all, d_upper)

        d_resid_norm, g_mlp_norm_part = norm2_pull(d_gated)
        d_resid = (grad_out.astype(F32) + d_resid_norm.astype(F32)).astype(BF16)
        g_out = lax.psum_scatter(dot_tn(mixed, d_resid), "tp", scatter_dimension=0, tiled=True)
        d_mixed = dot_nt(d_resid, wo_all).astype(BF16)
        d_query, d_keys_part, d_values_part = attention_backward(lens, query, kv_all, d_mixed, batch)
        d_keys = scatter_relative(d_keys_part).astype(BF16)
        d_values = scatter_relative(d_values_part).astype(BF16)
        d_q_raw = query_pull(d_query)[0].astype(BF16)
        d_k_raw = key_pull(d_keys)[0].astype(BF16)
        g_query = lax.psum_scatter(jnp.einsum("td,hte->hde", normed, d_q_raw, preferred_element_type=F32), "tp", scatter_dimension=0, tiled=False)
        g_key = lax.psum(dot_tn(normed, d_k_raw), "tp")
        g_value = lax.psum(dot_tn(normed, d_values), "tp")
        d_normed = (jnp.einsum("hte,hde->td", d_q_raw, wq_all, preferred_element_type=F32)
                    + dot_nt(d_k_raw, w_key) + dot_nt(d_values, w_value)).astype(BF16)
        d_hidden_norm, g_attn_norm_part = norm1_pull(d_normed)
        grad_hidden = (d_resid.astype(F32) + d_hidden_norm.astype(F32)).astype(BF16)
        g_norms = all_sum_small(jnp.stack([g_attn_norm_part, g_mlp_norm_part]))
        full = (batch, shard, dim)
        return (hidden_out.reshape(full), grad_hidden.reshape(full), g_norms[0], g_query, g_key, g_value, g_out, g_norms[1], g_gate, g_up, g_down)

    return jax.shard_map(local_layer, mesh=mesh, in_specs=in_specs, out_specs=out_specs, check_vma=False)
```

```python
import functools
import math
import jax
import jax.numpy as jnp
from jax import lax
from jax.experimental import pallas as pl
from jax.experimental.pallas import tpu as pltpu
from jax.sharding import PartitionSpec as P

NORM_EPS = 1e-6
BF16 = jnp.bfloat16
F32 = jnp.float32
GELU_C = math.sqrt(2.0 / math.pi)
GELU_K = 0.044715
MASKED = -1e30
NT = (((1,), (1,)), ((), ()))
TN = (((0,), (0,)), ((), ()))


def rms_norm(x_in, gain):
    x_f = x_in.astype(F32)
    inv_rms = lax.rsqrt(jnp.mean(x_f * x_f, axis=-1, keepdims=True) + NORM_EPS)
    return (x_f * inv_rms * (1.0 + gain)).astype(BF16)


def rope_tables(positions, head_dim):
    half_dim = head_dim // 2
    exponent = jnp.arange(half_dim, dtype=F32) * (2.0 / head_dim)
    inv_freq = jnp.exp(exponent * (-math.log(10000.0)))
    angles = positions.astype(F32)[:, None] * inv_freq[None, :]
    return jnp.cos(angles), jnp.sin(angles)


def apply_rope(x_f, cos_t, sin_t):
    half_dim = x_f.shape[-1] // 2
    first = x_f[..., :half_dim]
    second = x_f[..., half_dim:]
    return jnp.concatenate([first * cos_t - second * sin_t, second * cos_t + first * sin_t], axis=-1)


def dot_nn(a, b):
    return jnp.dot(a, b, preferred_element_type=F32)


def dot_nt(a, b):
    return lax.dot_general(a, b, NT, preferred_element_type=F32)


def dot_tn(a, b):
    return lax.dot_general(a, b, TN, preferred_element_type=F32)


def swap(x, bit):
    return lax.ppermute(x, "tp", [(t, t ^ bit) for t in range(8)])


def gather_relative(own):
    half = own.shape[0] // 2
    part = swap(own, 1)
    side = swap(own, 2)
    back = swap(own, 4)
    diag = jnp.concatenate([swap(side[:half], 4), swap(back[half:], 2)], axis=0)
    return [own, part, side, swap(side, 1), back, swap(back, 1), diag, swap(diag, 1)]


def scatter_relative(parts):
    def join(kept, came):
        return kept.astype(F32) + came.astype(F32)

    near = [join(parts[s], swap(parts[s + 1], 1)) for s in (0, 2, 4, 6)]
    own, side, back, diag = near
    half = diag.shape[0] // 2
    diag = diag.astype(parts[0].dtype)
    came_side = swap(diag[:half], 2)
    came_back = swap(diag[half:], 4)
    back = jnp.concatenate([join(back[:half], came_side), back[half:]], axis=0).astype(parts[0].dtype)
    side = jnp.concatenate([side[:half], join(side[half:], came_back)], axis=0).astype(parts[0].dtype)
    return own + swap(side, 2).astype(F32) + swap(back, 4).astype(F32)


def all_sum_small(x):
    for bit in (1, 2, 4):
        x = x + swap(x, bit)
    return x


def attn_fwd_kernel(lens_ref, kpos_ref, q_ref, k_ref, v_ref, o_ref, p_ref):
    heads, shard, head_dim = q_ref.shape
    tp = k_ref.shape[0]
    total = tp * shard
    s_id = pl.program_id(0)
    prefix = lens_ref[0, s_id]
    valid = lens_ref[1, s_id]
    first = lens_ref[2, 0] * shard
    keys = k_ref[...].reshape(total, head_dim)
    values = v_ref[...].reshape(total, head_dim)
    q_pos = first + lax.broadcasted_iota(jnp.int32, (shard, 1), 0)
    visible = kpos_ref[...] < jnp.minimum(valid, jnp.maximum(prefix, q_pos + 1))
    scale = head_dim ** -0.5
    query = q_ref[...].reshape(heads * shard, head_dim)
    scores = dot_nt(query, keys)
    for h in range(heads):
        rows = slice(h * shard, (h + 1) * shard)
        s = jnp.where(visible, scores[rows] * scale, MASKED)
        e = jnp.exp(s - jnp.max(s, axis=-1, keepdims=True))
        p_ref[rows, :] = (e / jnp.sum(e, axis=-1, keepdims=True)).astype(BF16)
    mixed = dot_nn(p_ref[...], values).astype(BF16)
    for h in range(heads):
        o_ref[:, h * head_dim:(h + 1) * head_dim] = mixed[h * shard:(h + 1) * shard]


def attn_bwd_kernel(lens_ref, q_ref, k_ref, v_ref, do_ref, dq_ref, dk_ref, dv_ref, dkv_acc):
    heads, shard, head_dim = q_ref.shape
    tp = k_ref.shape[0]
    total = tp * shard
    rows = heads * shard
    s_id = pl.program_id(0)
    g_id = pl.program_id(1)
    prefix = lens_ref[0, s_id]
    valid = lens_ref[1, s_id]
    first = lens_ref[2, 0] * shard
    keys = k_ref[...].reshape(total, head_dim)
    values = v_ref[...].reshape(total, head_dim)
    query = q_ref[...].reshape(rows, head_dim)
    d_out = jnp.concatenate([do_ref[:, h * head_dim:(h + 1) * head_dim] for h in range(heads)], axis=0)
    scale = head_dim ** -0.5
    step = lax.broadcasted_iota(jnp.int32, (shard, 1), 0)
    k_pos = jnp.concatenate([step + lens_ref[3 + r, 0] for r in range(tp)], axis=0)
    q_pos = first + lax.rem(lax.broadcasted_iota(jnp.int32, (1, rows), 1), shard)
    limit = jnp.minimum(valid, jnp.maximum(prefix, q_pos + 1))
    s = jnp.where(k_pos < limit, dot_nt(keys, query) * scale, MASKED)
    e = jnp.exp(s - jnp.max(s, axis=0, keepdims=True))
    p = e * (1.0 / jnp.sum(e, axis=0, keepdims=True))
    d_p = dot_nt(values, d_out)
    delta = jnp.sum(p * d_p, axis=0, keepdims=True)
    d_s = (p * (d_p - delta) * scale).astype(BF16)
    d_v = dot_nn(p.astype(BF16), d_out)
    d_k = dot_nn(d_s, query)
    dq_ref[...] = dot_tn(d_s, keys).astype(BF16).reshape(heads, shard, head_dim)

    @pl.when(g_id == 0)
    def _():
        dkv_acc[0] = d_k
        dkv_acc[1] = d_v

    @pl.when(g_id > 0)
    def _():
        dkv_acc[0] += d_k
        dkv_acc[1] += d_v

    @pl.when(g_id == pl.num_programs(1) - 1)
    def _():
        dk_ref[...] = dkv_acc[0].astype(BF16).reshape(tp, shard, head_dim)
        dv_ref[...] = dkv_acc[1].astype(BF16).reshape(tp, shard, head_dim)


def attention_forward(lens, k_pos, query, kv_all, batch, group=4):
    heads, rows, head_dim = query.shape
    tp = kv_all.shape[0]
    shard = rows // batch
    total = tp * shard
    q_spec = pl.BlockSpec((group, shard, head_dim), lambda s, g, *_: (g, s, 0))
    return pl.pallas_call(
        attn_fwd_kernel,
        out_shape=jax.ShapeDtypeStruct((rows, heads * head_dim), BF16),
        grid_spec=pltpu.PrefetchScalarGridSpec(
            num_scalar_prefetch=1, grid=(batch, heads // group),
            in_specs=[pl.BlockSpec((1, total), lambda s, g, *_: (0, 0)), q_spec,
                      pl.BlockSpec((tp, shard, head_dim), lambda s, g, *_: (0, s, 0)),
                      pl.BlockSpec((tp, shard, head_dim), lambda s, g, *_: (0, s, 1))],
            out_specs=pl.BlockSpec((shard, group * head_dim), lambda s, g, *_: (s, g)),
            scratch_shapes=[pltpu.VMEM((group * shard, total), BF16)]),
        compiler_params=pltpu.CompilerParams(dimension_semantics=("arbitrary", "arbitrary"), vmem_limit_bytes=48 << 20),
        cost_estimate=pl.CostEstimate(flops=4 * heads * rows * total * head_dim, bytes_accessed=12 << 20, transcendentals=heads * rows * total),
        name="attn_fwd",
    )(lens, k_pos, query, kv_all, kv_all)


def attention_backward(lens, query, kv_all, d_mixed, batch, group=4):
    heads, rows, head_dim = query.shape
    tp = kv_all.shape[0]
    shard = rows // batch
    total = tp * shard
    q_spec = pl.BlockSpec((group, shard, head_dim), lambda s, g, *_: (g, s, 0))
    kv_specs = [pl.BlockSpec((tp, shard, head_dim), lambda s, g, *_: (0, s, 0)),
                pl.BlockSpec((tp, shard, head_dim), lambda s, g, *_: (0, s, 1))]
    kv_out = pl.BlockSpec((tp, shard, head_dim), lambda s, g, *_: (0, s, 0))
    return pl.pallas_call(
        attn_bwd_kernel,
        out_shape=(jax.ShapeDtypeStruct((heads, rows, head_dim), BF16),
                   jax.ShapeDtypeStruct((tp, rows, head_dim), BF16),
                   jax.ShapeDtypeStruct((tp, rows, head_dim), BF16)),
        grid_spec=pltpu.PrefetchScalarGridSpec(
            num_scalar_prefetch=1, grid=(batch, heads // group),
            in_specs=[q_spec] + kv_specs + [pl.BlockSpec((shard, group * head_dim), lambda s, g, *_: (s, g))],
            out_specs=(q_spec, kv_out, kv_out),
            scratch_shapes=[pltpu.VMEM((2, total, head_dim), F32)]),
        compiler_params=pltpu.CompilerParams(dimension_semantics=("arbitrary", "arbitrary"), vmem_limit_bytes=56 << 20),
        cost_estimate=pl.CostEstimate(flops=10 * heads * rows * total * head_dim, bytes_accessed=20 << 20, transcendentals=heads * rows * total),
        name="attn_bwd",
    )(lens, query, kv_all, kv_all, d_mixed)


def flip(index, bit):
    return index + bit - 2 * bit * ((index // bit) % 2)


def neighbours():
    me = lax.axis_index("tp")
    return me, flip(me, 1), flip(me, 2), flip(me, 4)


def enter(peers):
    barrier = pltpu.get_barrier_semaphore()
    for peer in peers:
        pl.semaphore_signal(barrier, inc=1, device_id={"tp": peer}, device_id_type=pl.DeviceIdType.MESH)
    pl.semaphore_wait(barrier, len(peers))


def gated_tile(z, g, w_g, w_u, w_d):
    gate = dot_nn(z, w_g)
    upper = dot_nn(z, w_u)
    d_act = dot_nt(g, w_d).astype(BF16).astype(F32)
    sq = gate * gate
    th = jnp.tanh(gate * (GELU_C + (GELU_C * GELU_K) * sq))
    half = 0.5 + 0.5 * th
    gelu = gate * half
    slope = half + gate * (0.5 - 0.5 * (th * th)) * (GELU_C + (3.0 * GELU_C * GELU_K) * sq)
    return (gelu * upper).astype(BF16), (d_act * upper * slope).astype(BF16), (d_act * gelu).astype(BF16)


def gated_kernel(z_own, g_own, wg_hbm, wu_hbm, wd_hbm, z_all, g_all, act, d_gate, d_up,
                 wg, wu, wd, z_buf, g_buf, outs, w_sem, in_sem, own_sem, out_sem, send, recv, send0, recv0, *, bn):
    rows, dim = z_own.shape
    width = wg_hbm.shape[1]
    steps = width // bn
    piece = rows // 4
    me, core, side, back = neighbours()
    corner = flip(side, 4)
    own = (z_own, g_own)
    full = (z_all, g_all)

    def remote(src, dst, sems, peer):
        return pltpu.make_async_remote_copy(src_ref=src, dst_ref=dst, send_sem=sems[0], recv_sem=sems[1],
                                            device_id={"tp": peer}, device_id_type=pl.DeviceIdType.MESH)

    def part(slot, q):
        return pl.ds(pl.multiple_of(slot * rows + q * piece, 16), piece)

    def link_rows(u, path):
        turn = u // 2
        diag = turn % 2
        if path == 0:
            return side + (corner - side) * diag, (u % 2) + 2 * (turn // 2) + diag * 2
        return back + (corner - back) * diag, (u % 2) + 2 - 2 * (turn // 2) - diag * 2

    def link_copy(u, path, a):
        turn = u // 2
        peer = side if path == 0 else back
        sems = (send.at[path, u, a], recv.at[path, u, a])
        if turn == 1:
            slot = back if path == 0 else side
            q = (2 if path == 0 else 0) + u % 2
            return remote(full[a].at[part(slot, q)], full[a].at[part(slot, q)], sems, peer)
        q = u % 2 + (2 * (turn // 2) if path == 0 else 2 - 2 * (turn // 2))
        return remote(own[a].at[pl.ds(q * piece, piece)], full[a].at[part(me, q)], sems, peer)

    def core_copy(u, path, a):
        slot, q = link_rows(u, path)
        return remote(full[a].at[part(slot, q)], full[a].at[part(slot, q)], (send.at[2 + path, u, a], recv.at[2 + path, u, a]), core)

    def own_copy(a):
        return remote(own[a], full[a].at[pl.ds(pl.multiple_of(me * rows, 16), rows)], (send0.at[a], recv0.at[a]), core)

    def weight_copies(n):
        cols = pl.ds(pl.multiple_of(n * bn, 128), bn)
        return [pltpu.make_async_copy(wg_hbm.at[:, cols], wg.at[:, cols], w_sem.at[0, n]),
                pltpu.make_async_copy(wu_hbm.at[:, cols], wu.at[:, cols], w_sem.at[1, n]),
                pltpu.make_async_copy(wd_hbm.at[cols], wd.at[cols], w_sem.at[2, n])]

    bufs = (z_buf, g_buf)
    own_in = [pltpu.make_async_copy(own[a], bufs[a], own_sem.at[a]) for a in range(2)]
    own_out = [pltpu.make_async_copy(bufs[a], full[a].at[pl.ds(pl.multiple_of(me * rows, 16), rows)], own_sem.at[2 + a]) for a in range(2)]
    for cp in own_in:
        cp.start()
    for n in range(steps):
        for cp in weight_copies(n):
            cp.start()
    enter((core, side, back))
    for u in range(2):
        for path in range(2):
            for a in range(2):
                link_copy(u, path, a).start()
        if u == 0:
            for a in range(2):
                own_copy(a).start()

    def out_copies(slot, s_rows, n):
        cols = pl.ds(pl.multiple_of(n * bn, 128), bn)
        return [pltpu.make_async_copy(outs.at[slot, k, pl.ds(i * piece, piece)], ref.at[s_rows[i], cols], out_sem.at[slot, k, i])
                for k, ref in enumerate((act, d_gate, d_up)) for i in range(4)]

    def stage_rows(s):
        late = (s + 6) // 8
        u = (s - 2) * late
        first = me + (core - me) * s * (1 - late)
        (slot_x, q_x), (slot_y, q_y) = link_rows(u, 0), link_rows(u, 1)
        base_x, base_y = slot_x * rows + q_x * piece, slot_y * rows + q_y * piece
        pair_x, pair_y = flip(slot_x, 1) * rows + q_x * piece, flip(slot_y, 1) * rows + q_y * piece
        starts = [(1 - late) * (first * rows + i * piece) + late * base for i, base in enumerate((base_x, base_y, pair_x, pair_y))]
        return [pl.ds(pl.multiple_of(st, 16), piece) for st in starts]

    def compute(s):
        s_rows = stage_rows(s)

        def block(n, carry):
            step = s * steps + n
            slot = step % 2

            @pl.when(step >= 2)
            def _():
                for cp in out_copies(slot, s_rows, n):
                    cp.wait()

            @pl.when(s == 0)
            def _():
                for cp in weight_copies(n):
                    cp.wait()

            cols = pl.ds(pl.multiple_of(n * bn, 128), bn)
            res = gated_tile(z_buf[...], g_buf[...], wg[:, cols], wu[:, cols], wd[cols, :])
            for k in range(3):
                outs[slot, k] = res[k]
            for cp in out_copies(slot, s_rows, n):
                cp.start()
            return carry

        lax.fori_loop(0, steps, block, 0)

    def stage(s, carry):
        @pl.when(s == 0)
        def _():
            for cp in own_in:
                cp.wait()
            for cp in own_out:
                cp.start()

        @pl.when(s == 1)
        def _():
            for cp in own_out:
                cp.wait()
            for a in range(2):
                own_copy(a).wait_recv()

        for u in range(6):
            @pl.when(s == u + 2)
            def _(u=u):
                for path in range(2):
                    for a in range(2):
                        link_copy(u, path, a).wait_recv()
                        core_copy(u, path, a).start()
                if u < 2:
                    for path in range(2):
                        for a in range(2):
                            link_copy(u + 2, path, a).start()
                if u == 1:
                    for later in (4, 5):
                        for path in range(2):
                            for a in range(2):
                                link_copy(later, path, a).start()
                for path in range(2):
                    for a in range(2):
                        core_copy(u, path, a).wait_recv()

        @pl.when(s >= 1)
        def _():
            s_rows = stage_rows(s)
            copies = [pltpu.make_async_copy(full[a].at[s_rows[i]], bufs[a].at[pl.ds(i * piece, piece)], in_sem.at[a, i])
                      for a in range(2) for i in range(4)]
            for cp in copies:
                cp.start()
            for cp in copies:
                cp.wait()

        compute(s)
        return carry

    lax.fori_loop(0, 8, stage, 0)
    last = stage_rows(7)
    for slot in range(2):
        for cp in out_copies(slot, last, 0):
            cp.wait()
    for a in range(2):
        own_copy(a).wait_send()
        for path in range(2):
            for u in range(6):
                link_copy(u, path, a).wait_send()
                core_copy(u, path, a).wait_send()


def gated_layer(z_own, g_own, w_gate, w_up, w_down, tp, bn=512):
    rows, dim = z_own.shape
    width = w_gate.shape[1]
    total = rows * tp
    anyspace = pl.BlockSpec(memory_space=pl.ANY)
    gathered = jax.ShapeDtypeStruct((total, dim), BF16)
    made = jax.ShapeDtypeStruct((total, width), BF16)
    dma = pltpu.SemaphoreType.DMA
    return pl.pallas_call(
        functools.partial(gated_kernel, bn=bn),
        out_shape=(gathered, gathered, made, made, made),
        in_specs=[anyspace] * 5,
        out_specs=(anyspace,) * 5,
        scratch_shapes=[pltpu.VMEM((dim, width), BF16), pltpu.VMEM((dim, width), BF16), pltpu.VMEM((width, dim), BF16),
                        pltpu.VMEM((rows, dim), BF16), pltpu.VMEM((rows, dim), BF16), pltpu.VMEM((2, 3, rows, bn), BF16),
                        dma((3, width // bn)), dma((2, 4)), dma((4,)), dma((2, 3, 4)), dma((4, 6, 2)), dma((4, 6, 2)), dma((2,)), dma((2,))],
        compiler_params=pltpu.CompilerParams(vmem_limit_bytes=60 << 20, collective_id=0, has_side_effects=True),
        cost_estimate=pl.CostEstimate(flops=6 * total * dim * width, bytes_accessed=200 << 20, transcendentals=total * width),
        name="gated",
    )(z_own, g_own, w_gate, w_up, w_down)


def pair_kernel(a_ref, b_ref, wa_ref, wb_ref, o_ref):
    o_ref[...] = (dot_nt(a_ref[...], wa_ref[...]) + dot_nt(b_ref[...], wb_ref[...])).astype(BF16)


def pair_back(a, b, w_a, w_b, bm=1152, bn=512):
    rows, width = a.shape
    dim = w_a.shape[0]
    lhs = pl.BlockSpec((bm, width), lambda i, j: (i, 0))
    row = pl.BlockSpec((bn, width), lambda i, j: (j, 0))
    return pl.pallas_call(
        pair_kernel,
        out_shape=jax.ShapeDtypeStruct((rows, dim), BF16),
        grid=(rows // bm, dim // bn),
        in_specs=[lhs, lhs, row, row],
        out_specs=pl.BlockSpec((bm, bn), lambda i, j: (i, j)),
        compiler_params=pltpu.CompilerParams(dimension_semantics=("arbitrary", "arbitrary"), vmem_limit_bytes=56 << 20),
        cost_estimate=pl.CostEstimate(flops=4 * rows * dim * width, bytes_accessed=140 << 20, transcendentals=0),
        name="pair_back",
    )(a, b, w_a, w_b)


def solution(mesh):
    tp_size = mesh.shape["tp"]
    act_spec = P("dp", "tp", None)
    in_specs = (act_spec, act_spec, P("dp"), P("dp"), P(None), P(None, "tp"), P(None, None), P(None, None), P("tp", None), P(None), P(None, "tp"), P(None, "tp"), P("tp", None))
    out_specs = (act_spec, act_spec, P("dp"), P("dp", "tp"), P("dp", None), P("dp", None), P(("dp", "tp"), None), P("dp"), P("dp", "tp"), P("dp", "tp"), P(("dp", "tp"), None))

    def local_layer(hidden, grad_out, prefix_len, valid_len, attn_norm, w_query, w_key, w_value, w_out, mlp_norm, w_gate, w_up, w_down):
        batch, shard, dim = hidden.shape
        head_dim = w_key.shape[1]
        rows = batch * shard
        me = lax.axis_index("tp")
        starts = (me ^ jnp.arange(tp_size, dtype=jnp.int32)) * shard
        k_pos = (starts[:, None] + jnp.arange(shard, dtype=jnp.int32)).reshape(1, tp_size * shard)
        lens = jnp.concatenate([jnp.stack([prefix_len, valid_len, jnp.full((batch,), me, jnp.int32)]),
                                jnp.broadcast_to(starts[:, None], (tp_size, batch))])
        cos_t, sin_t = rope_tables(me * shard + jnp.arange(shard), head_dim)
        cos_t, sin_t = jnp.tile(cos_t, (batch, 1)), jnp.tile(sin_t, (batch, 1))

        def rope(raw_proj):
            return apply_rope(raw_proj, cos_t, sin_t).astype(BF16)

        wq_all = lax.all_gather(w_query, "tp", axis=0)
        hidden = hidden.reshape(rows, dim)
        grad_out = grad_out.reshape(rows, dim)
        normed, norm1_pull = jax.vjp(rms_norm, hidden, attn_norm.astype(F32))
        keys, key_pull = jax.vjp(rope, dot_nn(normed, w_key))
        values = dot_nn(normed, w_value).astype(BF16)
        kv_all = jnp.stack(gather_relative(jnp.concatenate([keys, values], axis=1)))
        wo_all = lax.all_gather(w_out, "tp", axis=0, tiled=True)
        q_raw = jnp.einsum("td,hde->hte", normed, wq_all, preferred_element_type=F32)
        query, query_pull = jax.vjp(rope, q_raw)
        mixed = attention_forward(lens, k_pos, query, kv_all, batch)
        attn_out = dot_nn(mixed, wo_all)
        resid = (hidden.astype(F32) + attn_out).astype(BF16)
        gated_in, norm2_pull = jax.vjp(rms_norm, resid, mlp_norm.astype(F32))
        gated_all, grad_all, act, d_gate, d_upper = gated_layer(gated_in, grad_out, w_gate, w_up, w_down, tp_size)
        d_gated_part = pair_back(d_gate, d_upper, w_gate, w_up)
        d_gated = lax.psum_scatter(d_gated_part, "tp", scatter_dimension=0, tiled=True)
        mlp_part = dot_nn(act, w_down).astype(BF16)
        mlp_sum = lax.psum_scatter(mlp_part, "tp", scatter_dimension=0, tiled=True)
        g_down = dot_tn(act, grad_all)
        g_gate = dot_tn(gated_all, d_gate)
        g_up = dot_tn(gated_all, d_upper)

        d_gated, g_down = lax.optimization_barrier((d_gated, g_down))
        d_resid_norm, g_mlp_norm_part = norm2_pull(d_gated)
        d_resid = (grad_out.astype(F32) + d_resid_norm.astype(F32)).astype(BF16)
        g_out = lax.psum_scatter(dot_tn(mixed, d_resid), "tp", scatter_dimension=0, tiled=True)
        d_mixed = dot_nt(d_resid, wo_all).astype(BF16)
        d_query, d_keys_part, d_values_part = attention_backward(lens, query, kv_all, d_mixed, batch)
        d_keys = scatter_relative(d_keys_part).astype(BF16)
        d_values = scatter_relative(d_values_part).astype(BF16)
        d_q_raw = query_pull(d_query)[0].astype(BF16)
        d_k_raw = key_pull(d_keys)[0].astype(BF16)
        g_query = lax.psum_scatter(jnp.einsum("td,hte->hde", normed, d_q_raw, preferred_element_type=F32), "tp", scatter_dimension=0, tiled=False)
        g_key = lax.psum(dot_tn(normed, d_k_raw), "tp")
        g_value = lax.psum(dot_tn(normed, d_values), "tp")
        d_normed = (jnp.einsum("hte,hde->td", d_q_raw, wq_all, preferred_element_type=F32)
                    + dot_nt(d_k_raw, w_key) + dot_nt(d_values, w_value)).astype(BF16)
        mlp_sum, d_normed = lax.optimization_barrier((mlp_sum, d_normed))
        d_hidden_norm, g_attn_norm_part = norm1_pull(d_normed)
        grad_hidden = (d_resid.astype(F32) + d_hidden_norm.astype(F32)).astype(BF16)
        hidden_out = (resid.astype(F32) + mlp_sum.astype(F32)).astype(BF16)
        g_norms = all_sum_small(jnp.stack([g_attn_norm_part, g_mlp_norm_part]))
        full = (batch, shard, dim)
        return (hidden_out.reshape(full), grad_hidden.reshape(full), g_norms[0], g_query, g_key, g_value, g_out, g_norms[1], g_gate, g_up, g_down)

    return jax.shard_map(local_layer, mesh=mesh, in_specs=in_specs, out_specs=out_specs, check_vma=False)
```

```python
import functools
import math
import jax
import jax.numpy as jnp
from jax import lax
from jax.experimental import pallas as pl
from jax.experimental.pallas import tpu as pltpu
from jax.sharding import PartitionSpec as P

NORM_EPS = 1e-6
BF16 = jnp.bfloat16
F32 = jnp.float32
GELU_C = math.sqrt(2.0 / math.pi)
GELU_K = 0.044715
MASKED = -1e30
NT = (((1,), (1,)), ((), ()))
TN = (((0,), (0,)), ((), ()))


def rms_norm(x_in, gain):
    x_f = x_in.astype(F32)
    inv_rms = lax.rsqrt(jnp.mean(x_f * x_f, axis=-1, keepdims=True) + NORM_EPS)
    return (x_f * inv_rms * (1.0 + gain)).astype(BF16)


def rope_tables(positions, head_dim):
    half_dim = head_dim // 2
    exponent = jnp.arange(half_dim, dtype=F32) * (2.0 / head_dim)
    inv_freq = jnp.exp(exponent * (-math.log(10000.0)))
    angles = positions.astype(F32)[:, None] * inv_freq[None, :]
    return jnp.cos(angles), jnp.sin(angles)


def apply_rope(x_f, cos_t, sin_t):
    half_dim = x_f.shape[-1] // 2
    first = x_f[..., :half_dim]
    second = x_f[..., half_dim:]
    return jnp.concatenate([first * cos_t - second * sin_t, second * cos_t + first * sin_t], axis=-1)


def dot_nn(a, b):
    return jnp.dot(a, b, preferred_element_type=F32)


def dot_nt(a, b):
    return lax.dot_general(a, b, NT, preferred_element_type=F32)


def dot_tn(a, b):
    return lax.dot_general(a, b, TN, preferred_element_type=F32)


def swap(x, bit):
    return lax.ppermute(x, "tp", [(t, t ^ bit) for t in range(8)])


def gather_near(own):
    half = own.shape[0] // 2
    side = swap(own, 2)
    back = swap(own, 4)
    diag = jnp.concatenate([swap(side[:half], 4), swap(back[half:], 2)], axis=0)
    mine = jnp.stack([own, side, back, diag])
    return mine, swap(mine, 1)


def all_sum_small(x):
    for bit in (1, 2, 4):
        x = x + swap(x, bit)
    return x


def keys_values(kv0_ref, kv1_ref, total, head_dim):
    both = jnp.concatenate([kv0_ref[...].reshape(total // 2, 2 * head_dim), kv1_ref[...].reshape(total // 2, 2 * head_dim)], axis=0)
    return both[:, :head_dim], both[:, head_dim:]


def attn_fwd_kernel(lens_ref, kpos_ref, q_ref, kv0_ref, kv1_ref, o_ref, p_ref):
    heads, shard, head_dim = q_ref.shape
    total = 2 * kv0_ref.shape[0] * shard
    s_id = pl.program_id(0)
    prefix = lens_ref[0, s_id]
    valid = lens_ref[1, s_id]
    first = lens_ref[2, 0] * shard
    keys, values = keys_values(kv0_ref, kv1_ref, total, head_dim)
    q_pos = first + lax.broadcasted_iota(jnp.int32, (shard, 1), 0)
    visible = kpos_ref[...] < jnp.minimum(valid, jnp.maximum(prefix, q_pos + 1))
    scale = head_dim ** -0.5
    query = q_ref[...].reshape(heads * shard, head_dim)
    scores = dot_nt(query, keys)
    for h in range(heads):
        rows = slice(h * shard, (h + 1) * shard)
        s = jnp.where(visible, scores[rows] * scale, MASKED)
        e = jnp.exp(s - jnp.max(s, axis=-1, keepdims=True))
        p_ref[rows, :] = (e / jnp.sum(e, axis=-1, keepdims=True)).astype(BF16)
    mixed = dot_nn(p_ref[...], values).astype(BF16)
    for h in range(heads):
        o_ref[:, h * head_dim:(h + 1) * head_dim] = mixed[h * shard:(h + 1) * shard]


def attn_bwd_kernel(lens_ref, q_ref, kv0_ref, kv1_ref, do_ref, dq_ref, dkv0_ref, dkv1_ref, dkv_acc):
    heads, shard, head_dim = q_ref.shape
    tp = 2 * kv0_ref.shape[0]
    total = tp * shard
    rows = heads * shard
    s_id = pl.program_id(0)
    g_id = pl.program_id(1)
    prefix = lens_ref[0, s_id]
    valid = lens_ref[1, s_id]
    first = lens_ref[2, 0] * shard
    keys, values = keys_values(kv0_ref, kv1_ref, total, head_dim)
    query = q_ref[...].reshape(rows, head_dim)
    d_out = jnp.concatenate([do_ref[:, h * head_dim:(h + 1) * head_dim] for h in range(heads)], axis=0)
    scale = head_dim ** -0.5
    step = lax.broadcasted_iota(jnp.int32, (shard, 1), 0)
    k_pos = jnp.concatenate([step + lens_ref[3 + r, 0] for r in range(tp)], axis=0)
    q_pos = first + lax.rem(lax.broadcasted_iota(jnp.int32, (1, rows), 1), shard)
    limit = jnp.minimum(valid, jnp.maximum(prefix, q_pos + 1))
    s = jnp.where(k_pos < limit, dot_nt(keys, query) * scale, MASKED)
    e = jnp.exp(s - jnp.max(s, axis=0, keepdims=True))
    p = e * (1.0 / jnp.sum(e, axis=0, keepdims=True))
    d_p = dot_nt(values, d_out)
    delta = jnp.sum(p * d_p, axis=0, keepdims=True)
    d_s = (p * (d_p - delta) * scale).astype(BF16)
    d_v = dot_nn(p.astype(BF16), d_out)
    d_k = dot_nn(d_s, query)
    dq_ref[...] = dot_tn(d_s, keys).astype(BF16).reshape(heads, shard, head_dim)

    d_kv = jnp.concatenate([d_k, d_v], axis=1)

    @pl.when(g_id == 0)
    def _():
        dkv_acc[...] = d_kv

    @pl.when(g_id > 0)
    def _():
        dkv_acc[...] += d_kv

    @pl.when(g_id == pl.num_programs(1) - 1)
    def _():
        near = (tp // 2, shard, 2 * head_dim)
        dkv0_ref[...] = dkv_acc[:total // 2].astype(BF16).reshape(near)
        dkv1_ref[...] = dkv_acc[total // 2:].astype(BF16).reshape(near)


def attention_forward(lens, k_pos, query, kv0, kv1, batch, group=4):
    heads, rows, head_dim = query.shape
    near = kv0.shape[0]
    shard = rows // batch
    total = 2 * near * shard
    q_spec = pl.BlockSpec((group, shard, head_dim), lambda s, g, *_: (g, s, 0))
    return pl.pallas_call(
        attn_fwd_kernel,
        out_shape=jax.ShapeDtypeStruct((rows, heads * head_dim), BF16),
        grid_spec=pltpu.PrefetchScalarGridSpec(
            num_scalar_prefetch=1, grid=(batch, heads // group),
            in_specs=[pl.BlockSpec((1, total), lambda s, g, *_: (0, 0)), q_spec,
                      pl.BlockSpec((near, shard, 2 * head_dim), lambda s, g, *_: (0, s, 0)),
                      pl.BlockSpec((near, shard, 2 * head_dim), lambda s, g, *_: (0, s, 0))],
            out_specs=pl.BlockSpec((shard, group * head_dim), lambda s, g, *_: (s, g)),
            scratch_shapes=[pltpu.VMEM((group * shard, total), BF16)]),
        compiler_params=pltpu.CompilerParams(dimension_semantics=("arbitrary", "arbitrary"), vmem_limit_bytes=48 << 20),
        cost_estimate=pl.CostEstimate(flops=4 * heads * rows * total * head_dim, bytes_accessed=12 << 20, transcendentals=heads * rows * total),
        name="attn_fwd",
    )(lens, k_pos, query, kv0, kv1)


def attention_backward(lens, query, kv0, kv1, d_mixed, batch, group=4):
    heads, rows, head_dim = query.shape
    near = kv0.shape[0]
    shard = rows // batch
    total = 2 * near * shard
    q_spec = pl.BlockSpec((group, shard, head_dim), lambda s, g, *_: (g, s, 0))
    kv_spec = pl.BlockSpec((near, shard, 2 * head_dim), lambda s, g, *_: (0, s, 0))
    kv_shape = jax.ShapeDtypeStruct((near, rows, 2 * head_dim), BF16)
    return pl.pallas_call(
        attn_bwd_kernel,
        out_shape=(jax.ShapeDtypeStruct((heads, rows, head_dim), BF16), kv_shape, kv_shape),
        grid_spec=pltpu.PrefetchScalarGridSpec(
            num_scalar_prefetch=1, grid=(batch, heads // group),
            in_specs=[q_spec, kv_spec, kv_spec, pl.BlockSpec((shard, group * head_dim), lambda s, g, *_: (s, g))],
            out_specs=(q_spec, kv_spec, kv_spec),
            scratch_shapes=[pltpu.VMEM((total, 2 * head_dim), F32)]),
        compiler_params=pltpu.CompilerParams(dimension_semantics=("arbitrary", "arbitrary"), vmem_limit_bytes=56 << 20),
        cost_estimate=pl.CostEstimate(flops=10 * heads * rows * total * head_dim, bytes_accessed=20 << 20, transcendentals=heads * rows * total),
        name="attn_bwd",
    )(lens, query, kv0, kv1, d_mixed)


def flip(index, bit):
    return index + bit - 2 * bit * ((index // bit) % 2)


def neighbours():
    me = lax.axis_index("tp")
    return me, flip(me, 1), flip(me, 2), flip(me, 4)


def enter(peers):
    barrier = pltpu.get_barrier_semaphore()
    for peer in peers:
        pl.semaphore_signal(barrier, inc=1, device_id={"tp": peer}, device_id_type=pl.DeviceIdType.MESH)
    pl.semaphore_wait(barrier, len(peers))


def gated_tile(z, g, w_g, w_u, w_d):
    gate = dot_nn(z, w_g)
    upper = dot_nn(z, w_u)
    d_act = dot_nt(g, w_d).astype(BF16).astype(F32)
    sq = gate * gate
    th = jnp.tanh(gate * (GELU_C + (GELU_C * GELU_K) * sq))
    half = 0.5 + 0.5 * th
    gelu = gate * half
    slope = half + gate * (0.5 - 0.5 * (th * th)) * (GELU_C + (3.0 * GELU_C * GELU_K) * sq)
    return (gelu * upper).astype(BF16), (d_act * upper * slope).astype(BF16), (d_act * gelu).astype(BF16)


def gated_kernel(z_own, g_own, wg_hbm, wu_hbm, wd_hbm, z_all, g_all, act, d_gate, d_up,
                 wg, wu, wd, z_buf, g_buf, outs, w_sem, in_sem, own_sem, out_sem, send, recv, send0, recv0, *, bn):
    rows, _ = z_own.shape
    width = wg_hbm.shape[1]
    steps = width // bn
    piece = rows // 4
    me, core, side, back = neighbours()
    corner = flip(side, 4)
    own = (z_own, g_own)
    full = (z_all, g_all)

    def remote(src, dst, sems, peer):
        return pltpu.make_async_remote_copy(src_ref=src, dst_ref=dst, send_sem=sems[0], recv_sem=sems[1],
                                            device_id={"tp": peer}, device_id_type=pl.DeviceIdType.MESH)

    def part(slot, q):
        return pl.ds(pl.multiple_of(slot * rows + q * piece, 16), piece)

    def link_rows(u, path):
        turn = u // 2
        diag = turn % 2
        if path == 0:
            return side + (corner - side) * diag, (u % 2) + 2 * (turn // 2) + diag * 2
        return back + (corner - back) * diag, (u % 2) + 2 - 2 * (turn // 2) - diag * 2

    def link_copy(u, path, a):
        turn = u // 2
        peer = side if path == 0 else back
        sems = (send.at[path, u, a], recv.at[path, u, a])
        if turn == 1:
            slot = back if path == 0 else side
            q = (2 if path == 0 else 0) + u % 2
            return remote(full[a].at[part(slot, q)], full[a].at[part(slot, q)], sems, peer)
        q = u % 2 + (2 * (turn // 2) if path == 0 else 2 - 2 * (turn // 2))
        return remote(own[a].at[pl.ds(q * piece, piece)], full[a].at[part(me, q)], sems, peer)

    def core_copy(u, path, a):
        slot, q = link_rows(u, path)
        return remote(full[a].at[part(slot, q)], full[a].at[part(slot, q)], (send.at[2 + path, u, a], recv.at[2 + path, u, a]), core)

    def own_copy(a):
        return remote(own[a], full[a].at[pl.ds(pl.multiple_of(me * rows, 16), rows)], (send0.at[a], recv0.at[a]), core)

    def weight_copies(n):
        cols = pl.ds(pl.multiple_of(n * bn, 128), bn)
        return [pltpu.make_async_copy(wg_hbm.at[:, cols], wg.at[:, cols], w_sem.at[0, n]),
                pltpu.make_async_copy(wu_hbm.at[:, cols], wu.at[:, cols], w_sem.at[1, n]),
                pltpu.make_async_copy(wd_hbm.at[cols], wd.at[cols], w_sem.at[2, n])]

    bufs = (z_buf, g_buf)
    own_in = [pltpu.make_async_copy(own[a], bufs[a], own_sem.at[a]) for a in range(2)]
    own_out = [pltpu.make_async_copy(bufs[a], full[a].at[pl.ds(pl.multiple_of(me * rows, 16), rows)], own_sem.at[2 + a]) for a in range(2)]
    for cp in own_in:
        cp.start()
    for n in range(steps):
        for cp in weight_copies(n):
            cp.start()
    enter((core, side, back))
    for u in range(2):
        for path in range(2):
            for a in range(2):
                link_copy(u, path, a).start()
        if u == 0:
            for a in range(2):
                own_copy(a).start()

    def out_copies(slot, s_rows, n):
        cols = pl.ds(pl.multiple_of(n * bn, 128), bn)
        return [pltpu.make_async_copy(outs.at[slot, k, pl.ds(i * piece, piece)], ref.at[s_rows[i], cols], out_sem.at[slot, k, i])
                for k, ref in enumerate((act, d_gate, d_up)) for i in range(4)]

    def stage_rows(s):
        late = (s + 6) // 8
        u = (s - 2) * late
        first = me + (core - me) * s * (1 - late)
        (slot_x, q_x), (slot_y, q_y) = link_rows(u, 0), link_rows(u, 1)
        base_x, base_y = slot_x * rows + q_x * piece, slot_y * rows + q_y * piece
        pair_x, pair_y = flip(slot_x, 1) * rows + q_x * piece, flip(slot_y, 1) * rows + q_y * piece
        starts = [(1 - late) * (first * rows + i * piece) + late * base for i, base in enumerate((base_x, base_y, pair_x, pair_y))]
        return [pl.ds(pl.multiple_of(st, 16), piece) for st in starts]

    def compute(s):
        s_rows = stage_rows(s)

        def block(n, carry):
            step = s * steps + n
            slot = step % 2

            @pl.when(step >= 2)
            def _():
                for cp in out_copies(slot, s_rows, n):
                    cp.wait()

            @pl.when(s == 0)
            def _():
                for cp in weight_copies(n):
                    cp.wait()

            cols = pl.ds(pl.multiple_of(n * bn, 128), bn)
            res = gated_tile(z_buf[...], g_buf[...], wg[:, cols], wu[:, cols], wd[cols, :])
            for k in range(3):
                outs[slot, k] = res[k]
            for cp in out_copies(slot, s_rows, n):
                cp.start()
            return carry

        lax.fori_loop(0, steps, block, 0)

    def stage(s, carry):
        @pl.when(s == 0)
        def _():
            for cp in own_in:
                cp.wait()
            for cp in own_out:
                cp.start()

        @pl.when(s == 1)
        def _():
            for cp in own_out:
                cp.wait()
            for a in range(2):
                own_copy(a).wait_recv()

        for u in range(6):
            @pl.when(s == u + 2)
            def _(u=u):
                for path in range(2):
                    for a in range(2):
                        link_copy(u, path, a).wait_recv()
                        core_copy(u, path, a).start()
                if u < 2:
                    for path in range(2):
                        for a in range(2):
                            link_copy(u + 2, path, a).start()
                if u == 1:
                    for later in (4, 5):
                        for path in range(2):
                            for a in range(2):
                                link_copy(later, path, a).start()
                for path in range(2):
                    for a in range(2):
                        core_copy(u, path, a).wait_recv()

        @pl.when(s >= 1)
        def _():
            s_rows = stage_rows(s)
            copies = [pltpu.make_async_copy(full[a].at[s_rows[i]], bufs[a].at[pl.ds(i * piece, piece)], in_sem.at[a, i])
                      for a in range(2) for i in range(4)]
            for cp in copies:
                cp.start()
            for cp in copies:
                cp.wait()

        compute(s)
        return carry

    lax.fori_loop(0, 8, stage, 0)
    last = stage_rows(7)
    for slot in range(2):
        for cp in out_copies(slot, last, 0):
            cp.wait()
    for a in range(2):
        own_copy(a).wait_send()
        for path in range(2):
            for u in range(6):
                link_copy(u, path, a).wait_send()
                core_copy(u, path, a).wait_send()


def gated_layer(z_own, g_own, w_gate, w_up, w_down, tp, bn=512):
    rows, dim = z_own.shape
    width = w_gate.shape[1]
    total = rows * tp
    anyspace = pl.BlockSpec(memory_space=pl.ANY)
    gathered = jax.ShapeDtypeStruct((total, dim), BF16)
    made = jax.ShapeDtypeStruct((total, width), BF16)
    dma = pltpu.SemaphoreType.DMA
    return pl.pallas_call(
        functools.partial(gated_kernel, bn=bn),
        out_shape=(gathered, gathered, made, made, made),
        in_specs=[anyspace] * 5,
        out_specs=(anyspace,) * 5,
        scratch_shapes=[pltpu.VMEM((dim, width), BF16), pltpu.VMEM((dim, width), BF16), pltpu.VMEM((width, dim), BF16),
                        pltpu.VMEM((rows, dim), BF16), pltpu.VMEM((rows, dim), BF16), pltpu.VMEM((2, 3, rows, bn), BF16),
                        dma((3, width // bn)), dma((2, 4)), dma((4,)), dma((2, 3, 4)), dma((4, 6, 2)), dma((4, 6, 2)), dma((2,)), dma((2,))],
        compiler_params=pltpu.CompilerParams(vmem_limit_bytes=60 << 20, collective_id=0, has_side_effects=True),
        cost_estimate=pl.CostEstimate(flops=6 * total * dim * width, bytes_accessed=200 << 20, transcendentals=total * width),
        name="gated",
    )(z_own, g_own, w_gate, w_up, w_down)


def back_kernel(act, d_gate, d_up, wg_hbm, wu_hbm, wd_hbm, own_out, x_in, y_in,
                wa, wb, lhs, st, from_core, from_diag, own_st, w_sem, l_sem, o_sem, c_send, c_recv, d_send, d_recv, f_send, f_recv, *, rows, bn):
    dim = wg_hbm.shape[0]
    steps = dim // bn
    half = rows // 2
    me, core, side, back = neighbours()

    def remote(src, dst, send, recv, peer):
        return pltpu.make_async_remote_copy(src_ref=src, dst_ref=dst, send_sem=send, recv_sem=recv,
                                            device_id={"tp": peer}, device_id_type=pl.DeviceIdType.MESH)

    def cols(j):
        return pl.ds(pl.multiple_of(j * bn, 128), bn)

    def pair_of(t):
        return ((t + 5) // 7) * ((t + 1) % 3 + 1)

    def lhs_copies(phase, t):
        pair = pair_of(t)
        theirs = 1 - t // 5 - ((t + 6) // 7 - (t + 5) // 7)
        dev = me + (1 - pair // 2) * (side - me) + (1 - pair % 2) * (back - me)
        dev = dev + theirs * (flip(dev, 1) - dev)
        src = pl.ds(pl.multiple_of(dev * rows, 16), rows)
        refs = (act,) if phase == 0 else (d_gate, d_up)
        return [pltpu.make_async_copy(ref.at[src], lhs.at[t % 2, k], l_sem.at[t % 2, k]) for k, ref in enumerate(refs)]

    def weight_copy(k, j):
        if k == 0:
            return pltpu.make_async_copy(wd_hbm.at[:, cols(j)], wa.at[:, cols(j)], w_sem.at[0, j])
        src, dst = (wg_hbm, wb) if k == 1 else (wu_hbm, wa)
        return pltpu.make_async_copy(src.at[cols(j)], dst.at[cols(j)], w_sem.at[k, j])

    def core_copy(pair, j):
        return remote(st.at[0, j], from_core.at[pair, j], c_send.at[j], c_recv.at[pair, j], core)

    def diag_copy(phase, k, j):
        return remote(st.at[1, j, pl.ds(k * half, half)], from_diag.at[phase, k, j], d_send.at[k, j], d_recv.at[phase, k, j], (side, back)[k])

    def final_copy(phase, k, j):
        return remote(st.at[2 + k, j], (x_in, y_in)[k].at[phase, :, cols(j)], f_send.at[k, j], f_recv.at[phase, k, j], (side, back)[k])

    def own_copy(phase, j):
        return pltpu.make_async_copy(own_st.at[j % 2], own_out.at[phase, :, cols(j)], o_sem.at[j % 2])

    def product(phase, slot, j):
        if phase == 0:
            return dot_nn(lhs[slot, 0], wa[:, cols(j)])
        return dot_nt(lhs[slot, 0], wb[cols(j), :]) + dot_nt(lhs[slot, 1], wa[cols(j), :])

    for cp in lhs_copies(0, 0):
        cp.start()
    for j in range(steps):
        weight_copy(0, j).start()
    enter((core, side, back))

    def tiles(body):
        def step(j, carry):
            body(j)
            return carry

        lax.fori_loop(0, steps, step, 0)

    for phase in (0, 1):
        def step(t, carry, phase=phase):
            for cp in lhs_copies(phase, t):
                cp.wait()

            @pl.when(t < 7)
            def _():
                for cp in lhs_copies(phase, t + 1):
                    cp.start()

            if phase == 0:
                @pl.when(t == 1)
                def _():
                    for j in range(steps):
                        weight_copy(1, j).start()

                @pl.when(t == 7)
                def _():
                    for cp in lhs_copies(1, 0):
                        cp.start()

            @pl.when((t == 0) | ((t >= 2) & (t <= 4)))
            def _():
                pair = pair_of(t)

                def body(j):
                    @pl.when(t == 0)
                    def _():
                        for k in ((0,) if phase == 0 else (1, 2)):
                            weight_copy(k, j).wait()

                    if phase == 0:
                        @pl.when(t > 0)
                        def _():
                            core_copy(0, j).wait_send()
                    else:
                        core_copy(0, j).wait_send()
                    st[0, j] = product(phase, t % 2, j).astype(BF16)
                    core_copy(pair, j).start()

                tiles(body)

            @pl.when(t == 1)
            def _():
                def body(j):
                    core_copy(0, j).wait_recv()
                    if phase == 1:
                        for k in range(2):
                            diag_copy(0, k, j).wait_send()
                    st[1, j] = (product(phase, 1, j) + from_core[0, j].astype(F32)).astype(BF16)
                    for k in range(2):
                        diag_copy(phase, k, j).start()

                tiles(body)

            for k in range(2):
                @pl.when(t == 5 + k)
                def _(k=k):
                    def body(j):
                        core_copy(1 + k, j).wait_recv()
                        diag_copy(phase, 1 - k, j).wait_recv()
                        if phase == 1:
                            final_copy(0, k, j).wait_send()
                        total = product(phase, (5 + k) % 2, j) + from_core[1 + k, j].astype(F32)
                        came = from_diag[phase, 1 - k, j].astype(F32)
                        split = slice(half, rows) if k == 0 else slice(0, half)
                        rest = slice(0, half) if k == 0 else slice(half, rows)
                        st[2 + k, j, split, :] = (total[split] + came).astype(BF16)
                        st[2 + k, j, rest, :] = total[rest].astype(BF16)
                        final_copy(phase, k, j).start()

                    tiles(body)

            @pl.when(t == 7)
            def _():
                def body(j):
                    core_copy(3, j).wait_recv()

                    @pl.when(j >= 2)
                    def _():
                        own_copy(phase, j).wait()

                    own_st[j % 2] = product(phase, 1, j) + from_core[3, j].astype(F32)
                    own_copy(phase, j).start()

                tiles(body)
                for j in (0, 1):
                    own_copy(phase, j).wait()
                if phase == 0:
                    for j in range(steps):
                        weight_copy(2, j).start()

            return carry

        lax.fori_loop(0, 8, step, 0)

    for j in range(steps):
        core_copy(0, j).wait_send()
        for k in range(2):
            diag_copy(1, k, j).wait_send()
            final_copy(1, k, j).wait_send()
            for phase in (0, 1):
                final_copy(phase, k, j).wait_recv()


def back_layer(act, d_gate, d_up, w_gate, w_up, w_down, tp, bn=512):
    total, width = act.shape
    dim = w_gate.shape[0]
    rows = total // tp
    steps = dim // bn
    anyspace = pl.BlockSpec(memory_space=pl.ANY)
    dma = pltpu.SemaphoreType.DMA
    came = jax.ShapeDtypeStruct((2, rows, dim), BF16)
    return pl.pallas_call(
        functools.partial(back_kernel, rows=rows, bn=bn),
        out_shape=(jax.ShapeDtypeStruct((2, rows, dim), F32), came, came),
        in_specs=[anyspace] * 6,
        out_specs=(anyspace,) * 3,
        scratch_shapes=[pltpu.VMEM((width, dim), BF16), pltpu.VMEM((dim, width), BF16), pltpu.VMEM((2, 2, rows, width), BF16),
                        pltpu.VMEM((4, steps, rows, bn), BF16), pltpu.VMEM((4, steps, rows, bn), BF16),
                        pltpu.VMEM((2, 2, steps, rows // 2, bn), BF16), pltpu.VMEM((2, rows, bn), F32),
                        dma((3, steps)), dma((2, 2)), dma((2,)), dma((steps,)), dma((4, steps)),
                        dma((2, steps)), dma((2, 2, steps)), dma((2, steps)), dma((2, 2, steps))],
        compiler_params=pltpu.CompilerParams(vmem_limit_bytes=67043328, collective_id=1, has_side_effects=True),
        cost_estimate=pl.CostEstimate(flops=6 * total * dim * width, bytes_accessed=200 << 20, transcendentals=0),
        name="back",
    )(act, d_gate, d_up, w_gate, w_up, w_down)


def solution(mesh):
    tp_size = mesh.shape["tp"]
    act_spec = P("dp", "tp", None)
    in_specs = (act_spec, act_spec, P("dp"), P("dp"), P(None), P(None, "tp"), P(None, None), P(None, None), P("tp", None), P(None), P(None, "tp"), P(None, "tp"), P("tp", None))
    out_specs = (act_spec, act_spec, P("dp"), P("dp", "tp"), P("dp", None), P("dp", None), P(("dp", "tp"), None), P("dp"), P("dp", "tp"), P("dp", "tp"), P(("dp", "tp"), None))

    def layer(hidden, grad_out, prefix_len, valid_len, attn_norm, w_query, w_key, w_value, w_out, mlp_norm, w_gate, w_up, w_down):
        batch, shard, dim = hidden.shape
        head_dim = w_key.shape[1]
        rows = batch * shard
        me = lax.axis_index("tp")
        starts = (me ^ jnp.array([0, 2, 4, 6, 1, 3, 5, 7], jnp.int32)) * shard
        k_pos = (starts[:, None] + jnp.arange(shard, dtype=jnp.int32)).reshape(1, tp_size * shard)
        lens = jnp.concatenate([jnp.stack([prefix_len, valid_len, jnp.full((batch,), me, jnp.int32)]),
                                jnp.broadcast_to(starts[:, None], (tp_size, batch))])
        cos_t, sin_t = rope_tables(me * shard + jnp.arange(shard), head_dim)
        cos_t, sin_t = jnp.tile(cos_t, (batch, 1)), jnp.tile(sin_t, (batch, 1))

        def rope(raw_proj):
            return apply_rope(raw_proj, cos_t, sin_t).astype(BF16)

        wq_all = lax.all_gather(w_query, "tp", axis=0)
        hidden = hidden.reshape(rows, dim)
        grad_out = grad_out.reshape(rows, dim)
        normed, norm1_pull = jax.vjp(rms_norm, hidden, attn_norm.astype(F32))
        keys, key_pull = jax.vjp(rope, dot_nn(normed, w_key))
        values = dot_nn(normed, w_value).astype(BF16)
        kv0, kv1 = gather_near(jnp.concatenate([keys, values], axis=1))
        wo_all = lax.all_gather(w_out, "tp", axis=0, tiled=True)
        q_raw = jnp.einsum("td,hde->hte", normed, wq_all, preferred_element_type=F32)
        query, query_pull = jax.vjp(rope, q_raw)
        mixed = attention_forward(lens, k_pos, query, kv0, kv1, batch)
        attn_out = dot_nn(mixed, wo_all)
        resid = (hidden.astype(F32) + attn_out).astype(BF16)
        gated_in, norm2_pull = jax.vjp(rms_norm, resid, mlp_norm.astype(F32))
        gated_all, grad_all, act, d_gate, d_upper = gated_layer(gated_in, grad_out, w_gate, w_up, w_down, tp_size)
        own_part, x_part, y_part = back_layer(act, d_gate, d_upper, w_gate, w_up, w_down, tp_size)
        mlp_sum, d_gated = [own_part[k] + x_part[k].astype(F32) + y_part[k].astype(F32) for k in range(2)]
        d_gated = d_gated.astype(BF16)
        hidden_out = (resid.astype(F32) + mlp_sum).astype(BF16)
        g_down = dot_tn(act, grad_all)
        g_gate = dot_tn(gated_all, d_gate)
        g_up = dot_tn(gated_all, d_upper)

        d_resid_norm, g_mlp_norm_part = norm2_pull(d_gated)
        d_resid = (grad_out.astype(F32) + d_resid_norm.astype(F32)).astype(BF16)
        g_out_part = dot_tn(mixed, d_resid)
        d_mixed = dot_nt(d_resid, wo_all).astype(BF16)
        d_mixed, g_out_part = lax.optimization_barrier((d_mixed, g_out_part))
        g_out = lax.psum_scatter(g_out_part, "tp", scatter_dimension=0, tiled=True)
        d_query, dkv_near, dkv_far = attention_backward(lens, query, kv0, kv1, d_mixed, batch)
        d_q_raw = query_pull(d_query)[0].astype(BF16)

        came = swap(dkv_far, 1)
        g_query_part = jnp.einsum("td,hte->hde", normed, d_q_raw, preferred_element_type=F32)
        came, g_query_part = lax.optimization_barrier((came, g_query_part))
        g_query = lax.psum_scatter(g_query_part, "tp", scatter_dimension=0, tiled=False)
        own, side, back, diag = [dkv_near[k].astype(F32) + came[k].astype(F32) for k in range(4)]
        diag = diag.astype(BF16)
        half = rows // 2
        came_side, came_back = swap(diag[:half], 2), swap(diag[half:], 4)
        d_normed_q = jnp.einsum("hte,hde->td", d_q_raw, wq_all, preferred_element_type=F32)
        came_side, came_back, d_normed_q = lax.optimization_barrier((came_side, came_back, d_normed_q))
        back = jnp.concatenate([back[:half] + came_side.astype(F32), back[half:]], axis=0).astype(BF16)
        side = jnp.concatenate([side[:half], side[half:] + came_back.astype(F32)], axis=0).astype(BF16)
        last_side, last_back = swap(side, 2), swap(back, 4)
        last_side, last_back, g_gate = lax.optimization_barrier((last_side, last_back, g_gate))
        d_kv = (own + last_side.astype(F32) + last_back.astype(F32)).astype(BF16)
        d_k_raw = key_pull(d_kv[:, :head_dim])[0].astype(BF16)
        d_values = d_kv[:, head_dim:]
        g_kv_part = dot_tn(normed, jnp.concatenate([d_k_raw, d_values], axis=1))
        g_kv = lax.psum_scatter(g_kv_part, "tp", scatter_dimension=0, tiled=True)
        g_kv, g_down, g_up = lax.optimization_barrier((g_kv, g_down, g_up))
        g_kv = lax.all_gather(g_kv, "tp", axis=0, tiled=True)
        g_key, g_value = g_kv[:, :head_dim], g_kv[:, head_dim:]
        d_normed = (d_normed_q + dot_nt(d_k_raw, w_key) + dot_nt(d_values, w_value)).astype(BF16)
        d_hidden_norm, g_attn_norm_part = norm1_pull(d_normed)
        grad_hidden = (d_resid.astype(F32) + d_hidden_norm.astype(F32)).astype(BF16)
        g_norms = all_sum_small(jnp.stack([g_attn_norm_part, g_mlp_norm_part]))
        full = (batch, shard, dim)
        return (hidden_out.reshape(full), grad_hidden.reshape(full), g_norms[0], g_query, g_key, g_value, g_out, g_norms[1], g_gate, g_up, g_down)

    return jax.shard_map(layer, mesh=mesh, in_specs=in_specs, out_specs=out_specs, check_vma=False)
```

```python
import functools
import math
import jax
import jax.numpy as jnp
from jax import lax
from jax.experimental import pallas as pl
from jax.experimental.pallas import tpu as pltpu
from jax.sharding import PartitionSpec as P

NORM_EPS = 1e-6
BF16 = jnp.bfloat16
F32 = jnp.float32
GELU_C = math.sqrt(2.0 / math.pi)
GELU_K = 0.044715
MASKED = -1e30
NT = (((1,), (1,)), ((), ()))
TN = (((0,), (0,)), ((), ()))


def rms_norm(x_in, gain):
    x_f = x_in.astype(F32)
    inv_rms = lax.rsqrt(jnp.mean(x_f * x_f, axis=-1, keepdims=True) + NORM_EPS)
    return (x_f * inv_rms * (1.0 + gain)).astype(BF16)


def rope_tables(positions, head_dim):
    half_dim = head_dim // 2
    exponent = jnp.arange(half_dim, dtype=F32) * (2.0 / head_dim)
    inv_freq = jnp.exp(exponent * (-math.log(10000.0)))
    angles = positions.astype(F32)[:, None] * inv_freq[None, :]
    return jnp.cos(angles), jnp.sin(angles)


def apply_rope(x_f, cos_t, sin_t):
    half_dim = x_f.shape[-1] // 2
    first = x_f[..., :half_dim]
    second = x_f[..., half_dim:]
    return jnp.concatenate([first * cos_t - second * sin_t, second * cos_t + first * sin_t], axis=-1)


def dot_nn(a, b):
    return jnp.dot(a, b, preferred_element_type=F32)


def dot_nt(a, b):
    return lax.dot_general(a, b, NT, preferred_element_type=F32)


def dot_tn(a, b):
    return lax.dot_general(a, b, TN, preferred_element_type=F32)


def swap(x, bit):
    return lax.ppermute(x, "tp", [(t, t ^ bit) for t in range(8)])


def gather_near(own):
    half = own.shape[0] // 2
    side = swap(own, 2)
    back = swap(own, 4)
    diag = jnp.concatenate([swap(side[:half], 4), swap(back[half:], 2)], axis=0)
    mine = jnp.stack([own, side, back, diag])
    return mine, swap(mine, 1)


def keys_values(kv0_ref, kv1_ref, total, head_dim):
    both = jnp.concatenate([kv0_ref[...].reshape(total // 2, 2 * head_dim), kv1_ref[...].reshape(total // 2, 2 * head_dim)], axis=0)
    return both[:, :head_dim], both[:, head_dim:]


def attn_fwd_kernel(lens_ref, kpos_ref, q_ref, kv0_ref, kv1_ref, o_ref, p_ref):
    heads, shard, head_dim = q_ref.shape
    total = 2 * kv0_ref.shape[0] * shard
    s_id = pl.program_id(0)
    prefix = lens_ref[0, s_id]
    valid = lens_ref[1, s_id]
    first = lens_ref[2, 0] * shard
    keys, values = keys_values(kv0_ref, kv1_ref, total, head_dim)
    q_pos = first + lax.broadcasted_iota(jnp.int32, (shard, 1), 0)
    visible = kpos_ref[...] < jnp.minimum(valid, jnp.maximum(prefix, q_pos + 1))
    query = q_ref[...].reshape(heads * shard, head_dim) * BF16(head_dim ** -0.5)
    scores = dot_nt(query, keys)
    for h in range(heads):
        rows = slice(h * shard, (h + 1) * shard)
        s = jnp.where(visible, scores[rows], MASKED)
        e = jnp.exp(s - jnp.max(s, axis=-1, keepdims=True))
        p_ref[rows, :] = (e * (1.0 / jnp.sum(e, axis=-1, keepdims=True))).astype(BF16)
    mixed = dot_nn(p_ref[...], values).astype(BF16)
    for h in range(heads):
        o_ref[:, h * head_dim:(h + 1) * head_dim] = mixed[h * shard:(h + 1) * shard]


def attn_bwd_kernel(lens_ref, cos_ref, sin_ref, q_ref, kv0_ref, kv1_ref, do_ref, dq_ref, dkv0_ref, dkv1_ref, dkv_acc):
    heads, shard, head_dim = q_ref.shape
    tp = 2 * kv0_ref.shape[0]
    total = tp * shard
    rows = heads * shard
    s_id = pl.program_id(0)
    g_id = pl.program_id(1)
    prefix = lens_ref[0, s_id]
    valid = lens_ref[1, s_id]
    first = lens_ref[2, 0] * shard
    keys, values = keys_values(kv0_ref, kv1_ref, total, head_dim)
    query = q_ref[...].reshape(rows, head_dim) * BF16(head_dim ** -0.5)
    d_out = jnp.concatenate([do_ref[:, h * head_dim:(h + 1) * head_dim] for h in range(heads)], axis=0)
    step = lax.broadcasted_iota(jnp.int32, (shard, 1), 0)
    k_pos = jnp.concatenate([step + lens_ref[3 + r, 0] for r in range(tp)], axis=0)
    q_pos = first + lax.rem(lax.broadcasted_iota(jnp.int32, (1, rows), 1), shard)
    limit = jnp.minimum(valid, jnp.maximum(prefix, q_pos + 1))
    s = jnp.where(k_pos < limit, dot_nt(keys, query), MASKED)
    e = jnp.exp(s - jnp.max(s, axis=0, keepdims=True))
    p = e * (1.0 / jnp.sum(e, axis=0, keepdims=True))
    d_p = dot_nt(values, d_out)
    delta = jnp.sum(p * d_p, axis=0, keepdims=True)
    d_s = (p * (d_p - delta)).astype(BF16)
    d_v = dot_nn(p.astype(BF16), d_out)
    d_k = dot_nn(d_s, query)
    d_q = (dot_tn(d_s, keys) * (head_dim ** -0.5)).reshape(heads, shard, head_dim)
    first, second = d_q[:, :, :head_dim // 2], d_q[:, :, head_dim // 2:]
    cos_t, sin_t = cos_ref[...][None], sin_ref[...][None]
    dq_ref[:, :, :head_dim // 2] = (first * cos_t + second * sin_t).astype(BF16)
    dq_ref[:, :, head_dim // 2:] = (second * cos_t - first * sin_t).astype(BF16)

    d_kv = jnp.concatenate([d_k, d_v], axis=1)

    @pl.when(g_id == 0)
    def _():
        dkv_acc[...] = d_kv

    @pl.when(g_id > 0)
    def _():
        dkv_acc[...] += d_kv

    @pl.when(g_id == pl.num_programs(1) - 1)
    def _():
        near = (tp // 2, shard, 2 * head_dim)
        dkv0_ref[...] = dkv_acc[:total // 2].astype(BF16).reshape(near)
        dkv1_ref[...] = dkv_acc[total // 2:].astype(BF16).reshape(near)


def attention_forward(lens, k_pos, query, kv0, kv1, batch, group=4):
    heads, rows, head_dim = query.shape
    near = kv0.shape[0]
    shard = rows // batch
    total = 2 * near * shard
    q_spec = pl.BlockSpec((group, shard, head_dim), lambda s, g, *_: (g, s, 0))
    return pl.pallas_call(
        attn_fwd_kernel,
        out_shape=jax.ShapeDtypeStruct((rows, heads * head_dim), BF16),
        grid_spec=pltpu.PrefetchScalarGridSpec(
            num_scalar_prefetch=1, grid=(batch, heads // group),
            in_specs=[pl.BlockSpec((1, total), lambda s, g, *_: (0, 0)), q_spec,
                      pl.BlockSpec((near, shard, 2 * head_dim), lambda s, g, *_: (0, s, 0)),
                      pl.BlockSpec((near, shard, 2 * head_dim), lambda s, g, *_: (0, s, 0))],
            out_specs=pl.BlockSpec((shard, group * head_dim), lambda s, g, *_: (s, g)),
            scratch_shapes=[pltpu.VMEM((group * shard, total), BF16)]),
        compiler_params=pltpu.CompilerParams(dimension_semantics=("arbitrary", "arbitrary"), vmem_limit_bytes=48 << 20),
        cost_estimate=pl.CostEstimate(flops=4 * heads * rows * total * head_dim, bytes_accessed=12 << 20, transcendentals=heads * rows * total),
        name="attn_fwd",
    )(lens, k_pos, query, kv0, kv1)


def attention_backward(lens, cos_t, sin_t, query, kv0, kv1, d_mixed, batch, group=4):
    heads, rows, head_dim = query.shape
    near = kv0.shape[0]
    shard = rows // batch
    total = 2 * near * shard
    q_spec = pl.BlockSpec((group, shard, head_dim), lambda s, g, *_: (g, s, 0))
    kv_spec = pl.BlockSpec((near, shard, 2 * head_dim), lambda s, g, *_: (0, s, 0))
    table = pl.BlockSpec((shard, head_dim // 2), lambda s, g, *_: (0, 0))
    kv_shape = jax.ShapeDtypeStruct((near, rows, 2 * head_dim), BF16)
    return pl.pallas_call(
        attn_bwd_kernel,
        out_shape=(jax.ShapeDtypeStruct((heads, rows, head_dim), BF16), kv_shape, kv_shape),
        grid_spec=pltpu.PrefetchScalarGridSpec(
            num_scalar_prefetch=1, grid=(batch, heads // group),
            in_specs=[table, table, q_spec, kv_spec, kv_spec, pl.BlockSpec((shard, group * head_dim), lambda s, g, *_: (s, g))],
            out_specs=(q_spec, kv_spec, kv_spec),
            scratch_shapes=[pltpu.VMEM((total, 2 * head_dim), F32)]),
        compiler_params=pltpu.CompilerParams(dimension_semantics=("arbitrary", "arbitrary"), vmem_limit_bytes=56 << 20),
        cost_estimate=pl.CostEstimate(flops=10 * heads * rows * total * head_dim, bytes_accessed=20 << 20, transcendentals=heads * rows * total),
        name="attn_bwd",
    )(lens, cos_t, sin_t, query, kv0, kv1, d_mixed)


def flip(index, bit):
    return index + bit - 2 * bit * ((index // bit) % 2)


def neighbours():
    me = lax.axis_index("tp")
    return me, flip(me, 1), flip(me, 2), flip(me, 4)


def enter(peers):
    barrier = pltpu.get_barrier_semaphore()
    for peer in peers:
        pl.semaphore_signal(barrier, inc=1, device_id={"tp": peer}, device_id_type=pl.DeviceIdType.MESH)
    pl.semaphore_wait(barrier, len(peers))


def gated_tile(z, g, w_g, w_u, w_d):
    gate = dot_nn(z, w_g)
    upper = dot_nn(z, w_u)
    d_act = dot_nt(g, w_d).astype(BF16).astype(F32)
    sq = gate * gate
    th = jnp.tanh(gate * (GELU_C + (GELU_C * GELU_K) * sq))
    half = 0.5 + 0.5 * th
    gelu = gate * half
    slope = half + gate * (0.5 - 0.5 * (th * th)) * (GELU_C + (3.0 * GELU_C * GELU_K) * sq)
    return (gelu * upper).astype(BF16), (d_act * upper * slope).astype(BF16), (d_act * gelu).astype(BF16)


def gated_kernel(z_own, g_own, wg_hbm, wu_hbm, wd_hbm, z_all, g_all, act, d_gate, d_up,
                 wg, wu, wd, z_buf, g_buf, outs, w_sem, in_sem, own_sem, out_sem, send, recv, send0, recv0, *, bn):
    rows, _ = z_own.shape
    width = wg_hbm.shape[1]
    steps = width // bn
    piece = rows // 4
    me, core, side, back = neighbours()
    corner = flip(side, 4)
    own = (z_own, g_own)
    full = (z_all, g_all)

    def remote(src, dst, sems, peer):
        return pltpu.make_async_remote_copy(src_ref=src, dst_ref=dst, send_sem=sems[0], recv_sem=sems[1],
                                            device_id={"tp": peer}, device_id_type=pl.DeviceIdType.MESH)

    def part(slot, q):
        return pl.ds(pl.multiple_of(slot * rows + q * piece, 16), piece)

    def link_rows(u, path):
        turn = u // 2
        diag = turn % 2
        if path == 0:
            return side + (corner - side) * diag, (u % 2) + 2 * (turn // 2) + diag * 2
        return back + (corner - back) * diag, (u % 2) + 2 - 2 * (turn // 2) - diag * 2

    def link_copy(u, path, a):
        turn = u // 2
        peer = side if path == 0 else back
        sems = (send.at[path, u, a], recv.at[path, u, a])
        if turn == 1:
            slot = back if path == 0 else side
            q = (2 if path == 0 else 0) + u % 2
            return remote(full[a].at[part(slot, q)], full[a].at[part(slot, q)], sems, peer)
        q = u % 2 + (2 * (turn // 2) if path == 0 else 2 - 2 * (turn // 2))
        return remote(own[a].at[pl.ds(q * piece, piece)], full[a].at[part(me, q)], sems, peer)

    def core_copy(u, path, a):
        slot, q = link_rows(u, path)
        return remote(full[a].at[part(slot, q)], full[a].at[part(slot, q)], (send.at[2 + path, u, a], recv.at[2 + path, u, a]), core)

    def own_copy(a):
        return remote(own[a], full[a].at[pl.ds(pl.multiple_of(me * rows, 16), rows)], (send0.at[a], recv0.at[a]), core)

    def weight_copies(n):
        cols = pl.ds(pl.multiple_of(n * bn, 128), bn)
        return [pltpu.make_async_copy(wg_hbm.at[:, cols], wg.at[:, cols], w_sem.at[0, n]),
                pltpu.make_async_copy(wu_hbm.at[:, cols], wu.at[:, cols], w_sem.at[1, n]),
                pltpu.make_async_copy(wd_hbm.at[cols], wd.at[cols], w_sem.at[2, n])]

    bufs = (z_buf, g_buf)
    own_in = [pltpu.make_async_copy(own[a], bufs[a], own_sem.at[a]) for a in range(2)]
    own_out = [pltpu.make_async_copy(bufs[a], full[a].at[pl.ds(pl.multiple_of(me * rows, 16), rows)], own_sem.at[2 + a]) for a in range(2)]
    for cp in own_in:
        cp.start()
    for n in range(steps):
        for cp in weight_copies(n):
            cp.start()
    enter((core, side, back))
    for u in range(2):
        for path in range(2):
            for a in range(2):
                link_copy(u, path, a).start()
        if u == 0:
            for a in range(2):
                own_copy(a).start()

    def out_copies(slot, s_rows, n):
        cols = pl.ds(pl.multiple_of(n * bn, 128), bn)
        return [pltpu.make_async_copy(outs.at[slot, k, pl.ds(i * piece, piece)], ref.at[s_rows[i], cols], out_sem.at[slot, k, i])
                for k, ref in enumerate((act, d_gate, d_up)) for i in range(4)]

    def stage_rows(s):
        late = (s + 6) // 8
        u = (s - 2) * late
        first = me + (core - me) * s * (1 - late)
        (slot_x, q_x), (slot_y, q_y) = link_rows(u, 0), link_rows(u, 1)
        base_x, base_y = slot_x * rows + q_x * piece, slot_y * rows + q_y * piece
        pair_x, pair_y = flip(slot_x, 1) * rows + q_x * piece, flip(slot_y, 1) * rows + q_y * piece
        starts = [(1 - late) * (first * rows + i * piece) + late * base for i, base in enumerate((base_x, base_y, pair_x, pair_y))]
        return [pl.ds(pl.multiple_of(st, 16), piece) for st in starts]

    def compute(s):
        s_rows = stage_rows(s)

        def block(n, carry):
            step = s * steps + n
            slot = step % 2

            @pl.when(step >= 2)
            def _():
                for cp in out_copies(slot, s_rows, n):
                    cp.wait()

            @pl.when(s == 0)
            def _():
                for cp in weight_copies(n):
                    cp.wait()

            cols = pl.ds(pl.multiple_of(n * bn, 128), bn)
            res = gated_tile(z_buf[...], g_buf[...], wg[:, cols], wu[:, cols], wd[cols, :])
            for k in range(3):
                outs[slot, k] = res[k]
            for cp in out_copies(slot, s_rows, n):
                cp.start()
            return carry

        lax.fori_loop(0, steps, block, 0)

    def stage(s, carry):
        @pl.when(s == 0)
        def _():
            for cp in own_in:
                cp.wait()
            for cp in own_out:
                cp.start()

        @pl.when(s == 1)
        def _():
            for cp in own_out:
                cp.wait()
            for a in range(2):
                own_copy(a).wait_recv()

        for u in range(6):
            @pl.when(s == u + 2)
            def _(u=u):
                for path in range(2):
                    for a in range(2):
                        link_copy(u, path, a).wait_recv()
                        core_copy(u, path, a).start()
                if u < 2:
                    for path in range(2):
                        for a in range(2):
                            link_copy(u + 2, path, a).start()
                if u == 1:
                    for later in (4, 5):
                        for path in range(2):
                            for a in range(2):
                                link_copy(later, path, a).start()
                for path in range(2):
                    for a in range(2):
                        core_copy(u, path, a).wait_recv()

        @pl.when(s >= 1)
        def _():
            s_rows = stage_rows(s)
            copies = [pltpu.make_async_copy(full[a].at[s_rows[i]], bufs[a].at[pl.ds(i * piece, piece)], in_sem.at[a, i])
                      for a in range(2) for i in range(4)]
            for cp in copies:
                cp.start()
            for cp in copies:
                cp.wait()

        compute(s)
        return carry

    lax.fori_loop(0, 8, stage, 0)
    last = stage_rows(7)
    for slot in range(2):
        for cp in out_copies(slot, last, 0):
            cp.wait()
    for a in range(2):
        own_copy(a).wait_send()
        for path in range(2):
            for u in range(6):
                link_copy(u, path, a).wait_send()
                core_copy(u, path, a).wait_send()


def gated_layer(z_own, g_own, w_gate, w_up, w_down, tp, bn=512):
    rows, dim = z_own.shape
    width = w_gate.shape[1]
    total = rows * tp
    anyspace = pl.BlockSpec(memory_space=pl.ANY)
    gathered = jax.ShapeDtypeStruct((total, dim), BF16)
    made = jax.ShapeDtypeStruct((total, width), BF16)
    dma = pltpu.SemaphoreType.DMA
    return pl.pallas_call(
        functools.partial(gated_kernel, bn=bn),
        out_shape=(gathered, gathered, made, made, made),
        in_specs=[anyspace] * 5,
        out_specs=(anyspace,) * 5,
        scratch_shapes=[pltpu.VMEM((dim, width), BF16), pltpu.VMEM((dim, width), BF16), pltpu.VMEM((width, dim), BF16),
                        pltpu.VMEM((rows, dim), BF16), pltpu.VMEM((rows, dim), BF16), pltpu.VMEM((2, 3, rows, bn), BF16),
                        dma((3, width // bn)), dma((2, 4)), dma((4,)), dma((2, 3, 4)), dma((4, 6, 2)), dma((4, 6, 2)), dma((2,)), dma((2,))],
        compiler_params=pltpu.CompilerParams(vmem_limit_bytes=60 << 20, collective_id=0, has_side_effects=True),
        cost_estimate=pl.CostEstimate(flops=6 * total * dim * width, bytes_accessed=200 << 20, transcendentals=total * width),
        name="gated",
    )(z_own, g_own, w_gate, w_up, w_down)


def back_kernel(act, d_gate, d_up, wg_hbm, wu_hbm, wd_hbm, own_out, x_in, y_in,
                wa, wb, lhs, st, from_core, from_diag, own_st, w_sem, l_sem, o_sem, c_send, c_recv, d_send, d_recv, f_send, f_recv, *, rows, bn):
    dim = wg_hbm.shape[0]
    steps = dim // bn
    half = rows // 2
    me, core, side, back = neighbours()

    def remote(src, dst, send, recv, peer):
        return pltpu.make_async_remote_copy(src_ref=src, dst_ref=dst, send_sem=send, recv_sem=recv,
                                            device_id={"tp": peer}, device_id_type=pl.DeviceIdType.MESH)

    def cols(j):
        return pl.ds(pl.multiple_of(j * bn, 128), bn)

    def pair_of(t):
        return ((t + 5) // 7) * ((t + 1) % 3 + 1)

    def lhs_copies(phase, t):
        pair = pair_of(t)
        theirs = 1 - t // 5 - ((t + 6) // 7 - (t + 5) // 7)
        dev = me + (1 - pair // 2) * (side - me) + (1 - pair % 2) * (back - me)
        dev = dev + theirs * (flip(dev, 1) - dev)
        src = pl.ds(pl.multiple_of(dev * rows, 16), rows)
        refs = (act,) if phase == 0 else (d_gate, d_up)
        return [pltpu.make_async_copy(ref.at[src], lhs.at[t % 2, k], l_sem.at[t % 2, k]) for k, ref in enumerate(refs)]

    def weight_copy(k, j):
        if k == 0:
            return pltpu.make_async_copy(wd_hbm.at[:, cols(j)], wa.at[:, cols(j)], w_sem.at[0, j])
        src, dst = (wg_hbm, wb) if k == 1 else (wu_hbm, wa)
        return pltpu.make_async_copy(src.at[cols(j)], dst.at[cols(j)], w_sem.at[k, j])

    def core_copy(pair, j):
        return remote(st.at[0, j], from_core.at[pair, j], c_send.at[j], c_recv.at[pair, j], core)

    def diag_copy(phase, k, j):
        return remote(st.at[1, j, pl.ds(k * half, half)], from_diag.at[phase, k, j], d_send.at[k, j], d_recv.at[phase, k, j], (side, back)[k])

    def final_copy(phase, k, j):
        return remote(st.at[2 + k, j], (x_in, y_in)[k].at[phase, :, cols(j)], f_send.at[k, j], f_recv.at[phase, k, j], (side, back)[k])

    def own_copy(phase, j):
        return pltpu.make_async_copy(own_st.at[j % 2], own_out.at[phase, :, cols(j)], o_sem.at[j % 2])

    def product(phase, slot, j):
        if phase == 0:
            return dot_nn(lhs[slot, 0], wa[:, cols(j)])
        return dot_nt(lhs[slot, 0], wb[cols(j), :]) + dot_nt(lhs[slot, 1], wa[cols(j), :])

    for cp in lhs_copies(0, 0):
        cp.start()
    for j in range(steps):
        weight_copy(0, j).start()
    enter((core, side, back))

    def tiles(body):
        def step(j, carry):
            body(j)
            return carry

        lax.fori_loop(0, steps, step, 0)

    for phase in (0, 1):
        def step(t, carry, phase=phase):
            for cp in lhs_copies(phase, t):
                cp.wait()

            @pl.when(t < 7)
            def _():
                for cp in lhs_copies(phase, t + 1):
                    cp.start()

            if phase == 0:
                @pl.when(t == 1)
                def _():
                    for j in range(steps):
                        weight_copy(1, j).start()

                @pl.when(t == 7)
                def _():
                    for cp in lhs_copies(1, 0):
                        cp.start()

            @pl.when((t == 0) | ((t >= 2) & (t <= 4)))
            def _():
                pair = pair_of(t)

                def body(j):
                    @pl.when(t == 0)
                    def _():
                        for k in ((0,) if phase == 0 else (1, 2)):
                            weight_copy(k, j).wait()

                    if phase == 0:
                        @pl.when(t > 0)
                        def _():
                            core_copy(0, j).wait_send()
                    else:
                        core_copy(0, j).wait_send()
                    st[0, j] = product(phase, t % 2, j).astype(BF16)
                    core_copy(pair, j).start()

                tiles(body)

            @pl.when(t == 1)
            def _():
                def body(j):
                    core_copy(0, j).wait_recv()
                    if phase == 1:
                        for k in range(2):
                            diag_copy(0, k, j).wait_send()
                    st[1, j] = (product(phase, 1, j) + from_core[0, j].astype(F32)).astype(BF16)
                    for k in range(2):
                        diag_copy(phase, k, j).start()

                tiles(body)

            for k in range(2):
                @pl.when(t == 5 + k)
                def _(k=k):
                    def body(j):
                        core_copy(1 + k, j).wait_recv()
                        diag_copy(phase, 1 - k, j).wait_recv()
                        if phase == 1:
                            final_copy(0, k, j).wait_send()
                        total = product(phase, (5 + k) % 2, j) + from_core[1 + k, j].astype(F32)
                        came = from_diag[phase, 1 - k, j].astype(F32)
                        split = slice(half, rows) if k == 0 else slice(0, half)
                        rest = slice(0, half) if k == 0 else slice(half, rows)
                        st[2 + k, j, split, :] = (total[split] + came).astype(BF16)
                        st[2 + k, j, rest, :] = total[rest].astype(BF16)
                        final_copy(phase, k, j).start()

                    tiles(body)

            @pl.when(t == 7)
            def _():
                def body(j):
                    core_copy(3, j).wait_recv()

                    @pl.when(j >= 2)
                    def _():
                        own_copy(phase, j).wait()

                    own_st[j % 2] = product(phase, 1, j) + from_core[3, j].astype(F32)
                    own_copy(phase, j).start()

                tiles(body)
                for j in (0, 1):
                    own_copy(phase, j).wait()
                if phase == 0:
                    for j in range(steps):
                        weight_copy(2, j).start()

            return carry

        lax.fori_loop(0, 8, step, 0)

    for j in range(steps):
        core_copy(0, j).wait_send()
        for k in range(2):
            diag_copy(1, k, j).wait_send()
            final_copy(1, k, j).wait_send()
            for phase in (0, 1):
                final_copy(phase, k, j).wait_recv()


def back_layer(act, d_gate, d_up, w_gate, w_up, w_down, tp, bn=512):
    total, width = act.shape
    dim = w_gate.shape[0]
    rows = total // tp
    steps = dim // bn
    anyspace = pl.BlockSpec(memory_space=pl.ANY)
    dma = pltpu.SemaphoreType.DMA
    came = jax.ShapeDtypeStruct((2, rows, dim), BF16)
    return pl.pallas_call(
        functools.partial(back_kernel, rows=rows, bn=bn),
        out_shape=(jax.ShapeDtypeStruct((2, rows, dim), F32), came, came),
        in_specs=[anyspace] * 6,
        out_specs=(anyspace,) * 3,
        scratch_shapes=[pltpu.VMEM((width, dim), BF16), pltpu.VMEM((dim, width), BF16), pltpu.VMEM((2, 2, rows, width), BF16),
                        pltpu.VMEM((4, steps, rows, bn), BF16), pltpu.VMEM((4, steps, rows, bn), BF16),
                        pltpu.VMEM((2, 2, steps, rows // 2, bn), BF16), pltpu.VMEM((2, rows, bn), F32),
                        dma((3, steps)), dma((2, 2)), dma((2,)), dma((steps,)), dma((4, steps)),
                        dma((2, steps)), dma((2, 2, steps)), dma((2, steps)), dma((2, 2, steps))],
        compiler_params=pltpu.CompilerParams(vmem_limit_bytes=67043328, collective_id=1, has_side_effects=True),
        cost_estimate=pl.CostEstimate(flops=6 * total * dim * width, bytes_accessed=200 << 20, transcendentals=0),
        name="back",
    )(act, d_gate, d_up, w_gate, w_up, w_down)


def product_kernel(a_ref, b_ref, o_ref):
    o_ref[...] = dot_tn(a_ref[...], b_ref[...])


def weight_grad(a, b, bm=512, bn=1024):
    rows, m = a.shape
    n = b.shape[1]
    return pl.pallas_call(
        product_kernel,
        out_shape=jax.ShapeDtypeStruct((m, n), F32),
        grid=(m // bm, n // bn),
        in_specs=[pl.BlockSpec((rows, bm), lambda i, j: (0, i)), pl.BlockSpec((rows, bn), lambda i, j: (0, j))],
        out_specs=pl.BlockSpec((bm, bn), lambda i, j: (i, j)),
        compiler_params=pltpu.CompilerParams(dimension_semantics=("arbitrary", "arbitrary"), vmem_limit_bytes=56 << 20),
        cost_estimate=pl.CostEstimate(flops=2 * rows * m * n, bytes_accessed=110 << 20, transcendentals=0),
        name="weight_grad",
    )(a, b)


def pick(x, index):
    return lax.dynamic_index_in_dim(x, index, axis=0, keepdims=False)


def hop_diagonal(diag):
    half = diag.shape[0] // 2
    return swap(diag[:half], 2), swap(diag[half:], 4)


def hop_near(side, back, came_side, came_back):
    half = side.shape[0] // 2
    kind = came_side.dtype
    side = jnp.concatenate([side[:half], side[half:] + came_back.astype(F32)], axis=0).astype(kind)
    back = jnp.concatenate([back[:half] + came_side.astype(F32), back[half:]], axis=0).astype(kind)
    return side, back


def solution(mesh):
    tp_size = mesh.shape["tp"]
    act_spec = P("dp", "tp", None)
    in_specs = (act_spec, act_spec, P("dp"), P("dp"), P(None), P(None, "tp"), P(None, None), P(None, None), P("tp", None), P(None), P(None, "tp"), P(None, "tp"), P("tp", None))
    out_specs = (act_spec, act_spec, P("dp"), P("dp", "tp"), P("dp", None), P("dp", None), P(("dp", "tp"), None), P("dp"), P("dp", "tp"), P("dp", "tp"), P(("dp", "tp"), None))

    def layer(hidden, grad_out, prefix_len, valid_len, attn_norm, w_query, w_key, w_value, w_out, mlp_norm, w_gate, w_up, w_down):
        batch, shard, dim = hidden.shape
        head_dim = w_key.shape[1]
        rows = batch * shard
        me = lax.axis_index("tp")
        starts = (me ^ jnp.array([0, 2, 4, 6, 1, 3, 5, 7], jnp.int32)) * shard
        k_pos = (starts[:, None] + jnp.arange(shard, dtype=jnp.int32)).reshape(1, tp_size * shard)
        lens = jnp.concatenate([jnp.stack([prefix_len, valid_len, jnp.full((batch,), me, jnp.int32)]),
                                jnp.broadcast_to(starts[:, None], (tp_size, batch))])
        cos_own, sin_own = rope_tables(me * shard + jnp.arange(shard), head_dim)
        cos_t, sin_t = jnp.tile(cos_own, (batch, 1)), jnp.tile(sin_own, (batch, 1))

        def rope(raw_proj):
            return apply_rope(raw_proj, cos_t, sin_t).astype(BF16)

        wq_all = lax.all_gather(w_query, "tp", axis=0)
        hidden = hidden.reshape(rows, dim)
        grad_out = grad_out.reshape(rows, dim)
        normed, norm1_pull = jax.vjp(rms_norm, hidden, attn_norm.astype(F32))
        keys, key_pull = jax.vjp(rope, dot_nn(normed, w_key))
        values = dot_nn(normed, w_value).astype(BF16)
        kv0, kv1 = gather_near(jnp.concatenate([keys, values], axis=1))
        wo_all = lax.all_gather(w_out, "tp", axis=0, tiled=True)
        q_raw = jnp.einsum("td,hde->hte", normed, wq_all, preferred_element_type=F32)
        query = rope(q_raw)
        mixed = attention_forward(lens, k_pos, query, kv0, kv1, batch)
        attn_out = dot_nn(mixed, wo_all)
        resid = (hidden.astype(F32) + attn_out).astype(BF16)
        gated_in, norm2_pull = jax.vjp(rms_norm, resid, mlp_norm.astype(F32))
        gated_all, grad_all, act, d_gate, d_upper = gated_layer(gated_in, grad_out, w_gate, w_up, w_down, tp_size)
        own_part, x_part, y_part = back_layer(act, d_gate, d_upper, w_gate, w_up, w_down, tp_size)
        mlp_sum, d_gated = [own_part[k] + x_part[k].astype(F32) + y_part[k].astype(F32) for k in range(2)]
        d_gated = d_gated.astype(BF16)
        hidden_out = (resid.astype(F32) + mlp_sum).astype(BF16)
        d_resid_norm, g_mlp_norm_part = norm2_pull(d_gated)
        d_resid = (grad_out.astype(F32) + d_resid_norm.astype(F32)).astype(BF16)
        g_out_part = dot_tn(mixed, d_resid)
        d_mixed = dot_nt(d_resid, wo_all).astype(BF16)
        d_mixed, g_out_part = lax.optimization_barrier((d_mixed, g_out_part))
        g_out = lax.psum_scatter(g_out_part, "tp", scatter_dimension=0, tiled=True)
        d_q_raw, dkv_near, dkv_far = attention_backward(lens, cos_own, sin_own, query, kv0, kv1, d_mixed, batch)
        came_kv = swap(dkv_far, 1)
        plane = me // 2
        by_core = d_q_raw.reshape(tp_size // 2, 2, rows, head_dim)
        theirs = lax.dynamic_index_in_dim(by_core, 1 - me % 2, axis=1, keepdims=False)
        mine = lax.dynamic_index_in_dim(by_core, me % 2, axis=1, keepdims=False)
        came_q = swap(jnp.einsum("td,kte->kde", normed, theirs, preferred_element_type=F32), 1)
        d_normed_q = jnp.einsum("hte,hde->td", d_q_raw, wq_all, preferred_element_type=F32)
        came_kv, d_normed_q = lax.optimization_barrier((came_kv, d_normed_q))
        kv_own, kv_side, kv_back, kv_diag = [dkv_near[k].astype(F32) + came_kv[k].astype(F32) for k in range(4)]
        kv_came = hop_diagonal(kv_diag.astype(BF16))
        g_query_sum = jnp.einsum("td,kte->kde", normed, mine, preferred_element_type=F32) + came_q
        kv_came, g_query_sum, d_gate = lax.optimization_barrier((kv_came, g_query_sum, d_gate))
        kv_next = hop_near(kv_side, kv_back, *kv_came)
        kv_last = (swap(kv_next[0], 2), swap(kv_next[1], 4))
        q_came = hop_diagonal(pick(g_query_sum, plane ^ 3))
        g_gate = weight_grad(gated_all, d_gate)
        kv_last, q_came, g_gate = lax.optimization_barrier((kv_last, q_came, g_gate))
        d_kv = (kv_own + kv_last[0].astype(F32) + kv_last[1].astype(F32)).astype(BF16)
        d_k_raw = key_pull(d_kv[:, :head_dim])[0].astype(BF16)
        d_values = d_kv[:, head_dim:]
        q_next = hop_near(pick(g_query_sum, plane ^ 1), pick(g_query_sum, plane ^ 2), *q_came)
        g_key_part, g_value_part = dot_tn(normed, d_k_raw), dot_tn(normed, d_values)
        q_next, g_key_part, g_value_part, d_upper = lax.optimization_barrier((q_next, g_key_part, g_value_part, d_upper))
        g_key, g_value = lax.psum((g_key_part, g_value_part), "tp")
        q_last = (swap(q_next[0], 2), swap(q_next[1], 4))
        g_up = weight_grad(gated_all, d_upper)
        d_normed = (d_normed_q + dot_nt(d_k_raw, w_key) + dot_nt(d_values, w_value)).astype(BF16)
        q_last, g_up, d_normed, act = lax.optimization_barrier((q_last, g_up, d_normed, act))
        g_query = pick(g_query_sum, plane) + q_last[0] + q_last[1]
        d_hidden_norm, g_attn_norm_part = norm1_pull(d_normed)
        norms = jnp.stack([g_attn_norm_part, g_mlp_norm_part])
        norms_near = [swap(norms, bit) for bit in (2, 4, 6)]
        g_down = weight_grad(act, grad_all)
        norms_near, g_down, d_hidden_norm = lax.optimization_barrier((norms_near, g_down, d_hidden_norm))
        norms = norms + norms_near[0] + norms_near[1] + norms_near[2]
        g_norms = norms + swap(norms, 1)
        grad_hidden = (d_resid.astype(F32) + d_hidden_norm.astype(F32)).astype(BF16)
        full = (batch, shard, dim)
        return (hidden_out.reshape(full), grad_hidden.reshape(full), g_norms[0], g_query, g_key, g_value, g_out, g_norms[1], g_gate, g_up, g_down)

    return jax.shard_map(layer, mesh=mesh, in_specs=in_specs, out_specs=out_specs, check_vma=False)
```

```python
import functools
import math
import jax
import jax.numpy as jnp
from jax import lax
from jax.experimental import pallas as pl
from jax.experimental.pallas import tpu as pltpu
from jax.sharding import PartitionSpec as P

NORM_EPS = 1e-6
BF16 = jnp.bfloat16
F32 = jnp.float32
GELU_C = math.sqrt(2.0 / math.pi)
GELU_K = 0.044715
MASKED = -1e30
NT = (((1,), (1,)), ((), ()))
TN = (((0,), (0,)), ((), ()))


def rms_norm(x_in, gain):
    x_f = x_in.astype(F32)
    inv_rms = lax.rsqrt(jnp.mean(x_f * x_f, axis=-1, keepdims=True) + NORM_EPS)
    return (x_f * inv_rms * (1.0 + gain)).astype(BF16)


def rope_tables(positions, head_dim):
    half_dim = head_dim // 2
    exponent = jnp.arange(half_dim, dtype=F32) * (2.0 / head_dim)
    inv_freq = jnp.exp(exponent * (-math.log(10000.0)))
    angles = positions.astype(F32)[:, None] * inv_freq[None, :]
    return jnp.cos(angles), jnp.sin(angles)


def apply_rope(x_f, cos_t, sin_t):
    half_dim = x_f.shape[-1] // 2
    first = x_f[..., :half_dim]
    second = x_f[..., half_dim:]
    return jnp.concatenate([first * cos_t - second * sin_t, second * cos_t + first * sin_t], axis=-1)


def dot_nn(a, b):
    return jnp.dot(a, b, preferred_element_type=F32)


def dot_nt(a, b):
    return lax.dot_general(a, b, NT, preferred_element_type=F32)


def dot_tn(a, b):
    return lax.dot_general(a, b, TN, preferred_element_type=F32)


def swap(x, bit):
    return lax.ppermute(x, "tp", [(t, t ^ bit) for t in range(8)])


def flip(index, bit):
    return index + bit - 2 * bit * ((index // bit) % 2)


def neighbours():
    me = lax.axis_index("tp")
    return me, flip(me, 1), flip(me, 2), flip(me, 4)


def enter(peers):
    barrier = pltpu.get_barrier_semaphore()
    for peer in peers:
        pl.semaphore_signal(barrier, inc=1, device_id={"tp": peer}, device_id_type=pl.DeviceIdType.MESH)
    pl.semaphore_wait(barrier, len(peers))


def attn_bwd_kernel(lens_ref, cos_ref, sin_ref, q_ref, kv_ref, do_ref, dq_ref, dkv0_ref, dkv1_ref, dkv_acc):
    heads, shard, head_dim = q_ref.shape
    tp = kv_ref.shape[0]
    total = tp * shard
    rows = heads * shard
    s_id = pl.program_id(0)
    g_id = pl.program_id(1)
    prefix = lens_ref[0, s_id]
    valid = lens_ref[1, s_id]
    first = lens_ref[2, 0] * shard
    keys = kv_ref[:, :, :head_dim].reshape(total, head_dim)
    values = kv_ref[:, :, head_dim:].reshape(total, head_dim)
    query = q_ref[...].reshape(rows, head_dim) * BF16(head_dim ** -0.5)
    d_out = jnp.concatenate([do_ref[:, h * head_dim:(h + 1) * head_dim] for h in range(heads)], axis=0)
    step = lax.broadcasted_iota(jnp.int32, (shard, 1), 0)
    k_pos = jnp.concatenate([step + lens_ref[3 + r, 0] for r in range(tp)], axis=0)
    q_pos = first + lax.rem(lax.broadcasted_iota(jnp.int32, (1, rows), 1), shard)
    limit = jnp.minimum(valid, jnp.maximum(prefix, q_pos + 1))
    s = jnp.where(k_pos < limit, dot_nt(keys, query), MASKED)
    e = jnp.exp(s - jnp.max(s, axis=0, keepdims=True))
    p = e * (1.0 / jnp.sum(e, axis=0, keepdims=True))
    d_p = dot_nt(values, d_out)
    delta = jnp.sum(p * d_p, axis=0, keepdims=True)
    d_s = (p * (d_p - delta)).astype(BF16)
    d_v = dot_nn(p.astype(BF16), d_out)
    d_k = dot_nn(d_s, query)
    d_q = (dot_tn(d_s, keys) * (head_dim ** -0.5)).reshape(heads, shard, head_dim)
    first, second = d_q[:, :, :head_dim // 2], d_q[:, :, head_dim // 2:]
    cos_t, sin_t = cos_ref[...][None], sin_ref[...][None]
    dq_ref[:, :, :head_dim // 2] = (first * cos_t + second * sin_t).astype(BF16)
    dq_ref[:, :, head_dim // 2:] = (second * cos_t - first * sin_t).astype(BF16)

    d_kv = jnp.concatenate([d_k, d_v], axis=1)

    @pl.when(g_id == 0)
    def _():
        dkv_acc[...] = d_kv

    @pl.when(g_id > 0)
    def _():
        dkv_acc[...] += d_kv

    @pl.when(g_id == pl.num_programs(1) - 1)
    def _():
        near = (tp // 2, shard, 2 * head_dim)
        dkv0_ref[...] = dkv_acc[:total // 2].astype(BF16).reshape(near)
        dkv1_ref[...] = dkv_acc[total // 2:].astype(BF16).reshape(near)


def remote(src, dst, send, recv, peer):
    return pltpu.make_async_remote_copy(src_ref=src, dst_ref=dst, send_sem=send, recv_sem=recv,
                                        device_id={"tp": peer}, device_id_type=pl.DeviceIdType.MESH)


def front_kernel(lens_ref, kpos_ref, cos_ref, sin_ref, gain1_ref, gain2_ref, hidden, w_query, w_key, w_value, w_out,
                 normed_out, wq_all, wo_all, kv_all, query_out, mixed_out, resid_out, gated_out,
                 x_buf, n_buf, wkv, wq, wo, kv, q, probs, mix, acc, load, store, send, recv, *, batch):
    rows, dim = x_buf.shape
    shard = rows // batch
    head_dim = w_key.shape[1]
    tp = wq.shape[0]
    near = tp // 2
    total = tp * shard
    half_dim = head_dim // 2
    me, core, side, back = neighbours()
    bufs = (wq, kv, wo)

    def to_side(a):
        return remote(bufs[a].at[0], bufs[a].at[1], send.at[a, 0], recv.at[a, 0], side)

    def to_back(a):
        return remote(bufs[a].at[0], bufs[a].at[2], send.at[a, 1], recv.at[a, 1], back)

    def onward(a, k):
        half = bufs[a].shape[1] // 2
        part = pl.ds(k * half, half)
        return remote(bufs[a].at[1 + k, part], bufs[a].at[3, part], send.at[a, 2 + k], recv.at[a, 2 + k], (back, side)[k])

    def to_core(a, k):
        return remote(bufs[a].at[k], bufs[a].at[near + k], send.at[a, 4 + k], recv.at[a, 4 + k], core)

    loads = [pltpu.make_async_copy(src, dst, load.at[i]) for i, (src, dst) in enumerate((
        (w_query, wq.at[0]), (hidden, x_buf), (w_key, wkv.at[:, :head_dim]), (w_value, wkv.at[:, head_dim:]), (w_out, wo.at[0])))]
    mixed_at = [me, side, back, flip(side, 4)]
    mixed_at = mixed_at + [flip(dev, 1) for dev in mixed_at]
    stores = {name: pltpu.make_async_copy(src, dst, store.at[i]) for i, (name, src, dst) in enumerate((
        ("normed", n_buf, normed_out), ("wq", wq, wq_all), ("wo", wo, wo_all), ("kv", kv, kv_all), ("query", q, query_out),
        ("resid", x_buf, resid_out), ("gated", n_buf, gated_out)))}
    mixed_stores = [pltpu.make_async_copy(mix.at[:, pl.ds(k * head_dim, head_dim)],
                                          mixed_out.at[:, pl.ds(pl.multiple_of(dev * head_dim, 128), head_dim)], store.at[7 + k])
                    for k, dev in enumerate(mixed_at)]

    for cp in loads:
        cp.start()
    enter((core, side, back))
    loads[0].wait()
    to_side(0).start()
    to_back(0).start()
    to_core(0, 0).start()

    def norm_rows(src, gain_ref):
        x_f = src.astype(F32)
        inv_rms = lax.rsqrt(jnp.mean(x_f * x_f, axis=-1, keepdims=True) + NORM_EPS)
        return (x_f * inv_rms * (1.0 + gain_ref[...].astype(F32))).astype(BF16)

    def seq_rows(i):
        return pl.ds(pl.multiple_of(i * shard, 16), shard)

    def rotate(x_f):
        first, second = x_f[:, :half_dim], x_f[:, half_dim:]
        cos_t, sin_t = cos_ref[...], sin_ref[...]
        return first * cos_t - second * sin_t, second * cos_t + first * sin_t

    def norm1(i, carry):
        n_buf[seq_rows(i), :] = norm_rows(x_buf[seq_rows(i), :], gain1_ref)
        return carry

    loads[1].wait()
    lax.fori_loop(0, batch, norm1, 0)
    stores["normed"].start()
    loads[2].wait()
    loads[3].wait()

    def own_kv(i, carry):
        raw = dot_nn(n_buf[seq_rows(i), :], wkv[...])
        first, second = rotate(raw[:, :head_dim])
        kv[0, seq_rows(i), :half_dim] = first.astype(BF16)
        kv[0, seq_rows(i), half_dim:head_dim] = second.astype(BF16)
        kv[0, seq_rows(i), head_dim:] = raw[:, head_dim:].astype(BF16)
        return carry

    lax.fori_loop(0, batch, own_kv, 0)
    to_side(1).start()
    to_back(1).start()
    to_core(1, 0).start()

    def own_query(k):
        def step(i, carry):
            for h in (k, near + k):
                first, second = rotate(dot_nn(n_buf[seq_rows(i), :], wq[h]))
                q[h, seq_rows(i), :half_dim] = first.astype(BF16)
                q[h, seq_rows(i), half_dim:] = second.astype(BF16)
            return carry

        to_core(0, k).wait_recv()
        lax.fori_loop(0, batch, step, 0)

    def pass_on(a):
        to_side(a).wait_recv()
        onward(a, 0).start()
        to_core(a, 1).start()
        to_back(a).wait_recv()
        onward(a, 1).start()
        to_core(a, 2).start()

    def pass_last(a):
        onward(a, 0).wait_recv()
        onward(a, 1).wait_recv()
        to_core(a, 3).start()

    own_query(0)
    pass_on(0)
    own_query(1)
    own_query(2)
    pass_on(1)
    loads[4].wait()
    to_side(2).start()
    to_back(2).start()
    to_core(2, 0).start()
    pass_last(0)
    own_query(3)
    stores["query"].start()
    stores["wq"].start()
    pass_last(1)
    for k in range(near):
        to_core(1, k).wait_recv()
    stores["kv"].start()

    q_pos = me * shard + lax.broadcasted_iota(jnp.int32, (shard, 1), 0)

    def attend(step, carry):
        i, g = step // 2, step % 2
        keys = kv[:, seq_rows(i), :head_dim].reshape(total, head_dim)
        values = kv[:, seq_rows(i), head_dim:].reshape(total, head_dim)
        query = q[pl.ds(g * near, near), seq_rows(i), :].reshape(near * shard, head_dim) * BF16(head_dim ** -0.5)
        visible = kpos_ref[...] < jnp.minimum(lens_ref[1, i], jnp.maximum(lens_ref[0, i], q_pos + 1))
        scores = dot_nt(query, keys)
        for h in range(near):
            part = slice(h * shard, (h + 1) * shard)
            s = jnp.where(visible, scores[part], MASKED)
            e = jnp.exp(s - jnp.max(s, axis=-1, keepdims=True))
            probs[part, :] = (e * (1.0 / jnp.sum(e, axis=-1, keepdims=True))).astype(BF16)
        mixed = dot_nn(probs[...], values).astype(BF16)
        for h in range(near):
            cols = pl.ds(pl.multiple_of((g * near + h) * head_dim, 128), head_dim)
            mix[seq_rows(i), cols] = mixed[h * shard:(h + 1) * shard]
        return carry

    lax.fori_loop(0, 2 * batch, attend, 0)
    for cp in mixed_stores:
        cp.start()
    pass_on(2)

    def project(k, first):
        def step(n, carry):
            cols = pl.ds(pl.multiple_of(n * 512, 128), 512)
            part = (dot_nn(mix[:, k * head_dim:(k + 1) * head_dim], wo[k, :, cols])
                    + dot_nn(mix[:, (near + k) * head_dim:(near + k + 1) * head_dim], wo[near + k, :, cols]))
            acc[:, cols] = part if first else acc[:, cols] + part
            return carry

        to_core(2, k).wait_recv()
        lax.fori_loop(0, dim // 512, step, 0)

    project(0, True)
    project(1, False)
    project(2, False)
    pass_last(2)
    project(3, False)
    stores["wo"].start()
    stores["normed"].wait()

    def norm2(i, carry):
        resid = (x_buf[seq_rows(i), :].astype(F32) + acc[seq_rows(i), :]).astype(BF16)
        x_buf[seq_rows(i), :] = resid
        n_buf[seq_rows(i), :] = norm_rows(resid, gain2_ref)
        return carry

    lax.fori_loop(0, batch, norm2, 0)
    stores["resid"].start()
    stores["gated"].start()
    for cp in mixed_stores:
        cp.wait()
    for name in ("wq", "wo", "kv", "query", "resid", "gated"):
        stores[name].wait()
    for a in range(3):
        to_side(a).wait_send()
        to_back(a).wait_send()
        for k in range(2):
            onward(a, k).wait_send()
        for k in range(near):
            to_core(a, k).wait_send()


def front_layer(lens, k_pos, cos_t, sin_t, attn_norm, mlp_norm, hidden, w_query, w_key, w_value, w_out, batch, tp):
    rows, dim = hidden.shape
    head_dim = w_key.shape[1]
    shard = rows // batch
    total = tp * shard
    anyspace = pl.BlockSpec(memory_space=pl.ANY)
    vmem = pl.BlockSpec(memory_space=pltpu.VMEM)
    dma = pltpu.SemaphoreType.DMA

    def shape(*dims):
        return jax.ShapeDtypeStruct(dims, BF16)

    return pl.pallas_call(
        functools.partial(front_kernel, batch=batch),
        out_shape=(shape(rows, dim), shape(tp, dim, head_dim), shape(tp, head_dim, dim), shape(tp, rows, 2 * head_dim),
                   shape(tp, rows, head_dim), shape(rows, tp * head_dim), shape(rows, dim), shape(rows, dim)),
        in_specs=[pl.BlockSpec(memory_space=pltpu.SMEM)] + [vmem] * 5 + [anyspace] * 5,
        out_specs=(anyspace,) * 8,
        scratch_shapes=[pltpu.VMEM((rows, dim), BF16), pltpu.VMEM((rows, dim), BF16), pltpu.VMEM((dim, 2 * head_dim), BF16),
                        pltpu.VMEM((tp, dim, head_dim), BF16), pltpu.VMEM((tp, head_dim, dim), BF16),
                        pltpu.VMEM((tp, rows, 2 * head_dim), BF16), pltpu.VMEM((tp, rows, head_dim), BF16),
                        pltpu.VMEM((tp // 2 * shard, total), BF16), pltpu.VMEM((rows, tp * head_dim), BF16), pltpu.VMEM((rows, dim), F32),
                        dma((5,)), dma((15,)), dma((3, 8)), dma((3, 8))],
        compiler_params=pltpu.CompilerParams(vmem_limit_bytes=62 << 20, collective_id=2, has_side_effects=True),
        cost_estimate=pl.CostEstimate(flops=8 * rows * dim * tp * head_dim, bytes_accessed=60 << 20, transcendentals=tp * rows * total),
        name="front",
    )(lens, k_pos, cos_t, sin_t, attn_norm.reshape(1, dim), mlp_norm.reshape(1, dim), hidden, w_query, w_key, w_value, w_out)


def attention_backward(lens, cos_t, sin_t, query, kv_all, d_mixed, batch, group=4):
    heads, rows, head_dim = query.shape
    near = kv_all.shape[0] // 2
    shard = rows // batch
    total = 2 * near * shard
    q_spec = pl.BlockSpec((group, shard, head_dim), lambda s, g, *_: (g, s, 0))
    kv_spec = pl.BlockSpec((near, shard, 2 * head_dim), lambda s, g, *_: (0, s, 0))
    table = pl.BlockSpec((shard, head_dim // 2), lambda s, g, *_: (0, 0))
    kv_shape = jax.ShapeDtypeStruct((near, rows, 2 * head_dim), BF16)
    return pl.pallas_call(
        attn_bwd_kernel,
        out_shape=(jax.ShapeDtypeStruct((heads, rows, head_dim), BF16), kv_shape, kv_shape),
        grid_spec=pltpu.PrefetchScalarGridSpec(
            num_scalar_prefetch=1, grid=(batch, heads // group),
            in_specs=[table, table, q_spec, pl.BlockSpec((2 * near, shard, 2 * head_dim), lambda s, g, *_: (0, s, 0)), pl.BlockSpec((shard, group * head_dim), lambda s, g, *_: (s, g))],
            out_specs=(q_spec, kv_spec, kv_spec),
            scratch_shapes=[pltpu.VMEM((total, 2 * head_dim), F32)]),
        compiler_params=pltpu.CompilerParams(dimension_semantics=("arbitrary", "arbitrary"), vmem_limit_bytes=56 << 20),
        cost_estimate=pl.CostEstimate(flops=10 * heads * rows * total * head_dim, bytes_accessed=20 << 20, transcendentals=heads * rows * total),
        name="attn_bwd",
    )(lens, cos_t, sin_t, query, kv_all, d_mixed)


def gated_tile(z, g, w_g, w_u, w_d):
    gate = dot_nn(z, w_g)
    upper = dot_nn(z, w_u)
    d_act = dot_nt(g, w_d).astype(BF16).astype(F32)
    sq = gate * gate
    th = jnp.tanh(gate * (GELU_C + (GELU_C * GELU_K) * sq))
    half = 0.5 + 0.5 * th
    gelu = gate * half
    slope = half + gate * (0.5 - 0.5 * (th * th)) * (GELU_C + (3.0 * GELU_C * GELU_K) * sq)
    return (gelu * upper).astype(BF16), (d_act * upper * slope).astype(BF16), (d_act * gelu).astype(BF16)


def gated_kernel(z_own, g_own, wg_hbm, wu_hbm, wd_hbm, z_all, g_all, act, d_gate, d_up,
                 wg, wu, wd, z_buf, g_buf, outs, w_sem, in_sem, own_sem, out_sem, send, recv, send0, recv0, *, bn):
    rows, _ = z_own.shape
    width = wg_hbm.shape[1]
    steps = width // bn
    piece = rows // 4
    me, core, side, back = neighbours()
    corner = flip(side, 4)
    own = (z_own, g_own)
    full = (z_all, g_all)

    def part(slot, q):
        return pl.ds(pl.multiple_of(slot * rows + q * piece, 16), piece)

    def link_rows(u, path):
        turn = u // 2
        diag = turn % 2
        if path == 0:
            return side + (corner - side) * diag, (u % 2) + 2 * (turn // 2) + diag * 2
        return back + (corner - back) * diag, (u % 2) + 2 - 2 * (turn // 2) - diag * 2

    def link_copy(u, path, a):
        turn = u // 2
        peer = side if path == 0 else back
        sems = (send.at[path, u, a], recv.at[path, u, a])
        if turn == 1:
            slot = back if path == 0 else side
            q = (2 if path == 0 else 0) + u % 2
            return remote(full[a].at[part(slot, q)], full[a].at[part(slot, q)], *sems, peer)
        q = u % 2 + (2 * (turn // 2) if path == 0 else 2 - 2 * (turn // 2))
        return remote(own[a].at[pl.ds(q * piece, piece)], full[a].at[part(me, q)], *sems, peer)

    def core_copy(u, path, a):
        slot, q = link_rows(u, path)
        return remote(full[a].at[part(slot, q)], full[a].at[part(slot, q)], send.at[2 + path, u, a], recv.at[2 + path, u, a], core)

    def own_copy(a):
        return remote(own[a], full[a].at[pl.ds(pl.multiple_of(me * rows, 16), rows)], send0.at[a], recv0.at[a], core)

    def weight_copies(n):
        cols = pl.ds(pl.multiple_of(n * bn, 128), bn)
        return [pltpu.make_async_copy(wg_hbm.at[:, cols], wg.at[:, cols], w_sem.at[0, n]),
                pltpu.make_async_copy(wu_hbm.at[:, cols], wu.at[:, cols], w_sem.at[1, n]),
                pltpu.make_async_copy(wd_hbm.at[cols], wd.at[cols], w_sem.at[2, n])]

    bufs = (z_buf, g_buf)
    own_in = [pltpu.make_async_copy(own[a], bufs[a], own_sem.at[a]) for a in range(2)]
    own_out = [pltpu.make_async_copy(bufs[a], full[a].at[pl.ds(pl.multiple_of(me * rows, 16), rows)], own_sem.at[2 + a]) for a in range(2)]
    for cp in own_in:
        cp.start()
    for n in range(steps):
        for cp in weight_copies(n):
            cp.start()
    enter((core, side, back))
    for u in range(2):
        for path in range(2):
            for a in range(2):
                link_copy(u, path, a).start()
        if u == 0:
            for a in range(2):
                own_copy(a).start()

    def out_copies(slot, s_rows, n):
        cols = pl.ds(pl.multiple_of(n * bn, 128), bn)
        return [pltpu.make_async_copy(outs.at[slot, k, pl.ds(i * piece, piece)], ref.at[s_rows[i], cols], out_sem.at[slot, k, i])
                for k, ref in enumerate((act, d_gate, d_up)) for i in range(4)]

    def stage_rows(s):
        late = (s + 6) // 8
        u = (s - 2) * late
        first = me + (core - me) * s * (1 - late)
        (slot_x, q_x), (slot_y, q_y) = link_rows(u, 0), link_rows(u, 1)
        base_x, base_y = slot_x * rows + q_x * piece, slot_y * rows + q_y * piece
        pair_x, pair_y = flip(slot_x, 1) * rows + q_x * piece, flip(slot_y, 1) * rows + q_y * piece
        starts = [(1 - late) * (first * rows + i * piece) + late * base for i, base in enumerate((base_x, base_y, pair_x, pair_y))]
        return [pl.ds(pl.multiple_of(st, 16), piece) for st in starts]

    def compute(s):
        s_rows = stage_rows(s)

        def block(n, carry):
            step = s * steps + n
            slot = step % 2

            @pl.when(step >= 2)
            def _():
                for cp in out_copies(slot, s_rows, n):
                    cp.wait()

            @pl.when(s == 0)
            def _():
                for cp in weight_copies(n):
                    cp.wait()

            cols = pl.ds(pl.multiple_of(n * bn, 128), bn)
            res = gated_tile(z_buf[...], g_buf[...], wg[:, cols], wu[:, cols], wd[cols, :])
            for k in range(3):
                outs[slot, k] = res[k]
            for cp in out_copies(slot, s_rows, n):
                cp.start()
            return carry

        lax.fori_loop(0, steps, block, 0)

    def stage(s, carry):
        @pl.when(s == 0)
        def _():
            for cp in own_in:
                cp.wait()
            for cp in own_out:
                cp.start()

        @pl.when(s == 1)
        def _():
            for cp in own_out:
                cp.wait()
            for a in range(2):
                own_copy(a).wait_recv()

        for u in range(6):
            @pl.when(s == u + 2)
            def _(u=u):
                for path in range(2):
                    for a in range(2):
                        link_copy(u, path, a).wait_recv()
                        core_copy(u, path, a).start()
                if u < 2:
                    for path in range(2):
                        for a in range(2):
                            link_copy(u + 2, path, a).start()
                if u == 1:
                    for later in (4, 5):
                        for path in range(2):
                            for a in range(2):
                                link_copy(later, path, a).start()
                for path in range(2):
                    for a in range(2):
                        core_copy(u, path, a).wait_recv()

        @pl.when(s >= 1)
        def _():
            s_rows = stage_rows(s)
            copies = [pltpu.make_async_copy(full[a].at[s_rows[i]], bufs[a].at[pl.ds(i * piece, piece)], in_sem.at[a, i])
                      for a in range(2) for i in range(4)]
            for cp in copies:
                cp.start()
            for cp in copies:
                cp.wait()

        compute(s)
        return carry

    lax.fori_loop(0, 8, stage, 0)
    last = stage_rows(7)
    for slot in range(2):
        for cp in out_copies(slot, last, 0):
            cp.wait()
    for a in range(2):
        own_copy(a).wait_send()
        for path in range(2):
            for u in range(6):
                link_copy(u, path, a).wait_send()
                core_copy(u, path, a).wait_send()


def gated_layer(z_own, g_own, w_gate, w_up, w_down, tp, bn=512):
    rows, dim = z_own.shape
    width = w_gate.shape[1]
    total = rows * tp
    anyspace = pl.BlockSpec(memory_space=pl.ANY)
    gathered = jax.ShapeDtypeStruct((total, dim), BF16)
    made = jax.ShapeDtypeStruct((total, width), BF16)
    dma = pltpu.SemaphoreType.DMA
    return pl.pallas_call(
        functools.partial(gated_kernel, bn=bn),
        out_shape=(gathered, gathered, made, made, made),
        in_specs=[anyspace] * 5,
        out_specs=(anyspace,) * 5,
        scratch_shapes=[pltpu.VMEM((dim, width), BF16), pltpu.VMEM((dim, width), BF16), pltpu.VMEM((width, dim), BF16),
                        pltpu.VMEM((rows, dim), BF16), pltpu.VMEM((rows, dim), BF16), pltpu.VMEM((2, 3, rows, bn), BF16),
                        dma((3, width // bn)), dma((2, 4)), dma((4,)), dma((2, 3, 4)), dma((4, 6, 2)), dma((4, 6, 2)), dma((2,)), dma((2,))],
        compiler_params=pltpu.CompilerParams(vmem_limit_bytes=60 << 20, collective_id=0, has_side_effects=True),
        cost_estimate=pl.CostEstimate(flops=6 * total * dim * width, bytes_accessed=200 << 20, transcendentals=total * width),
        name="gated",
    )(z_own, g_own, w_gate, w_up, w_down)


def back_kernel(act, d_gate, d_up, wg_hbm, wu_hbm, wd_hbm, own_out, x_in, y_in,
                wa, wb, lhs, st, from_core, from_diag, own_st, w_sem, l_sem, o_sem, c_send, c_recv, d_send, d_recv, f_send, f_recv, *, rows, bn):
    dim = wg_hbm.shape[0]
    steps = dim // bn
    half = rows // 2
    me, core, side, back = neighbours()

    def cols(j):
        return pl.ds(pl.multiple_of(j * bn, 128), bn)

    def pair_of(t):
        return ((t + 5) // 7) * ((t + 1) % 3 + 1)

    def lhs_copies(phase, t):
        pair = pair_of(t)
        theirs = 1 - t // 5 - ((t + 6) // 7 - (t + 5) // 7)
        dev = me + (1 - pair // 2) * (side - me) + (1 - pair % 2) * (back - me)
        dev = dev + theirs * (flip(dev, 1) - dev)
        src = pl.ds(pl.multiple_of(dev * rows, 16), rows)
        refs = (act,) if phase == 0 else (d_gate, d_up)
        return [pltpu.make_async_copy(ref.at[src], lhs.at[t % 2, k], l_sem.at[t % 2, k]) for k, ref in enumerate(refs)]

    def weight_copy(k, j):
        if k == 0:
            return pltpu.make_async_copy(wd_hbm.at[:, cols(j)], wa.at[:, cols(j)], w_sem.at[0, j])
        src, dst = (wg_hbm, wb) if k == 1 else (wu_hbm, wa)
        return pltpu.make_async_copy(src.at[cols(j)], dst.at[cols(j)], w_sem.at[k, j])

    def core_copy(pair, j):
        return remote(st.at[0, j], from_core.at[pair, j], c_send.at[j], c_recv.at[pair, j], core)

    def diag_copy(phase, k, j):
        return remote(st.at[1, j, pl.ds(k * half, half)], from_diag.at[phase, k, j], d_send.at[k, j], d_recv.at[phase, k, j], (side, back)[k])

    def final_copy(phase, k, j):
        return remote(st.at[2 + k, j], (x_in, y_in)[k].at[phase, :, cols(j)], f_send.at[k, j], f_recv.at[phase, k, j], (side, back)[k])

    def own_copy(phase, j):
        return pltpu.make_async_copy(own_st.at[j % 2], own_out.at[phase, :, cols(j)], o_sem.at[j % 2])

    def product(phase, slot, j):
        if phase == 0:
            return dot_nn(lhs[slot, 0], wa[:, cols(j)])
        return dot_nt(lhs[slot, 0], wb[cols(j), :]) + dot_nt(lhs[slot, 1], wa[cols(j), :])

    for cp in lhs_copies(0, 0):
        cp.start()
    for j in range(steps):
        weight_copy(0, j).start()
    enter((core, side, back))

    def tiles(body):
        def step(j, carry):
            body(j)
            return carry

        lax.fori_loop(0, steps, step, 0)

    for phase in (0, 1):
        def step(t, carry, phase=phase):
            for cp in lhs_copies(phase, t):
                cp.wait()

            @pl.when(t < 7)
            def _():
                for cp in lhs_copies(phase, t + 1):
                    cp.start()

            if phase == 0:
                @pl.when(t == 1)
                def _():
                    for j in range(steps):
                        weight_copy(1, j).start()

                @pl.when(t == 7)
                def _():
                    for cp in lhs_copies(1, 0):
                        cp.start()

            @pl.when((t == 0) | ((t >= 2) & (t <= 4)))
            def _():
                pair = pair_of(t)

                def body(j):
                    @pl.when(t == 0)
                    def _():
                        for k in ((0,) if phase == 0 else (1, 2)):
                            weight_copy(k, j).wait()

                    if phase == 0:
                        @pl.when(t > 0)
                        def _():
                            core_copy(0, j).wait_send()
                    else:
                        core_copy(0, j).wait_send()
                    st[0, j] = product(phase, t % 2, j).astype(BF16)
                    core_copy(pair, j).start()

                tiles(body)

            @pl.when(t == 1)
            def _():
                def body(j):
                    core_copy(0, j).wait_recv()
                    if phase == 1:
                        for k in range(2):
                            diag_copy(0, k, j).wait_send()
                    st[1, j] = (product(phase, 1, j) + from_core[0, j].astype(F32)).astype(BF16)
                    for k in range(2):
                        diag_copy(phase, k, j).start()

                tiles(body)

            for k in range(2):
                @pl.when(t == 5 + k)
                def _(k=k):
                    def body(j):
                        core_copy(1 + k, j).wait_recv()
                        diag_copy(phase, 1 - k, j).wait_recv()
                        if phase == 1:
                            final_copy(0, k, j).wait_send()
                        total = product(phase, (5 + k) % 2, j) + from_core[1 + k, j].astype(F32)
                        came = from_diag[phase, 1 - k, j].astype(F32)
                        split = slice(half, rows) if k == 0 else slice(0, half)
                        rest = slice(0, half) if k == 0 else slice(half, rows)
                        st[2 + k, j, split, :] = (total[split] + came).astype(BF16)
                        st[2 + k, j, rest, :] = total[rest].astype(BF16)
                        final_copy(phase, k, j).start()

                    tiles(body)

            @pl.when(t == 7)
            def _():
                def body(j):
                    core_copy(3, j).wait_recv()

                    @pl.when(j >= 2)
                    def _():
                        own_copy(phase, j).wait()

                    own_st[j % 2] = product(phase, 1, j) + from_core[3, j].astype(F32)
                    own_copy(phase, j).start()

                tiles(body)
                for j in (0, 1):
                    own_copy(phase, j).wait()
                if phase == 0:
                    for j in range(steps):
                        weight_copy(2, j).start()

            return carry

        lax.fori_loop(0, 8, step, 0)

    for j in range(steps):
        core_copy(0, j).wait_send()
        for k in range(2):
            diag_copy(1, k, j).wait_send()
            final_copy(1, k, j).wait_send()
            for phase in (0, 1):
                final_copy(phase, k, j).wait_recv()


def back_layer(act, d_gate, d_up, w_gate, w_up, w_down, tp, bn=512):
    total, width = act.shape
    dim = w_gate.shape[0]
    rows = total // tp
    steps = dim // bn
    anyspace = pl.BlockSpec(memory_space=pl.ANY)
    dma = pltpu.SemaphoreType.DMA
    came = jax.ShapeDtypeStruct((2, rows, dim), BF16)
    return pl.pallas_call(
        functools.partial(back_kernel, rows=rows, bn=bn),
        out_shape=(jax.ShapeDtypeStruct((2, rows, dim), F32), came, came),
        in_specs=[anyspace] * 6,
        out_specs=(anyspace,) * 3,
        scratch_shapes=[pltpu.VMEM((width, dim), BF16), pltpu.VMEM((dim, width), BF16), pltpu.VMEM((2, 2, rows, width), BF16),
                        pltpu.VMEM((4, steps, rows, bn), BF16), pltpu.VMEM((4, steps, rows, bn), BF16),
                        pltpu.VMEM((2, 2, steps, rows // 2, bn), BF16), pltpu.VMEM((2, rows, bn), F32),
                        dma((3, steps)), dma((2, 2)), dma((2,)), dma((steps,)), dma((4, steps)),
                        dma((2, steps)), dma((2, 2, steps)), dma((2, steps)), dma((2, 2, steps))],
        compiler_params=pltpu.CompilerParams(vmem_limit_bytes=67043328, collective_id=1, has_side_effects=True),
        cost_estimate=pl.CostEstimate(flops=6 * total * dim * width, bytes_accessed=200 << 20, transcendentals=0),
        name="back",
    )(act, d_gate, d_up, w_gate, w_up, w_down)


def product_kernel(a_ref, b_ref, o_ref):
    o_ref[...] = dot_tn(a_ref[...], b_ref[...])


def weight_grad(a, b, bm=512, bn=1024):
    rows, m = a.shape
    n = b.shape[1]
    return pl.pallas_call(
        product_kernel,
        out_shape=jax.ShapeDtypeStruct((m, n), F32),
        grid=(m // bm, n // bn),
        in_specs=[pl.BlockSpec((rows, bm), lambda i, j: (0, i)), pl.BlockSpec((rows, bn), lambda i, j: (0, j))],
        out_specs=pl.BlockSpec((bm, bn), lambda i, j: (i, j)),
        compiler_params=pltpu.CompilerParams(dimension_semantics=("arbitrary", "arbitrary"), vmem_limit_bytes=56 << 20),
        cost_estimate=pl.CostEstimate(flops=2 * rows * m * n, bytes_accessed=110 << 20, transcendentals=0),
        name="weight_grad",
    )(a, b)


def hop_diagonal(diag):
    half = diag.shape[0] // 2
    return swap(diag[:half], 2), swap(diag[half:], 4)


def hop_near(side, back, came_side, came_back):
    half = side.shape[0] // 2
    kind = came_side.dtype
    side = jnp.concatenate([side[:half], side[half:] + came_back.astype(F32)], axis=0).astype(kind)
    back = jnp.concatenate([back[:half] + came_side.astype(F32), back[half:]], axis=0).astype(kind)
    return side, back


def solution(mesh):
    tp_size = mesh.shape["tp"]
    act_spec = P("dp", "tp", None)
    in_specs = (act_spec, act_spec, P("dp"), P("dp"), P(None), P(None, "tp"), P(None, None), P(None, None), P("tp", None), P(None), P(None, "tp"), P(None, "tp"), P("tp", None))
    out_specs = (act_spec, act_spec, P("dp"), P("dp", "tp"), P("dp", None), P("dp", None), P(("dp", "tp"), None), P("dp"), P("dp", "tp"), P("dp", "tp"), P(("dp", "tp"), None))

    def layer(hidden, grad_out, prefix_len, valid_len, attn_norm, w_query, w_key, w_value, w_out, mlp_norm, w_gate, w_up, w_down):
        batch, shard, dim = hidden.shape
        head_dim = w_key.shape[1]
        rows = batch * shard
        me = lax.axis_index("tp")
        starts = (me ^ jnp.array([0, 2, 4, 6, 1, 3, 5, 7], jnp.int32)) * shard
        k_pos = (starts[:, None] + jnp.arange(shard, dtype=jnp.int32)).reshape(1, tp_size * shard)
        lens = jnp.stack([prefix_len, valid_len])
        cos_own, sin_own = rope_tables(me * shard + jnp.arange(shard), head_dim)
        hidden = hidden.reshape(rows, dim)
        grad_out = grad_out.reshape(rows, dim)
        normed, wq_all, wo_all, kv_all, query, mixed, resid, gated_in = front_layer(
            lens, k_pos, cos_own, sin_own, attn_norm, mlp_norm, hidden, w_query, w_key, w_value, w_out, batch, tp_size)
        wo_all = wo_all.reshape(tp_size * head_dim, dim)

        def rope(raw_proj):
            return apply_rope(raw_proj, jnp.tile(cos_own, (batch, 1)), jnp.tile(sin_own, (batch, 1)))

        gated_all, grad_all, act, d_gate, d_upper = gated_layer(gated_in, grad_out, w_gate, w_up, w_down, tp_size)
        own_part, x_part, y_part = back_layer(act, d_gate, d_upper, w_gate, w_up, w_down, tp_size)
        hidden, resid, own_part = lax.optimization_barrier((hidden, resid, own_part))
        norm1_pull = jax.vjp(rms_norm, hidden, attn_norm.astype(F32))[1]
        norm2_pull = jax.vjp(rms_norm, resid, mlp_norm.astype(F32))[1]
        key_pull = jax.linear_transpose(rope, jax.ShapeDtypeStruct((rows, head_dim), F32))
        mlp_sum, d_gated = [own_part[k] + x_part[k].astype(F32) + y_part[k].astype(F32) for k in range(2)]
        d_gated = d_gated.astype(BF16)
        hidden_out = (resid.astype(F32) + mlp_sum).astype(BF16)
        d_resid_norm, g_mlp_norm_part = norm2_pull(d_gated)
        d_resid = (grad_out.astype(F32) + d_resid_norm.astype(F32)).astype(BF16)
        g_out_part = dot_tn(mixed, d_resid)
        d_mixed = dot_nt(d_resid, wo_all).astype(BF16)
        lens_back = jnp.concatenate([lens, jnp.full((1, batch), me, jnp.int32), jnp.broadcast_to(starts[:, None], (tp_size, batch))])
        d_mixed, g_out_part = lax.optimization_barrier((d_mixed, g_out_part))
        g_out = lax.psum_scatter(g_out_part, "tp", scatter_dimension=0, tiled=True)
        d_q_raw, dkv_near, dkv_far = attention_backward(lens_back, cos_own, sin_own, query, kv_all, d_mixed, batch)
        came_kv = swap(dkv_far, 1)
        near = tp_size // 2
        came_q = swap(jnp.einsum("td,kte->kde", normed, d_q_raw[near:], preferred_element_type=F32), 1)
        d_normed_q = jnp.einsum("hte,hde->td", d_q_raw, wq_all, preferred_element_type=F32)
        came_kv, d_normed_q = lax.optimization_barrier((came_kv, d_normed_q))
        kv_own, kv_side, kv_back, kv_diag = [dkv_near[k].astype(F32) + came_kv[k].astype(F32) for k in range(4)]
        kv_came = hop_diagonal(kv_diag.astype(BF16))
        g_query_sum = jnp.einsum("td,kte->kde", normed, d_q_raw[:near], preferred_element_type=F32) + came_q
        kv_came, g_query_sum, d_gate = lax.optimization_barrier((kv_came, g_query_sum, d_gate))
        kv_next = hop_near(kv_side, kv_back, *kv_came)
        kv_last = (swap(kv_next[0], 2), swap(kv_next[1], 4))
        q_came = hop_diagonal(g_query_sum[3])
        g_gate = weight_grad(gated_all, d_gate)
        kv_last, q_came, g_gate = lax.optimization_barrier((kv_last, q_came, g_gate))
        d_kv = (kv_own + kv_last[0].astype(F32) + kv_last[1].astype(F32)).astype(BF16)
        d_k_raw = key_pull(d_kv[:, :head_dim].astype(F32))[0].astype(BF16)
        d_values = d_kv[:, head_dim:]
        q_next = hop_near(g_query_sum[1], g_query_sum[2], *q_came)
        g_key_part, g_value_part = dot_tn(normed, d_k_raw), dot_tn(normed, d_values)
        q_next, g_key_part, g_value_part, d_upper = lax.optimization_barrier((q_next, g_key_part, g_value_part, d_upper))
        g_key, g_value = lax.psum((g_key_part, g_value_part), "tp")
        q_last = (swap(q_next[0], 2), swap(q_next[1], 4))
        g_up = weight_grad(gated_all, d_upper)
        d_normed = (d_normed_q + dot_nt(d_k_raw, w_key) + dot_nt(d_values, w_value)).astype(BF16)
        q_last, g_up, d_normed, act = lax.optimization_barrier((q_last, g_up, d_normed, act))
        g_query = g_query_sum[0] + q_last[0] + q_last[1]
        d_hidden_norm, g_attn_norm_part = norm1_pull(d_normed)
        norms = jnp.stack([g_attn_norm_part, g_mlp_norm_part])
        norms_near = [swap(norms, bit) for bit in (2, 4, 6)]
        g_down = weight_grad(act, grad_all)
        norms_near, g_down, d_hidden_norm = lax.optimization_barrier((norms_near, g_down, d_hidden_norm))
        norms = norms + norms_near[0] + norms_near[1] + norms_near[2]
        g_norms = norms + swap(norms, 1)
        grad_hidden = (d_resid.astype(F32) + d_hidden_norm.astype(F32)).astype(BF16)
        full = (batch, shard, dim)
        return (hidden_out.reshape(full), grad_hidden.reshape(full), g_norms[0], g_query, g_key, g_value, g_out, g_norms[1], g_gate, g_up, g_down)

    return jax.shard_map(layer, mesh=mesh, in_specs=in_specs, out_specs=out_specs, check_vma=False)
```

```python
import functools
import math
import jax
import jax.numpy as jnp
from jax import lax
from jax.experimental import pallas as pl
from jax.experimental.pallas import tpu as pltpu
from jax.sharding import PartitionSpec as P

NORM_EPS = 1e-6
BF16 = jnp.bfloat16
F32 = jnp.float32
GELU_C = math.sqrt(2.0 / math.pi)
GELU_K = 0.044715
MASKED = -1e30
NT = (((1,), (1,)), ((), ()))
TN = (((0,), (0,)), ((), ()))


def rms_norm(x_in, gain):
    x_f = x_in.astype(F32)
    inv_rms = lax.rsqrt(jnp.mean(x_f * x_f, axis=-1, keepdims=True) + NORM_EPS)
    return (x_f * inv_rms * (1.0 + gain)).astype(BF16)


def rope_tables(positions, head_dim):
    half_dim = head_dim // 2
    exponent = jnp.arange(half_dim, dtype=F32) * (2.0 / head_dim)
    inv_freq = jnp.exp(exponent * (-math.log(10000.0)))
    angles = positions.astype(F32)[:, None] * inv_freq[None, :]
    return jnp.cos(angles), jnp.sin(angles)


def apply_rope(x_f, cos_t, sin_t):
    half_dim = x_f.shape[-1] // 2
    first = x_f[..., :half_dim]
    second = x_f[..., half_dim:]
    return jnp.concatenate([first * cos_t - second * sin_t, second * cos_t + first * sin_t], axis=-1)


def dot_nn(a, b):
    return jnp.dot(a, b, preferred_element_type=F32)


def dot_nt(a, b):
    return lax.dot_general(a, b, NT, preferred_element_type=F32)


def dot_tn(a, b):
    return lax.dot_general(a, b, TN, preferred_element_type=F32)


def swap(x, bit):
    return lax.ppermute(x, "tp", [(t, t ^ bit) for t in range(8)])


def flip(index, bit):
    return index + bit - 2 * bit * ((index // bit) % 2)


def neighbours():
    me = lax.axis_index("tp")
    return me, flip(me, 1), flip(me, 2), flip(me, 4)


def enter(peers):
    barrier = pltpu.get_barrier_semaphore()
    for peer in peers:
        pl.semaphore_signal(barrier, inc=1, device_id={"tp": peer}, device_id_type=pl.DeviceIdType.MESH)
    pl.semaphore_wait(barrier, len(peers))


def attn_bwd_kernel(lens_ref, cos_ref, sin_ref, q_ref, kv_ref, do_ref, dq_ref, dkv0_ref, dkv1_ref, dkv_acc):
    heads, shard, head_dim = q_ref.shape
    tp = kv_ref.shape[0]
    total = tp * shard
    rows = heads * shard
    s_id = pl.program_id(0)
    g_id = pl.program_id(1)
    prefix = lens_ref[0, s_id]
    valid = lens_ref[1, s_id]
    first = lens_ref[2, 0] * shard
    keys = kv_ref[:, :, :head_dim].reshape(total, head_dim)
    values = kv_ref[:, :, head_dim:].reshape(total, head_dim)
    query = q_ref[...].reshape(rows, head_dim) * BF16(head_dim ** -0.5)
    d_out = jnp.concatenate([do_ref[:, h * head_dim:(h + 1) * head_dim] for h in range(heads)], axis=0)
    step = lax.broadcasted_iota(jnp.int32, (shard, 1), 0)
    k_pos = jnp.concatenate([step + lens_ref[3 + r, 0] for r in range(tp)], axis=0)
    q_pos = first + lax.rem(lax.broadcasted_iota(jnp.int32, (1, rows), 1), shard)
    limit = jnp.minimum(valid, jnp.maximum(prefix, q_pos + 1))
    cos_t, sin_t = cos_ref[...][None], sin_ref[...][None]
    d_k = d_v = None
    count = heads // 2
    width = count * shard
    for c in range(2):
        cols = slice(c * width, (c + 1) * width)
        q_c, do_c = query[cols], d_out[cols]
        s = jnp.where(k_pos < limit[:, cols], dot_nt(keys, q_c), MASKED)
        e = jnp.exp(s - jnp.max(s, axis=0, keepdims=True))
        p = e * (1.0 / jnp.sum(e, axis=0, keepdims=True))
        d_p = dot_nt(values, do_c)
        delta = jnp.sum(p * d_p, axis=0, keepdims=True)
        d_s = (p * (d_p - delta)).astype(BF16)
        d_v_c = dot_nn(p.astype(BF16), do_c)
        d_k_c = dot_nn(d_s, q_c)
        d_k, d_v = (d_k_c, d_v_c) if d_k is None else (d_k + d_k_c, d_v + d_v_c)
        d_q = (dot_tn(d_s, keys) * (head_dim ** -0.5)).reshape(count, shard, head_dim)
        first, second = d_q[:, :, :head_dim // 2], d_q[:, :, head_dim // 2:]
        some = slice(c * count, (c + 1) * count)
        dq_ref[some, :, :head_dim // 2] = (first * cos_t + second * sin_t).astype(BF16)
        dq_ref[some, :, head_dim // 2:] = (second * cos_t - first * sin_t).astype(BF16)
    d_kv = jnp.concatenate([d_k, d_v], axis=1)

    @pl.when(g_id == 0)
    def _():
        dkv_acc[...] = d_kv

    @pl.when(g_id > 0)
    def _():
        dkv_acc[...] += d_kv

    @pl.when(g_id == pl.num_programs(1) - 1)
    def _():
        near = (tp // 2, shard, 2 * head_dim)
        dkv0_ref[...] = dkv_acc[:total // 2].astype(BF16).reshape(near)
        dkv1_ref[...] = dkv_acc[total // 2:].astype(BF16).reshape(near)


def remote(src, dst, send, recv, peer):
    return pltpu.make_async_remote_copy(src_ref=src, dst_ref=dst, send_sem=send, recv_sem=recv,
                                        device_id={"tp": peer}, device_id_type=pl.DeviceIdType.MESH)


def front_kernel(lens_ref, kpos_ref, cos_ref, sin_ref, gain1_ref, gain2_ref, hidden, w_query, w_key, w_value, w_out,
                 normed_out, wq_all, wo_all, kv_all, query_out, mixed_out, resid_out, gated_out,
                 x_buf, n_buf, wkv, wq, wo, kv, q, probs, mix, acc, load, store, send, recv, *, batch):
    rows, dim = x_buf.shape
    shard = rows // batch
    head_dim = w_key.shape[1]
    tp = wq.shape[0]
    near = tp // 2
    total = tp * shard
    half_dim = head_dim // 2
    me, core, side, back = neighbours()
    bufs = (wq, kv, wo)

    def to_side(a):
        return remote(bufs[a].at[0], bufs[a].at[1], send.at[a, 0], recv.at[a, 0], side)

    def to_back(a):
        return remote(bufs[a].at[0], bufs[a].at[2], send.at[a, 1], recv.at[a, 1], back)

    def onward(a, k):
        half = bufs[a].shape[1] // 2
        part = pl.ds(k * half, half)
        return remote(bufs[a].at[1 + k, part], bufs[a].at[3, part], send.at[a, 2 + k], recv.at[a, 2 + k], (back, side)[k])

    def to_core(a, k):
        return remote(bufs[a].at[k], bufs[a].at[near + k], send.at[a, 4 + k], recv.at[a, 4 + k], core)

    loads = [pltpu.make_async_copy(src, dst, load.at[i]) for i, (src, dst) in enumerate((
        (w_query, wq.at[0]), (hidden, x_buf), (w_key, wkv.at[:, :head_dim]), (w_value, wkv.at[:, head_dim:]), (w_out, wo.at[0])))]
    mixed_at = [me, side, back, flip(side, 4)]
    mixed_at = mixed_at + [flip(dev, 1) for dev in mixed_at]
    stores = {name: pltpu.make_async_copy(src, dst, store.at[i]) for i, (name, src, dst) in enumerate((
        ("normed", n_buf, normed_out), ("wq", wq, wq_all), ("wo", wo, wo_all), ("kv", kv, kv_all), ("query", q, query_out),
        ("resid", x_buf, resid_out), ("gated", n_buf, gated_out)))}
    mixed_stores = [pltpu.make_async_copy(mix.at[:, pl.ds(k * head_dim, head_dim)],
                                          mixed_out.at[:, pl.ds(pl.multiple_of(dev * head_dim, 128), head_dim)], store.at[7 + k])
                    for k, dev in enumerate(mixed_at)]

    for cp in loads:
        cp.start()
    enter((core, side, back))
    loads[0].wait()
    to_side(0).start()
    to_back(0).start()
    to_core(0, 0).start()

    def norm_rows(src, gain_ref):
        x_f = src.astype(F32)
        inv_rms = lax.rsqrt(jnp.mean(x_f * x_f, axis=-1, keepdims=True) + NORM_EPS)
        return (x_f * inv_rms * (1.0 + gain_ref[...].astype(F32))).astype(BF16)

    def seq_rows(i):
        return pl.ds(pl.multiple_of(i * shard, 16), shard)

    def rotate(x_f):
        first, second = x_f[:, :half_dim], x_f[:, half_dim:]
        cos_t, sin_t = cos_ref[...], sin_ref[...]
        return first * cos_t - second * sin_t, second * cos_t + first * sin_t

    def norm1(i, carry):
        n_buf[seq_rows(i), :] = norm_rows(x_buf[seq_rows(i), :], gain1_ref)
        return carry

    loads[1].wait()
    lax.fori_loop(0, batch, norm1, 0)
    stores["normed"].start()
    loads[2].wait()
    loads[3].wait()

    def own_kv(i, carry):
        raw = dot_nn(n_buf[seq_rows(i), :], wkv[...])
        first, second = rotate(raw[:, :head_dim])
        kv[0, seq_rows(i), :half_dim] = first.astype(BF16)
        kv[0, seq_rows(i), half_dim:head_dim] = second.astype(BF16)
        kv[0, seq_rows(i), head_dim:] = raw[:, head_dim:].astype(BF16)
        return carry

    lax.fori_loop(0, batch, own_kv, 0)
    to_side(1).start()
    to_back(1).start()
    to_core(1, 0).start()

    def own_query(k):
        def step(i, carry):
            for h in (k, near + k):
                first, second = rotate(dot_nn(n_buf[seq_rows(i), :], wq[h]))
                q[h, seq_rows(i), :half_dim] = first.astype(BF16)
                q[h, seq_rows(i), half_dim:] = second.astype(BF16)
            return carry

        to_core(0, k).wait_recv()
        lax.fori_loop(0, batch, step, 0)

    def pass_on(a):
        to_side(a).wait_recv()
        onward(a, 0).start()
        to_core(a, 1).start()
        to_back(a).wait_recv()
        onward(a, 1).start()
        to_core(a, 2).start()

    def pass_last(a):
        onward(a, 0).wait_recv()
        onward(a, 1).wait_recv()
        to_core(a, 3).start()

    own_query(0)
    pass_on(0)
    own_query(1)
    own_query(2)
    pass_on(1)
    loads[4].wait()
    to_side(2).start()
    to_back(2).start()
    to_core(2, 0).start()
    pass_last(0)
    own_query(3)
    stores["query"].start()
    stores["wq"].start()
    pass_last(1)
    for k in range(near):
        to_core(1, k).wait_recv()
    stores["kv"].start()

    q_pos = me * shard + lax.broadcasted_iota(jnp.int32, (shard, 1), 0)

    def attend(i, carry):
        keys = kv[:, seq_rows(i), :head_dim].reshape(total, head_dim)
        values = kv[:, seq_rows(i), head_dim:].reshape(total, head_dim)
        visible = kpos_ref[...] < jnp.minimum(lens_ref[1, i], jnp.maximum(lens_ref[0, i], q_pos + 1))
        for g in range(2):
            query = q[g * near:(g + 1) * near, seq_rows(i), :].reshape(near * shard, head_dim) * BF16(head_dim ** -0.5)
            scores = dot_nt(query, keys)
            for h in range(near):
                part = slice(h * shard, (h + 1) * shard)
                s = jnp.where(visible, scores[part], MASKED)
                e = jnp.exp(s - jnp.max(s, axis=-1, keepdims=True))
                probs[g, part, :] = (e * (1.0 / jnp.sum(e, axis=-1, keepdims=True))).astype(BF16)
            mixed = dot_nn(probs[g], values).astype(BF16)
            for h in range(near):
                head = g * near + h
                mix[seq_rows(i), head * head_dim:(head + 1) * head_dim] = mixed[h * shard:(h + 1) * shard]
        return carry

    lax.fori_loop(0, batch, attend, 0)
    for cp in mixed_stores:
        cp.start()
    pass_on(2)

    def project(k, first):
        def step(n, carry):
            cols = pl.ds(pl.multiple_of(n * 512, 128), 512)
            part = (dot_nn(mix[:, k * head_dim:(k + 1) * head_dim], wo[k, :, cols])
                    + dot_nn(mix[:, (near + k) * head_dim:(near + k + 1) * head_dim], wo[near + k, :, cols]))
            acc[:, cols] = part if first else acc[:, cols] + part
            return carry

        to_core(2, k).wait_recv()
        lax.fori_loop(0, dim // 512, step, 0)

    project(0, True)
    project(1, False)
    project(2, False)
    pass_last(2)
    project(3, False)
    stores["wo"].start()
    stores["normed"].wait()

    def norm2(i, carry):
        resid = (x_buf[seq_rows(i), :].astype(F32) + acc[seq_rows(i), :]).astype(BF16)
        x_buf[seq_rows(i), :] = resid
        n_buf[seq_rows(i), :] = norm_rows(resid, gain2_ref)
        return carry

    lax.fori_loop(0, batch, norm2, 0)
    stores["resid"].start()
    stores["gated"].start()
    for cp in mixed_stores:
        cp.wait()
    for name in ("wq", "wo", "kv", "query", "resid", "gated"):
        stores[name].wait()
    for a in range(3):
        to_side(a).wait_send()
        to_back(a).wait_send()
        for k in range(2):
            onward(a, k).wait_send()
        for k in range(near):
            to_core(a, k).wait_send()


def front_layer(lens, k_pos, cos_t, sin_t, attn_norm, mlp_norm, hidden, w_query, w_key, w_value, w_out, batch, tp):
    rows, dim = hidden.shape
    head_dim = w_key.shape[1]
    shard = rows // batch
    total = tp * shard
    anyspace = pl.BlockSpec(memory_space=pl.ANY)
    vmem = pl.BlockSpec(memory_space=pltpu.VMEM)
    dma = pltpu.SemaphoreType.DMA

    def shape(*dims):
        return jax.ShapeDtypeStruct(dims, BF16)

    return pl.pallas_call(
        functools.partial(front_kernel, batch=batch),
        out_shape=(shape(rows, dim), shape(tp, dim, head_dim), shape(tp, head_dim, dim), shape(tp, rows, 2 * head_dim),
                   shape(tp, rows, head_dim), shape(rows, tp * head_dim), shape(rows, dim), shape(rows, dim)),
        in_specs=[pl.BlockSpec(memory_space=pltpu.SMEM)] + [vmem] * 5 + [anyspace] * 5,
        out_specs=(anyspace,) * 8,
        scratch_shapes=[pltpu.VMEM((rows, dim), BF16), pltpu.VMEM((rows, dim), BF16), pltpu.VMEM((dim, 2 * head_dim), BF16),
                        pltpu.VMEM((tp, dim, head_dim), BF16), pltpu.VMEM((tp, head_dim, dim), BF16),
                        pltpu.VMEM((tp, rows, 2 * head_dim), BF16), pltpu.VMEM((tp, rows, head_dim), BF16),
                        pltpu.VMEM((2, tp // 2 * shard, total), BF16), pltpu.VMEM((rows, tp * head_dim), BF16), pltpu.VMEM((rows, dim), F32),
                        dma((5,)), dma((15,)), dma((3, 8)), dma((3, 8))],
        compiler_params=pltpu.CompilerParams(vmem_limit_bytes=62 << 20, collective_id=2, has_side_effects=True),
        cost_estimate=pl.CostEstimate(flops=8 * rows * dim * tp * head_dim, bytes_accessed=60 << 20, transcendentals=tp * rows * total),
        name="front",
    )(lens, k_pos, cos_t, sin_t, attn_norm.reshape(1, dim), mlp_norm.reshape(1, dim), hidden, w_query, w_key, w_value, w_out)


def attention_backward(lens, cos_t, sin_t, query, kv_all, d_mixed, batch, group=8):
    heads, rows, head_dim = query.shape
    near = kv_all.shape[0] // 2
    shard = rows // batch
    total = 2 * near * shard
    q_spec = pl.BlockSpec((group, shard, head_dim), lambda s, g, *_: (g, s, 0))
    kv_spec = pl.BlockSpec((near, shard, 2 * head_dim), lambda s, g, *_: (0, s, 0))
    table = pl.BlockSpec((shard, head_dim // 2), lambda s, g, *_: (0, 0))
    kv_shape = jax.ShapeDtypeStruct((near, rows, 2 * head_dim), BF16)
    return pl.pallas_call(
        attn_bwd_kernel,
        out_shape=(jax.ShapeDtypeStruct((heads, rows, head_dim), BF16), kv_shape, kv_shape),
        grid_spec=pltpu.PrefetchScalarGridSpec(
            num_scalar_prefetch=1, grid=(batch, heads // group),
            in_specs=[table, table, q_spec, pl.BlockSpec((2 * near, shard, 2 * head_dim), lambda s, g, *_: (0, s, 0)), pl.BlockSpec((shard, group * head_dim), lambda s, g, *_: (s, g))],
            out_specs=(q_spec, kv_spec, kv_spec),
            scratch_shapes=[pltpu.VMEM((total, 2 * head_dim), F32)]),
        compiler_params=pltpu.CompilerParams(dimension_semantics=("arbitrary", "arbitrary"), vmem_limit_bytes=56 << 20),
        cost_estimate=pl.CostEstimate(flops=10 * heads * rows * total * head_dim, bytes_accessed=20 << 20, transcendentals=heads * rows * total),
        name="attn_bwd",
    )(lens, cos_t, sin_t, query, kv_all, d_mixed)


def gated_tile(z, g, w_g, w_u, w_d):
    gate = dot_nn(z, w_g)
    upper = dot_nn(z, w_u)
    d_act = dot_nt(g, w_d).astype(BF16).astype(F32)
    sq = gate * gate
    th = jnp.tanh(gate * (GELU_C + (GELU_C * GELU_K) * sq))
    half = 0.5 + 0.5 * th
    gelu = gate * half
    slope = half + gate * (0.5 - 0.5 * (th * th)) * (GELU_C + (3.0 * GELU_C * GELU_K) * sq)
    return (gelu * upper).astype(BF16), (d_act * upper * slope).astype(BF16), (d_act * gelu).astype(BF16)


def gated_kernel(z_own, g_own, wg_hbm, wu_hbm, wd_hbm, z_all, g_all, act, d_gate, d_up, g_down,
                 wg, wu, wd, z_buf, g_buf, outs, acc, acc_sem, w_sem, in_sem, own_sem, out_sem, send, recv, send0, recv0, *, bn):
    rows, dim = z_own.shape
    width = wg_hbm.shape[1]
    steps = width // bn
    piece = rows // 4
    me, core, side, back = neighbours()
    corner = flip(side, 4)
    own = (z_own, g_own)
    full = (z_all, g_all)

    def part(slot, q):
        return pl.ds(pl.multiple_of(slot * rows + q * piece, 16), piece)

    def link_rows(u, path):
        turn = u // 2
        diag = turn % 2
        if path == 0:
            return side + (corner - side) * diag, (u % 2) + 2 * (turn // 2) + diag * 2
        return back + (corner - back) * diag, (u % 2) + 2 - 2 * (turn // 2) - diag * 2

    def link_copy(u, path, a):
        turn = u // 2
        peer = side if path == 0 else back
        sems = (send.at[path, u, a], recv.at[path, u, a])
        if turn == 1:
            slot = back if path == 0 else side
            q = (2 if path == 0 else 0) + u % 2
            return remote(full[a].at[part(slot, q)], full[a].at[part(slot, q)], *sems, peer)
        q = u % 2 + (2 * (turn // 2) if path == 0 else 2 - 2 * (turn // 2))
        return remote(own[a].at[pl.ds(q * piece, piece)], full[a].at[part(me, q)], *sems, peer)

    def core_copy(u, path, a):
        slot, q = link_rows(u, path)
        return remote(full[a].at[part(slot, q)], full[a].at[part(slot, q)], send.at[2 + path, u, a], recv.at[2 + path, u, a], core)

    def own_copy(a):
        return remote(own[a], full[a].at[pl.ds(pl.multiple_of(me * rows, 16), rows)], send0.at[a], recv0.at[a], core)

    def weight_copies(n):
        cols = pl.ds(pl.multiple_of(n * bn, 128), bn)
        return [pltpu.make_async_copy(wg_hbm.at[:, cols], wg.at[:, cols], w_sem.at[0, n]),
                pltpu.make_async_copy(wu_hbm.at[:, cols], wu.at[:, cols], w_sem.at[1, n]),
                pltpu.make_async_copy(wd_hbm.at[cols], wd.at[cols], w_sem.at[2, n])]

    bufs = (z_buf, g_buf)
    own_in = [pltpu.make_async_copy(own[a], bufs[a], own_sem.at[a]) for a in range(2)]
    own_out = [pltpu.make_async_copy(bufs[a], full[a].at[pl.ds(pl.multiple_of(me * rows, 16), rows)], own_sem.at[2 + a]) for a in range(2)]
    for cp in own_in:
        cp.start()
    for n in range(steps):
        for cp in weight_copies(n):
            cp.start()
    enter((core, side, back))
    for u in range(2):
        for path in range(2):
            for a in range(2):
                link_copy(u, path, a).start()
        if u == 0:
            for a in range(2):
                own_copy(a).start()

    def out_copies(slot, s_rows, n):
        cols = pl.ds(pl.multiple_of(n * bn, 128), bn)
        return [pltpu.make_async_copy(outs.at[slot, k, pl.ds(i * piece, piece)], ref.at[s_rows[i], cols], out_sem.at[slot, k, i])
                for k, ref in enumerate((act, d_gate, d_up)) for i in range(4)]

    def acc_copy(n):
        part = pl.ds(pl.multiple_of(n * bn, 128), bn)
        return pltpu.make_async_copy(acc.at[part], g_down.at[part], acc_sem.at[n])

    def stage_rows(s):
        late = (s + 6) // 8
        u = (s - 2) * late
        first = me + (core - me) * s * (1 - late)
        (slot_x, q_x), (slot_y, q_y) = link_rows(u, 0), link_rows(u, 1)
        base_x, base_y = slot_x * rows + q_x * piece, slot_y * rows + q_y * piece
        pair_x, pair_y = flip(slot_x, 1) * rows + q_x * piece, flip(slot_y, 1) * rows + q_y * piece
        starts = [(1 - late) * (first * rows + i * piece) + late * base for i, base in enumerate((base_x, base_y, pair_x, pair_y))]
        return [pl.ds(pl.multiple_of(st, 16), piece) for st in starts]

    def compute(s):
        s_rows = stage_rows(s)

        def block(n, carry):
            step = s * steps + n
            slot = step % 2

            @pl.when(step >= 2)
            def _():
                for cp in out_copies(slot, s_rows, n):
                    cp.wait()

            @pl.when(s == 0)
            def _():
                for cp in weight_copies(n):
                    cp.wait()

            cols = pl.ds(pl.multiple_of(n * bn, 128), bn)
            res = gated_tile(z_buf[...], g_buf[...], wg[:, cols], wu[:, cols], wd[cols, :])
            for k in range(3):
                outs[slot, k] = res[k]
            for cp in out_copies(slot, s_rows, n):
                cp.start()

            @pl.when(s >= 2)
            def _():
                for c in range(2):
                    part = slice(c * (dim // 2), (c + 1) * (dim // 2))
                    acc[cols, part] += dot_tn(outs[slot, 0], g_buf[:, part])

                @pl.when(s == 7)
                def _():
                    acc_copy(n).start()

            return carry

        lax.fori_loop(0, steps, block, 0)

    def stage(s, carry):
        @pl.when(s == 0)
        def _():
            for cp in own_in:
                cp.wait()
            for cp in own_out:
                cp.start()

        @pl.when(s == 1)
        def _():
            acc[...] = jnp.zeros_like(acc)
            for cp in own_out:
                cp.wait()
            for a in range(2):
                own_copy(a).wait_recv()

        for u in range(6):
            @pl.when(s == u + 2)
            def _(u=u):
                for path in range(2):
                    for a in range(2):
                        link_copy(u, path, a).wait_recv()
                        core_copy(u, path, a).start()
                if u < 2:
                    for path in range(2):
                        for a in range(2):
                            link_copy(u + 2, path, a).start()
                if u == 1:
                    for later in (4, 5):
                        for path in range(2):
                            for a in range(2):
                                link_copy(later, path, a).start()
                for path in range(2):
                    for a in range(2):
                        core_copy(u, path, a).wait_recv()

        @pl.when(s >= 1)
        def _():
            s_rows = stage_rows(s)
            copies = [pltpu.make_async_copy(full[a].at[s_rows[i]], bufs[a].at[pl.ds(i * piece, piece)], in_sem.at[a, i])
                      for a in range(2) for i in range(4)]
            for cp in copies:
                cp.start()
            for cp in copies:
                cp.wait()

        compute(s)
        return carry

    lax.fori_loop(0, 8, stage, 0)
    last = stage_rows(7)
    for slot in range(2):
        for cp in out_copies(slot, last, 0):
            cp.wait()
    for n in range(steps):
        acc_copy(n).wait()
    for a in range(2):
        own_copy(a).wait_send()
        for path in range(2):
            for u in range(6):
                link_copy(u, path, a).wait_send()
                core_copy(u, path, a).wait_send()


def gated_layer(z_own, g_own, w_gate, w_up, w_down, tp, bn=512):
    rows, dim = z_own.shape
    width = w_gate.shape[1]
    total = rows * tp
    anyspace = pl.BlockSpec(memory_space=pl.ANY)
    gathered = jax.ShapeDtypeStruct((total, dim), BF16)
    made = jax.ShapeDtypeStruct((total, width), BF16)
    dma = pltpu.SemaphoreType.DMA
    return pl.pallas_call(
        functools.partial(gated_kernel, bn=bn),
        out_shape=(gathered, gathered, made, made, made, jax.ShapeDtypeStruct((width, dim), F32)),
        in_specs=[anyspace] * 5,
        out_specs=(anyspace,) * 6,
        scratch_shapes=[pltpu.VMEM((dim, width), BF16), pltpu.VMEM((dim, width), BF16), pltpu.VMEM((width, dim), BF16),
                        pltpu.VMEM((rows, dim), BF16), pltpu.VMEM((rows, dim), BF16), pltpu.VMEM((2, 3, rows, bn), BF16),
                        pltpu.VMEM((width, dim), F32), dma((width // bn,)), dma((3, width // bn)), dma((2, 4)), dma((4,)), dma((2, 3, 4)), dma((4, 6, 2)), dma((4, 6, 2)), dma((2,)), dma((2,))],
        compiler_params=pltpu.CompilerParams(vmem_limit_bytes=67043328, collective_id=0, has_side_effects=True),
        cost_estimate=pl.CostEstimate(flops=6 * total * dim * width, bytes_accessed=200 << 20, transcendentals=total * width),
        name="gated",
    )(z_own, g_own, w_gate, w_up, w_down)


def back_kernel(act, d_gate, d_up, z_all, wg_hbm, wu_hbm, wd_hbm, own_out, x_in, y_in, g_gate,
                wa, wb, lhs, st, from_core, from_diag, own_st, z_sem, w_sem, l_sem, o_sem, c_send, c_recv, d_send, d_recv, f_send, f_recv, *, rows, bn):
    dim, width = wg_hbm.shape
    steps = dim // bn
    half = rows // 2
    me, core, side, back = neighbours()

    def cols(j):
        return pl.ds(pl.multiple_of(j * bn, 128), bn)

    def pair_of(t):
        return ((t + 5) // 7) * ((t + 1) % 3 + 1)

    def lhs_copies(phase, t):
        pair = pair_of(t)
        theirs = 1 - t // 5 - ((t + 6) // 7 - (t + 5) // 7)
        dev = me + (1 - pair // 2) * (side - me) + (1 - pair % 2) * (back - me)
        dev = dev + theirs * (flip(dev, 1) - dev)
        src = pl.ds(pl.multiple_of(dev * rows, 16), rows)
        refs = (act,) if phase == 0 else (d_gate, d_up)
        return [pltpu.make_async_copy(ref.at[src], lhs.at[t % 2, k], l_sem.at[t % 2, k]) for k, ref in enumerate(refs)]

    def weight_copy(k, j):
        if k == 0:
            return pltpu.make_async_copy(wd_hbm.at[:, cols(j)], wa.at[pl.ds(0, width), cols(j)], w_sem.at[0, j])
        src, dst = (wg_hbm, wb) if k == 1 else (wu_hbm, wa)
        return pltpu.make_async_copy(src.at[cols(j)], dst.at[cols(j)], w_sem.at[k, j])

    def core_copy(pair, j):
        return remote(st.at[0, j], from_core.at[pair, j], c_send.at[j], c_recv.at[pair, j], core)

    def diag_copy(phase, k, j):
        return remote(st.at[1, j, pl.ds(k * half, half)], from_diag.at[phase, k, j], d_send.at[k, j], d_recv.at[phase, k, j], (side, back)[k])

    def final_copy(phase, k, j):
        return remote(st.at[2 + k, j], (x_in, y_in)[k].at[phase, :, cols(j)], f_send.at[k, j], f_recv.at[phase, k, j], (side, back)[k])

    def own_copy(phase, j):
        return pltpu.make_async_copy(own_st.at[j % 2], own_out.at[phase, :, cols(j)], o_sem.at[j % 2])

    def product(phase, slot, j):
        if phase == 0:
            return dot_nn(lhs[slot, 0], wa[:width, cols(j)])
        return dot_nt(lhs[slot, 0], wb[cols(j), :]) + dot_nt(lhs[slot, 1], wa[cols(j), :])

    for cp in lhs_copies(0, 0):
        cp.start()
    for j in range(steps):
        weight_copy(0, j).start()
    enter((core, side, back))

    def tiles(body):
        def step(j, carry):
            body(j)
            return carry

        lax.fori_loop(0, steps, step, 0)

    for phase in (0, 1):
        def step(t, carry, phase=phase):
            for cp in lhs_copies(phase, t):
                cp.wait()

            @pl.when(t < 7)
            def _():
                for cp in lhs_copies(phase, t + 1):
                    cp.start()

            if phase == 0:
                @pl.when(t == 1)
                def _():
                    for j in range(steps):
                        weight_copy(1, j).start()

                @pl.when(t == 7)
                def _():
                    for cp in lhs_copies(1, 0):
                        cp.start()

            @pl.when((t == 0) | ((t >= 2) & (t <= 4)))
            def _():
                pair = pair_of(t)

                def body(j):
                    @pl.when(t == 0)
                    def _():
                        for k in ((0,) if phase == 0 else (1, 2)):
                            weight_copy(k, j).wait()

                    if phase == 0:
                        @pl.when(t > 0)
                        def _():
                            core_copy(0, j).wait_send()
                    else:
                        core_copy(0, j).wait_send()
                    st[0, j] = product(phase, t % 2, j).astype(BF16)
                    core_copy(pair, j).start()

                tiles(body)

            @pl.when(t == 1)
            def _():
                def body(j):
                    core_copy(0, j).wait_recv()
                    if phase == 1:
                        for k in range(2):
                            diag_copy(0, k, j).wait_send()
                    st[1, j] = (product(phase, 1, j) + from_core[0, j].astype(F32)).astype(BF16)
                    for k in range(2):
                        diag_copy(phase, k, j).start()

                tiles(body)

            for k in range(2):
                @pl.when(t == 5 + k)
                def _(k=k):
                    def body(j):
                        core_copy(1 + k, j).wait_recv()
                        diag_copy(phase, 1 - k, j).wait_recv()
                        if phase == 1:
                            final_copy(0, k, j).wait_send()
                        total = product(phase, (5 + k) % 2, j) + from_core[1 + k, j].astype(F32)
                        came = from_diag[phase, 1 - k, j].astype(F32)
                        split = slice(half, rows) if k == 0 else slice(0, half)
                        rest = slice(0, half) if k == 0 else slice(half, rows)
                        st[2 + k, j, split, :] = (total[split] + came).astype(BF16)
                        st[2 + k, j, rest, :] = total[rest].astype(BF16)
                        final_copy(phase, k, j).start()

                    tiles(body)

            @pl.when(t == 7)
            def _():
                def body(j):
                    core_copy(3, j).wait_recv()

                    @pl.when(j >= 2)
                    def _():
                        own_copy(phase, j).wait()

                    own_st[j % 2] = product(phase, 1, j) + from_core[3, j].astype(F32)
                    own_copy(phase, j).start()

                tiles(body)
                for j in (0, 1):
                    own_copy(phase, j).wait()
                if phase == 0:
                    for j in range(steps):
                        weight_copy(2, j).start()

            return carry

        lax.fori_loop(0, 8, step, 0)

    def z_copy(j, c):
        return pltpu.make_async_copy(z_all.at[pl.ds(c * rows, rows), cols(j)], lhs.at[c // 2, c % 2, :, cols(j)], z_sem.at[j, c])

    def gate_copy(j):
        return pltpu.make_async_copy(d_gate.at[pl.ds(0, 4 * rows), cols(j)], wa.at[:, cols(j)], w_sem.at[0, j])

    def grad_copy(i, j):
        slot = j % 2
        return pltpu.make_async_copy(own_st.at[slot, pl.ds(0, bn)], g_gate.at[cols(i), cols(j)], o_sem.at[slot])

    for j in range(steps):
        for c in range(4):
            z_copy(j, c).start()
        gate_copy(j).start()

    def grad_tile(step, carry):
        i, j = step // steps, step % steps

        @pl.when(i == 0)
        def _():
            gate_copy(j).wait()

        @pl.when(j == 0)
        def _():
            for c in range(4):
                z_copy(i, c).wait()

        @pl.when(step >= 2)
        def _():
            grad_copy(i, j).wait()

        own_st[j % 2, :bn] = dot_tn(lhs[:, :, :, cols(i)].reshape(4 * rows, bn), wa[:, cols(j)])
        grad_copy(i, j).start()
        return carry

    lax.fori_loop(0, steps * steps, grad_tile, 0)
    for j in range(2):
        grad_copy(0, j).wait()
    for j in range(steps):
        core_copy(0, j).wait_send()
        for k in range(2):
            diag_copy(1, k, j).wait_send()
            final_copy(1, k, j).wait_send()
            for phase in (0, 1):
                final_copy(phase, k, j).wait_recv()


def back_layer(act, d_gate, d_up, z_all, w_gate, w_up, w_down, tp, bn=512):
    total, width = act.shape
    dim = w_gate.shape[0]
    rows = total // tp
    steps = dim // bn
    anyspace = pl.BlockSpec(memory_space=pl.ANY)
    dma = pltpu.SemaphoreType.DMA
    came = jax.ShapeDtypeStruct((2, rows, dim), BF16)
    return pl.pallas_call(
        functools.partial(back_kernel, rows=rows, bn=bn),
        out_shape=(jax.ShapeDtypeStruct((2, rows, dim), F32), came, came, jax.ShapeDtypeStruct((dim, width), F32)),
        in_specs=[anyspace] * 7,
        out_specs=(anyspace,) * 4,
        scratch_shapes=[pltpu.VMEM((4 * rows, dim), BF16), pltpu.VMEM((dim, width), BF16), pltpu.VMEM((2, 2, rows, width), BF16),
                        pltpu.VMEM((4, steps, rows, bn), BF16), pltpu.VMEM((4, steps, rows, bn), BF16),
                        pltpu.VMEM((2, 2, steps, rows // 2, bn), BF16), pltpu.VMEM((2, rows, bn), F32),
                        dma((steps, 4)), dma((3, steps)), dma((2, 2)), dma((2,)), dma((steps,)), dma((4, steps)),
                        dma((2, steps)), dma((2, 2, steps)), dma((2, steps)), dma((2, 2, steps))],
        compiler_params=pltpu.CompilerParams(vmem_limit_bytes=67043328, collective_id=1, has_side_effects=True),
        cost_estimate=pl.CostEstimate(flops=6 * total * dim * width, bytes_accessed=200 << 20, transcendentals=0),
        name="back",
    )(act, d_gate, d_up, z_all, w_gate, w_up, w_down)


def product_kernel(a_ref, b_ref, o_ref):
    o_ref[...] = dot_tn(a_ref[...], b_ref[...])


def weight_grad(a, b, bm=512, bn=1024):
    rows, m = a.shape
    n = b.shape[1]
    return pl.pallas_call(
        product_kernel,
        out_shape=jax.ShapeDtypeStruct((m, n), F32),
        grid=(m // bm, n // bn),
        in_specs=[pl.BlockSpec((rows, bm), lambda i, j: (0, i)), pl.BlockSpec((rows, bn), lambda i, j: (0, j))],
        out_specs=pl.BlockSpec((bm, bn), lambda i, j: (i, j)),
        compiler_params=pltpu.CompilerParams(dimension_semantics=("arbitrary", "arbitrary"), vmem_limit_bytes=56 << 20),
        cost_estimate=pl.CostEstimate(flops=2 * rows * m * n, bytes_accessed=110 << 20, transcendentals=0),
        name="weight_grad",
    )(a, b)


def rest_kernel(at_ref, a_ref, b_ref, part_ref, o_ref):
    o_ref[...] = part_ref[...] + dot_tn(a_ref[...], b_ref[...])


def weight_grad_rest(a, b, part, block, count, bm=512, bn=1024):
    m, n = part.shape
    out = pl.BlockSpec((bm, bn), lambda i, j, at: (i, j))
    return pl.pallas_call(
        rest_kernel,
        out_shape=jax.ShapeDtypeStruct((m, n), F32),
        grid_spec=pltpu.PrefetchScalarGridSpec(
            num_scalar_prefetch=1, grid=(m // bm, n // bn),
            in_specs=[pl.BlockSpec((count, bm), lambda i, j, at: (at[0], i)), pl.BlockSpec((count, bn), lambda i, j, at: (at[0], j)), out],
            out_specs=out),
        compiler_params=pltpu.CompilerParams(dimension_semantics=("arbitrary", "arbitrary"), vmem_limit_bytes=56 << 20),
        cost_estimate=pl.CostEstimate(flops=2 * count * m * n, bytes_accessed=80 << 20, transcendentals=0),
        name="weight_grad_rest",
    )(jnp.asarray(block, jnp.int32).reshape(1), a, b, part)


def hop_diagonal(diag):
    half = diag.shape[0] // 2
    return swap(diag[:half], 2), swap(diag[half:], 4)


def hop_near(side, back, came_side, came_back):
    half = side.shape[0] // 2
    kind = came_side.dtype
    side = jnp.concatenate([side[:half], side[half:] + came_back.astype(F32)], axis=0).astype(kind)
    back = jnp.concatenate([back[:half] + came_side.astype(F32), back[half:]], axis=0).astype(kind)
    return side, back


def solution(mesh):
    tp_size = mesh.shape["tp"]
    act_spec = P("dp", "tp", None)
    in_specs = (act_spec, act_spec, P("dp"), P("dp"), P(None), P(None, "tp"), P(None, None), P(None, None), P("tp", None), P(None), P(None, "tp"), P(None, "tp"), P("tp", None))
    out_specs = (act_spec, act_spec, P("dp"), P("dp", "tp"), P("dp", None), P("dp", None), P(("dp", "tp"), None), P("dp"), P("dp", "tp"), P("dp", "tp"), P(("dp", "tp"), None))

    def layer(hidden, grad_out, prefix_len, valid_len, attn_norm, w_query, w_key, w_value, w_out, mlp_norm, w_gate, w_up, w_down):
        batch, shard, dim = hidden.shape
        head_dim = w_key.shape[1]
        rows = batch * shard
        me = lax.axis_index("tp")
        starts = (me ^ jnp.array([0, 2, 4, 6, 1, 3, 5, 7], jnp.int32)) * shard
        k_pos = (starts[:, None] + jnp.arange(shard, dtype=jnp.int32)).reshape(1, tp_size * shard)
        lens = jnp.stack([prefix_len, valid_len])
        cos_own, sin_own = rope_tables(me * shard + jnp.arange(shard), head_dim)
        hidden = hidden.reshape(rows, dim)
        grad_out = grad_out.reshape(rows, dim)
        normed, wq_all, wo_all, kv_all, query, mixed, resid, gated_in = front_layer(
            lens, k_pos, cos_own, sin_own, attn_norm, mlp_norm, hidden, w_query, w_key, w_value, w_out, batch, tp_size)
        wo_all = wo_all.reshape(tp_size * head_dim, dim)

        def rope(raw_proj):
            return apply_rope(raw_proj, jnp.tile(cos_own, (batch, 1)), jnp.tile(sin_own, (batch, 1)))

        gated_all, grad_all, act, d_gate, d_upper, g_down_part = gated_layer(gated_in, grad_out, w_gate, w_up, w_down, tp_size)
        own_part, x_part, y_part, g_gate_part = back_layer(act, d_gate, d_upper, gated_all, w_gate, w_up, w_down, tp_size)
        hidden, resid, own_part = lax.optimization_barrier((hidden, resid, own_part))
        norm1_pull = jax.vjp(rms_norm, hidden, attn_norm.astype(F32))[1]
        norm2_pull = jax.vjp(rms_norm, resid, mlp_norm.astype(F32))[1]
        key_pull = jax.linear_transpose(rope, jax.ShapeDtypeStruct((rows, head_dim), F32))
        mlp_sum, d_gated = [own_part[k] + x_part[k].astype(F32) + y_part[k].astype(F32) for k in range(2)]
        d_gated = d_gated.astype(BF16)
        hidden_out = (resid.astype(F32) + mlp_sum).astype(BF16)
        d_resid_norm, g_mlp_norm_part = norm2_pull(d_gated)
        d_resid = (grad_out.astype(F32) + d_resid_norm.astype(F32)).astype(BF16)
        g_out_part = dot_tn(mixed, d_resid)
        d_mixed = dot_nt(d_resid, wo_all).astype(BF16)
        lens_back = jnp.concatenate([lens, jnp.full((1, batch), me, jnp.int32), jnp.broadcast_to(starts[:, None], (tp_size, batch))])
        d_mixed, g_out_part = lax.optimization_barrier((d_mixed, g_out_part))
        g_out = lax.psum_scatter(g_out_part, "tp", scatter_dimension=0, tiled=True)
        d_q_raw, dkv_near, dkv_far = attention_backward(lens_back, cos_own, sin_own, query, kv_all, d_mixed, batch)
        came_kv = swap(dkv_far, 1)
        near = tp_size // 2
        came_q = swap(jnp.einsum("td,kte->kde", normed, d_q_raw[near:], preferred_element_type=F32), 1)
        d_normed_q = jnp.einsum("hte,hde->td", d_q_raw, wq_all, preferred_element_type=F32)
        came_kv, d_normed_q = lax.optimization_barrier((came_kv, d_normed_q))
        kv_own, kv_side, kv_back, kv_diag = [dkv_near[k].astype(F32) + came_kv[k].astype(F32) for k in range(4)]
        kv_came = hop_diagonal(kv_diag.astype(BF16))
        g_query_sum = jnp.einsum("td,kte->kde", normed, d_q_raw[:near], preferred_element_type=F32) + came_q
        kv_came, g_query_sum, act = lax.optimization_barrier((kv_came, g_query_sum, act))
        kv_next = hop_near(kv_side, kv_back, *kv_came)
        kv_last = (swap(kv_next[0], 2), swap(kv_next[1], 4))
        q_came = hop_diagonal(g_query_sum[3])
        g_down = weight_grad_rest(act, grad_all, g_down_part, me // 2, 2 * rows)
        kv_last, g_down = lax.optimization_barrier((kv_last, g_down))
        d_kv = (kv_own + kv_last[0].astype(F32) + kv_last[1].astype(F32)).astype(BF16)
        d_k_raw = key_pull(d_kv[:, :head_dim].astype(F32))[0].astype(BF16)
        d_values = d_kv[:, head_dim:]
        g_key_part, g_value_part = dot_tn(normed, d_k_raw), dot_tn(normed, d_values)
        g_key_part, g_value_part, d_gate = lax.optimization_barrier((g_key_part, g_value_part, d_gate))
        g_key, g_value = lax.psum((g_key_part, g_value_part), "tp")
        g_gate = weight_grad_rest(gated_all, d_gate, g_gate_part, 1, 4 * rows)
        q_came, g_gate = lax.optimization_barrier((q_came, g_gate))
        q_next = hop_near(g_query_sum[1], g_query_sum[2], *q_came)
        d_normed = (d_normed_q + dot_nt(d_k_raw, w_key) + dot_nt(d_values, w_value)).astype(BF16)
        d_hidden_norm, g_attn_norm_part = norm1_pull(d_normed)
        norms = jnp.stack([g_attn_norm_part, g_mlp_norm_part])
        q_next, norms, d_upper = lax.optimization_barrier((q_next, norms, d_upper))
        q_last = (swap(q_next[0], 2), swap(q_next[1], 4))
        norms_near = [swap(norms, bit) for bit in (2, 4, 6)]
        g_up = weight_grad(gated_all, d_upper)
        norms_near, q_last, g_up, d_hidden_norm = lax.optimization_barrier((norms_near, q_last, g_up, d_hidden_norm))
        norms = norms + norms_near[0] + norms_near[1] + norms_near[2]
        g_norms = norms + swap(norms, 1)
        g_query = g_query_sum[0] + q_last[0] + q_last[1]
        grad_hidden = (d_resid.astype(F32) + d_hidden_norm.astype(F32)).astype(BF16)
        full = (batch, shard, dim)
        return (hidden_out.reshape(full), grad_hidden.reshape(full), g_norms[0], g_query, g_key, g_value, g_out, g_norms[1], g_gate, g_up, g_down)

    return jax.shard_map(layer, mesh=mesh, in_specs=in_specs, out_specs=out_specs, check_vma=False)
```

```python
import functools
import math
import jax
import jax.numpy as jnp
from jax import lax
from jax.experimental import pallas as pl
from jax.experimental.pallas import tpu as pltpu
from jax.sharding import PartitionSpec as P

NORM_EPS = 1e-6
BF16 = jnp.bfloat16
F32 = jnp.float32
GELU_C = math.sqrt(2.0 / math.pi)
GELU_K = 0.044715
MASKED = -1e30
NT = (((1,), (1,)), ((), ()))
TN = (((0,), (0,)), ((), ()))


def rms_norm(x_in, gain):
    x_f = x_in.astype(F32)
    inv_rms = lax.rsqrt(jnp.mean(x_f * x_f, axis=-1, keepdims=True) + NORM_EPS)
    return (x_f * inv_rms * (1.0 + gain)).astype(BF16)


def rope_tables(positions, head_dim):
    half_dim = head_dim // 2
    exponent = jnp.arange(half_dim, dtype=F32) * (2.0 / head_dim)
    inv_freq = jnp.exp(exponent * (-math.log(10000.0)))
    angles = positions.astype(F32)[:, None] * inv_freq[None, :]
    return jnp.cos(angles), jnp.sin(angles)


def apply_rope(x_f, cos_t, sin_t):
    half_dim = x_f.shape[-1] // 2
    first = x_f[..., :half_dim]
    second = x_f[..., half_dim:]
    return jnp.concatenate([first * cos_t - second * sin_t, second * cos_t + first * sin_t], axis=-1)


def dot_nn(a, b):
    return jnp.dot(a, b, preferred_element_type=F32)


def dot_nt(a, b):
    return lax.dot_general(a, b, NT, preferred_element_type=F32)


def dot_tn(a, b):
    return lax.dot_general(a, b, TN, preferred_element_type=F32)


def swap(x, bit):
    return lax.ppermute(x, "tp", [(t, t ^ bit) for t in range(8)])


def flip(index, bit):
    return index + bit - 2 * bit * ((index // bit) % 2)


def neighbours():
    me = lax.axis_index("tp")
    return me, flip(me, 1), flip(me, 2), flip(me, 4)


def enter(peers):
    barrier = pltpu.get_barrier_semaphore()
    for peer in peers:
        pl.semaphore_signal(barrier, inc=1, device_id={"tp": peer}, device_id_type=pl.DeviceIdType.MESH)
    pl.semaphore_wait(barrier, len(peers))


def attn_bwd_kernel(lens_ref, cos_ref, sin_ref, q_ref, kv_ref, do_ref, dq_ref, dkv0_ref, dkv1_ref, dkv_acc):
    heads, shard, head_dim = q_ref.shape
    tp = kv_ref.shape[0]
    total = tp * shard
    rows = heads * shard
    s_id = pl.program_id(0)
    g_id = pl.program_id(1)
    prefix = lens_ref[0, s_id]
    valid = lens_ref[1, s_id]
    first = lens_ref[2, 0] * shard
    keys = kv_ref[:, :, :head_dim].reshape(total, head_dim)
    values = kv_ref[:, :, head_dim:].reshape(total, head_dim)
    query = q_ref[...].reshape(rows, head_dim) * BF16(head_dim ** -0.5)
    d_out = jnp.concatenate([do_ref[:, h * head_dim:(h + 1) * head_dim] for h in range(heads)], axis=0)
    step = lax.broadcasted_iota(jnp.int32, (shard, 1), 0)
    k_pos = jnp.concatenate([step + lens_ref[3 + r, 0] for r in range(tp)], axis=0)
    q_pos = first + lax.rem(lax.broadcasted_iota(jnp.int32, (1, rows), 1), shard)
    limit = jnp.minimum(valid, jnp.maximum(prefix, q_pos + 1))
    cos_t, sin_t = cos_ref[...][None], sin_ref[...][None]
    d_k = d_v = None
    count = heads // 2
    width = count * shard
    for c in range(2):
        cols = slice(c * width, (c + 1) * width)
        q_c, do_c = query[cols], d_out[cols]
        s = jnp.where(k_pos < limit[:, cols], dot_nt(keys, q_c), MASKED)
        e = jnp.exp(s - jnp.max(s, axis=0, keepdims=True))
        p = e * (1.0 / jnp.sum(e, axis=0, keepdims=True))
        d_p = dot_nt(values, do_c)
        delta = jnp.sum(p * d_p, axis=0, keepdims=True)
        d_s = (p * (d_p - delta)).astype(BF16)
        d_v_c = dot_nn(p.astype(BF16), do_c)
        d_k_c = dot_nn(d_s, q_c)
        d_k, d_v = (d_k_c, d_v_c) if d_k is None else (d_k + d_k_c, d_v + d_v_c)
        d_q = (dot_tn(d_s, keys) * (head_dim ** -0.5)).reshape(count, shard, head_dim)
        first, second = d_q[:, :, :head_dim // 2], d_q[:, :, head_dim // 2:]
        some = slice(c * count, (c + 1) * count)
        dq_ref[some, :, :head_dim // 2] = (first * cos_t + second * sin_t).astype(BF16)
        dq_ref[some, :, head_dim // 2:] = (second * cos_t - first * sin_t).astype(BF16)
    d_kv = jnp.concatenate([d_k, d_v], axis=1)

    @pl.when(g_id == 0)
    def _():
        dkv_acc[...] = d_kv

    @pl.when(g_id > 0)
    def _():
        dkv_acc[...] += d_kv

    @pl.when(g_id == pl.num_programs(1) - 1)
    def _():
        near = (tp // 2, shard, 2 * head_dim)
        dkv0_ref[...] = dkv_acc[:total // 2].astype(BF16).reshape(near)
        dkv1_ref[...] = dkv_acc[total // 2:].astype(BF16).reshape(near)


def remote(src, dst, send, recv, peer):
    return pltpu.make_async_remote_copy(src_ref=src, dst_ref=dst, send_sem=send, recv_sem=recv,
                                        device_id={"tp": peer}, device_id_type=pl.DeviceIdType.MESH)


def front_kernel(lens_ref, kpos_ref, cos_ref, sin_ref, gain1_ref, gain2_ref, hidden, w_query, w_key, w_value, w_out,
                 normed_out, wq_all, wo_all, kv_all, query_out, mixed_out, resid_out, gated_out,
                 x_buf, n_buf, wkv, wq, wo, kv, q, probs, mix, acc, load, store, send, recv, *, batch):
    rows, dim = x_buf.shape
    shard = rows // batch
    head_dim = w_key.shape[1]
    tp = wq.shape[0]
    near = tp // 2
    total = tp * shard
    half_dim = head_dim // 2
    me, core, side, back = neighbours()
    bufs = (wq, kv, wo)

    def to_side(a):
        return remote(bufs[a].at[0], bufs[a].at[1], send.at[a, 0], recv.at[a, 0], side)

    def to_back(a):
        return remote(bufs[a].at[0], bufs[a].at[2], send.at[a, 1], recv.at[a, 1], back)

    def onward(a, k):
        half = bufs[a].shape[1] // 2
        part = pl.ds(k * half, half)
        return remote(bufs[a].at[1 + k, part], bufs[a].at[3, part], send.at[a, 2 + k], recv.at[a, 2 + k], (back, side)[k])

    def to_core(a, k):
        return remote(bufs[a].at[k], bufs[a].at[near + k], send.at[a, 4 + k], recv.at[a, 4 + k], core)

    loads = [pltpu.make_async_copy(src, dst, load.at[i]) for i, (src, dst) in enumerate((
        (w_query, wq.at[0]), (hidden, x_buf), (w_key, wkv.at[:, :head_dim]), (w_value, wkv.at[:, head_dim:]), (w_out, wo.at[0])))]
    mixed_at = [me, side, back, flip(side, 4)]
    mixed_at = mixed_at + [flip(dev, 1) for dev in mixed_at]
    stores = {name: pltpu.make_async_copy(src, dst, store.at[i]) for i, (name, src, dst) in enumerate((
        ("normed", n_buf, normed_out), ("wq", wq, wq_all), ("wo", wo, wo_all), ("kv", kv, kv_all), ("query", q, query_out),
        ("resid", x_buf, resid_out), ("gated", n_buf, gated_out)))}
    mixed_stores = [pltpu.make_async_copy(mix.at[:, pl.ds(k * head_dim, head_dim)],
                                          mixed_out.at[:, pl.ds(pl.multiple_of(dev * head_dim, 128), head_dim)], store.at[7 + k])
                    for k, dev in enumerate(mixed_at)]

    for cp in loads:
        cp.start()
    enter((core, side, back))
    loads[0].wait()
    to_side(0).start()
    to_back(0).start()
    to_core(0, 0).start()

    def norm_rows(src, gain_ref):
        x_f = src.astype(F32)
        inv_rms = lax.rsqrt(jnp.mean(x_f * x_f, axis=-1, keepdims=True) + NORM_EPS)
        return (x_f * inv_rms * (1.0 + gain_ref[...].astype(F32))).astype(BF16)

    def seq_rows(i):
        return pl.ds(pl.multiple_of(i * shard, 16), shard)

    def rotate(x_f):
        first, second = x_f[:, :half_dim], x_f[:, half_dim:]
        cos_t, sin_t = cos_ref[...], sin_ref[...]
        return first * cos_t - second * sin_t, second * cos_t + first * sin_t

    def norm1(i, carry):
        n_buf[seq_rows(i), :] = norm_rows(x_buf[seq_rows(i), :], gain1_ref)
        return carry

    loads[1].wait()
    lax.fori_loop(0, batch, norm1, 0)
    stores["normed"].start()
    loads[2].wait()
    loads[3].wait()

    def own_kv(i, carry):
        raw = dot_nn(n_buf[seq_rows(i), :], wkv[...])
        first, second = rotate(raw[:, :head_dim])
        kv[0, seq_rows(i), :half_dim] = first.astype(BF16)
        kv[0, seq_rows(i), half_dim:head_dim] = second.astype(BF16)
        kv[0, seq_rows(i), head_dim:] = raw[:, head_dim:].astype(BF16)
        return carry

    lax.fori_loop(0, batch, own_kv, 0)
    to_side(1).start()
    to_back(1).start()
    to_core(1, 0).start()

    def own_query(k):
        def step(i, carry):
            for h in (k, near + k):
                first, second = rotate(dot_nn(n_buf[seq_rows(i), :], wq[h]))
                q[h, seq_rows(i), :half_dim] = first.astype(BF16)
                q[h, seq_rows(i), half_dim:] = second.astype(BF16)
            return carry

        to_core(0, k).wait_recv()
        lax.fori_loop(0, batch, step, 0)

    def pass_on(a):
        to_side(a).wait_recv()
        onward(a, 0).start()
        to_core(a, 1).start()
        to_back(a).wait_recv()
        onward(a, 1).start()
        to_core(a, 2).start()

    def pass_last(a):
        onward(a, 0).wait_recv()
        onward(a, 1).wait_recv()
        to_core(a, 3).start()

    own_query(0)
    pass_on(0)
    own_query(1)
    own_query(2)
    pass_on(1)
    loads[4].wait()
    to_side(2).start()
    to_back(2).start()
    to_core(2, 0).start()
    pass_last(0)
    own_query(3)
    stores["query"].start()
    stores["wq"].start()
    pass_last(1)
    for k in range(near):
        to_core(1, k).wait_recv()
    stores["kv"].start()

    q_pos = me * shard + lax.broadcasted_iota(jnp.int32, (shard, 1), 0)

    def attend(i, carry):
        keys = kv[:, seq_rows(i), :head_dim].reshape(total, head_dim)
        values = kv[:, seq_rows(i), head_dim:].reshape(total, head_dim)
        visible = kpos_ref[...] < jnp.minimum(lens_ref[1, i], jnp.maximum(lens_ref[0, i], q_pos + 1))
        for g in range(2):
            query = q[g * near:(g + 1) * near, seq_rows(i), :].reshape(near * shard, head_dim) * BF16(head_dim ** -0.5)
            scores = dot_nt(query, keys)
            for h in range(near):
                part = slice(h * shard, (h + 1) * shard)
                s = jnp.where(visible, scores[part], MASKED)
                e = jnp.exp(s - jnp.max(s, axis=-1, keepdims=True))
                probs[g, part, :] = (e * (1.0 / jnp.sum(e, axis=-1, keepdims=True))).astype(BF16)
            mixed = dot_nn(probs[g], values).astype(BF16)
            for h in range(near):
                head = g * near + h
                mix[seq_rows(i), head * head_dim:(head + 1) * head_dim] = mixed[h * shard:(h + 1) * shard]
        return carry

    lax.fori_loop(0, batch, attend, 0)
    for cp in mixed_stores:
        cp.start()
    pass_on(2)

    def project(k, first):
        def step(n, carry):
            cols = pl.ds(pl.multiple_of(n * 512, 128), 512)
            part = (dot_nn(mix[:, k * head_dim:(k + 1) * head_dim], wo[k, :, cols])
                    + dot_nn(mix[:, (near + k) * head_dim:(near + k + 1) * head_dim], wo[near + k, :, cols]))
            acc[:, cols] = part if first else acc[:, cols] + part
            return carry

        to_core(2, k).wait_recv()
        lax.fori_loop(0, dim // 512, step, 0)

    project(0, True)
    project(1, False)
    project(2, False)
    pass_last(2)
    project(3, False)
    stores["wo"].start()
    stores["normed"].wait()

    def norm2(i, carry):
        resid = (x_buf[seq_rows(i), :].astype(F32) + acc[seq_rows(i), :]).astype(BF16)
        x_buf[seq_rows(i), :] = resid
        n_buf[seq_rows(i), :] = norm_rows(resid, gain2_ref)
        return carry

    lax.fori_loop(0, batch, norm2, 0)
    stores["resid"].start()
    stores["gated"].start()
    for cp in mixed_stores:
        cp.wait()
    for name in ("wq", "wo", "kv", "query", "resid", "gated"):
        stores[name].wait()
    for a in range(3):
        to_side(a).wait_send()
        to_back(a).wait_send()
        for k in range(2):
            onward(a, k).wait_send()
        for k in range(near):
            to_core(a, k).wait_send()


def front_layer(lens, k_pos, cos_t, sin_t, attn_norm, mlp_norm, hidden, w_query, w_key, w_value, w_out, batch, tp):
    rows, dim = hidden.shape
    head_dim = w_key.shape[1]
    shard = rows // batch
    total = tp * shard
    anyspace = pl.BlockSpec(memory_space=pl.ANY)
    vmem = pl.BlockSpec(memory_space=pltpu.VMEM)
    dma = pltpu.SemaphoreType.DMA

    def shape(*dims):
        return jax.ShapeDtypeStruct(dims, BF16)

    return pl.pallas_call(
        functools.partial(front_kernel, batch=batch),
        out_shape=(shape(rows, dim), shape(tp, dim, head_dim), shape(tp, head_dim, dim), shape(tp, rows, 2 * head_dim),
                   shape(tp, rows, head_dim), shape(rows, tp * head_dim), shape(rows, dim), shape(rows, dim)),
        in_specs=[pl.BlockSpec(memory_space=pltpu.SMEM)] + [vmem] * 5 + [anyspace] * 5,
        out_specs=(anyspace,) * 8,
        scratch_shapes=[pltpu.VMEM((rows, dim), BF16), pltpu.VMEM((rows, dim), BF16), pltpu.VMEM((dim, 2 * head_dim), BF16),
                        pltpu.VMEM((tp, dim, head_dim), BF16), pltpu.VMEM((tp, head_dim, dim), BF16),
                        pltpu.VMEM((tp, rows, 2 * head_dim), BF16), pltpu.VMEM((tp, rows, head_dim), BF16),
                        pltpu.VMEM((2, tp // 2 * shard, total), BF16), pltpu.VMEM((rows, tp * head_dim), BF16), pltpu.VMEM((rows, dim), F32),
                        dma((5,)), dma((15,)), dma((3, 8)), dma((3, 8))],
        compiler_params=pltpu.CompilerParams(vmem_limit_bytes=62 << 20, collective_id=2, has_side_effects=True),
        cost_estimate=pl.CostEstimate(flops=8 * rows * dim * tp * head_dim, bytes_accessed=60 << 20, transcendentals=tp * rows * total),
        name="front",
    )(lens, k_pos, cos_t, sin_t, attn_norm.reshape(1, dim), mlp_norm.reshape(1, dim), hidden, w_query, w_key, w_value, w_out)


def attention_backward(lens, cos_t, sin_t, query, kv_all, d_mixed, batch, group=8):
    heads, rows, head_dim = query.shape
    near = kv_all.shape[0] // 2
    shard = rows // batch
    total = 2 * near * shard
    q_spec = pl.BlockSpec((group, shard, head_dim), lambda s, g, *_: (g, s, 0))
    kv_spec = pl.BlockSpec((near, shard, 2 * head_dim), lambda s, g, *_: (0, s, 0))
    table = pl.BlockSpec((shard, head_dim // 2), lambda s, g, *_: (0, 0))
    kv_shape = jax.ShapeDtypeStruct((near, rows, 2 * head_dim), BF16)
    return pl.pallas_call(
        attn_bwd_kernel,
        out_shape=(jax.ShapeDtypeStruct((heads, rows, head_dim), BF16), kv_shape, kv_shape),
        grid_spec=pltpu.PrefetchScalarGridSpec(
            num_scalar_prefetch=1, grid=(batch, heads // group),
            in_specs=[table, table, q_spec, pl.BlockSpec((2 * near, shard, 2 * head_dim), lambda s, g, *_: (0, s, 0)), pl.BlockSpec((shard, group * head_dim), lambda s, g, *_: (s, g))],
            out_specs=(q_spec, kv_spec, kv_spec),
            scratch_shapes=[pltpu.VMEM((total, 2 * head_dim), F32)]),
        compiler_params=pltpu.CompilerParams(dimension_semantics=("arbitrary", "arbitrary"), vmem_limit_bytes=56 << 20),
        cost_estimate=pl.CostEstimate(flops=10 * heads * rows * total * head_dim, bytes_accessed=20 << 20, transcendentals=heads * rows * total),
        name="attn_bwd",
    )(lens, cos_t, sin_t, query, kv_all, d_mixed)


def gated_tile(z, g, w_g, w_u, w_d):
    gate = dot_nn(z, w_g)
    upper = dot_nn(z, w_u)
    d_act = dot_nt(g, w_d).astype(BF16).astype(F32)
    sq = gate * gate
    th = jnp.tanh(gate * (GELU_C + (GELU_C * GELU_K) * sq))
    half = 0.5 + 0.5 * th
    gelu = gate * half
    slope = half + gate * (0.5 - 0.5 * (th * th)) * (GELU_C + (3.0 * GELU_C * GELU_K) * sq)
    return (gelu * upper).astype(BF16), (d_act * upper * slope).astype(BF16), (d_act * gelu).astype(BF16)


def gated_kernel(z_own, g_own, wg_hbm, wu_hbm, wd_hbm, z_all, g_all, act, d_gate, d_up,
                 wg, wu, wd, z_buf, g_buf, outs, w_sem, in_sem, own_sem, out_sem, send, recv, send0, recv0, *, bn):
    rows, _ = z_own.shape
    width = wg_hbm.shape[1]
    steps = width // bn
    piece = rows // 4
    me, core, side, back = neighbours()
    corner = flip(side, 4)
    own = (z_own, g_own)
    full = (z_all, g_all)

    def part(slot, q):
        return pl.ds(pl.multiple_of(slot * rows + q * piece, 16), piece)

    def link_rows(u, path):
        turn = u // 2
        diag = turn % 2
        if path == 0:
            return side + (corner - side) * diag, (u % 2) + 2 * (turn // 2) + diag * 2
        return back + (corner - back) * diag, (u % 2) + 2 - 2 * (turn // 2) - diag * 2

    def link_copy(u, path, a):
        turn = u // 2
        peer = side if path == 0 else back
        sems = (send.at[path, u, a], recv.at[path, u, a])
        if turn == 1:
            slot = back if path == 0 else side
            q = (2 if path == 0 else 0) + u % 2
            return remote(full[a].at[part(slot, q)], full[a].at[part(slot, q)], *sems, peer)
        q = u % 2 + (2 * (turn // 2) if path == 0 else 2 - 2 * (turn // 2))
        return remote(own[a].at[pl.ds(q * piece, piece)], full[a].at[part(me, q)], *sems, peer)

    def core_copy(u, path, a):
        slot, q = link_rows(u, path)
        return remote(full[a].at[part(slot, q)], full[a].at[part(slot, q)], send.at[2 + path, u, a], recv.at[2 + path, u, a], core)

    def own_copy(a):
        return remote(own[a], full[a].at[pl.ds(pl.multiple_of(me * rows, 16), rows)], send0.at[a], recv0.at[a], core)

    def weight_copies(n):
        cols = pl.ds(pl.multiple_of(n * bn, 128), bn)
        return [pltpu.make_async_copy(wg_hbm.at[:, cols], wg.at[:, cols], w_sem.at[0, n]),
                pltpu.make_async_copy(wu_hbm.at[:, cols], wu.at[:, cols], w_sem.at[1, n]),
                pltpu.make_async_copy(wd_hbm.at[cols], wd.at[cols], w_sem.at[2, n])]

    bufs = (z_buf, g_buf)
    own_in = [pltpu.make_async_copy(own[a], bufs[a], own_sem.at[a]) for a in range(2)]
    own_out = [pltpu.make_async_copy(bufs[a], full[a].at[pl.ds(pl.multiple_of(me * rows, 16), rows)], own_sem.at[2 + a]) for a in range(2)]
    for cp in own_in:
        cp.start()
    for n in range(steps):
        for cp in weight_copies(n):
            cp.start()
    enter((core, side, back))
    for u in range(2):
        for path in range(2):
            for a in range(2):
                link_copy(u, path, a).start()
        if u == 0:
            for a in range(2):
                own_copy(a).start()

    def out_copies(slot, s_rows, n):
        cols = pl.ds(pl.multiple_of(n * bn, 128), bn)
        return [pltpu.make_async_copy(outs.at[slot, k, pl.ds(i * piece, piece)], ref.at[s_rows[i], cols], out_sem.at[slot, k, i])
                for k, ref in enumerate((act, d_gate, d_up)) for i in range(4)]

    def stage_rows(s):
        late = (s + 6) // 8
        u = (s - 2) * late
        first = me + (core - me) * s * (1 - late)
        (slot_x, q_x), (slot_y, q_y) = link_rows(u, 0), link_rows(u, 1)
        base_x, base_y = slot_x * rows + q_x * piece, slot_y * rows + q_y * piece
        pair_x, pair_y = flip(slot_x, 1) * rows + q_x * piece, flip(slot_y, 1) * rows + q_y * piece
        starts = [(1 - late) * (first * rows + i * piece) + late * base for i, base in enumerate((base_x, base_y, pair_x, pair_y))]
        return [pl.ds(pl.multiple_of(st, 16), piece) for st in starts]

    def compute(s):
        s_rows = stage_rows(s)

        def block(n, carry):
            step = s * steps + n
            slot = step % 2

            @pl.when(step >= 2)
            def _():
                for cp in out_copies(slot, s_rows, n):
                    cp.wait()

            @pl.when(s == 0)
            def _():
                for cp in weight_copies(n):
                    cp.wait()

            cols = pl.ds(pl.multiple_of(n * bn, 128), bn)
            res = gated_tile(z_buf[...], g_buf[...], wg[:, cols], wu[:, cols], wd[cols, :])
            for k in range(3):
                outs[slot, k] = res[k]
            for cp in out_copies(slot, s_rows, n):
                cp.start()
            return carry

        lax.fori_loop(0, steps, block, 0)

    def stage(s, carry):
        @pl.when(s == 0)
        def _():
            for cp in own_in:
                cp.wait()
            for cp in own_out:
                cp.start()

        @pl.when(s == 1)
        def _():
            for cp in own_out:
                cp.wait()
            for a in range(2):
                own_copy(a).wait_recv()

        for u in range(6):
            @pl.when(s == u + 2)
            def _(u=u):
                for path in range(2):
                    for a in range(2):
                        link_copy(u, path, a).wait_recv()
                        core_copy(u, path, a).start()
                if u < 2:
                    for path in range(2):
                        for a in range(2):
                            link_copy(u + 2, path, a).start()
                if u == 1:
                    for later in (4, 5):
                        for path in range(2):
                            for a in range(2):
                                link_copy(later, path, a).start()
                for path in range(2):
                    for a in range(2):
                        core_copy(u, path, a).wait_recv()

        @pl.when(s >= 1)
        def _():
            s_rows = stage_rows(s)
            copies = [pltpu.make_async_copy(full[a].at[s_rows[i]], bufs[a].at[pl.ds(i * piece, piece)], in_sem.at[a, i])
                      for a in range(2) for i in range(4)]
            for cp in copies:
                cp.start()
            for cp in copies:
                cp.wait()

        compute(s)
        return carry

    lax.fori_loop(0, 8, stage, 0)
    last = stage_rows(7)
    for slot in range(2):
        for cp in out_copies(slot, last, 0):
            cp.wait()
    for a in range(2):
        own_copy(a).wait_send()
        for path in range(2):
            for u in range(6):
                link_copy(u, path, a).wait_send()
                core_copy(u, path, a).wait_send()


def gated_layer(z_own, g_own, w_gate, w_up, w_down, tp, bn=512):
    rows, dim = z_own.shape
    width = w_gate.shape[1]
    total = rows * tp
    anyspace = pl.BlockSpec(memory_space=pl.ANY)
    gathered = jax.ShapeDtypeStruct((total, dim), BF16)
    made = jax.ShapeDtypeStruct((total, width), BF16)
    dma = pltpu.SemaphoreType.DMA
    return pl.pallas_call(
        functools.partial(gated_kernel, bn=bn),
        out_shape=(gathered, gathered, made, made, made),
        in_specs=[anyspace] * 5,
        out_specs=(anyspace,) * 5,
        scratch_shapes=[pltpu.VMEM((dim, width), BF16), pltpu.VMEM((dim, width), BF16), pltpu.VMEM((width, dim), BF16),
                        pltpu.VMEM((rows, dim), BF16), pltpu.VMEM((rows, dim), BF16), pltpu.VMEM((2, 3, rows, bn), BF16),
                        dma((3, width // bn)), dma((2, 4)), dma((4,)), dma((2, 3, 4)), dma((4, 6, 2)), dma((4, 6, 2)), dma((2,)), dma((2,))],
        compiler_params=pltpu.CompilerParams(vmem_limit_bytes=67043328, collective_id=0, has_side_effects=True),
        cost_estimate=pl.CostEstimate(flops=6 * total * dim * width, bytes_accessed=200 << 20, transcendentals=total * width),
        name="gated",
    )(z_own, g_own, w_gate, w_up, w_down)


def back_kernel(act, d_gate, d_up, z_all, wg_hbm, wu_hbm, wd_hbm, own_out, x_in, y_in, g_gate,
                wa, wb, lhs, st, from_core, from_diag, own_st, z_sem, w_sem, l_sem, o_sem, c_send, c_recv, d_send, d_recv, f_send, f_recv, *, rows, bn):
    dim, width = wg_hbm.shape
    steps = dim // bn
    half = rows // 2
    me, core, side, back = neighbours()

    def cols(j):
        return pl.ds(pl.multiple_of(j * bn, 128), bn)

    def pair_of(t):
        return ((t + 5) // 7) * ((t + 1) % 3 + 1)

    def lhs_copies(phase, t):
        pair = pair_of(t)
        theirs = 1 - t // 5 - ((t + 6) // 7 - (t + 5) // 7)
        dev = me + (1 - pair // 2) * (side - me) + (1 - pair % 2) * (back - me)
        dev = dev + theirs * (flip(dev, 1) - dev)
        src = pl.ds(pl.multiple_of(dev * rows, 16), rows)
        refs = (act,) if phase == 0 else (d_gate, d_up)
        return [pltpu.make_async_copy(ref.at[src], lhs.at[t % 2, k], l_sem.at[t % 2, k]) for k, ref in enumerate(refs)]

    def weight_copy(k, j):
        if k == 0:
            return pltpu.make_async_copy(wd_hbm.at[:, cols(j)], wa.at[pl.ds(0, width), cols(j)], w_sem.at[0, j])
        src, dst = (wg_hbm, wb) if k == 1 else (wu_hbm, wa)
        return pltpu.make_async_copy(src.at[cols(j)], dst.at[cols(j)], w_sem.at[k, j])

    def core_copy(pair, j):
        return remote(st.at[0, j], from_core.at[pair, j], c_send.at[j], c_recv.at[pair, j], core)

    def diag_copy(phase, k, j):
        return remote(st.at[1, j, pl.ds(k * half, half)], from_diag.at[phase, k, j], d_send.at[k, j], d_recv.at[phase, k, j], (side, back)[k])

    def final_copy(phase, k, j):
        return remote(st.at[2 + k, j], (x_in, y_in)[k].at[phase, :, cols(j)], f_send.at[k, j], f_recv.at[phase, k, j], (side, back)[k])

    def own_copy(phase, j):
        return pltpu.make_async_copy(own_st.at[j % 2], own_out.at[phase, :, cols(j)], o_sem.at[j % 2])

    def product(phase, slot, j):
        if phase == 0:
            return dot_nn(lhs[slot, 0], wa[:width, cols(j)])
        return dot_nt(lhs[slot, 0], wb[cols(j), :]) + dot_nt(lhs[slot, 1], wa[cols(j), :])

    for cp in lhs_copies(0, 0):
        cp.start()
    for j in range(steps):
        weight_copy(0, j).start()
    enter((core, side, back))

    def tiles(body):
        def step(j, carry):
            body(j)
            return carry

        lax.fori_loop(0, steps, step, 0)

    for phase in (0, 1):
        def step(t, carry, phase=phase):
            for cp in lhs_copies(phase, t):
                cp.wait()

            @pl.when(t < 7)
            def _():
                for cp in lhs_copies(phase, t + 1):
                    cp.start()

            if phase == 0:
                @pl.when(t == 1)
                def _():
                    for j in range(steps):
                        weight_copy(1, j).start()

                @pl.when(t == 7)
                def _():
                    for cp in lhs_copies(1, 0):
                        cp.start()

            @pl.when((t == 0) | ((t >= 2) & (t <= 4)))
            def _():
                pair = pair_of(t)

                def body(j):
                    @pl.when(t == 0)
                    def _():
                        for k in ((0,) if phase == 0 else (1, 2)):
                            weight_copy(k, j).wait()

                    if phase == 0:
                        @pl.when(t > 0)
                        def _():
                            core_copy(0, j).wait_send()
                    else:
                        core_copy(0, j).wait_send()
                    st[0, j] = product(phase, t % 2, j).astype(BF16)
                    core_copy(pair, j).start()

                tiles(body)

            @pl.when(t == 1)
            def _():
                def body(j):
                    core_copy(0, j).wait_recv()
                    if phase == 1:
                        for k in range(2):
                            diag_copy(0, k, j).wait_send()
                    st[1, j] = (product(phase, 1, j) + from_core[0, j].astype(F32)).astype(BF16)
                    for k in range(2):
                        diag_copy(phase, k, j).start()

                tiles(body)

            for k in range(2):
                @pl.when(t == 5 + k)
                def _(k=k):
                    def body(j):
                        core_copy(1 + k, j).wait_recv()
                        diag_copy(phase, 1 - k, j).wait_recv()
                        if phase == 1:
                            final_copy(0, k, j).wait_send()
                        total = product(phase, (5 + k) % 2, j) + from_core[1 + k, j].astype(F32)
                        came = from_diag[phase, 1 - k, j].astype(F32)
                        split = slice(half, rows) if k == 0 else slice(0, half)
                        rest = slice(0, half) if k == 0 else slice(half, rows)
                        st[2 + k, j, split, :] = (total[split] + came).astype(BF16)
                        st[2 + k, j, rest, :] = total[rest].astype(BF16)
                        final_copy(phase, k, j).start()

                    tiles(body)

            @pl.when(t == 7)
            def _():
                def body(j):
                    core_copy(3, j).wait_recv()

                    @pl.when(j >= 2)
                    def _():
                        own_copy(phase, j).wait()

                    own_st[j % 2] = product(phase, 1, j) + from_core[3, j].astype(F32)
                    own_copy(phase, j).start()

                tiles(body)
                for j in (0, 1):
                    own_copy(phase, j).wait()
                if phase == 0:
                    for j in range(steps):
                        weight_copy(2, j).start()

            return carry

        lax.fori_loop(0, 8, step, 0)

    def z_copy(j, c):
        return pltpu.make_async_copy(z_all.at[pl.ds(c * rows, rows), cols(j)], lhs.at[c // 2, c % 2, :, cols(j)], z_sem.at[j, c])

    def gate_copy(j):
        return pltpu.make_async_copy(d_gate.at[pl.ds(0, 4 * rows), cols(j)], wa.at[:, cols(j)], w_sem.at[0, j])

    def grad_copy(i, j):
        slot = j % 2
        return pltpu.make_async_copy(own_st.at[slot, pl.ds(0, bn)], g_gate.at[cols(i), cols(j)], o_sem.at[slot])

    for j in range(steps):
        for c in range(4):
            z_copy(j, c).start()
        gate_copy(j).start()

    def grad_tile(step, carry):
        i, j = step // steps, step % steps

        @pl.when(i == 0)
        def _():
            gate_copy(j).wait()

        @pl.when(j == 0)
        def _():
            for c in range(4):
                z_copy(i, c).wait()

        @pl.when(step >= 2)
        def _():
            grad_copy(i, j).wait()

        own_st[j % 2, :bn] = dot_tn(lhs[:, :, :, cols(i)].reshape(4 * rows, bn), wa[:, cols(j)])
        grad_copy(i, j).start()
        return carry

    lax.fori_loop(0, steps * steps, grad_tile, 0)
    for j in range(2):
        grad_copy(0, j).wait()
    for j in range(steps):
        core_copy(0, j).wait_send()
        for k in range(2):
            diag_copy(1, k, j).wait_send()
            final_copy(1, k, j).wait_send()
            for phase in (0, 1):
                final_copy(phase, k, j).wait_recv()


def back_layer(act, d_gate, d_up, z_all, w_gate, w_up, w_down, tp, bn=512):
    total, width = act.shape
    dim = w_gate.shape[0]
    rows = total // tp
    steps = dim // bn
    anyspace = pl.BlockSpec(memory_space=pl.ANY)
    dma = pltpu.SemaphoreType.DMA
    came = jax.ShapeDtypeStruct((2, rows, dim), BF16)
    return pl.pallas_call(
        functools.partial(back_kernel, rows=rows, bn=bn),
        out_shape=(jax.ShapeDtypeStruct((2, rows, dim), F32), came, came, jax.ShapeDtypeStruct((dim, width), F32)),
        in_specs=[anyspace] * 7,
        out_specs=(anyspace,) * 4,
        scratch_shapes=[pltpu.VMEM((4 * rows, dim), BF16), pltpu.VMEM((dim, width), BF16), pltpu.VMEM((2, 2, rows, width), BF16),
                        pltpu.VMEM((4, steps, rows, bn), BF16), pltpu.VMEM((4, steps, rows, bn), BF16),
                        pltpu.VMEM((2, 2, steps, rows // 2, bn), BF16), pltpu.VMEM((2, rows, bn), F32),
                        dma((steps, 4)), dma((3, steps)), dma((2, 2)), dma((2,)), dma((steps,)), dma((4, steps)),
                        dma((2, steps)), dma((2, 2, steps)), dma((2, steps)), dma((2, 2, steps))],
        compiler_params=pltpu.CompilerParams(vmem_limit_bytes=67043328, collective_id=1, has_side_effects=True),
        cost_estimate=pl.CostEstimate(flops=6 * total * dim * width, bytes_accessed=200 << 20, transcendentals=0),
        name="back",
    )(act, d_gate, d_up, z_all, w_gate, w_up, w_down)


def join_kernel(own_ref, x_ref, y_ref, resid_ref, grad_ref, gain_ref, out_ref, d_resid_ref, g_gain_ref):
    mlp_sum, d_gated = [own_ref[k] + x_ref[k].astype(F32) + y_ref[k].astype(F32) for k in range(2)]
    resid = resid_ref[...].astype(F32)
    out_ref[...] = (resid + mlp_sum).astype(BF16)
    d_gated = d_gated.astype(BF16).astype(F32)
    inv_rms = lax.rsqrt(jnp.mean(resid * resid, axis=-1, keepdims=True) + NORM_EPS)
    unit = resid * inv_rms
    scaled = d_gated * (1.0 + gain_ref[...].astype(F32))
    d_norm = inv_rms * (scaled - unit * jnp.mean(unit * scaled, axis=-1, keepdims=True))
    d_resid_ref[...] = (grad_ref[...].astype(F32) + d_norm).astype(BF16)

    @pl.when(pl.program_id(0) == 0)
    def _():
        g_gain_ref[...] = jnp.zeros_like(g_gain_ref)

    g_gain_ref[...] += jnp.sum(d_gated * unit, axis=0, keepdims=True)


def join_layer(own_part, x_part, y_part, resid, grad_out, gain, bm=96):
    rows, dim = resid.shape
    pair = pl.BlockSpec((2, bm, dim), lambda i: (0, i, 0))
    row = pl.BlockSpec((bm, dim), lambda i: (i, 0))
    one = pl.BlockSpec((1, dim), lambda i: (0, 0))
    return pl.pallas_call(
        join_kernel,
        out_shape=(jax.ShapeDtypeStruct((rows, dim), BF16), jax.ShapeDtypeStruct((rows, dim), BF16), jax.ShapeDtypeStruct((1, dim), F32)),
        grid=(rows // bm,),
        in_specs=[pair, pair, pair, row, row, one],
        out_specs=(row, row, one),
        compiler_params=pltpu.CompilerParams(dimension_semantics=("arbitrary",), vmem_limit_bytes=32 << 20),
        cost_estimate=pl.CostEstimate(flops=40 * rows * dim, bytes_accessed=28 << 20, transcendentals=rows),
        name="join",
    )(own_part, x_part, y_part, resid, grad_out, gain.reshape(1, dim))


def product_kernel(a_ref, b_ref, o_ref):
    o_ref[...] = dot_tn(a_ref[...], b_ref[...])


def weight_grad(a, b, bm=512, bn=1024):
    rows, m = a.shape
    n = b.shape[1]
    return pl.pallas_call(
        product_kernel,
        out_shape=jax.ShapeDtypeStruct((m, n), F32),
        grid=(m // bm, n // bn),
        in_specs=[pl.BlockSpec((rows, bm), lambda i, j: (0, i)), pl.BlockSpec((rows, bn), lambda i, j: (0, j))],
        out_specs=pl.BlockSpec((bm, bn), lambda i, j: (i, j)),
        compiler_params=pltpu.CompilerParams(dimension_semantics=("arbitrary", "arbitrary"), vmem_limit_bytes=56 << 20),
        cost_estimate=pl.CostEstimate(flops=2 * rows * m * n, bytes_accessed=110 << 20, transcendentals=0),
        name="weight_grad",
    )(a, b)


def rest_kernel(at_ref, a_ref, b_ref, part_ref, o_ref):
    o_ref[...] = part_ref[...] + dot_tn(a_ref[...], b_ref[...])


def weight_grad_rest(a, b, part, block, count, bm=512, bn=1024):
    m, n = part.shape
    out = pl.BlockSpec((bm, bn), lambda i, j, at: (i, j))
    return pl.pallas_call(
        rest_kernel,
        out_shape=jax.ShapeDtypeStruct((m, n), F32),
        grid_spec=pltpu.PrefetchScalarGridSpec(
            num_scalar_prefetch=1, grid=(m // bm, n // bn),
            in_specs=[pl.BlockSpec((count, bm), lambda i, j, at: (at[0], i)), pl.BlockSpec((count, bn), lambda i, j, at: (at[0], j)), out],
            out_specs=out),
        compiler_params=pltpu.CompilerParams(dimension_semantics=("arbitrary", "arbitrary"), vmem_limit_bytes=56 << 20),
        cost_estimate=pl.CostEstimate(flops=2 * count * m * n, bytes_accessed=80 << 20, transcendentals=0),
        name="weight_grad_rest",
    )(jnp.asarray(block, jnp.int32).reshape(1), a, b, part)


def hop_diagonal(diag):
    half = diag.shape[0] // 2
    return swap(diag[:half], 2), swap(diag[half:], 4)


def hop_near(side, back, came_side, came_back):
    half = side.shape[0] // 2
    kind = came_side.dtype
    side = jnp.concatenate([side[:half], side[half:] + came_back.astype(F32)], axis=0).astype(kind)
    back = jnp.concatenate([back[:half] + came_side.astype(F32), back[half:]], axis=0).astype(kind)
    return side, back


def solution(mesh):
    tp_size = mesh.shape["tp"]
    act_spec = P("dp", "tp", None)
    in_specs = (act_spec, act_spec, P("dp"), P("dp"), P(None), P(None, "tp"), P(None, None), P(None, None), P("tp", None), P(None), P(None, "tp"), P(None, "tp"), P("tp", None))
    out_specs = (act_spec, act_spec, P("dp"), P("dp", "tp"), P("dp", None), P("dp", None), P(("dp", "tp"), None), P("dp"), P("dp", "tp"), P("dp", "tp"), P(("dp", "tp"), None))

    def layer(hidden, grad_out, prefix_len, valid_len, attn_norm, w_query, w_key, w_value, w_out, mlp_norm, w_gate, w_up, w_down):
        batch, shard, dim = hidden.shape
        head_dim = w_key.shape[1]
        rows = batch * shard
        me = lax.axis_index("tp")
        starts = (me ^ jnp.array([0, 2, 4, 6, 1, 3, 5, 7], jnp.int32)) * shard
        k_pos = (starts[:, None] + jnp.arange(shard, dtype=jnp.int32)).reshape(1, tp_size * shard)
        lens = jnp.stack([prefix_len, valid_len])
        cos_own, sin_own = rope_tables(me * shard + jnp.arange(shard), head_dim)
        hidden = hidden.reshape(rows, dim)
        grad_out = grad_out.reshape(rows, dim)
        normed, wq_all, wo_all, kv_all, query, mixed, resid, gated_in = front_layer(
            lens, k_pos, cos_own, sin_own, attn_norm, mlp_norm, hidden, w_query, w_key, w_value, w_out, batch, tp_size)
        wo_all = wo_all.reshape(tp_size * head_dim, dim)

        def rope(raw_proj):
            return apply_rope(raw_proj, jnp.tile(cos_own, (batch, 1)), jnp.tile(sin_own, (batch, 1)))

        gated_all, grad_all, act, d_gate, d_upper = gated_layer(gated_in, grad_out, w_gate, w_up, w_down, tp_size)
        own_part, x_part, y_part, g_gate_part = back_layer(act, d_gate, d_upper, gated_all, w_gate, w_up, w_down, tp_size)
        hidden, own_part = lax.optimization_barrier((hidden, own_part))
        norm1_pull = jax.vjp(rms_norm, hidden, attn_norm.astype(F32))[1]
        key_pull = jax.linear_transpose(rope, jax.ShapeDtypeStruct((rows, head_dim), F32))
        hidden_out, d_resid, g_mlp_norm_part = join_layer(own_part, x_part, y_part, resid, grad_out, mlp_norm)
        g_out_part = dot_tn(mixed, d_resid)
        g_out_part, d_resid = lax.optimization_barrier((g_out_part, d_resid))
        g_out = lax.psum_scatter(g_out_part, "tp", scatter_dimension=0, tiled=True)
        d_mixed = dot_nt(d_resid, wo_all).astype(BF16)
        lens_back = jnp.concatenate([lens, jnp.full((1, batch), me, jnp.int32), jnp.broadcast_to(starts[:, None], (tp_size, batch))])
        d_q_raw, dkv_near, dkv_far = attention_backward(lens_back, cos_own, sin_own, query, kv_all, d_mixed, batch)
        near = tp_size // 2
        came_kv = swap(dkv_far, 1)
        g_far = jnp.einsum("kte,td->ked", d_q_raw[near:], normed, preferred_element_type=F32)
        came_kv, g_far = lax.optimization_barrier((came_kv, g_far))
        came_q = swap(g_far, 1)
        kv_own, kv_side, kv_back, kv_diag = [dkv_near[k].astype(F32) + came_kv[k].astype(F32) for k in range(4)]
        kv_came = hop_diagonal(kv_diag.astype(BF16))
        d_normed_q = jnp.einsum("hte,hde->td", d_q_raw, wq_all, preferred_element_type=F32)
        kv_came, d_normed_q = lax.optimization_barrier((kv_came, d_normed_q))
        kv_next = hop_near(kv_side, kv_back, *kv_came)
        kv_last = (swap(kv_next[0], 2), swap(kv_next[1], 4))
        came_q, dq_near = lax.optimization_barrier((came_q, d_q_raw[:near]))
        g_query_sum = jnp.einsum("kte,td->ked", dq_near, normed, preferred_element_type=F32) + came_q
        g_query_sum, act = lax.optimization_barrier((g_query_sum, act))
        q_came = hop_diagonal(g_query_sum[3])
        g_down = weight_grad(act, grad_all)
        kv_last, q_came, g_down = lax.optimization_barrier((kv_last, q_came, g_down))
        d_kv = (kv_own + kv_last[0].astype(F32) + kv_last[1].astype(F32)).astype(BF16)
        d_k_raw = key_pull(d_kv[:, :head_dim].astype(F32))[0].astype(BF16)
        d_values = d_kv[:, head_dim:]
        q_next = hop_near(g_query_sum[1], g_query_sum[2], *q_came)
        g_key_part, g_value_part = dot_tn(normed, d_k_raw), dot_tn(normed, d_values)
        q_next, g_key_part, g_value_part, d_gate = lax.optimization_barrier((q_next, g_key_part, g_value_part, d_gate))
        last_side = swap(q_next[0], 2)
        q_last = (last_side, swap(q_next[1], 4))
        g_key, g_value = lax.psum((g_key_part, g_value_part), "tp")
        g_gate = weight_grad_rest(gated_all, d_gate, g_gate_part, 1, 4 * rows)
        d_normed = (d_normed_q + dot_nt(d_k_raw, w_key) + dot_nt(d_values, w_value)).astype(BF16)
        d_normed, g_gate = lax.optimization_barrier((d_normed, g_gate))
        d_hidden_norm, g_attn_norm_part = norm1_pull(d_normed)
        norms = jnp.concatenate([g_attn_norm_part.reshape(1, dim), g_mlp_norm_part])
        norms, d_upper = lax.optimization_barrier((norms, d_upper))
        norms_near = [swap(norms, bit) for bit in (2, 4, 6)]
        g_up = weight_grad(gated_all, d_upper)
        norms_near, q_last, g_up, d_hidden_norm = lax.optimization_barrier((norms_near, q_last, g_up, d_hidden_norm))
        norms = norms + norms_near[0] + norms_near[1] + norms_near[2]
        g_norms = norms + swap(norms, 1)
        g_query = (g_query_sum[0] + q_last[0] + q_last[1]).T
        grad_hidden = (d_resid.astype(F32) + d_hidden_norm.astype(F32)).astype(BF16)
        full = (batch, shard, dim)
        return (hidden_out.reshape(full), grad_hidden.reshape(full), g_norms[0], g_query, g_key, g_value, g_out, g_norms[1], g_gate, g_up, g_down)

    return jax.shard_map(layer, mesh=mesh, in_specs=in_specs, out_specs=out_specs, check_vma=False)
```

```python
import functools
import math
import jax
import jax.numpy as jnp
from jax import lax
from jax.experimental import pallas as pl
from jax.experimental.pallas import tpu as pltpu
from jax.sharding import PartitionSpec as P

NORM_EPS = 1e-6
BF16 = jnp.bfloat16
F32 = jnp.float32
GELU_C = math.sqrt(2.0 / math.pi)
GELU_K = 0.044715
MASKED = -1e30
NT = (((1,), (1,)), ((), ()))
TN = (((0,), (0,)), ((), ()))


def rope_tables(positions, head_dim):
    half_dim = head_dim // 2
    exponent = jnp.arange(half_dim, dtype=F32) * (2.0 / head_dim)
    inv_freq = jnp.exp(exponent * (-math.log(10000.0)))
    angles = positions.astype(F32)[:, None] * inv_freq[None, :]
    return jnp.cos(angles), jnp.sin(angles)


def dot_nn(a, b):
    return jnp.dot(a, b, preferred_element_type=F32)


def dot_nt(a, b):
    return lax.dot_general(a, b, NT, preferred_element_type=F32)


def dot_tn(a, b):
    return lax.dot_general(a, b, TN, preferred_element_type=F32)


def swap(x, bit):
    return lax.ppermute(x, "tp", [(t, t ^ bit) for t in range(8)])


def flip(index, bit):
    return index + bit - 2 * bit * ((index // bit) % 2)


def neighbours():
    me = lax.axis_index("tp")
    return me, flip(me, 1), flip(me, 2), flip(me, 4)


def enter(peers):
    barrier = pltpu.get_barrier_semaphore()
    for peer in peers:
        pl.semaphore_signal(barrier, inc=1, device_id={"tp": peer}, device_id_type=pl.DeviceIdType.MESH)
    pl.semaphore_wait(barrier, len(peers))


def attn_bwd_kernel(lens_ref, cos_ref, sin_ref, q_ref, kv_ref, do_ref, dq_ref, dkv0_ref, dkv1_ref, dkv_acc):
    heads, shard, head_dim = q_ref.shape
    tp = kv_ref.shape[0]
    total = tp * shard
    rows = heads * shard
    s_id = pl.program_id(0)
    g_id = pl.program_id(1)
    prefix = lens_ref[0, s_id]
    valid = lens_ref[1, s_id]
    first = lens_ref[2, 0] * shard
    keys = kv_ref[:, :, :head_dim].reshape(total, head_dim)
    values = kv_ref[:, :, head_dim:].reshape(total, head_dim)
    query = q_ref[...].reshape(rows, head_dim) * BF16(head_dim ** -0.5)
    d_out = jnp.concatenate([do_ref[:, h * head_dim:(h + 1) * head_dim] for h in range(heads)], axis=0)
    step = lax.broadcasted_iota(jnp.int32, (shard, 1), 0)
    k_pos = jnp.concatenate([step + lens_ref[3 + r, 0] for r in range(tp)], axis=0)
    q_pos = first + lax.rem(lax.broadcasted_iota(jnp.int32, (1, rows), 1), shard)
    limit = jnp.minimum(valid, jnp.maximum(prefix, q_pos + 1))
    cos_t, sin_t = cos_ref[...][None], sin_ref[...][None]
    d_k = d_v = None
    count = heads // 2
    width = count * shard
    for c in range(2):
        cols = slice(c * width, (c + 1) * width)
        q_c, do_c = query[cols], d_out[cols]
        s = jnp.where(k_pos < limit[:, cols], dot_nt(keys, q_c), MASKED)
        e = jnp.exp(s - jnp.max(s, axis=0, keepdims=True))
        p = e * (1.0 / jnp.sum(e, axis=0, keepdims=True))
        d_p = dot_nt(values, do_c)
        delta = jnp.sum(p * d_p, axis=0, keepdims=True)
        d_s = (p * (d_p - delta)).astype(BF16)
        d_v_c = dot_nn(p.astype(BF16), do_c)
        d_k_c = dot_nn(d_s, q_c)
        d_k, d_v = (d_k_c, d_v_c) if d_k is None else (d_k + d_k_c, d_v + d_v_c)
        d_q = (dot_tn(d_s, keys) * (head_dim ** -0.5)).reshape(count, shard, head_dim)
        first, second = d_q[:, :, :head_dim // 2], d_q[:, :, head_dim // 2:]
        some = slice(c * count, (c + 1) * count)
        dq_ref[some, :, :head_dim // 2] = (first * cos_t + second * sin_t).astype(BF16)
        dq_ref[some, :, head_dim // 2:] = (second * cos_t - first * sin_t).astype(BF16)
    d_kv = jnp.concatenate([d_k, d_v], axis=1)

    @pl.when(g_id == 0)
    def _():
        dkv_acc[...] = d_kv

    @pl.when(g_id > 0)
    def _():
        dkv_acc[...] += d_kv

    @pl.when(g_id == pl.num_programs(1) - 1)
    def _():
        near = (tp // 2, shard, 2 * head_dim)
        dkv0_ref[...] = dkv_acc[:total // 2].astype(BF16).reshape(near)
        dkv1_ref[...] = dkv_acc[total // 2:].astype(BF16).reshape(near)


def remote(src, dst, send, recv, peer):
    return pltpu.make_async_remote_copy(src_ref=src, dst_ref=dst, send_sem=send, recv_sem=recv,
                                        device_id={"tp": peer}, device_id_type=pl.DeviceIdType.MESH)


def front_kernel(prefix_ref, valid_ref, kpos_ref, cos_ref, sin_ref, gain1_ref, gain2_ref, hidden, w_query, w_key, w_value, w_out,
                 normed_out, wq_all, wo_all, kv_all, query_out, mixed_out, resid_out, gated_out,
                 x_buf, n_buf, wkv, wq, wo, kv, q, probs, mix, acc, load, store, send, recv, *, batch):
    rows, dim = x_buf.shape
    shard = rows // batch
    head_dim = w_key.shape[1]
    tp = wq.shape[0]
    near = tp // 2
    total = tp * shard
    half_dim = head_dim // 2
    me, core, side, back = neighbours()
    bufs = (wq, kv, wo)

    def to_side(a):
        return remote(bufs[a].at[0], bufs[a].at[1], send.at[a, 0], recv.at[a, 0], side)

    def to_back(a):
        return remote(bufs[a].at[0], bufs[a].at[2], send.at[a, 1], recv.at[a, 1], back)

    def onward(a, k):
        half = bufs[a].shape[1] // 2
        part = pl.ds(k * half, half)
        return remote(bufs[a].at[1 + k, part], bufs[a].at[3, part], send.at[a, 2 + k], recv.at[a, 2 + k], (back, side)[k])

    def to_core(a, k):
        return remote(bufs[a].at[k], bufs[a].at[near + k], send.at[a, 4 + k], recv.at[a, 4 + k], core)

    loads = [pltpu.make_async_copy(src, dst, load.at[i]) for i, (src, dst) in enumerate((
        (w_query, wq.at[0]), (hidden, x_buf), (w_key, wkv.at[:, :head_dim]), (w_value, wkv.at[:, head_dim:]), (w_out, wo.at[0])))]
    mixed_at = [me, side, back, flip(side, 4)]
    mixed_at = mixed_at + [flip(dev, 1) for dev in mixed_at]
    stores = {name: pltpu.make_async_copy(src, dst, store.at[i]) for i, (name, src, dst) in enumerate((
        ("normed", n_buf, normed_out), ("wq", wq, wq_all), ("wo", wo, wo_all), ("kv", kv, kv_all), ("query", q, query_out),
        ("resid", x_buf, resid_out), ("gated", n_buf, gated_out)))}
    mixed_stores = [pltpu.make_async_copy(mix.at[:, pl.ds(k * head_dim, head_dim)],
                                          mixed_out.at[:, pl.ds(pl.multiple_of(dev * head_dim, 128), head_dim)], store.at[7 + k])
                    for k, dev in enumerate(mixed_at)]

    for cp in loads:
        cp.start()
    enter((core, side, back))
    loads[0].wait()
    to_side(0).start()
    to_back(0).start()
    to_core(0, 0).start()

    def norm_rows(src, gain_ref):
        x_f = src.astype(F32)
        inv_rms = lax.rsqrt(jnp.mean(x_f * x_f, axis=-1, keepdims=True) + NORM_EPS)
        return (x_f * inv_rms * (1.0 + gain_ref[...].astype(F32))).astype(BF16)

    def seq_rows(i):
        return pl.ds(pl.multiple_of(i * shard, 16), shard)

    def rotate(x_f):
        first, second = x_f[:, :half_dim], x_f[:, half_dim:]
        cos_t, sin_t = cos_ref[...], sin_ref[...]
        return first * cos_t - second * sin_t, second * cos_t + first * sin_t

    def norm1(i, carry):
        n_buf[seq_rows(i), :] = norm_rows(x_buf[seq_rows(i), :], gain1_ref)
        return carry

    loads[1].wait()
    lax.fori_loop(0, batch, norm1, 0)
    stores["normed"].start()
    loads[2].wait()
    loads[3].wait()

    def own_kv(i, carry):
        raw = dot_nn(n_buf[seq_rows(i), :], wkv[...])
        first, second = rotate(raw[:, :head_dim])
        kv[0, seq_rows(i), :half_dim] = first.astype(BF16)
        kv[0, seq_rows(i), half_dim:head_dim] = second.astype(BF16)
        kv[0, seq_rows(i), head_dim:] = raw[:, head_dim:].astype(BF16)
        return carry

    lax.fori_loop(0, batch, own_kv, 0)
    to_side(1).start()
    to_back(1).start()
    to_core(1, 0).start()

    def own_query(k):
        def step(i, carry):
            for h in (k, near + k):
                first, second = rotate(dot_nn(n_buf[seq_rows(i), :], wq[h]))
                q[h, seq_rows(i), :half_dim] = first.astype(BF16)
                q[h, seq_rows(i), half_dim:] = second.astype(BF16)
            return carry

        to_core(0, k).wait_recv()
        lax.fori_loop(0, batch, step, 0)

    def pass_on(a):
        to_side(a).wait_recv()
        onward(a, 0).start()
        to_core(a, 1).start()
        to_back(a).wait_recv()
        onward(a, 1).start()
        to_core(a, 2).start()

    def pass_last(a):
        onward(a, 0).wait_recv()
        onward(a, 1).wait_recv()
        to_core(a, 3).start()

    own_query(0)
    pass_on(0)
    own_query(1)
    own_query(2)
    pass_on(1)
    loads[4].wait()
    to_side(2).start()
    to_back(2).start()
    to_core(2, 0).start()
    pass_last(0)
    own_query(3)
    stores["query"].start()
    stores["wq"].start()
    pass_last(1)
    for k in range(near):
        to_core(1, k).wait_recv()
    stores["kv"].start()

    q_pos = me * shard + lax.broadcasted_iota(jnp.int32, (shard, 1), 0)

    def attend(i, carry):
        keys = kv[:, seq_rows(i), :head_dim].reshape(total, head_dim)
        values = kv[:, seq_rows(i), head_dim:].reshape(total, head_dim)
        visible = kpos_ref[...] < jnp.minimum(valid_ref[i], jnp.maximum(prefix_ref[i], q_pos + 1))
        for g in range(2):
            query = q[g * near:(g + 1) * near, seq_rows(i), :].reshape(near * shard, head_dim) * BF16(head_dim ** -0.5)
            scores = dot_nt(query, keys)
            for h in range(near):
                part = slice(h * shard, (h + 1) * shard)
                s = jnp.where(visible, scores[part], MASKED)
                e = jnp.exp(s - jnp.max(s, axis=-1, keepdims=True))
                probs[g, part, :] = (e * (1.0 / jnp.sum(e, axis=-1, keepdims=True))).astype(BF16)
            mixed = dot_nn(probs[g], values).astype(BF16)
            for h in range(near):
                head = g * near + h
                mix[seq_rows(i), head * head_dim:(head + 1) * head_dim] = mixed[h * shard:(h + 1) * shard]
        return carry

    lax.fori_loop(0, batch, attend, 0)
    for cp in mixed_stores:
        cp.start()
    pass_on(2)

    def project(k, first):
        def step(n, carry):
            cols = pl.ds(pl.multiple_of(n * 512, 128), 512)
            part = (dot_nn(mix[:, k * head_dim:(k + 1) * head_dim], wo[k, :, cols])
                    + dot_nn(mix[:, (near + k) * head_dim:(near + k + 1) * head_dim], wo[near + k, :, cols]))
            acc[:, cols] = part if first else acc[:, cols] + part
            return carry

        to_core(2, k).wait_recv()
        lax.fori_loop(0, dim // 512, step, 0)

    project(0, True)
    project(1, False)
    project(2, False)
    pass_last(2)
    project(3, False)
    stores["wo"].start()
    stores["normed"].wait()

    def norm2(i, carry):
        resid = (x_buf[seq_rows(i), :].astype(F32) + acc[seq_rows(i), :]).astype(BF16)
        x_buf[seq_rows(i), :] = resid
        n_buf[seq_rows(i), :] = norm_rows(resid, gain2_ref)
        return carry

    lax.fori_loop(0, batch, norm2, 0)
    stores["resid"].start()
    stores["gated"].start()
    for cp in mixed_stores:
        cp.wait()
    for name in ("wq", "wo", "kv", "query", "resid", "gated"):
        stores[name].wait()
    for a in range(3):
        to_side(a).wait_send()
        to_back(a).wait_send()
        for k in range(2):
            onward(a, k).wait_send()
        for k in range(near):
            to_core(a, k).wait_send()


def front_layer(prefix_len, valid_len, k_pos, cos_t, sin_t, attn_norm, mlp_norm, hidden, w_query, w_key, w_value, w_out, batch, tp):
    rows, dim = hidden.shape
    head_dim = w_key.shape[1]
    shard = rows // batch
    total = tp * shard
    anyspace = pl.BlockSpec(memory_space=pl.ANY)
    vmem = pl.BlockSpec(memory_space=pltpu.VMEM)
    dma = pltpu.SemaphoreType.DMA

    def shape(*dims):
        return jax.ShapeDtypeStruct(dims, BF16)

    return pl.pallas_call(
        functools.partial(front_kernel, batch=batch),
        out_shape=(shape(rows, dim), shape(tp, dim, head_dim), shape(tp, head_dim, dim), shape(tp, rows, 2 * head_dim),
                   shape(tp, rows, head_dim), shape(rows, tp * head_dim), shape(rows, dim), shape(rows, dim)),
        in_specs=[pl.BlockSpec(memory_space=pltpu.SMEM)] * 2 + [vmem] * 5 + [anyspace] * 5,
        out_specs=(anyspace,) * 8,
        scratch_shapes=[pltpu.VMEM((rows, dim), BF16), pltpu.VMEM((rows, dim), BF16), pltpu.VMEM((dim, 2 * head_dim), BF16),
                        pltpu.VMEM((tp, dim, head_dim), BF16), pltpu.VMEM((tp, head_dim, dim), BF16),
                        pltpu.VMEM((tp, rows, 2 * head_dim), BF16), pltpu.VMEM((tp, rows, head_dim), BF16),
                        pltpu.VMEM((2, tp // 2 * shard, total), BF16), pltpu.VMEM((rows, tp * head_dim), BF16), pltpu.VMEM((rows, dim), F32),
                        dma((5,)), dma((15,)), dma((3, 8)), dma((3, 8))],
        compiler_params=pltpu.CompilerParams(vmem_limit_bytes=62 << 20, collective_id=2, has_side_effects=True),
        cost_estimate=pl.CostEstimate(flops=8 * rows * dim * tp * head_dim, bytes_accessed=60 << 20, transcendentals=tp * rows * total),
        name="front",
    )(prefix_len, valid_len, k_pos, cos_t, sin_t, attn_norm.reshape(1, dim), mlp_norm.reshape(1, dim), hidden, w_query, w_key, w_value, w_out)


def attention_backward(lens, cos_t, sin_t, query, kv_all, d_mixed, batch, group=8):
    heads, rows, head_dim = query.shape
    near = kv_all.shape[0] // 2
    shard = rows // batch
    total = 2 * near * shard
    q_spec = pl.BlockSpec((group, shard, head_dim), lambda s, g, *_: (g, s, 0))
    kv_spec = pl.BlockSpec((near, shard, 2 * head_dim), lambda s, g, *_: (0, s, 0))
    table = pl.BlockSpec((shard, head_dim // 2), lambda s, g, *_: (0, 0))
    kv_shape = jax.ShapeDtypeStruct((near, rows, 2 * head_dim), BF16)
    return pl.pallas_call(
        attn_bwd_kernel,
        out_shape=(jax.ShapeDtypeStruct((heads, rows, head_dim), BF16), kv_shape, kv_shape),
        grid_spec=pltpu.PrefetchScalarGridSpec(
            num_scalar_prefetch=1, grid=(batch, heads // group),
            in_specs=[table, table, q_spec, pl.BlockSpec((2 * near, shard, 2 * head_dim), lambda s, g, *_: (0, s, 0)), pl.BlockSpec((shard, group * head_dim), lambda s, g, *_: (s, g))],
            out_specs=(q_spec, kv_spec, kv_spec),
            scratch_shapes=[pltpu.VMEM((total, 2 * head_dim), F32)]),
        compiler_params=pltpu.CompilerParams(dimension_semantics=("arbitrary", "arbitrary"), vmem_limit_bytes=62 << 20),
        cost_estimate=pl.CostEstimate(flops=10 * heads * rows * total * head_dim, bytes_accessed=20 << 20, transcendentals=heads * rows * total),
        name="attn_bwd",
    )(lens, cos_t, sin_t, query, kv_all, d_mixed)


def gated_tile(z, g, w_g, w_u, w_d):
    gate = dot_nn(z, w_g)
    upper = dot_nn(z, w_u)
    d_act = dot_nt(g, w_d).astype(BF16).astype(F32)
    sq = gate * gate
    th = jnp.tanh(gate * (GELU_C + (GELU_C * GELU_K) * sq))
    half = 0.5 + 0.5 * th
    gelu = gate * half
    slope = half + gate * (0.5 - 0.5 * (th * th)) * (GELU_C + (3.0 * GELU_C * GELU_K) * sq)
    return (gelu * upper).astype(BF16), (d_act * upper * slope).astype(BF16), (d_act * gelu).astype(BF16)


def gated_kernel(z_own, g_own, wg_hbm, wu_hbm, wd_hbm, z_all, g_all, act, d_gate, d_up,
                 wg, wu, wd, z_buf, g_buf, outs, w_sem, in_sem, own_sem, out_sem, send, recv, send0, recv0, *, bn):
    rows, _ = z_own.shape
    width = wg_hbm.shape[1]
    steps = width // bn
    piece = rows // 4
    me, core, side, back = neighbours()
    corner = flip(side, 4)
    own = (z_own, g_own)
    full = (z_all, g_all)

    def part(slot, q):
        return pl.ds(pl.multiple_of(slot * rows + q * piece, 16), piece)

    def link_rows(u, path):
        turn = u // 2
        diag = turn % 2
        if path == 0:
            return side + (corner - side) * diag, (u % 2) + 2 * (turn // 2) + diag * 2
        return back + (corner - back) * diag, (u % 2) + 2 - 2 * (turn // 2) - diag * 2

    def link_copy(u, path, a):
        turn = u // 2
        peer = side if path == 0 else back
        sems = (send.at[path, u, a], recv.at[path, u, a])
        if turn == 1:
            slot = back if path == 0 else side
            q = (2 if path == 0 else 0) + u % 2
            return remote(full[a].at[part(slot, q)], full[a].at[part(slot, q)], *sems, peer)
        q = u % 2 + (2 * (turn // 2) if path == 0 else 2 - 2 * (turn // 2))
        return remote(own[a].at[pl.ds(q * piece, piece)], full[a].at[part(me, q)], *sems, peer)

    def core_copy(u, path, a):
        slot, q = link_rows(u, path)
        return remote(full[a].at[part(slot, q)], full[a].at[part(slot, q)], send.at[2 + path, u, a], recv.at[2 + path, u, a], core)

    def own_copy(a):
        return remote(own[a], full[a].at[pl.ds(pl.multiple_of(me * rows, 16), rows)], send0.at[a], recv0.at[a], core)

    def weight_copies(n):
        cols = pl.ds(pl.multiple_of(n * bn, 128), bn)
        return [pltpu.make_async_copy(wg_hbm.at[:, cols], wg.at[:, cols], w_sem.at[0, n]),
                pltpu.make_async_copy(wu_hbm.at[:, cols], wu.at[:, cols], w_sem.at[1, n]),
                pltpu.make_async_copy(wd_hbm.at[cols], wd.at[cols], w_sem.at[2, n])]

    bufs = (z_buf, g_buf)
    own_in = [pltpu.make_async_copy(own[a], bufs[a], own_sem.at[a]) for a in range(2)]
    own_out = [pltpu.make_async_copy(bufs[a], full[a].at[pl.ds(pl.multiple_of(me * rows, 16), rows)], own_sem.at[2 + a]) for a in range(2)]
    for cp in own_in:
        cp.start()
    for n in range(steps):
        for cp in weight_copies(n):
            cp.start()
    enter((core, side, back))
    for u in range(2):
        for path in range(2):
            for a in range(2):
                link_copy(u, path, a).start()
        if u == 0:
            for a in range(2):
                own_copy(a).start()

    def out_copies(slot, s_rows, n):
        cols = pl.ds(pl.multiple_of(n * bn, 128), bn)
        return [pltpu.make_async_copy(outs.at[slot, k, pl.ds(i * piece, piece)], ref.at[s_rows[i], cols], out_sem.at[slot, k, i])
                for k, ref in enumerate((act, d_gate, d_up)) for i in range(4)]

    def stage_rows(s):
        late = (s + 6) // 8
        u = (s - 2) * late
        first = me + (core - me) * s * (1 - late)
        (slot_x, q_x), (slot_y, q_y) = link_rows(u, 0), link_rows(u, 1)
        base_x, base_y = slot_x * rows + q_x * piece, slot_y * rows + q_y * piece
        pair_x, pair_y = flip(slot_x, 1) * rows + q_x * piece, flip(slot_y, 1) * rows + q_y * piece
        starts = [(1 - late) * (first * rows + i * piece) + late * base for i, base in enumerate((base_x, base_y, pair_x, pair_y))]
        return [pl.ds(pl.multiple_of(st, 16), piece) for st in starts]

    def compute(s):
        s_rows = stage_rows(s)

        def block(n, carry):
            step = s * steps + n
            slot = step % 2

            @pl.when(step >= 2)
            def _():
                for cp in out_copies(slot, s_rows, n):
                    cp.wait()

            @pl.when(s == 0)
            def _():
                for cp in weight_copies(n):
                    cp.wait()

            cols = pl.ds(pl.multiple_of(n * bn, 128), bn)
            res = gated_tile(z_buf[...], g_buf[...], wg[:, cols], wu[:, cols], wd[cols, :])
            for k in range(3):
                outs[slot, k] = res[k]
            for cp in out_copies(slot, s_rows, n):
                cp.start()
            return carry

        lax.fori_loop(0, steps, block, 0)

    def stage(s, carry):
        @pl.when(s == 0)
        def _():
            for cp in own_in:
                cp.wait()
            for cp in own_out:
                cp.start()

        @pl.when(s == 1)
        def _():
            for cp in own_out:
                cp.wait()
            for a in range(2):
                own_copy(a).wait_recv()

        for u in range(6):
            @pl.when(s == u + 2)
            def _(u=u):
                for path in range(2):
                    for a in range(2):
                        link_copy(u, path, a).wait_recv()
                        core_copy(u, path, a).start()
                if u < 2:
                    for path in range(2):
                        for a in range(2):
                            link_copy(u + 2, path, a).start()
                if u == 1:
                    for later in (4, 5):
                        for path in range(2):
                            for a in range(2):
                                link_copy(later, path, a).start()
                for path in range(2):
                    for a in range(2):
                        core_copy(u, path, a).wait_recv()

        @pl.when(s >= 1)
        def _():
            s_rows = stage_rows(s)
            copies = [pltpu.make_async_copy(full[a].at[s_rows[i]], bufs[a].at[pl.ds(i * piece, piece)], in_sem.at[a, i])
                      for a in range(2) for i in range(4)]
            for cp in copies:
                cp.start()
            for cp in copies:
                cp.wait()

        compute(s)
        return carry

    lax.fori_loop(0, 8, stage, 0)
    last = stage_rows(7)
    for slot in range(2):
        for cp in out_copies(slot, last, 0):
            cp.wait()
    for a in range(2):
        own_copy(a).wait_send()
        for path in range(2):
            for u in range(6):
                link_copy(u, path, a).wait_send()
                core_copy(u, path, a).wait_send()


def gated_layer(z_own, g_own, w_gate, w_up, w_down, tp, bn=512):
    rows, dim = z_own.shape
    width = w_gate.shape[1]
    total = rows * tp
    anyspace = pl.BlockSpec(memory_space=pl.ANY)
    gathered = jax.ShapeDtypeStruct((total, dim), BF16)
    made = jax.ShapeDtypeStruct((total, width), BF16)
    dma = pltpu.SemaphoreType.DMA
    return pl.pallas_call(
        functools.partial(gated_kernel, bn=bn),
        out_shape=(gathered, gathered, made, made, made),
        in_specs=[anyspace] * 5,
        out_specs=(anyspace,) * 5,
        scratch_shapes=[pltpu.VMEM((dim, width), BF16), pltpu.VMEM((dim, width), BF16), pltpu.VMEM((width, dim), BF16),
                        pltpu.VMEM((rows, dim), BF16), pltpu.VMEM((rows, dim), BF16), pltpu.VMEM((2, 3, rows, bn), BF16),
                        dma((3, width // bn)), dma((2, 4)), dma((4,)), dma((2, 3, 4)), dma((4, 6, 2)), dma((4, 6, 2)), dma((2,)), dma((2,))],
        compiler_params=pltpu.CompilerParams(vmem_limit_bytes=67043328, collective_id=0, has_side_effects=True),
        cost_estimate=pl.CostEstimate(flops=6 * total * dim * width, bytes_accessed=200 << 20, transcendentals=total * width),
        name="gated",
    )(z_own, g_own, w_gate, w_up, w_down)


def back_kernel(act, d_gate, d_up, z_all, wg_hbm, wu_hbm, wd_hbm, own_out, x_in, y_in, g_gate,
                wa, wb, lhs, st, from_core, from_diag, own_st, z_sem, w_sem, l_sem, o_sem, c_send, c_recv, d_send, d_recv, f_send, f_recv, *, rows, bn):
    dim, width = wg_hbm.shape
    steps = dim // bn
    half = rows // 2
    me, core, side, back = neighbours()

    def cols(j):
        return pl.ds(pl.multiple_of(j * bn, 128), bn)

    def pair_of(t):
        return ((t + 5) // 7) * ((t + 1) % 3 + 1)

    def lhs_copies(phase, t):
        pair = pair_of(t)
        theirs = 1 - t // 5 - ((t + 6) // 7 - (t + 5) // 7)
        dev = me + (1 - pair // 2) * (side - me) + (1 - pair % 2) * (back - me)
        dev = dev + theirs * (flip(dev, 1) - dev)
        src = pl.ds(pl.multiple_of(dev * rows, 16), rows)
        refs = (act,) if phase == 0 else (d_gate, d_up)
        return [pltpu.make_async_copy(ref.at[src], lhs.at[t % 2, k], l_sem.at[t % 2, k]) for k, ref in enumerate(refs)]

    def weight_copy(k, j):
        if k == 0:
            return pltpu.make_async_copy(wd_hbm.at[:, cols(j)], wa.at[pl.ds(0, width), cols(j)], w_sem.at[0, j])
        src, dst = (wg_hbm, wb) if k == 1 else (wu_hbm, wa)
        return pltpu.make_async_copy(src.at[cols(j)], dst.at[cols(j)], w_sem.at[k, j])

    def core_copy(pair, j):
        return remote(st.at[0, j], from_core.at[pair, j], c_send.at[j], c_recv.at[pair, j], core)

    def diag_copy(phase, k, j):
        return remote(st.at[1, j, pl.ds(k * half, half)], from_diag.at[phase, k, j], d_send.at[k, j], d_recv.at[phase, k, j], (side, back)[k])

    def final_copy(phase, k, j):
        return remote(st.at[2 + k, j], (x_in, y_in)[k].at[phase, :, cols(j)], f_send.at[k, j], f_recv.at[phase, k, j], (side, back)[k])

    def own_copy(phase, j):
        return pltpu.make_async_copy(own_st.at[j % 2], own_out.at[phase, :, cols(j)], o_sem.at[j % 2])

    def product(phase, slot, j):
        if phase == 0:
            return dot_nn(lhs[slot, 0], wa[:width, cols(j)])
        return dot_nt(lhs[slot, 0], wb[cols(j), :]) + dot_nt(lhs[slot, 1], wa[cols(j), :])

    for cp in lhs_copies(0, 0):
        cp.start()
    for j in range(steps):
        weight_copy(0, j).start()
    enter((core, side, back))

    def tiles(body):
        def step(j, carry):
            body(j)
            return carry

        lax.fori_loop(0, steps, step, 0)

    for phase in (0, 1):
        def step(t, carry, phase=phase):
            for cp in lhs_copies(phase, t):
                cp.wait()

            @pl.when(t < 7)
            def _():
                for cp in lhs_copies(phase, t + 1):
                    cp.start()

            if phase == 0:
                @pl.when(t == 1)
                def _():
                    for j in range(steps):
                        weight_copy(1, j).start()

                @pl.when(t == 7)
                def _():
                    for cp in lhs_copies(1, 0):
                        cp.start()

            @pl.when((t == 0) | ((t >= 2) & (t <= 4)))
            def _():
                pair = pair_of(t)

                def body(j):
                    @pl.when(t == 0)
                    def _():
                        for k in ((0,) if phase == 0 else (1, 2)):
                            weight_copy(k, j).wait()

                    if phase == 0:
                        @pl.when(t > 0)
                        def _():
                            core_copy(0, j).wait_send()
                    else:
                        core_copy(0, j).wait_send()
                    st[0, j] = product(phase, t % 2, j).astype(BF16)
                    core_copy(pair, j).start()

                tiles(body)

            @pl.when(t == 1)
            def _():
                def body(j):
                    core_copy(0, j).wait_recv()
                    if phase == 1:
                        for k in range(2):
                            diag_copy(0, k, j).wait_send()
                    st[1, j] = (product(phase, 1, j) + from_core[0, j].astype(F32)).astype(BF16)
                    for k in range(2):
                        diag_copy(phase, k, j).start()

                tiles(body)

            for k in range(2):
                @pl.when(t == 5 + k)
                def _(k=k):
                    def body(j):
                        core_copy(1 + k, j).wait_recv()
                        diag_copy(phase, 1 - k, j).wait_recv()
                        if phase == 1:
                            final_copy(0, k, j).wait_send()
                        total = product(phase, (5 + k) % 2, j) + from_core[1 + k, j].astype(F32)
                        came = from_diag[phase, 1 - k, j].astype(F32)
                        split = slice(half, rows) if k == 0 else slice(0, half)
                        rest = slice(0, half) if k == 0 else slice(half, rows)
                        st[2 + k, j, split, :] = (total[split] + came).astype(BF16)
                        st[2 + k, j, rest, :] = total[rest].astype(BF16)
                        final_copy(phase, k, j).start()

                    tiles(body)

            @pl.when(t == 7)
            def _():
                def body(j):
                    core_copy(3, j).wait_recv()

                    @pl.when(j >= 2)
                    def _():
                        own_copy(phase, j).wait()

                    own_st[j % 2] = product(phase, 1, j) + from_core[3, j].astype(F32)
                    own_copy(phase, j).start()

                tiles(body)
                for j in (0, 1):
                    own_copy(phase, j).wait()
                if phase == 0:
                    for j in range(steps):
                        weight_copy(2, j).start()

            return carry

        lax.fori_loop(0, 8, step, 0)

    def z_copy(j, c):
        return pltpu.make_async_copy(z_all.at[pl.ds(c * rows, rows), cols(j)], lhs.at[c // 2, c % 2, :, cols(j)], z_sem.at[j, c])

    def gate_copy(j):
        return pltpu.make_async_copy(d_gate.at[pl.ds(0, 4 * rows), cols(j)], wa.at[:, cols(j)], w_sem.at[0, j])

    def grad_copy(i, j):
        slot = j % 2
        return pltpu.make_async_copy(own_st.at[slot, pl.ds(0, bn)], g_gate.at[cols(i), cols(j)], o_sem.at[slot])

    for j in range(steps):
        for c in range(4):
            z_copy(j, c).start()
        gate_copy(j).start()

    def grad_tile(step, carry):
        i, j = step // steps, step % steps

        @pl.when(i == 0)
        def _():
            gate_copy(j).wait()

        @pl.when(j == 0)
        def _():
            for c in range(4):
                z_copy(i, c).wait()

        @pl.when(step >= 2)
        def _():
            grad_copy(i, j).wait()

        own_st[j % 2, :bn] = dot_tn(lhs[:, :, :, cols(i)].reshape(4 * rows, bn), wa[:, cols(j)])
        grad_copy(i, j).start()
        return carry

    lax.fori_loop(0, steps * steps, grad_tile, 0)
    for j in range(2):
        grad_copy(0, j).wait()
    for j in range(steps):
        core_copy(0, j).wait_send()
        for k in range(2):
            diag_copy(1, k, j).wait_send()
            final_copy(1, k, j).wait_send()
            for phase in (0, 1):
                final_copy(phase, k, j).wait_recv()


def back_layer(act, d_gate, d_up, z_all, w_gate, w_up, w_down, tp, bn=512):
    total, width = act.shape
    dim = w_gate.shape[0]
    rows = total // tp
    steps = dim // bn
    anyspace = pl.BlockSpec(memory_space=pl.ANY)
    dma = pltpu.SemaphoreType.DMA
    came = jax.ShapeDtypeStruct((2, rows, dim), BF16)
    return pl.pallas_call(
        functools.partial(back_kernel, rows=rows, bn=bn),
        out_shape=(jax.ShapeDtypeStruct((2, rows, dim), F32), came, came, jax.ShapeDtypeStruct((dim, width), F32)),
        in_specs=[anyspace] * 7,
        out_specs=(anyspace,) * 4,
        scratch_shapes=[pltpu.VMEM((4 * rows, dim), BF16), pltpu.VMEM((dim, width), BF16), pltpu.VMEM((2, 2, rows, width), BF16),
                        pltpu.VMEM((4, steps, rows, bn), BF16), pltpu.VMEM((4, steps, rows, bn), BF16),
                        pltpu.VMEM((2, 2, steps, rows // 2, bn), BF16), pltpu.VMEM((2, rows, bn), F32),
                        dma((steps, 4)), dma((3, steps)), dma((2, 2)), dma((2,)), dma((steps,)), dma((4, steps)),
                        dma((2, steps)), dma((2, 2, steps)), dma((2, steps)), dma((2, 2, steps))],
        compiler_params=pltpu.CompilerParams(vmem_limit_bytes=67043328, collective_id=1, has_side_effects=True),
        cost_estimate=pl.CostEstimate(flops=6 * total * dim * width, bytes_accessed=200 << 20, transcendentals=0),
        name="back",
    )(act, d_gate, d_up, z_all, w_gate, w_up, w_down)


def norm_back(x, gain, d_out):
    inv_rms = lax.rsqrt(jnp.mean(x * x, axis=-1, keepdims=True) + NORM_EPS)
    unit = x * inv_rms
    scaled = d_out * (1.0 + gain.astype(F32))
    return inv_rms * (scaled - unit * jnp.mean(unit * scaled, axis=-1, keepdims=True)), d_out * unit


def join_kernel(own_ref, x_ref, y_ref, resid_ref, grad_ref, gain_ref, wo_ref, mixed_ref,
                out_ref, d_resid_ref, g_gain_ref, d_mixed_ref, g_out_ref, keep, *, joins):
    step = pl.program_id(0)
    bm = resid_ref.shape[0]

    @pl.when(step == 0)
    def _():
        g_gain_ref[...] = jnp.zeros_like(g_gain_ref)

    @pl.when(step < joins)
    def _():
        mlp_sum, d_gated = [own_ref[k] + x_ref[k].astype(F32) + y_ref[k].astype(F32) for k in range(2)]
        resid = resid_ref[...].astype(F32)
        out_ref[...] = (resid + mlp_sum).astype(BF16)
        d_norm, terms = norm_back(resid, gain_ref[...], d_gated.astype(BF16).astype(F32))
        d_resid = (grad_ref[...].astype(F32) + d_norm).astype(BF16)
        d_resid_ref[...] = d_resid
        keep[pl.ds(pl.multiple_of(step * bm, 16), bm), :] = d_resid
        g_gain_ref[...] += jnp.sum(terms, axis=0, keepdims=True)

    @pl.when(step >= joins)
    def _():
        d_mixed_ref[...] = dot_nt(keep[...], wo_ref[...]).astype(BF16)
        g_out_ref[...] = dot_tn(mixed_ref[...], keep[...])


def join_layer(own_part, x_part, y_part, resid, grad_out, gain, wo_all, mixed, bm=96, bn=512):
    rows, dim = resid.shape
    width = mixed.shape[1]
    joins = rows // bm
    pair = pl.BlockSpec((2, bm, dim), lambda i: (0, jnp.minimum(i, joins - 1), 0))
    row = pl.BlockSpec((bm, dim), lambda i: (jnp.minimum(i, joins - 1), 0))
    one = pl.BlockSpec((1, dim), lambda i: (0, 0))
    col = pl.BlockSpec((rows, bn), lambda i: (0, jnp.maximum(i - joins, 0)))
    block = pl.BlockSpec((bn, dim), lambda i: (jnp.maximum(i - joins, 0), 0))
    act = jax.ShapeDtypeStruct((rows, dim), BF16)
    return pl.pallas_call(
        functools.partial(join_kernel, joins=joins),
        out_shape=(act, act, jax.ShapeDtypeStruct((1, dim), F32), jax.ShapeDtypeStruct((rows, width), BF16),
                   jax.ShapeDtypeStruct((width, dim), F32)),
        grid=(joins + width // bn,),
        in_specs=[pair, pair, pair, row, row, one, block, col],
        out_specs=(row, row, one, col, block),
        scratch_shapes=[pltpu.VMEM((rows, dim), BF16)],
        compiler_params=pltpu.CompilerParams(dimension_semantics=("arbitrary",), vmem_limit_bytes=62 << 20),
        cost_estimate=pl.CostEstimate(flops=4 * rows * dim * width, bytes_accessed=60 << 20, transcendentals=rows),
        name="join",
    )(own_part, x_part, y_part, resid, grad_out, gain.reshape(1, dim), wo_all, mixed)


def finish_kernel(kv_ref, side_ref, back_ref, cos_ref, sin_ref, normed_ref, wk_ref, wv_ref, part_ref, hidden_ref, d_resid_ref, gain_ref,
                  g_key_ref, g_value_ref, out_ref, g_gain_ref):
    head_dim = wk_ref.shape[1]
    half_dim = head_dim // 2
    d_kv = (kv_ref[...] + side_ref[...].astype(F32) + back_ref[...].astype(F32)).astype(BF16)
    first, second = d_kv[:, :half_dim].astype(F32), d_kv[:, half_dim:head_dim].astype(F32)
    cos_t, sin_t = cos_ref[...], sin_ref[...]
    d_key = jnp.concatenate([first * cos_t + second * sin_t, second * cos_t - first * sin_t], axis=1).astype(BF16)
    d_value = d_kv[:, head_dim:]
    d_normed = (part_ref[...] + dot_nt(d_key, wk_ref[...]) + dot_nt(d_value, wv_ref[...])).astype(BF16).astype(F32)
    d_norm, terms = norm_back(hidden_ref[...].astype(F32), gain_ref[...], d_normed)
    out_ref[...] = (d_resid_ref[...].astype(F32) + d_norm).astype(BF16)
    g_key = dot_tn(normed_ref[...], d_key)
    g_value = dot_tn(normed_ref[...], d_value)
    g_gain = jnp.sum(terms, axis=0, keepdims=True)

    @pl.when(pl.program_id(0) == 0)
    def _():
        g_key_ref[...] = g_key
        g_value_ref[...] = g_value
        g_gain_ref[...] = g_gain

    @pl.when(pl.program_id(0) > 0)
    def _():
        g_key_ref[...] += g_key
        g_value_ref[...] += g_value
        g_gain_ref[...] += g_gain


def finish_layer(kv_own, kv_side, kv_back, cos_t, sin_t, normed, w_key, w_value, part, hidden, d_resid, gain):
    rows, dim = hidden.shape
    shard, half_dim = cos_t.shape
    head_dim = w_key.shape[1]

    def row(width):
        return pl.BlockSpec((shard, width), lambda i: (i, 0))

    def whole(*shape):
        return pl.BlockSpec(shape, lambda i: (0, 0))

    kv, act, table, weight, one = row(2 * head_dim), row(dim), whole(shard, half_dim), whole(dim, head_dim), whole(1, dim)
    grad = jax.ShapeDtypeStruct((dim, head_dim), F32)
    return pl.pallas_call(
        finish_kernel,
        out_shape=(grad, grad, jax.ShapeDtypeStruct((rows, dim), BF16), jax.ShapeDtypeStruct((1, dim), F32)),
        grid=(rows // shard,),
        in_specs=[kv, kv, kv, table, table, act, weight, weight, act, act, act, one],
        out_specs=(weight, weight, act, one),
        compiler_params=pltpu.CompilerParams(dimension_semantics=("arbitrary",), vmem_limit_bytes=62 << 20),
        cost_estimate=pl.CostEstimate(flops=8 * rows * dim * head_dim, bytes_accessed=24 << 20, transcendentals=rows),
        name="finish",
    )(kv_own, kv_side, kv_back, cos_t, sin_t, normed, w_key, w_value, part, hidden, d_resid, gain.reshape(1, dim))


def product_kernel(a_ref, b_ref, o_ref):
    o_ref[...] = dot_tn(a_ref[...], b_ref[...])


def weight_grad(a, b, bm=1024, bn=512):
    rows, m = a.shape
    n = b.shape[1]
    return pl.pallas_call(
        product_kernel,
        out_shape=jax.ShapeDtypeStruct((m, n), F32),
        grid=(m // bm, n // bn),
        in_specs=[pl.BlockSpec((rows, bm), lambda i, j: (0, i)), pl.BlockSpec((rows, bn), lambda i, j: (0, j))],
        out_specs=pl.BlockSpec((bm, bn), lambda i, j: (i, j)),
        compiler_params=pltpu.CompilerParams(dimension_semantics=("arbitrary", "arbitrary"), vmem_limit_bytes=62 << 20),
        cost_estimate=pl.CostEstimate(flops=2 * rows * m * n, bytes_accessed=110 << 20, transcendentals=0),
        name="weight_grad",
    )(a, b)


def rest_kernel(at_ref, a_ref, b_ref, part_ref, o_ref):
    o_ref[...] = part_ref[...] + dot_tn(a_ref[...], b_ref[...])


def weight_grad_rest(a, b, part, block, count, bm=1024, bn=512):
    m, n = part.shape
    out = pl.BlockSpec((bm, bn), lambda i, j, at: (i, j))
    return pl.pallas_call(
        rest_kernel,
        out_shape=jax.ShapeDtypeStruct((m, n), F32),
        grid_spec=pltpu.PrefetchScalarGridSpec(
            num_scalar_prefetch=1, grid=(m // bm, n // bn),
            in_specs=[pl.BlockSpec((count, bm), lambda i, j, at: (at[0], i)), pl.BlockSpec((count, bn), lambda i, j, at: (at[0], j)), out],
            out_specs=out),
        compiler_params=pltpu.CompilerParams(dimension_semantics=("arbitrary", "arbitrary"), vmem_limit_bytes=62 << 20),
        cost_estimate=pl.CostEstimate(flops=2 * count * m * n, bytes_accessed=80 << 20, transcendentals=0),
        name="weight_grad_rest",
    )(jnp.asarray(block, jnp.int32).reshape(1), a, b, part)


def hop_diagonal(diag):
    half = diag.shape[0] // 2
    return swap(diag[:half], 2), swap(diag[half:], 4)


def hop_near(side, back, came_side, came_back):
    half = side.shape[0] // 2
    kind = came_side.dtype
    side = jnp.concatenate([side[:half], side[half:] + came_back.astype(F32)], axis=0).astype(kind)
    back = jnp.concatenate([back[:half] + came_side.astype(F32), back[half:]], axis=0).astype(kind)
    return side, back


def solution(mesh):
    tp_size = mesh.shape["tp"]
    act_spec = P("dp", "tp", None)
    in_specs = (act_spec, act_spec, P("dp"), P("dp"), P(None), P(None, "tp"), P(None, None), P(None, None), P("tp", None), P(None), P(None, "tp"), P(None, "tp"), P("tp", None))
    out_specs = (act_spec, act_spec, P("dp"), P("dp", "tp"), P("dp", None), P("dp", None), P(("dp", "tp"), None), P("dp"), P("dp", "tp"), P("dp", "tp"), P(("dp", "tp"), None))

    def layer(hidden, grad_out, prefix_len, valid_len, attn_norm, w_query, w_key, w_value, w_out, mlp_norm, w_gate, w_up, w_down):
        batch, shard, dim = hidden.shape
        head_dim = w_key.shape[1]
        rows = batch * shard
        me = lax.axis_index("tp")
        starts = (me ^ jnp.array([0, 2, 4, 6, 1, 3, 5, 7], jnp.int32)) * shard
        k_pos = (starts[:, None] + jnp.arange(shard, dtype=jnp.int32)).reshape(1, tp_size * shard)
        cos_own, sin_own = rope_tables(me * shard + jnp.arange(shard), head_dim)
        hidden = hidden.reshape(rows, dim)
        grad_out = grad_out.reshape(rows, dim)
        normed, wq_all, wo_all, kv_all, query, mixed, resid, gated_in = front_layer(
            prefix_len, valid_len, k_pos, cos_own, sin_own, attn_norm, mlp_norm, hidden, w_query, w_key, w_value, w_out, batch, tp_size)
        wo_all = wo_all.reshape(tp_size * head_dim, dim)

        gated_all, grad_all, act, d_gate, d_upper = gated_layer(gated_in, grad_out, w_gate, w_up, w_down, tp_size)
        own_part, x_part, y_part, g_gate_part = back_layer(act, d_gate, d_upper, gated_all, w_gate, w_up, w_down, tp_size)
        hidden_out, d_resid, g_mlp_norm_part, d_mixed, g_out_part = join_layer(
            own_part, x_part, y_part, resid, grad_out, mlp_norm, wo_all, mixed)
        g_out = lax.psum_scatter(g_out_part, "tp", scatter_dimension=0, tiled=True)
        lens_back = jnp.concatenate([jnp.stack([prefix_len, valid_len, jnp.full((batch,), me, jnp.int32)]),
                                     jnp.broadcast_to(starts[:, None], (tp_size, batch))])
        d_q_raw, dkv_near, dkv_far = attention_backward(lens_back, cos_own, sin_own, query, kv_all, d_mixed, batch)
        near = tp_size // 2
        came_kv = swap(dkv_far, 1)
        g_far = jnp.einsum("kte,td->ked", d_q_raw[near:], normed, preferred_element_type=F32)
        came_kv, g_far = lax.optimization_barrier((came_kv, g_far))
        came_q = swap(g_far, 1)
        kv_own, kv_side, kv_back, kv_diag = [dkv_near[k].astype(F32) + came_kv[k].astype(F32) for k in range(4)]
        kv_came = hop_diagonal(kv_diag.astype(BF16))
        d_normed_q = jnp.einsum("hte,hde->td", d_q_raw, wq_all, preferred_element_type=F32)
        kv_came, d_normed_q = lax.optimization_barrier((kv_came, d_normed_q))
        kv_next = hop_near(kv_side, kv_back, *kv_came)
        kv_last = (swap(kv_next[0], 2), swap(kv_next[1], 4))
        came_q, dq_near = lax.optimization_barrier((came_q, d_q_raw[:near]))
        g_query_sum = jnp.einsum("kte,td->ked", dq_near, normed, preferred_element_type=F32) + came_q
        g_query_sum, act = lax.optimization_barrier((g_query_sum, act))
        q_came = hop_diagonal(g_query_sum[3])
        g_down = weight_grad(act, grad_all)
        kv_last, q_came, g_down = lax.optimization_barrier((kv_last, q_came, g_down))
        q_next = hop_near(g_query_sum[1], g_query_sum[2], *q_came)
        g_key_part, g_value_part, grad_hidden, g_attn_norm_part = finish_layer(
            kv_own, kv_last[0], kv_last[1], cos_own, sin_own, normed, w_key, w_value, d_normed_q, hidden, d_resid, attn_norm)
        norms = jnp.concatenate([g_attn_norm_part, g_mlp_norm_part])
        q_next, g_key_part, g_value_part, norms, d_gate = lax.optimization_barrier((q_next, g_key_part, g_value_part, norms, d_gate))
        g_key, g_value = lax.psum((g_key_part, g_value_part), "tp")
        last_side = swap(q_next[0], 2)
        q_last = (last_side, swap(q_next[1], 4))
        norms_near = [swap(norms, bit) for bit in (2, 4, 6)]
        g_gate = weight_grad_rest(gated_all, d_gate, g_gate_part, 1, 4 * rows)
        norms_near, g_gate, d_upper = lax.optimization_barrier((norms_near, g_gate, d_upper))
        norms = norms + norms_near[0] + norms_near[1] + norms_near[2]
        norms, d_upper = lax.optimization_barrier((norms, d_upper))
        norms_core = swap(norms, 1)
        g_up = weight_grad(gated_all, d_upper)
        norms_core, q_last, g_up = lax.optimization_barrier((norms_core, q_last, g_up))
        g_norms = norms + norms_core
        g_query = (g_query_sum[0] + q_last[0] + q_last[1]).T
        full = (batch, shard, dim)
        return (hidden_out.reshape(full), grad_hidden.reshape(full), g_norms[0], g_query, g_key, g_value, g_out, g_norms[1], g_gate, g_up, g_down)

    return jax.shard_map(layer, mesh=mesh, in_specs=in_specs, out_specs=out_specs, check_vma=False)
```

```python
import functools
import math
import jax
import jax.numpy as jnp
from jax import lax
from jax.experimental import pallas as pl
from jax.experimental.pallas import tpu as pltpu
from jax.sharding import PartitionSpec as P

NORM_EPS = 1e-6
BF16 = jnp.bfloat16
F32 = jnp.float32
GELU_C = math.sqrt(2.0 / math.pi)
GELU_K = 0.044715
MASKED = -1e30
NT = (((1,), (1,)), ((), ()))
TN = (((0,), (0,)), ((), ()))


def rope_tables(positions, head_dim):
    half_dim = head_dim // 2
    exponent = jnp.arange(half_dim, dtype=F32) * (2.0 / head_dim)
    inv_freq = jnp.exp(exponent * (-math.log(10000.0)))
    angles = positions.astype(F32)[:, None] * inv_freq[None, :]
    return jnp.cos(angles), jnp.sin(angles)


def dot_nn(a, b):
    return jnp.dot(a, b, preferred_element_type=F32)


def dot_nt(a, b):
    return lax.dot_general(a, b, NT, preferred_element_type=F32)


def dot_tn(a, b):
    return lax.dot_general(a, b, TN, preferred_element_type=F32)


def swap(x, bit):
    return lax.ppermute(x, "tp", [(t, t ^ bit) for t in range(8)])


def flip(index, bit):
    return index + bit - 2 * bit * ((index // bit) % 2)


def neighbours():
    me = lax.axis_index("tp")
    return me, flip(me, 1), flip(me, 2), flip(me, 4)


def enter(peers):
    barrier = pltpu.get_barrier_semaphore()
    for peer in peers:
        pl.semaphore_signal(barrier, inc=1, device_id={"tp": peer}, device_id_type=pl.DeviceIdType.MESH)
    pl.semaphore_wait(barrier, len(peers))


def attn_bwd_kernel(lens_ref, cos_ref, sin_ref, q_ref, kv_ref, do_ref, dq_ref, dkv0_ref, dkv1_ref, dkv_acc):
    heads, shard, head_dim = q_ref.shape
    tp = kv_ref.shape[0]
    total = tp * shard
    rows = heads * shard
    s_id = pl.program_id(0)
    g_id = pl.program_id(1)
    prefix = lens_ref[0, s_id]
    valid = lens_ref[1, s_id]
    first = lens_ref[2, 0] * shard
    keys = kv_ref[:, :, :head_dim].reshape(total, head_dim)
    values = kv_ref[:, :, head_dim:].reshape(total, head_dim)
    query = q_ref[...].reshape(rows, head_dim) * BF16(head_dim ** -0.5)
    d_out = jnp.concatenate([do_ref[:, h * head_dim:(h + 1) * head_dim] for h in range(heads)], axis=0)
    step = lax.broadcasted_iota(jnp.int32, (shard, 1), 0)
    k_pos = jnp.concatenate([step + lens_ref[3 + r, 0] for r in range(tp)], axis=0)
    q_pos = first + lax.rem(lax.broadcasted_iota(jnp.int32, (1, rows), 1), shard)
    limit = jnp.minimum(valid, jnp.maximum(prefix, q_pos + 1))
    cos_t, sin_t = cos_ref[...][None], sin_ref[...][None]
    d_k = d_v = None
    count = heads // 2
    width = count * shard
    for c in range(2):
        cols = slice(c * width, (c + 1) * width)
        q_c, do_c = query[cols], d_out[cols]
        s = jnp.where(k_pos < limit[:, cols], dot_nt(keys, q_c), MASKED)
        e = jnp.exp(s - jnp.max(s, axis=0, keepdims=True))
        p = e * (1.0 / jnp.sum(e, axis=0, keepdims=True))
        d_p = dot_nt(values, do_c)
        delta = jnp.sum(p * d_p, axis=0, keepdims=True)
        d_s = (p * (d_p - delta)).astype(BF16)
        d_v_c = dot_nn(p.astype(BF16), do_c)
        d_k_c = dot_nn(d_s, q_c)
        d_k, d_v = (d_k_c, d_v_c) if d_k is None else (d_k + d_k_c, d_v + d_v_c)
        d_q = (dot_tn(d_s, keys) * (head_dim ** -0.5)).reshape(count, shard, head_dim)
        first, second = d_q[:, :, :head_dim // 2], d_q[:, :, head_dim // 2:]
        some = slice(c * count, (c + 1) * count)
        dq_ref[some, :, :head_dim // 2] = (first * cos_t + second * sin_t).astype(BF16)
        dq_ref[some, :, head_dim // 2:] = (second * cos_t - first * sin_t).astype(BF16)
    d_kv = jnp.concatenate([d_k, d_v], axis=1)

    @pl.when(g_id == 0)
    def _():
        dkv_acc[...] = d_kv

    @pl.when(g_id > 0)
    def _():
        dkv_acc[...] += d_kv

    @pl.when(g_id == pl.num_programs(1) - 1)
    def _():
        near = (tp // 2, shard, 2 * head_dim)
        dkv0_ref[...] = dkv_acc[:total // 2].astype(BF16).reshape(near)
        dkv1_ref[...] = dkv_acc[total // 2:].astype(BF16).reshape(near)


def remote(src, dst, send, recv, peer):
    return pltpu.make_async_remote_copy(src_ref=src, dst_ref=dst, send_sem=send, recv_sem=recv,
                                        device_id={"tp": peer}, device_id_type=pl.DeviceIdType.MESH)


def front_kernel(prefix_ref, valid_ref, kpos_ref, cos_ref, sin_ref, gain1_ref, gain2_ref, hidden, w_query, w_key, w_value, w_out,
                 normed_out, wq_all, wo_all, kv_all, query_out, mixed_out, resid_out, gated_out,
                 x_buf, n_buf, wkv, wq, wo, kv, q, probs, mix, acc, load, store, send, recv, *, batch):
    rows, dim = x_buf.shape
    shard = rows // batch
    head_dim = w_key.shape[1]
    tp = wq.shape[0]
    near = tp // 2
    total = tp * shard
    half_dim = head_dim // 2
    me, core, side, back = neighbours()
    bufs = (wq, kv, wo)

    def to_side(a):
        return remote(bufs[a].at[0], bufs[a].at[1], send.at[a, 0], recv.at[a, 0], side)

    def to_back(a):
        return remote(bufs[a].at[0], bufs[a].at[2], send.at[a, 1], recv.at[a, 1], back)

    def onward(a, k):
        half = bufs[a].shape[1] // 2
        part = pl.ds(k * half, half)
        return remote(bufs[a].at[1 + k, part], bufs[a].at[3, part], send.at[a, 2 + k], recv.at[a, 2 + k], (back, side)[k])

    def to_core(a, k):
        return remote(bufs[a].at[k], bufs[a].at[near + k], send.at[a, 4 + k], recv.at[a, 4 + k], core)

    loads = [pltpu.make_async_copy(src, dst, load.at[i]) for i, (src, dst) in enumerate((
        (w_query, wq.at[0]), (hidden, x_buf), (w_key, wkv.at[:, :head_dim]), (w_value, wkv.at[:, head_dim:]), (w_out, wo.at[0])))]
    mixed_at = [me, side, back, flip(side, 4)]
    mixed_at = mixed_at + [flip(dev, 1) for dev in mixed_at]
    stores = {name: pltpu.make_async_copy(src, dst, store.at[i]) for i, (name, src, dst) in enumerate((
        ("normed", n_buf, normed_out), ("wq", wq, wq_all), ("wo", wo, wo_all), ("kv", kv, kv_all), ("query", q, query_out),
        ("resid", x_buf, resid_out), ("gated", n_buf, gated_out)))}
    mixed_stores = [pltpu.make_async_copy(mix.at[:, pl.ds(k * head_dim, head_dim)],
                                          mixed_out.at[:, pl.ds(pl.multiple_of(dev * head_dim, 128), head_dim)], store.at[7 + k])
                    for k, dev in enumerate(mixed_at)]

    for cp in loads:
        cp.start()
    enter((core, side, back))
    loads[0].wait()
    to_side(0).start()
    to_back(0).start()
    to_core(0, 0).start()

    def norm_rows(src, gain_ref):
        x_f = src.astype(F32)
        inv_rms = lax.rsqrt(jnp.mean(x_f * x_f, axis=-1, keepdims=True) + NORM_EPS)
        return (x_f * inv_rms * (1.0 + gain_ref[...].astype(F32))).astype(BF16)

    def seq_rows(i):
        return pl.ds(pl.multiple_of(i * shard, 16), shard)

    def rotate(x_f):
        first, second = x_f[:, :half_dim], x_f[:, half_dim:]
        cos_t, sin_t = cos_ref[...], sin_ref[...]
        return first * cos_t - second * sin_t, second * cos_t + first * sin_t

    def norm1(i, carry):
        n_buf[seq_rows(i), :] = norm_rows(x_buf[seq_rows(i), :], gain1_ref)
        return carry

    loads[1].wait()
    lax.fori_loop(0, batch, norm1, 0)
    stores["normed"].start()
    loads[2].wait()
    loads[3].wait()

    def own_kv(i, carry):
        raw = dot_nn(n_buf[seq_rows(i), :], wkv[...])
        first, second = rotate(raw[:, :head_dim])
        kv[0, seq_rows(i), :half_dim] = first.astype(BF16)
        kv[0, seq_rows(i), half_dim:head_dim] = second.astype(BF16)
        kv[0, seq_rows(i), head_dim:] = raw[:, head_dim:].astype(BF16)
        return carry

    lax.fori_loop(0, batch, own_kv, 0)
    to_side(1).start()
    to_back(1).start()
    to_core(1, 0).start()

    def own_query(k):
        def step(i, carry):
            for h in (k, near + k):
                first, second = rotate(dot_nn(n_buf[seq_rows(i), :], wq[h]))
                q[h, seq_rows(i), :half_dim] = first.astype(BF16)
                q[h, seq_rows(i), half_dim:] = second.astype(BF16)
            return carry

        to_core(0, k).wait_recv()
        lax.fori_loop(0, batch, step, 0)

    def pass_on(a):
        to_side(a).wait_recv()
        onward(a, 0).start()
        to_core(a, 1).start()
        to_back(a).wait_recv()
        onward(a, 1).start()
        to_core(a, 2).start()

    def pass_last(a):
        onward(a, 0).wait_recv()
        onward(a, 1).wait_recv()
        to_core(a, 3).start()

    own_query(0)
    pass_on(0)
    own_query(1)
    own_query(2)
    pass_on(1)
    loads[4].wait()
    to_side(2).start()
    to_back(2).start()
    to_core(2, 0).start()
    pass_last(0)
    own_query(3)
    stores["query"].start()
    stores["wq"].start()
    pass_last(1)
    for k in range(near):
        to_core(1, k).wait_recv()
    stores["kv"].start()

    q_pos = me * shard + lax.broadcasted_iota(jnp.int32, (shard, 1), 0)

    def attend(i, carry):
        keys = kv[:, seq_rows(i), :head_dim].reshape(total, head_dim)
        values = kv[:, seq_rows(i), head_dim:].reshape(total, head_dim)
        visible = kpos_ref[...] < jnp.minimum(valid_ref[i], jnp.maximum(prefix_ref[i], q_pos + 1))
        for g in range(2):
            query = q[g * near:(g + 1) * near, seq_rows(i), :].reshape(near * shard, head_dim) * BF16(head_dim ** -0.5)
            scores = dot_nt(query, keys)
            for h in range(near):
                part = slice(h * shard, (h + 1) * shard)
                s = jnp.where(visible, scores[part], MASKED)
                e = jnp.exp(s - jnp.max(s, axis=-1, keepdims=True))
                probs[g, part, :] = (e * (1.0 / jnp.sum(e, axis=-1, keepdims=True))).astype(BF16)
            mixed = dot_nn(probs[g], values).astype(BF16)
            for h in range(near):
                head = g * near + h
                mix[seq_rows(i), head * head_dim:(head + 1) * head_dim] = mixed[h * shard:(h + 1) * shard]
        return carry

    lax.fori_loop(0, batch, attend, 0)
    for cp in mixed_stores:
        cp.start()
    pass_on(2)

    def project(k, first):
        def step(n, carry):
            cols = pl.ds(pl.multiple_of(n * 512, 128), 512)
            part = (dot_nn(mix[:, k * head_dim:(k + 1) * head_dim], wo[k, :, cols])
                    + dot_nn(mix[:, (near + k) * head_dim:(near + k + 1) * head_dim], wo[near + k, :, cols]))
            acc[:, cols] = part if first else acc[:, cols] + part
            return carry

        to_core(2, k).wait_recv()
        lax.fori_loop(0, dim // 512, step, 0)

    project(0, True)
    project(1, False)
    project(2, False)
    pass_last(2)
    project(3, False)
    stores["wo"].start()
    stores["normed"].wait()

    def norm2(i, carry):
        resid = (x_buf[seq_rows(i), :].astype(F32) + acc[seq_rows(i), :]).astype(BF16)
        x_buf[seq_rows(i), :] = resid
        n_buf[seq_rows(i), :] = norm_rows(resid, gain2_ref)
        return carry

    lax.fori_loop(0, batch, norm2, 0)
    stores["resid"].start()
    stores["gated"].start()
    for cp in mixed_stores:
        cp.wait()
    for name in ("wq", "wo", "kv", "query", "resid", "gated"):
        stores[name].wait()
    for a in range(3):
        to_side(a).wait_send()
        to_back(a).wait_send()
        for k in range(2):
            onward(a, k).wait_send()
        for k in range(near):
            to_core(a, k).wait_send()


def front_layer(prefix_len, valid_len, k_pos, cos_t, sin_t, attn_norm, mlp_norm, hidden, w_query, w_key, w_value, w_out, batch, tp):
    rows, dim = hidden.shape
    head_dim = w_key.shape[1]
    shard = rows // batch
    total = tp * shard
    anyspace = pl.BlockSpec(memory_space=pl.ANY)
    vmem = pl.BlockSpec(memory_space=pltpu.VMEM)
    dma = pltpu.SemaphoreType.DMA

    def shape(*dims):
        return jax.ShapeDtypeStruct(dims, BF16)

    return pl.pallas_call(
        functools.partial(front_kernel, batch=batch),
        out_shape=(shape(rows, dim), shape(tp, dim, head_dim), shape(tp, head_dim, dim), shape(tp, rows, 2 * head_dim),
                   shape(tp, rows, head_dim), shape(rows, tp * head_dim), shape(rows, dim), shape(rows, dim)),
        in_specs=[pl.BlockSpec(memory_space=pltpu.SMEM)] * 2 + [vmem] * 5 + [anyspace] * 5,
        out_specs=(anyspace,) * 8,
        scratch_shapes=[pltpu.VMEM((rows, dim), BF16), pltpu.VMEM((rows, dim), BF16), pltpu.VMEM((dim, 2 * head_dim), BF16),
                        pltpu.VMEM((tp, dim, head_dim), BF16), pltpu.VMEM((tp, head_dim, dim), BF16),
                        pltpu.VMEM((tp, rows, 2 * head_dim), BF16), pltpu.VMEM((tp, rows, head_dim), BF16),
                        pltpu.VMEM((2, tp // 2 * shard, total), BF16), pltpu.VMEM((rows, tp * head_dim), BF16), pltpu.VMEM((rows, dim), F32),
                        dma((5,)), dma((15,)), dma((3, 8)), dma((3, 8))],
        compiler_params=pltpu.CompilerParams(vmem_limit_bytes=62 << 20, collective_id=2, has_side_effects=True),
        cost_estimate=pl.CostEstimate(flops=8 * rows * dim * tp * head_dim, bytes_accessed=60 << 20, transcendentals=tp * rows * total),
        name="front",
    )(prefix_len, valid_len, k_pos, cos_t, sin_t, attn_norm.reshape(1, dim), mlp_norm.reshape(1, dim), hidden, w_query, w_key, w_value, w_out)


def attention_backward(lens, cos_t, sin_t, query, kv_all, d_mixed, batch, group=8):
    heads, rows, head_dim = query.shape
    near = kv_all.shape[0] // 2
    shard = rows // batch
    total = 2 * near * shard
    q_spec = pl.BlockSpec((group, shard, head_dim), lambda s, g, *_: (g, s, 0))
    kv_spec = pl.BlockSpec((near, shard, 2 * head_dim), lambda s, g, *_: (0, s, 0))
    table = pl.BlockSpec((shard, head_dim // 2), lambda s, g, *_: (0, 0))
    kv_shape = jax.ShapeDtypeStruct((near, rows, 2 * head_dim), BF16)
    return pl.pallas_call(
        attn_bwd_kernel,
        out_shape=(jax.ShapeDtypeStruct((heads, rows, head_dim), BF16), kv_shape, kv_shape),
        grid_spec=pltpu.PrefetchScalarGridSpec(
            num_scalar_prefetch=1, grid=(batch, heads // group),
            in_specs=[table, table, q_spec, pl.BlockSpec((2 * near, shard, 2 * head_dim), lambda s, g, *_: (0, s, 0)), pl.BlockSpec((shard, group * head_dim), lambda s, g, *_: (s, g))],
            out_specs=(q_spec, kv_spec, kv_spec),
            scratch_shapes=[pltpu.VMEM((total, 2 * head_dim), F32)]),
        compiler_params=pltpu.CompilerParams(dimension_semantics=("arbitrary", "arbitrary"), vmem_limit_bytes=62 << 20),
        cost_estimate=pl.CostEstimate(flops=10 * heads * rows * total * head_dim, bytes_accessed=20 << 20, transcendentals=heads * rows * total),
        name="attn_bwd",
    )(lens, cos_t, sin_t, query, kv_all, d_mixed)


def gated_tile(z, g, w_g, w_u, w_d):
    gate = dot_nn(z, w_g)
    upper = dot_nn(z, w_u)
    d_act = dot_nt(g, w_d).astype(BF16).astype(F32)
    sq = gate * gate
    th = jnp.tanh(gate * (GELU_C + (GELU_C * GELU_K) * sq))
    half = 0.5 + 0.5 * th
    gelu = gate * half
    slope = half + gate * (0.5 - 0.5 * (th * th)) * (GELU_C + (3.0 * GELU_C * GELU_K) * sq)
    return (gelu * upper).astype(BF16), (d_act * upper * slope).astype(BF16), (d_act * gelu).astype(BF16)


def gated_kernel(z_own, g_own, wg_hbm, wu_hbm, wd_hbm, z_all, g_all, act, d_gate, d_up, diag_in,
                 wg, wu, wd, z_buf, g_buf, outs, st, from_core, far_send, far_recv, diag_send, diag_recv, w_sem, in_sem, own_sem, out_sem, send, recv, send0, recv0, *, bn):
    rows, dim = z_own.shape
    width = wg_hbm.shape[1]
    steps = width // bn
    piece = rows // 4
    me, core, side, back = neighbours()
    corner = flip(side, 4)
    own = (z_own, g_own)
    full = (z_all, g_all)

    def part(slot, q):
        return pl.ds(pl.multiple_of(slot * rows + q * piece, 16), piece)

    def link_rows(u, path):
        turn = u // 2
        diag = turn % 2
        if path == 0:
            return side + (corner - side) * diag, (u % 2) + 2 * (turn // 2) + diag * 2
        return back + (corner - back) * diag, (u % 2) + 2 - 2 * (turn // 2) - diag * 2

    def link_copy(u, path, a):
        turn = u // 2
        peer = side if path == 0 else back
        sems = (send.at[path, u, a], recv.at[path, u, a])
        if turn == 1:
            slot = back if path == 0 else side
            q = (2 if path == 0 else 0) + u % 2
            return remote(full[a].at[part(slot, q)], full[a].at[part(slot, q)], *sems, peer)
        q = u % 2 + (2 * (turn // 2) if path == 0 else 2 - 2 * (turn // 2))
        return remote(own[a].at[pl.ds(q * piece, piece)], full[a].at[part(me, q)], *sems, peer)

    def core_copy(u, path, a):
        slot, q = link_rows(u, path)
        return remote(full[a].at[part(slot, q)], full[a].at[part(slot, q)], send.at[2 + path, u, a], recv.at[2 + path, u, a], core)

    def own_copy(a):
        return remote(own[a], full[a].at[pl.ds(pl.multiple_of(me * rows, 16), rows)], send0.at[a], recv0.at[a], core)

    def weight_copies(n):
        cols = pl.ds(pl.multiple_of(n * bn, 128), bn)
        return [pltpu.make_async_copy(wg_hbm.at[:, cols], wg.at[:, cols], w_sem.at[0, n]),
                pltpu.make_async_copy(wu_hbm.at[:, cols], wu.at[:, cols], w_sem.at[1, n]),
                pltpu.make_async_copy(wd_hbm.at[cols], wd.at[cols], w_sem.at[2, n])]

    bufs = (z_buf, g_buf)
    own_in = [pltpu.make_async_copy(own[a], bufs[a], own_sem.at[a]) for a in range(2)]
    own_out = [pltpu.make_async_copy(bufs[a], full[a].at[pl.ds(pl.multiple_of(me * rows, 16), rows)], own_sem.at[2 + a]) for a in range(2)]
    for cp in own_in:
        cp.start()
    for n in range(steps):
        for cp in weight_copies(n):
            cp.start()
    enter((core, side, back))
    for u in range(2):
        for path in range(2):
            for a in range(2):
                link_copy(u, path, a).start()
        if u == 0:
            for a in range(2):
                own_copy(a).start()

    def out_copies(slot, s_rows, n):
        cols = pl.ds(pl.multiple_of(n * bn, 128), bn)
        return [pltpu.make_async_copy(outs.at[slot, k, pl.ds(i * piece, piece)], ref.at[s_rows[i], cols], out_sem.at[slot, k, i])
                for k, ref in enumerate((act, d_gate, d_up)) for i in range(4)]

    def stage_rows(s):
        late = (s + 6) // 8
        u = (s - 2) * late
        first = me + (core - me) * s * (1 - late)
        (slot_x, q_x), (slot_y, q_y) = link_rows(u, 0), link_rows(u, 1)
        base_x, base_y = slot_x * rows + q_x * piece, slot_y * rows + q_y * piece
        pair_x, pair_y = flip(slot_x, 1) * rows + q_x * piece, flip(slot_y, 1) * rows + q_y * piece
        starts = [(1 - late) * (first * rows + i * piece) + late * base for i, base in enumerate((base_x, base_y, pair_x, pair_y))]
        return [pl.ds(pl.multiple_of(st, 16), piece) for st in starts]

    def pass_on(u):
        for path in range(2):
            for a in range(2):
                link_copy(u, path, a).wait_recv()
                core_copy(u, path, a).start()

    def far_copy(j):
        return remote(st.at[0, j], from_core.at[j], far_send.at[j], far_recv.at[j], core)

    def diag_copy(k, j):
        half = rows // 2
        return remote(st.at[1, j, pl.ds(k * half, half)], diag_in.at[k, :, pl.ds(pl.multiple_of(j * bn, 128), bn)],
                      diag_send.at[k, j], diag_recv.at[k, j], (side, back)[k])

    def down_diagonal():
        for slot in range(2):
            for cp in out_copies(slot, stage_rows(5), 0):
                cp.wait()
        loads = [pltpu.make_async_copy(act.at[pl.ds(pl.multiple_of(dev * rows, 16), rows)], bufs[a], in_sem.at[a, 0])
                 for a, dev in enumerate((flip(corner, 1), corner))]
        for cp in loads:
            cp.start()

        def theirs(j, carry):
            st[0, j] = dot_nn(z_buf[...], wd[:, pl.ds(pl.multiple_of(j * bn, 128), bn)]).astype(BF16)
            far_copy(j).start()
            return carry

        def mine(j, carry):
            far_copy(j).wait_recv()
            total = dot_nn(g_buf[...], wd[:, pl.ds(pl.multiple_of(j * bn, 128), bn)]) + from_core[j].astype(F32)
            st[1, j] = total.astype(BF16)
            for k in range(2):
                diag_copy(k, j).start()
            return carry

        loads[0].wait()
        lax.fori_loop(0, dim // bn, theirs, 0)
        loads[1].wait()
        lax.fori_loop(0, dim // bn, mine, 0)

    def compute(s):
        s_rows = stage_rows(s)

        def block(n, carry):
            step = s * steps + n
            slot = step % 2

            @pl.when((step >= 2) & (step // 2 != 6 * steps // 2))
            def _():
                for cp in out_copies(slot, s_rows, n):
                    cp.wait()

            @pl.when(s == 0)
            def _():
                for cp in weight_copies(n):
                    cp.wait()

            @pl.when((s == 6) & (n == steps - 1))
            def _():
                pass_on(5)

            cols = pl.ds(pl.multiple_of(n * bn, 128), bn)
            res = gated_tile(z_buf[...], g_buf[...], wg[:, cols], wu[:, cols], wd[cols, :])
            for k in range(3):
                outs[slot, k] = res[k]
            for cp in out_copies(slot, s_rows, n):
                cp.start()
            return carry

        lax.fori_loop(0, steps, block, 0)

    def stage(s, carry):
        @pl.when(s == 0)
        def _():
            for cp in own_in:
                cp.wait()
            for cp in own_out:
                cp.start()

        @pl.when(s == 1)
        def _():
            for cp in own_out:
                cp.wait()
            for a in range(2):
                own_copy(a).wait_recv()

        for u in range(6):
            @pl.when(s == u + 2)
            def _(u=u):
                if u < 5:
                    pass_on(u)
                if u == 4:
                    down_diagonal()
                if u < 2:
                    for path in range(2):
                        for a in range(2):
                            link_copy(u + 2, path, a).start()
                if u == 1:
                    for later in (4, 5):
                        for path in range(2):
                            for a in range(2):
                                link_copy(later, path, a).start()
                for path in range(2):
                    for a in range(2):
                        core_copy(u, path, a).wait_recv()

        @pl.when(s >= 1)
        def _():
            s_rows = stage_rows(s)
            copies = [pltpu.make_async_copy(full[a].at[s_rows[i]], bufs[a].at[pl.ds(i * piece, piece)], in_sem.at[a, i])
                      for a in range(2) for i in range(4)]
            for cp in copies:
                cp.start()
            for cp in copies:
                cp.wait()

        compute(s)
        return carry

    lax.fori_loop(0, 8, stage, 0)
    last = stage_rows(7)
    for slot in range(2):
        for cp in out_copies(slot, last, 0):
            cp.wait()
    for j in range(dim // bn):
        far_copy(j).wait_send()
        for k in range(2):
            diag_copy(k, j).wait_send()
            diag_copy(k, j).wait_recv()
    for a in range(2):
        own_copy(a).wait_send()
        for path in range(2):
            for u in range(6):
                link_copy(u, path, a).wait_send()
                core_copy(u, path, a).wait_send()


def gated_layer(z_own, g_own, w_gate, w_up, w_down, tp, bn=512):
    rows, dim = z_own.shape
    width = w_gate.shape[1]
    total = rows * tp
    anyspace = pl.BlockSpec(memory_space=pl.ANY)
    gathered = jax.ShapeDtypeStruct((total, dim), BF16)
    made = jax.ShapeDtypeStruct((total, width), BF16)
    dma = pltpu.SemaphoreType.DMA
    return pl.pallas_call(
        functools.partial(gated_kernel, bn=bn),
        out_shape=(gathered, gathered, made, made, made, jax.ShapeDtypeStruct((2, rows // 2, dim), BF16)),
        in_specs=[anyspace] * 5,
        out_specs=(anyspace,) * 6,
        scratch_shapes=[pltpu.VMEM((dim, width), BF16), pltpu.VMEM((dim, width), BF16), pltpu.VMEM((width, dim), BF16),
                        pltpu.VMEM((rows, dim), BF16), pltpu.VMEM((rows, dim), BF16), pltpu.VMEM((2, 3, rows, bn), BF16),
                        pltpu.VMEM((2, dim // bn, rows, bn), BF16), pltpu.VMEM((dim // bn, rows, bn), BF16),
                        dma((dim // bn,)), dma((dim // bn,)), dma((2, dim // bn)), dma((2, dim // bn)), dma((3, width // bn)), dma((2, 4)), dma((4,)), dma((2, 3, 4)), dma((4, 6, 2)), dma((4, 6, 2)), dma((2,)), dma((2,))],
        compiler_params=pltpu.CompilerParams(vmem_limit_bytes=67043328, collective_id=0, has_side_effects=True),
        cost_estimate=pl.CostEstimate(flops=6 * total * dim * width, bytes_accessed=200 << 20, transcendentals=total * width),
        name="gated",
    )(z_own, g_own, w_gate, w_up, w_down)


def back_kernel(act, d_gate, d_up, z_all, diag_in, wg_hbm, wu_hbm, wd_hbm, own_out, x_in, y_in, g_gate,
                wa, wb, lhs, st, from_core, from_diag, own_st, in_sem, z_sem, w_sem, l_sem, o_sem, c_send, c_recv, d_send, d_recv, f_send, f_recv, *, rows, bn):
    dim, width = wg_hbm.shape
    steps = dim // bn
    half = rows // 2
    me, core, side, back = neighbours()

    def cols(j):
        return pl.ds(pl.multiple_of(j * bn, 128), bn)

    def pair_of(t):
        return ((t + 5) // 7) * ((t + 1) % 3 + 1)

    def lhs_copies(phase, t):
        pair = pair_of(t)
        theirs = 1 - t // 5 - ((t + 6) // 7 - (t + 5) // 7)
        dev = me + (1 - pair // 2) * (side - me) + (1 - pair % 2) * (back - me)
        dev = dev + theirs * (flip(dev, 1) - dev)
        src = pl.ds(pl.multiple_of(dev * rows, 16), rows)
        refs = (act,) if phase == 0 else (d_gate, d_up)
        return [pltpu.make_async_copy(ref.at[src], lhs.at[t % 2, k], l_sem.at[t % 2, k]) for k, ref in enumerate(refs)]

    def weight_copy(k, j):
        if k == 0:
            return pltpu.make_async_copy(wd_hbm.at[:, cols(j)], wa.at[pl.ds(0, width), cols(j)], w_sem.at[0, j])
        src, dst = (wg_hbm, wb) if k == 1 else (wu_hbm, wa)
        return pltpu.make_async_copy(src.at[cols(j)], dst.at[cols(j)], w_sem.at[k, j])

    def core_copy(pair, j):
        return remote(st.at[0, j], from_core.at[pair, j], c_send.at[j], c_recv.at[pair, j], core)

    def diag_copy(phase, k, j):
        return remote(st.at[1, j, pl.ds(k * half, half)], from_diag.at[phase, k, j], d_send.at[k, j], d_recv.at[phase, k, j], (side, back)[k])

    def final_copy(phase, k, j):
        return remote(st.at[2 + k, j], (x_in, y_in)[k].at[phase, :, cols(j)], f_send.at[k, j], f_recv.at[phase, k, j], (side, back)[k])

    def own_copy(phase, j):
        return pltpu.make_async_copy(own_st.at[j % 2], own_out.at[phase, :, cols(j)], o_sem.at[j % 2])

    def product(phase, slot, j):
        if phase == 0:
            return dot_nn(lhs[slot, 0], wa[:width, cols(j)])
        return dot_nt(lhs[slot, 0], wb[cols(j), :]) + dot_nt(lhs[slot, 1], wa[cols(j), :])

    def diag_load(k, j):
        return pltpu.make_async_copy(diag_in.at[k, :, cols(j)], from_diag.at[0, k, j], in_sem.at[k, j])

    for cp in lhs_copies(0, 2):
        cp.start()
    for j in range(steps):
        weight_copy(0, j).start()
    for k in range(2):
        for j in range(steps):
            diag_load(k, j).start()
    enter((core, side, back))

    def tiles(body):
        def step(j, carry):
            body(j)
            return carry

        lax.fori_loop(0, steps, step, 0)

    for phase in (0, 1):
        def step(t, carry, phase=phase):
            for cp in lhs_copies(phase, t):
                cp.wait()

            @pl.when(t < 7)
            def _():
                for cp in lhs_copies(phase, t + 1):
                    cp.start()

            if phase == 0:
                @pl.when(t == 3)
                def _():
                    for j in range(steps):
                        weight_copy(1, j).start()

                @pl.when(t == 7)
                def _():
                    for cp in lhs_copies(1, 0):
                        cp.start()

            @pl.when((t == 0) | ((t >= 2) & (t <= 4)))
            def _():
                pair = pair_of(t)

                def body(j):
                    @pl.when(t == (2 if phase == 0 else 0))
                    def _():
                        for k in ((0,) if phase == 0 else (1, 2)):
                            weight_copy(k, j).wait()

                    if phase == 0:
                        @pl.when(t > 2)
                        def _():
                            core_copy(0, j).wait_send()
                    else:
                        core_copy(0, j).wait_send()
                    st[0, j] = product(phase, t % 2, j).astype(BF16)
                    core_copy(pair, j).start()

                tiles(body)

            if phase == 1:
                @pl.when(t == 1)
                def _():
                    def body(j):
                        core_copy(0, j).wait_recv()
                        st[1, j] = (product(phase, 1, j) + from_core[0, j].astype(F32)).astype(BF16)
                        for k in range(2):
                            diag_copy(phase, k, j).start()

                    tiles(body)

            for k in range(2):
                @pl.when(t == 5 + k)
                def _(k=k):
                    def body(j):
                        core_copy(1 + k, j).wait_recv()
                        if phase == 0:
                            diag_load(1 - k, j).wait()
                        else:
                            diag_copy(phase, 1 - k, j).wait_recv()
                            final_copy(0, k, j).wait_send()
                        total = product(phase, (5 + k) % 2, j) + from_core[1 + k, j].astype(F32)
                        came = from_diag[phase, 1 - k, j].astype(F32)
                        split = slice(half, rows) if k == 0 else slice(0, half)
                        rest = slice(0, half) if k == 0 else slice(half, rows)
                        st[2 + k, j, split, :] = (total[split] + came).astype(BF16)
                        st[2 + k, j, rest, :] = total[rest].astype(BF16)
                        final_copy(phase, k, j).start()

                    tiles(body)

            @pl.when(t == 7)
            def _():
                def body(j):
                    core_copy(3, j).wait_recv()

                    @pl.when(j >= 2)
                    def _():
                        own_copy(phase, j).wait()

                    own_st[j % 2] = product(phase, 1, j) + from_core[3, j].astype(F32)
                    own_copy(phase, j).start()

                tiles(body)
                for j in (0, 1):
                    own_copy(phase, j).wait()
                if phase == 0:
                    for j in range(steps):
                        weight_copy(2, j).start()

            return carry

        lax.fori_loop(2 if phase == 0 else 0, 8, step, 0)

    def z_copy(j, c):
        return pltpu.make_async_copy(z_all.at[pl.ds(c * rows, rows), cols(j)], lhs.at[c // 2, c % 2, :, cols(j)], z_sem.at[j, c])

    def gate_copy(j):
        return pltpu.make_async_copy(d_gate.at[pl.ds(0, 4 * rows), cols(j)], wa.at[:, cols(j)], w_sem.at[0, j])

    def grad_copy(i, j):
        slot = j % 2
        return pltpu.make_async_copy(own_st.at[slot, pl.ds(0, bn)], g_gate.at[cols(i), cols(j)], o_sem.at[slot])

    for j in range(steps):
        for c in range(4):
            z_copy(j, c).start()
        gate_copy(j).start()

    def grad_tile(step, carry):
        i, j = step // steps, step % steps

        @pl.when(i == 0)
        def _():
            gate_copy(j).wait()

        @pl.when(j == 0)
        def _():
            for c in range(4):
                z_copy(i, c).wait()

        @pl.when(step >= 2)
        def _():
            grad_copy(i, j).wait()

        own_st[j % 2, :bn] = dot_tn(lhs[:, :, :, cols(i)].reshape(4 * rows, bn), wa[:, cols(j)])
        grad_copy(i, j).start()
        return carry

    lax.fori_loop(0, steps * steps, grad_tile, 0)
    for j in range(2):
        grad_copy(0, j).wait()
    for j in range(steps):
        core_copy(0, j).wait_send()
        for k in range(2):
            diag_copy(1, k, j).wait_send()
            final_copy(1, k, j).wait_send()
            for phase in (0, 1):
                final_copy(phase, k, j).wait_recv()


def back_layer(act, d_gate, d_up, z_all, diag_in, w_gate, w_up, w_down, tp, bn=512):
    total, width = act.shape
    dim = w_gate.shape[0]
    rows = total // tp
    steps = dim // bn
    anyspace = pl.BlockSpec(memory_space=pl.ANY)
    dma = pltpu.SemaphoreType.DMA
    came = jax.ShapeDtypeStruct((2, rows, dim), BF16)
    return pl.pallas_call(
        functools.partial(back_kernel, rows=rows, bn=bn),
        out_shape=(jax.ShapeDtypeStruct((2, rows, dim), F32), came, came, jax.ShapeDtypeStruct((dim, width), F32)),
        in_specs=[anyspace] * 8,
        out_specs=(anyspace,) * 4,
        scratch_shapes=[pltpu.VMEM((4 * rows, dim), BF16), pltpu.VMEM((dim, width), BF16), pltpu.VMEM((2, 2, rows, width), BF16),
                        pltpu.VMEM((4, steps, rows, bn), BF16), pltpu.VMEM((4, steps, rows, bn), BF16),
                        pltpu.VMEM((2, 2, steps, rows // 2, bn), BF16), pltpu.VMEM((2, rows, bn), F32),
                        dma((2, steps)), dma((steps, 4)), dma((3, steps)), dma((2, 2)), dma((2,)), dma((steps,)), dma((4, steps)),
                        dma((2, steps)), dma((2, 2, steps)), dma((2, steps)), dma((2, 2, steps))],
        compiler_params=pltpu.CompilerParams(vmem_limit_bytes=67043328, collective_id=1, has_side_effects=True),
        cost_estimate=pl.CostEstimate(flops=6 * total * dim * width, bytes_accessed=200 << 20, transcendentals=0),
        name="back",
    )(act, d_gate, d_up, z_all, diag_in, w_gate, w_up, w_down)


def norm_back(x, gain, d_out):
    inv_rms = lax.rsqrt(jnp.mean(x * x, axis=-1, keepdims=True) + NORM_EPS)
    unit = x * inv_rms
    scaled = d_out * (1.0 + gain.astype(F32))
    return inv_rms * (scaled - unit * jnp.mean(unit * scaled, axis=-1, keepdims=True)), d_out * unit


def join_kernel(own_ref, x_ref, y_ref, resid_ref, grad_ref, gain_ref, wo_ref, mixed_ref,
                out_ref, d_resid_ref, g_gain_ref, d_mixed_ref, g_out_ref, keep, *, joins):
    step = pl.program_id(0)
    bm = resid_ref.shape[0]

    @pl.when(step == 0)
    def _():
        g_gain_ref[...] = jnp.zeros_like(g_gain_ref)

    @pl.when(step < joins)
    def _():
        mlp_sum, d_gated = [own_ref[k] + x_ref[k].astype(F32) + y_ref[k].astype(F32) for k in range(2)]
        resid = resid_ref[...].astype(F32)
        out_ref[...] = (resid + mlp_sum).astype(BF16)
        d_norm, terms = norm_back(resid, gain_ref[...], d_gated.astype(BF16).astype(F32))
        d_resid = (grad_ref[...].astype(F32) + d_norm).astype(BF16)
        d_resid_ref[...] = d_resid
        keep[pl.ds(pl.multiple_of(step * bm, 16), bm), :] = d_resid
        g_gain_ref[...] += jnp.sum(terms, axis=0, keepdims=True)

    @pl.when(step >= joins)
    def _():
        d_mixed_ref[...] = dot_nt(keep[...], wo_ref[...]).astype(BF16)
        g_out_ref[...] = dot_tn(mixed_ref[...], keep[...])


def join_layer(own_part, x_part, y_part, resid, grad_out, gain, wo_all, mixed, bm=96, bn=512):
    rows, dim = resid.shape
    width = mixed.shape[1]
    joins = rows // bm
    pair = pl.BlockSpec((2, bm, dim), lambda i: (0, jnp.minimum(i, joins - 1), 0))
    row = pl.BlockSpec((bm, dim), lambda i: (jnp.minimum(i, joins - 1), 0))
    one = pl.BlockSpec((1, dim), lambda i: (0, 0))
    col = pl.BlockSpec((rows, bn), lambda i: (0, jnp.maximum(i - joins, 0)))
    block = pl.BlockSpec((bn, dim), lambda i: (jnp.maximum(i - joins, 0), 0))
    act = jax.ShapeDtypeStruct((rows, dim), BF16)
    return pl.pallas_call(
        functools.partial(join_kernel, joins=joins),
        out_shape=(act, act, jax.ShapeDtypeStruct((1, dim), F32), jax.ShapeDtypeStruct((rows, width), BF16),
                   jax.ShapeDtypeStruct((width, dim), F32)),
        grid=(joins + width // bn,),
        in_specs=[pair, pair, pair, row, row, one, block, col],
        out_specs=(row, row, one, col, block),
        scratch_shapes=[pltpu.VMEM((rows, dim), BF16)],
        compiler_params=pltpu.CompilerParams(dimension_semantics=("arbitrary",), vmem_limit_bytes=62 << 20),
        cost_estimate=pl.CostEstimate(flops=4 * rows * dim * width, bytes_accessed=60 << 20, transcendentals=rows),
        name="join",
    )(own_part, x_part, y_part, resid, grad_out, gain.reshape(1, dim), wo_all, mixed)


def finish_kernel(kv_ref, side_ref, back_ref, cos_ref, sin_ref, normed_ref, wk_ref, wv_ref, part_ref, hidden_ref, d_resid_ref, gain_ref,
                  g_key_ref, g_value_ref, out_ref, g_gain_ref):
    head_dim = wk_ref.shape[1]
    half_dim = head_dim // 2
    d_kv = (kv_ref[...] + side_ref[...].astype(F32) + back_ref[...].astype(F32)).astype(BF16)
    first, second = d_kv[:, :half_dim].astype(F32), d_kv[:, half_dim:head_dim].astype(F32)
    cos_t, sin_t = cos_ref[...], sin_ref[...]
    d_key = jnp.concatenate([first * cos_t + second * sin_t, second * cos_t - first * sin_t], axis=1).astype(BF16)
    d_value = d_kv[:, head_dim:]
    d_normed = (part_ref[...] + dot_nt(d_key, wk_ref[...]) + dot_nt(d_value, wv_ref[...])).astype(BF16).astype(F32)
    d_norm, terms = norm_back(hidden_ref[...].astype(F32), gain_ref[...], d_normed)
    out_ref[...] = (d_resid_ref[...].astype(F32) + d_norm).astype(BF16)
    g_key = dot_tn(normed_ref[...], d_key)
    g_value = dot_tn(normed_ref[...], d_value)
    g_gain = jnp.sum(terms, axis=0, keepdims=True)

    @pl.when(pl.program_id(0) == 0)
    def _():
        g_key_ref[...] = g_key
        g_value_ref[...] = g_value
        g_gain_ref[...] = g_gain

    @pl.when(pl.program_id(0) > 0)
    def _():
        g_key_ref[...] += g_key
        g_value_ref[...] += g_value
        g_gain_ref[...] += g_gain


def finish_layer(kv_own, kv_side, kv_back, cos_t, sin_t, normed, w_key, w_value, part, hidden, d_resid, gain):
    rows, dim = hidden.shape
    shard, half_dim = cos_t.shape
    head_dim = w_key.shape[1]

    def row(width):
        return pl.BlockSpec((shard, width), lambda i: (i, 0))

    def whole(*shape):
        return pl.BlockSpec(shape, lambda i: (0, 0))

    kv, act, table, weight, one = row(2 * head_dim), row(dim), whole(shard, half_dim), whole(dim, head_dim), whole(1, dim)
    grad = jax.ShapeDtypeStruct((dim, head_dim), F32)
    return pl.pallas_call(
        finish_kernel,
        out_shape=(grad, grad, jax.ShapeDtypeStruct((rows, dim), BF16), jax.ShapeDtypeStruct((1, dim), F32)),
        grid=(rows // shard,),
        in_specs=[kv, kv, kv, table, table, act, weight, weight, act, act, act, one],
        out_specs=(weight, weight, act, one),
        compiler_params=pltpu.CompilerParams(dimension_semantics=("arbitrary",), vmem_limit_bytes=62 << 20),
        cost_estimate=pl.CostEstimate(flops=8 * rows * dim * head_dim, bytes_accessed=24 << 20, transcendentals=rows),
        name="finish",
    )(kv_own, kv_side, kv_back, cos_t, sin_t, normed, w_key, w_value, part, hidden, d_resid, gain.reshape(1, dim))


def product_kernel(a_ref, b_ref, o_ref):
    o_ref[...] = dot_tn(a_ref[...], b_ref[...])


def weight_grad(a, b, bm=1024, bn=512):
    rows, m = a.shape
    n = b.shape[1]
    return pl.pallas_call(
        product_kernel,
        out_shape=jax.ShapeDtypeStruct((m, n), F32),
        grid=(m // bm, n // bn),
        in_specs=[pl.BlockSpec((rows, bm), lambda i, j: (0, i)), pl.BlockSpec((rows, bn), lambda i, j: (0, j))],
        out_specs=pl.BlockSpec((bm, bn), lambda i, j: (i, j)),
        compiler_params=pltpu.CompilerParams(dimension_semantics=("arbitrary", "arbitrary"), vmem_limit_bytes=62 << 20),
        cost_estimate=pl.CostEstimate(flops=2 * rows * m * n, bytes_accessed=110 << 20, transcendentals=0),
        name="weight_grad",
    )(a, b)


def rest_kernel(at_ref, a_ref, b_ref, part_ref, o_ref):
    o_ref[...] = part_ref[...] + dot_tn(a_ref[...], b_ref[...])


def weight_grad_rest(a, b, part, block, count, bm=1024, bn=512):
    m, n = part.shape
    out = pl.BlockSpec((bm, bn), lambda i, j, at: (i, j))
    return pl.pallas_call(
        rest_kernel,
        out_shape=jax.ShapeDtypeStruct((m, n), F32),
        grid_spec=pltpu.PrefetchScalarGridSpec(
            num_scalar_prefetch=1, grid=(m // bm, n // bn),
            in_specs=[pl.BlockSpec((count, bm), lambda i, j, at: (at[0], i)), pl.BlockSpec((count, bn), lambda i, j, at: (at[0], j)), out],
            out_specs=out),
        compiler_params=pltpu.CompilerParams(dimension_semantics=("arbitrary", "arbitrary"), vmem_limit_bytes=62 << 20),
        cost_estimate=pl.CostEstimate(flops=2 * count * m * n, bytes_accessed=80 << 20, transcendentals=0),
        name="weight_grad_rest",
    )(jnp.asarray(block, jnp.int32).reshape(1), a, b, part)


def hop_diagonal(diag):
    half = diag.shape[0] // 2
    return swap(diag[:half], 2), swap(diag[half:], 4)


def hop_near(side, back, came_side, came_back):
    half = side.shape[0] // 2
    kind = came_side.dtype
    side = jnp.concatenate([side[:half], side[half:] + came_back.astype(F32)], axis=0).astype(kind)
    back = jnp.concatenate([back[:half] + came_side.astype(F32), back[half:]], axis=0).astype(kind)
    return side, back


def solution(mesh):
    tp_size = mesh.shape["tp"]
    act_spec = P("dp", "tp", None)
    in_specs = (act_spec, act_spec, P("dp"), P("dp"), P(None), P(None, "tp"), P(None, None), P(None, None), P("tp", None), P(None), P(None, "tp"), P(None, "tp"), P("tp", None))
    out_specs = (act_spec, act_spec, P("dp"), P("dp", "tp"), P("dp", None), P("dp", None), P(("dp", "tp"), None), P("dp"), P("dp", "tp"), P("dp", "tp"), P(("dp", "tp"), None))

    def layer(hidden, grad_out, prefix_len, valid_len, attn_norm, w_query, w_key, w_value, w_out, mlp_norm, w_gate, w_up, w_down):
        batch, shard, dim = hidden.shape
        head_dim = w_key.shape[1]
        rows = batch * shard
        me = lax.axis_index("tp")
        starts = (me ^ jnp.array([0, 2, 4, 6, 1, 3, 5, 7], jnp.int32)) * shard
        k_pos = (starts[:, None] + jnp.arange(shard, dtype=jnp.int32)).reshape(1, tp_size * shard)
        cos_own, sin_own = rope_tables(me * shard + jnp.arange(shard), head_dim)
        hidden = hidden.reshape(rows, dim)
        grad_out = grad_out.reshape(rows, dim)
        normed, wq_all, wo_all, kv_all, query, mixed, resid, gated_in = front_layer(
            prefix_len, valid_len, k_pos, cos_own, sin_own, attn_norm, mlp_norm, hidden, w_query, w_key, w_value, w_out, batch, tp_size)
        wo_all = wo_all.reshape(tp_size * head_dim, dim)

        gated_all, grad_all, act, d_gate, d_upper, diag_in = gated_layer(gated_in, grad_out, w_gate, w_up, w_down, tp_size)
        own_part, x_part, y_part, g_gate_part = back_layer(act, d_gate, d_upper, gated_all, diag_in, w_gate, w_up, w_down, tp_size)
        hidden_out, d_resid, g_mlp_norm_part, d_mixed, g_out_part = join_layer(
            own_part, x_part, y_part, resid, grad_out, mlp_norm, wo_all, mixed)
        g_out = lax.psum_scatter(g_out_part, "tp", scatter_dimension=0, tiled=True)
        lens_back = jnp.concatenate([jnp.stack([prefix_len, valid_len, jnp.full((batch,), me, jnp.int32)]),
                                     jnp.broadcast_to(starts[:, None], (tp_size, batch))])
        d_q_raw, dkv_near, dkv_far = attention_backward(lens_back, cos_own, sin_own, query, kv_all, d_mixed, batch)
        near = tp_size // 2
        came_kv = swap(dkv_far, 1)
        g_far = jnp.einsum("kte,td->ked", d_q_raw[near:], normed, preferred_element_type=F32)
        came_kv, g_far = lax.optimization_barrier((came_kv, g_far))
        came_q = swap(g_far, 1)
        kv_own, kv_side, kv_back, kv_diag = [dkv_near[k].astype(F32) + came_kv[k].astype(F32) for k in range(4)]
        kv_came = hop_diagonal(kv_diag.astype(BF16))
        d_normed_q = jnp.einsum("hte,hde->td", d_q_raw, wq_all, preferred_element_type=F32)
        kv_came, d_normed_q = lax.optimization_barrier((kv_came, d_normed_q))
        kv_next = hop_near(kv_side, kv_back, *kv_came)
        kv_last = (swap(kv_next[0], 2), swap(kv_next[1], 4))
        came_q, dq_near = lax.optimization_barrier((came_q, d_q_raw[:near]))
        g_query_sum = jnp.einsum("kte,td->ked", dq_near, normed, preferred_element_type=F32) + came_q
        g_query_sum, act = lax.optimization_barrier((g_query_sum, act))
        q_came = hop_diagonal(g_query_sum[3])
        g_down = weight_grad(act, grad_all)
        kv_last, q_came, g_down = lax.optimization_barrier((kv_last, q_came, g_down))
        q_next = hop_near(g_query_sum[1], g_query_sum[2], *q_came)
        g_key_part, g_value_part, grad_hidden, g_attn_norm_part = finish_layer(
            kv_own, kv_last[0], kv_last[1], cos_own, sin_own, normed, w_key, w_value, d_normed_q, hidden, d_resid, attn_norm)
        norms = jnp.concatenate([g_attn_norm_part, g_mlp_norm_part])
        q_next, g_key_part, g_value_part, norms, d_gate = lax.optimization_barrier((q_next, g_key_part, g_value_part, norms, d_gate))
        g_key, g_value = lax.psum((g_key_part, g_value_part), "tp")
        last_side = swap(q_next[0], 2)
        q_last = (last_side, swap(q_next[1], 4))
        norms_near = [swap(norms, bit) for bit in (2, 4, 6)]
        g_gate = weight_grad_rest(gated_all, d_gate, g_gate_part, 1, 4 * rows)
        norms_near, g_gate, d_upper = lax.optimization_barrier((norms_near, g_gate, d_upper))
        norms = norms + norms_near[0] + norms_near[1] + norms_near[2]
        norms, d_upper = lax.optimization_barrier((norms, d_upper))
        norms_core = swap(norms, 1)
        g_up = weight_grad(gated_all, d_upper)
        norms_core, q_last, g_up = lax.optimization_barrier((norms_core, q_last, g_up))
        g_norms = norms + norms_core
        g_query = (g_query_sum[0] + q_last[0] + q_last[1]).T
        full = (batch, shard, dim)
        return (hidden_out.reshape(full), grad_hidden.reshape(full), g_norms[0], g_query, g_key, g_value, g_out, g_norms[1], g_gate, g_up, g_down)

    return jax.shard_map(layer, mesh=mesh, in_specs=in_specs, out_specs=out_specs, check_vma=False)
```

```python
import functools
import math
import jax
import jax.numpy as jnp
from jax import lax
from jax.experimental import pallas as pl
from jax.experimental.pallas import tpu as pltpu
from jax.sharding import PartitionSpec as P

NORM_EPS = 1e-6
BF16 = jnp.bfloat16
F32 = jnp.float32
GELU_C = math.sqrt(2.0 / math.pi)
GELU_K = 0.044715
MASKED = -1e30
NT = (((1,), (1,)), ((), ()))
TN = (((0,), (0,)), ((), ()))


def rope_tables(positions, head_dim):
    half_dim = head_dim // 2
    exponent = jnp.arange(half_dim, dtype=F32) * (2.0 / head_dim)
    inv_freq = jnp.exp(exponent * (-math.log(10000.0)))
    angles = positions.astype(F32)[:, None] * inv_freq[None, :]
    return jnp.cos(angles), jnp.sin(angles)


def dot_nn(a, b):
    return jnp.dot(a, b, preferred_element_type=F32)


def dot_nt(a, b):
    return lax.dot_general(a, b, NT, preferred_element_type=F32)


def dot_tn(a, b):
    return lax.dot_general(a, b, TN, preferred_element_type=F32)


def swap(x, bit):
    return lax.ppermute(x, "tp", [(t, t ^ bit) for t in range(8)])


def flip(index, bit):
    return index + bit - 2 * bit * ((index // bit) % 2)


def neighbours():
    me = lax.axis_index("tp")
    return me, flip(me, 1), flip(me, 2), flip(me, 4)


def enter(peers):
    barrier = pltpu.get_barrier_semaphore()
    for peer in peers:
        pl.semaphore_signal(barrier, inc=1, device_id={"tp": peer}, device_id_type=pl.DeviceIdType.MESH)
    pl.semaphore_wait(barrier, len(peers))


def attn_bwd_kernel(lens_ref, cos_ref, sin_ref, q_ref, kv_ref, do_ref, dq_ref, dkv0_ref, dkv1_ref, dkv_acc):
    heads, shard, head_dim = q_ref.shape
    tp = kv_ref.shape[0]
    total = tp * shard
    rows = heads * shard
    s_id = pl.program_id(0)
    g_id = pl.program_id(1)
    prefix = lens_ref[0, s_id]
    valid = lens_ref[1, s_id]
    first = lens_ref[2, 0] * shard
    keys = kv_ref[:, :, :head_dim].reshape(total, head_dim)
    values = kv_ref[:, :, head_dim:].reshape(total, head_dim)
    query = q_ref[...].reshape(rows, head_dim) * BF16(head_dim ** -0.5)
    d_out = jnp.concatenate([do_ref[:, h * head_dim:(h + 1) * head_dim] for h in range(heads)], axis=0)
    step = lax.broadcasted_iota(jnp.int32, (shard, 1), 0)
    k_pos = jnp.concatenate([step + lens_ref[3 + r, 0] for r in range(tp)], axis=0)
    q_pos = first + lax.rem(lax.broadcasted_iota(jnp.int32, (1, rows), 1), shard)
    limit = jnp.minimum(valid, jnp.maximum(prefix, q_pos + 1))
    cos_t, sin_t = cos_ref[...][None], sin_ref[...][None]
    d_k = d_v = None
    count = heads // 2
    width = count * shard
    for c in range(2):
        cols = slice(c * width, (c + 1) * width)
        q_c, do_c = query[cols], d_out[cols]
        s = jnp.where(k_pos < limit[:, cols], dot_nt(keys, q_c), MASKED)
        e = jnp.exp(s - jnp.max(s, axis=0, keepdims=True))
        p = e * (1.0 / jnp.sum(e, axis=0, keepdims=True))
        d_p = dot_nt(values, do_c)
        delta = jnp.sum(p * d_p, axis=0, keepdims=True)
        d_s = (p * (d_p - delta)).astype(BF16)
        d_v_c = dot_nn(p.astype(BF16), do_c)
        d_k_c = dot_nn(d_s, q_c)
        d_k, d_v = (d_k_c, d_v_c) if d_k is None else (d_k + d_k_c, d_v + d_v_c)
        d_q = (dot_tn(d_s, keys) * (head_dim ** -0.5)).reshape(count, shard, head_dim)
        first, second = d_q[:, :, :head_dim // 2], d_q[:, :, head_dim // 2:]
        some = slice(c * count, (c + 1) * count)
        dq_ref[some, :, :head_dim // 2] = (first * cos_t + second * sin_t).astype(BF16)
        dq_ref[some, :, head_dim // 2:] = (second * cos_t - first * sin_t).astype(BF16)
    d_kv = jnp.concatenate([d_k, d_v], axis=1)

    @pl.when(g_id == 0)
    def _():
        dkv_acc[...] = d_kv

    @pl.when(g_id > 0)
    def _():
        dkv_acc[...] += d_kv

    @pl.when(g_id == pl.num_programs(1) - 1)
    def _():
        near = (tp // 2, shard, 2 * head_dim)
        dkv0_ref[...] = dkv_acc[:total // 2].astype(BF16).reshape(near)
        dkv1_ref[...] = dkv_acc[total // 2:].astype(BF16).reshape(near)


def remote(src, dst, send, recv, peer):
    return pltpu.make_async_remote_copy(src_ref=src, dst_ref=dst, send_sem=send, recv_sem=recv,
                                        device_id={"tp": peer}, device_id_type=pl.DeviceIdType.MESH)


def front_kernel(prefix_ref, valid_ref, kpos_ref, cos_ref, sin_ref, gain1_ref, gain2_ref, hidden, grad, w_query, w_key, w_value, w_out,
                 normed_out, wq_all, wo_all, kv_all, query_out, mixed_out, resid_out, gated_out, g_all,
                 x_buf, n_buf, wkv, wq, wo, kv, q, probs, mix, acc, load, store, send, recv, early_send, early_recv, *, batch):
    rows, dim = x_buf.shape
    shard = rows // batch
    head_dim = w_key.shape[1]
    tp = wq.shape[0]
    near = tp // 2
    total = tp * shard
    half_dim = head_dim // 2
    me, core, side, back = neighbours()
    bufs = (wq, kv, wo)

    def to_side(a):
        return remote(bufs[a].at[0], bufs[a].at[1], send.at[a, 0], recv.at[a, 0], side)

    def to_back(a):
        return remote(bufs[a].at[0], bufs[a].at[2], send.at[a, 1], recv.at[a, 1], back)

    def onward(a, k):
        half = bufs[a].shape[1] // 2
        part = pl.ds(k * half, half)
        return remote(bufs[a].at[1 + k, part], bufs[a].at[3, part], send.at[a, 2 + k], recv.at[a, 2 + k], (back, side)[k])

    def to_core(a, k):
        return remote(bufs[a].at[k], bufs[a].at[near + k], send.at[a, 4 + k], recv.at[a, 4 + k], core)

    piece = rows // 4

    def early(k, onto_core):
        shard_at = ((side, back)[k] if onto_core else me) * rows + 2 * k * piece
        there = g_all.at[pl.ds(pl.multiple_of(shard_at, 16), piece)]
        src = there if onto_core else grad.at[pl.ds(2 * k * piece, piece)]
        at = 2 * int(onto_core) + k
        return remote(src, there, early_send.at[at], early_recv.at[at], core if onto_core else (side, back)[k])

    loads = [pltpu.make_async_copy(src, dst, load.at[i]) for i, (src, dst) in enumerate((
        (w_query, wq.at[0]), (hidden, x_buf), (w_key, wkv.at[:, :head_dim]), (w_value, wkv.at[:, head_dim:]), (w_out, wo.at[0])))]
    mixed_at = [me, side, back, flip(side, 4)]
    mixed_at = mixed_at + [flip(dev, 1) for dev in mixed_at]
    stores = {name: pltpu.make_async_copy(src, dst, store.at[i]) for i, (name, src, dst) in enumerate((
        ("normed", n_buf, normed_out), ("wq", wq, wq_all), ("wo", wo, wo_all), ("kv", kv, kv_all), ("query", q, query_out),
        ("resid", x_buf, resid_out), ("gated", n_buf, gated_out)))}
    mixed_stores = [pltpu.make_async_copy(mix.at[:, pl.ds(k * head_dim, head_dim)],
                                          mixed_out.at[:, pl.ds(pl.multiple_of(dev * head_dim, 128), head_dim)], store.at[7 + k])
                    for k, dev in enumerate(mixed_at)]

    for cp in loads:
        cp.start()
    enter((core, side, back))
    loads[0].wait()
    to_side(0).start()
    to_back(0).start()
    to_core(0, 0).start()

    def norm_rows(src, gain_ref):
        x_f = src.astype(F32)
        inv_rms = lax.rsqrt(jnp.mean(x_f * x_f, axis=-1, keepdims=True) + NORM_EPS)
        return (x_f * inv_rms * (1.0 + gain_ref[...].astype(F32))).astype(BF16)

    def seq_rows(i):
        return pl.ds(pl.multiple_of(i * shard, 16), shard)

    def rotate(x_f):
        first, second = x_f[:, :half_dim], x_f[:, half_dim:]
        cos_t, sin_t = cos_ref[...], sin_ref[...]
        return first * cos_t - second * sin_t, second * cos_t + first * sin_t

    def norm1(i, carry):
        n_buf[seq_rows(i), :] = norm_rows(x_buf[seq_rows(i), :], gain1_ref)
        return carry

    loads[1].wait()
    lax.fori_loop(0, batch, norm1, 0)
    stores["normed"].start()
    loads[2].wait()
    loads[3].wait()

    def own_kv(i, carry):
        raw = dot_nn(n_buf[seq_rows(i), :], wkv[...])
        first, second = rotate(raw[:, :head_dim])
        kv[0, seq_rows(i), :half_dim] = first.astype(BF16)
        kv[0, seq_rows(i), half_dim:head_dim] = second.astype(BF16)
        kv[0, seq_rows(i), head_dim:] = raw[:, head_dim:].astype(BF16)
        return carry

    lax.fori_loop(0, batch, own_kv, 0)
    to_side(1).start()
    to_back(1).start()
    to_core(1, 0).start()

    def own_query(k):
        def step(i, carry):
            for h in (k, near + k):
                first, second = rotate(dot_nn(n_buf[seq_rows(i), :], wq[h]))
                q[h, seq_rows(i), :half_dim] = first.astype(BF16)
                q[h, seq_rows(i), half_dim:] = second.astype(BF16)
            return carry

        to_core(0, k).wait_recv()
        lax.fori_loop(0, batch, step, 0)

    def pass_on(a):
        to_side(a).wait_recv()
        onward(a, 0).start()
        to_core(a, 1).start()
        to_back(a).wait_recv()
        onward(a, 1).start()
        to_core(a, 2).start()

    def pass_last(a):
        onward(a, 0).wait_recv()
        onward(a, 1).wait_recv()
        to_core(a, 3).start()

    own_query(0)
    pass_on(0)
    own_query(1)
    own_query(2)
    pass_on(1)
    loads[4].wait()
    to_side(2).start()
    to_back(2).start()
    to_core(2, 0).start()
    pass_last(0)
    own_query(3)
    stores["query"].start()
    stores["wq"].start()
    pass_last(1)
    for k in range(near):
        to_core(1, k).wait_recv()
    stores["kv"].start()

    q_pos = me * shard + lax.broadcasted_iota(jnp.int32, (shard, 1), 0)

    def attend(i, carry):
        keys = kv[:, seq_rows(i), :head_dim].reshape(total, head_dim)
        values = kv[:, seq_rows(i), head_dim:].reshape(total, head_dim)
        visible = kpos_ref[...] < jnp.minimum(valid_ref[i], jnp.maximum(prefix_ref[i], q_pos + 1))
        for g in range(2):
            query = q[g * near:(g + 1) * near, seq_rows(i), :].reshape(near * shard, head_dim) * BF16(head_dim ** -0.5)
            scores = dot_nt(query, keys)
            for h in range(near):
                part = slice(h * shard, (h + 1) * shard)
                s = jnp.where(visible, scores[part], MASKED)
                e = jnp.exp(s - jnp.max(s, axis=-1, keepdims=True))
                probs[g, part, :] = (e * (1.0 / jnp.sum(e, axis=-1, keepdims=True))).astype(BF16)
            mixed = dot_nn(probs[g], values).astype(BF16)
            for h in range(near):
                head = g * near + h
                mix[seq_rows(i), head * head_dim:(head + 1) * head_dim] = mixed[h * shard:(h + 1) * shard]
        return carry

    lax.fori_loop(0, batch, attend, 0)
    for cp in mixed_stores:
        cp.start()
    pass_on(2)
    for k in range(2):
        early(k, False).start()

    def project(k, first):
        def step(n, carry):
            cols = pl.ds(pl.multiple_of(n * 512, 128), 512)
            part = (dot_nn(mix[:, k * head_dim:(k + 1) * head_dim], wo[k, :, cols])
                    + dot_nn(mix[:, (near + k) * head_dim:(near + k + 1) * head_dim], wo[near + k, :, cols]))
            acc[:, cols] = part if first else acc[:, cols] + part
            return carry

        to_core(2, k).wait_recv()
        lax.fori_loop(0, dim // 512, step, 0)

    project(0, True)
    project(1, False)
    project(2, False)
    pass_last(2)
    project(3, False)
    stores["wo"].start()
    for k in range(2):
        early(k, False).wait_recv()
        early(k, True).start()
    stores["normed"].wait()

    def norm2(i, carry):
        resid = (x_buf[seq_rows(i), :].astype(F32) + acc[seq_rows(i), :]).astype(BF16)
        x_buf[seq_rows(i), :] = resid
        n_buf[seq_rows(i), :] = norm_rows(resid, gain2_ref)
        return carry

    lax.fori_loop(0, batch, norm2, 0)
    stores["resid"].start()
    stores["gated"].start()
    for cp in mixed_stores:
        cp.wait()
    for name in ("wq", "wo", "kv", "query", "resid", "gated"):
        stores[name].wait()
    for k in range(2):
        early(k, False).wait_send()
        early(k, True).wait_send()
        early(k, True).wait_recv()
    for a in range(3):
        to_side(a).wait_send()
        to_back(a).wait_send()
        for k in range(2):
            onward(a, k).wait_send()
        for k in range(near):
            to_core(a, k).wait_send()


def front_layer(prefix_len, valid_len, k_pos, cos_t, sin_t, attn_norm, mlp_norm, hidden, grad, w_query, w_key, w_value, w_out, batch, tp):
    rows, dim = hidden.shape
    head_dim = w_key.shape[1]
    shard = rows // batch
    total = tp * shard
    anyspace = pl.BlockSpec(memory_space=pl.ANY)
    vmem = pl.BlockSpec(memory_space=pltpu.VMEM)
    dma = pltpu.SemaphoreType.DMA

    def shape(*dims):
        return jax.ShapeDtypeStruct(dims, BF16)

    return pl.pallas_call(
        functools.partial(front_kernel, batch=batch),
        out_shape=(shape(rows, dim), shape(tp, dim, head_dim), shape(tp, head_dim, dim), shape(tp, rows, 2 * head_dim),
                   shape(tp, rows, head_dim), shape(rows, tp * head_dim), shape(rows, dim), shape(rows, dim), shape(tp * rows, dim)),
        in_specs=[pl.BlockSpec(memory_space=pltpu.SMEM)] * 2 + [vmem] * 5 + [anyspace] * 6,
        out_specs=(anyspace,) * 9,
        scratch_shapes=[pltpu.VMEM((rows, dim), BF16), pltpu.VMEM((rows, dim), BF16), pltpu.VMEM((dim, 2 * head_dim), BF16),
                        pltpu.VMEM((tp, dim, head_dim), BF16), pltpu.VMEM((tp, head_dim, dim), BF16),
                        pltpu.VMEM((tp, rows, 2 * head_dim), BF16), pltpu.VMEM((tp, rows, head_dim), BF16),
                        pltpu.VMEM((2, tp // 2 * shard, total), BF16), pltpu.VMEM((rows, tp * head_dim), BF16), pltpu.VMEM((rows, dim), F32),
                        dma((5,)), dma((15,)), dma((3, 8)), dma((3, 8)), dma((4,)), dma((4,))],
        compiler_params=pltpu.CompilerParams(vmem_limit_bytes=62 << 20, collective_id=2, has_side_effects=True),
        cost_estimate=pl.CostEstimate(flops=8 * rows * dim * tp * head_dim, bytes_accessed=60 << 20, transcendentals=tp * rows * total),
        name="front",
    )(prefix_len, valid_len, k_pos, cos_t, sin_t, attn_norm.reshape(1, dim), mlp_norm.reshape(1, dim), hidden, grad, w_query, w_key, w_value, w_out)


def attention_backward(lens, cos_t, sin_t, query, kv_all, d_mixed, batch, group=8):
    heads, rows, head_dim = query.shape
    near = kv_all.shape[0] // 2
    shard = rows // batch
    total = 2 * near * shard
    q_spec = pl.BlockSpec((group, shard, head_dim), lambda s, g, *_: (g, s, 0))
    kv_spec = pl.BlockSpec((near, shard, 2 * head_dim), lambda s, g, *_: (0, s, 0))
    table = pl.BlockSpec((shard, head_dim // 2), lambda s, g, *_: (0, 0))
    kv_shape = jax.ShapeDtypeStruct((near, rows, 2 * head_dim), BF16)
    return pl.pallas_call(
        attn_bwd_kernel,
        out_shape=(jax.ShapeDtypeStruct((heads, rows, head_dim), BF16), kv_shape, kv_shape),
        grid_spec=pltpu.PrefetchScalarGridSpec(
            num_scalar_prefetch=1, grid=(batch, heads // group),
            in_specs=[table, table, q_spec, pl.BlockSpec((2 * near, shard, 2 * head_dim), lambda s, g, *_: (0, s, 0)), pl.BlockSpec((shard, group * head_dim), lambda s, g, *_: (s, g))],
            out_specs=(q_spec, kv_spec, kv_spec),
            scratch_shapes=[pltpu.VMEM((total, 2 * head_dim), F32)]),
        compiler_params=pltpu.CompilerParams(dimension_semantics=("arbitrary", "arbitrary"), vmem_limit_bytes=62 << 20),
        cost_estimate=pl.CostEstimate(flops=10 * heads * rows * total * head_dim, bytes_accessed=20 << 20, transcendentals=heads * rows * total),
        name="attn_bwd",
    )(lens, cos_t, sin_t, query, kv_all, d_mixed)


def gated_tile(z, g, w_g, w_u, w_d):
    gate = dot_nn(z, w_g)
    upper = dot_nn(z, w_u)
    d_act = dot_nt(g, w_d).astype(BF16).astype(F32)
    sq = gate * gate
    th = jnp.tanh(gate * (GELU_C + (GELU_C * GELU_K) * sq))
    half = 0.5 + 0.5 * th
    gelu = gate * half
    slope = half + gate * (0.5 - 0.5 * (th * th)) * (GELU_C + (3.0 * GELU_C * GELU_K) * sq)
    return (gelu * upper).astype(BF16), (d_act * upper * slope).astype(BF16), (d_act * gelu).astype(BF16)


def gated_kernel(z_own, g_own, g_early, wg_hbm, wu_hbm, wd_hbm, z_all, g_all, act, d_gate, d_up, diag_in,
                 wg, wu, wd, z_buf, g_buf, outs, st, from_core, far_send, far_recv, diag_send, diag_recv, w_sem, in_sem, own_sem, out_sem, send, recv, send0, recv0, *, bn):
    rows, dim = z_own.shape
    width = wg_hbm.shape[1]
    steps = width // bn
    piece = rows // 4
    me, core, side, back = neighbours()
    corner = flip(side, 4)
    own = (z_own, g_own)
    full = (z_all, g_all)

    def part(slot, q):
        return pl.ds(pl.multiple_of(slot * rows + q * piece, 16), piece)

    def link_rows(u, path):
        turn = u // 2
        diag = turn % 2
        if path == 0:
            return side + (corner - side) * diag, (u % 2) + 2 * (turn // 2) + diag * 2
        return back + (corner - back) * diag, (u % 2) + 2 - 2 * (turn // 2) - diag * 2

    def link_copy(u, path, a):
        turn = u // 2
        peer = side if path == 0 else back
        sems = (send.at[path, u, a], recv.at[path, u, a])
        if turn == 1:
            slot = back if path == 0 else side
            q = (2 if path == 0 else 0) + u % 2
            return remote(full[a].at[part(slot, q)], full[a].at[part(slot, q)], *sems, peer)
        q = u % 2 + (2 * (turn // 2) if path == 0 else 2 - 2 * (turn // 2))
        return remote(own[a].at[pl.ds(q * piece, piece)], full[a].at[part(me, q)], *sems, peer)

    def core_copy(u, path, a):
        slot, q = link_rows(u, path)
        return remote(full[a].at[part(slot, q)], full[a].at[part(slot, q)], send.at[2 + path, u, a], recv.at[2 + path, u, a], core)

    def own_copy(a):
        return remote(own[a], full[a].at[pl.ds(pl.multiple_of(me * rows, 16), rows)], send0.at[a], recv0.at[a], core)

    def weight_copies(n):
        cols = pl.ds(pl.multiple_of(n * bn, 128), bn)
        return [pltpu.make_async_copy(wg_hbm.at[:, cols], wg.at[:, cols], w_sem.at[0, n]),
                pltpu.make_async_copy(wu_hbm.at[:, cols], wu.at[:, cols], w_sem.at[1, n]),
                pltpu.make_async_copy(wd_hbm.at[cols], wd.at[cols], w_sem.at[2, n])]

    bufs = (z_buf, g_buf)
    own_in = [pltpu.make_async_copy(own[a], bufs[a], own_sem.at[a]) for a in range(2)]
    own_out = [pltpu.make_async_copy(bufs[a], full[a].at[pl.ds(pl.multiple_of(me * rows, 16), rows)], own_sem.at[2 + a]) for a in range(2)]
    for cp in own_in:
        cp.start()
    for n in range(steps):
        for cp in weight_copies(n):
            cp.start()
    enter((core, side, back))
    for u in range(2):
        for path in range(2):
            for a in ((0,) if u == 0 else (0, 1)):
                link_copy(u, path, a).start()
        if u == 0:
            for a in range(2):
                own_copy(a).start()

    def out_copies(slot, s_rows, n):
        cols = pl.ds(pl.multiple_of(n * bn, 128), bn)
        return [pltpu.make_async_copy(outs.at[slot, k, pl.ds(i * piece, piece)], ref.at[s_rows[i], cols], out_sem.at[slot, k, i])
                for k, ref in enumerate((act, d_gate, d_up)) for i in range(4)]

    def stage_rows(s):
        late = (s + 6) // 8
        u = (s - 2) * late
        first = me + (core - me) * s * (1 - late)
        (slot_x, q_x), (slot_y, q_y) = link_rows(u, 0), link_rows(u, 1)
        base_x, base_y = slot_x * rows + q_x * piece, slot_y * rows + q_y * piece
        pair_x, pair_y = flip(slot_x, 1) * rows + q_x * piece, flip(slot_y, 1) * rows + q_y * piece
        starts = [(1 - late) * (first * rows + i * piece) + late * base for i, base in enumerate((base_x, base_y, pair_x, pair_y))]
        return [pl.ds(pl.multiple_of(st, 16), piece) for st in starts]

    def kinds(u):
        return (0,) if u == 0 else (0, 1)

    def pass_on(u):
        for path in range(2):
            for a in kinds(u):
                link_copy(u, path, a).wait_recv()
                core_copy(u, path, a).start()

    def far_copy(j):
        return remote(st.at[0, j], from_core.at[j], far_send.at[j], far_recv.at[j], core)

    def diag_copy(k, j):
        half = rows // 2
        return remote(st.at[1, j, pl.ds(k * half, half)], diag_in.at[k, :, pl.ds(pl.multiple_of(j * bn, 128), bn)],
                      diag_send.at[k, j], diag_recv.at[k, j], (side, back)[k])

    def down_diagonal():
        for slot in range(2):
            for cp in out_copies(slot, stage_rows(5), 0):
                cp.wait()
        loads = [pltpu.make_async_copy(act.at[pl.ds(pl.multiple_of(dev * rows, 16), rows)], bufs[a], in_sem.at[a, 0])
                 for a, dev in enumerate((flip(corner, 1), corner))]
        for cp in loads:
            cp.start()

        def theirs(j, carry):
            st[0, j] = dot_nn(z_buf[...], wd[:, pl.ds(pl.multiple_of(j * bn, 128), bn)]).astype(BF16)
            far_copy(j).start()
            return carry

        def mine(j, carry):
            far_copy(j).wait_recv()
            total = dot_nn(g_buf[...], wd[:, pl.ds(pl.multiple_of(j * bn, 128), bn)]) + from_core[j].astype(F32)
            st[1, j] = total.astype(BF16)
            for k in range(2):
                diag_copy(k, j).start()
            return carry

        loads[0].wait()
        lax.fori_loop(0, dim // bn, theirs, 0)
        loads[1].wait()
        lax.fori_loop(0, dim // bn, mine, 0)

    def compute(s):
        s_rows = stage_rows(s)

        def block(n, carry):
            step = s * steps + n
            slot = step % 2

            @pl.when((step >= 2) & (step // 2 != 6 * steps // 2))
            def _():
                for cp in out_copies(slot, s_rows, n):
                    cp.wait()

            @pl.when(s == 0)
            def _():
                for cp in weight_copies(n):
                    cp.wait()

            @pl.when((s == 6) & (n == steps - 1))
            def _():
                pass_on(5)

            cols = pl.ds(pl.multiple_of(n * bn, 128), bn)
            res = gated_tile(z_buf[...], g_buf[...], wg[:, cols], wu[:, cols], wd[cols, :])
            for k in range(3):
                outs[slot, k] = res[k]
            for cp in out_copies(slot, s_rows, n):
                cp.start()
            return carry

        lax.fori_loop(0, steps, block, 0)

    def stage(s, carry):
        @pl.when(s == 0)
        def _():
            for cp in own_in:
                cp.wait()
            for cp in own_out:
                cp.start()

        @pl.when(s == 1)
        def _():
            for cp in own_out:
                cp.wait()
            for a in range(2):
                own_copy(a).wait_recv()

        for u in range(6):
            @pl.when(s == u + 2)
            def _(u=u):
                if u < 5:
                    pass_on(u)
                if u == 4:
                    down_diagonal()
                if u < 2:
                    for path in range(2):
                        for a in range(2):
                            link_copy(u + 2, path, a).start()
                if u == 1:
                    for later in (4, 5):
                        for path in range(2):
                            for a in range(2):
                                link_copy(later, path, a).start()
                for path in range(2):
                    for a in kinds(u):
                        core_copy(u, path, a).wait_recv()

        @pl.when(s >= 1)
        def _():
            s_rows = stage_rows(s)
            copies = [pltpu.make_async_copy(full[a].at[s_rows[i]], bufs[a].at[pl.ds(i * piece, piece)], in_sem.at[a, i])
                      for a in range(2) for i in range(4)]
            for cp in copies:
                cp.start()
            for cp in copies:
                cp.wait()

        compute(s)
        return carry

    lax.fori_loop(0, 8, stage, 0)
    last = stage_rows(7)
    for slot in range(2):
        for cp in out_copies(slot, last, 0):
            cp.wait()
    for j in range(dim // bn):
        far_copy(j).wait_send()
        for k in range(2):
            diag_copy(k, j).wait_send()
            diag_copy(k, j).wait_recv()
    for a in range(2):
        own_copy(a).wait_send()
        for path in range(2):
            for u in range(a, 6):
                link_copy(u, path, a).wait_send()
                core_copy(u, path, a).wait_send()


def gated_layer(z_own, g_own, g_early, w_gate, w_up, w_down, tp, bn=512):
    rows, dim = z_own.shape
    width = w_gate.shape[1]
    total = rows * tp
    anyspace = pl.BlockSpec(memory_space=pl.ANY)
    gathered = jax.ShapeDtypeStruct((total, dim), BF16)
    made = jax.ShapeDtypeStruct((total, width), BF16)
    dma = pltpu.SemaphoreType.DMA
    return pl.pallas_call(
        functools.partial(gated_kernel, bn=bn),
        out_shape=(gathered, gathered, made, made, made, jax.ShapeDtypeStruct((2, rows // 2, dim), BF16)),
        in_specs=[anyspace] * 6,
        out_specs=(anyspace,) * 6,
        input_output_aliases={2: 1},
        scratch_shapes=[pltpu.VMEM((dim, width), BF16), pltpu.VMEM((dim, width), BF16), pltpu.VMEM((width, dim), BF16),
                        pltpu.VMEM((rows, dim), BF16), pltpu.VMEM((rows, dim), BF16), pltpu.VMEM((2, 3, rows, bn), BF16),
                        pltpu.VMEM((2, dim // bn, rows, bn), BF16), pltpu.VMEM((dim // bn, rows, bn), BF16),
                        dma((dim // bn,)), dma((dim // bn,)), dma((2, dim // bn)), dma((2, dim // bn)), dma((3, width // bn)), dma((2, 4)), dma((4,)), dma((2, 3, 4)), dma((4, 6, 2)), dma((4, 6, 2)), dma((2,)), dma((2,))],
        compiler_params=pltpu.CompilerParams(vmem_limit_bytes=67043328, collective_id=0, has_side_effects=True),
        cost_estimate=pl.CostEstimate(flops=6 * total * dim * width, bytes_accessed=200 << 20, transcendentals=total * width),
        name="gated",
    )(z_own, g_own, g_early, w_gate, w_up, w_down)


def back_kernel(act, d_gate, d_up, z_all, diag_in, wg_hbm, wu_hbm, wd_hbm, own_out, x_in, y_in, g_gate,
                wa, wb, lhs, st, from_core, from_diag, own_st, in_sem, z_sem, w_sem, l_sem, o_sem, c_send, c_recv, d_send, d_recv, f_send, f_recv, *, rows, bn):
    dim, width = wg_hbm.shape
    steps = dim // bn
    half = rows // 2
    me, core, side, back = neighbours()

    def cols(j):
        return pl.ds(pl.multiple_of(j * bn, 128), bn)

    def shard_of(phase, t):
        if phase == 0:
            return 1 + t // 2, 1 - t % 2
        ge = [(t + 8 - k) // 8 for k in range(8)]
        return ge[2] + ge[3] - ge[5] + 2 * ge[6], 1 - ge[1] + ge[2] - ge[4] + ge[6] - ge[7]

    def lhs_copies(phase, t):
        pair, theirs = shard_of(phase, t)
        dev = me + (1 - pair // 2) * (side - me) + (1 - pair % 2) * (back - me)
        dev = dev + theirs * (flip(dev, 1) - dev)
        src = pl.ds(pl.multiple_of(dev * rows, 16), rows)
        refs = (act,) if phase == 0 else (d_gate, d_up)
        return [pltpu.make_async_copy(ref.at[src], lhs.at[t % 2, k], l_sem.at[t % 2, k]) for k, ref in enumerate(refs)]

    def weight_copy(k, j):
        if k == 0:
            return pltpu.make_async_copy(wd_hbm.at[:, cols(j)], wa.at[pl.ds(0, width), cols(j)], w_sem.at[0, j])
        src, dst = (wg_hbm, wb) if k == 1 else (wu_hbm, wa)
        return pltpu.make_async_copy(src.at[cols(j)], dst.at[cols(j)], w_sem.at[k, j])

    def core_copy(pair, j):
        return remote(st.at[0, j], from_core.at[pair, j], c_send.at[j], c_recv.at[pair, j], core)

    def diag_copy(phase, k, j):
        return remote(st.at[1, j, pl.ds(k * half, half)], from_diag.at[phase, k, j], d_send.at[k, j], d_recv.at[phase, k, j], (side, back)[k])

    def final_copy(phase, k, j):
        return remote(st.at[2 + k, j], (x_in, y_in)[k].at[phase, :, cols(j)], f_send.at[k, j], f_recv.at[phase, k, j], (side, back)[k])

    def own_copy(phase, j):
        return pltpu.make_async_copy(own_st.at[j % 2], own_out.at[phase, :, cols(j)], o_sem.at[j % 2])

    def product(phase, slot, j):
        if phase == 0:
            return dot_nn(lhs[slot, 0], wa[:width, cols(j)])
        return dot_nt(lhs[slot, 0], wb[cols(j), :]) + dot_nt(lhs[slot, 1], wa[cols(j), :])

    def diag_load(k, j):
        return pltpu.make_async_copy(diag_in.at[k, :, cols(j)], from_diag.at[0, k, j], in_sem.at[k, j])

    for cp in lhs_copies(0, 0):
        cp.start()
    for j in range(steps):
        weight_copy(0, j).start()
    for k in range(2):
        for j in range(steps):
            diag_load(k, j).start()
    enter((core, side, back))

    def tiles(body):
        def step(j, carry):
            body(j)
            return carry

        lax.fori_loop(0, steps, step, 0)

    for phase in (0, 1):
        def step(t, carry, phase=phase):
            for cp in lhs_copies(phase, t):
                cp.wait()

            last = 5 if phase == 0 else 7

            @pl.when(t < last)
            def _():
                for cp in lhs_copies(phase, t + 1):
                    cp.start()

            if phase == 0:
                @pl.when(t == 1)
                def _():
                    for j in range(steps):
                        weight_copy(1, j).start()

                @pl.when(t == last)
                def _():
                    for cp in lhs_copies(1, 0):
                        cp.start()

            theirs = (t % 2 == 0) if phase == 0 else ((t % 6 == 0) | (t // 2 == 1))

            @pl.when(theirs)
            def _():
                pair = shard_of(phase, t)[0]

                def body(j):
                    @pl.when(t == 0)
                    def _():
                        for k in ((0,) if phase == 0 else (1, 2)):
                            weight_copy(k, j).wait()

                    if phase == 0:
                        @pl.when(t > 0)
                        def _():
                            core_copy(0, j).wait_send()
                    else:
                        core_copy(0, j).wait_send()
                    st[0, j] = product(phase, t % 2, j).astype(BF16)
                    core_copy(pair, j).start()

                tiles(body)

            if phase == 1:
                @pl.when(t == 1)
                def _():
                    def body(j):
                        core_copy(0, j).wait_recv()
                        st[1, j] = (product(phase, 1, j) + from_core[0, j].astype(F32)).astype(BF16)
                        for k in range(2):
                            diag_copy(phase, k, j).start()

                    tiles(body)

            for k in range(2):
                @pl.when(t == (1 + 2 * k if phase == 0 else 5 - k))
                def _(k=k):
                    def body(j):
                        core_copy(1 + k, j).wait_recv()
                        if phase == 0:
                            diag_load(1 - k, j).wait()
                        else:
                            diag_copy(phase, 1 - k, j).wait_recv()
                            final_copy(0, k, j).wait_send()
                        total = product(phase, 1 if phase == 0 else 1 - k, j) + from_core[1 + k, j].astype(F32)
                        came = from_diag[phase, 1 - k, j].astype(F32)
                        split = slice(half, rows) if k == 0 else slice(0, half)
                        rest = slice(0, half) if k == 0 else slice(half, rows)
                        st[2 + k, j, split, :] = (total[split] + came).astype(BF16)
                        st[2 + k, j, rest, :] = total[rest].astype(BF16)
                        final_copy(phase, k, j).start()

                    tiles(body)

            @pl.when(t == last)
            def _():
                def body(j):
                    core_copy(3, j).wait_recv()

                    @pl.when(j >= 2)
                    def _():
                        own_copy(phase, j).wait()

                    own_st[j % 2] = product(phase, 1, j) + from_core[3, j].astype(F32)
                    own_copy(phase, j).start()

                tiles(body)
                for j in (0, 1):
                    own_copy(phase, j).wait()
                if phase == 0:
                    for j in range(steps):
                        weight_copy(2, j).start()

            return carry

        lax.fori_loop(0, 6 if phase == 0 else 8, step, 0)

    first = z_all.shape[0] - 2 * rows

    def z_copy(j, c):
        return pltpu.make_async_copy(z_all.at[pl.ds(first + c * rows, rows), cols(j)], lhs.at[0, c, :, cols(j)], z_sem.at[j, c])

    def gate_copy(j):
        return pltpu.make_async_copy(d_gate.at[pl.ds(first, 2 * rows), cols(j)], wa.at[pl.ds(0, 2 * rows), cols(j)], w_sem.at[0, j])

    def grad_copy(i, j):
        slot = j % 2
        return pltpu.make_async_copy(own_st.at[slot, pl.ds(0, bn)], g_gate.at[cols(i), cols(j)], o_sem.at[slot])

    for j in range(steps):
        for c in range(2):
            z_copy(j, c).start()
        gate_copy(j).start()

    def grad_tile(step, carry):
        i, j = step // steps, step % steps

        @pl.when(i == 0)
        def _():
            gate_copy(j).wait()

        @pl.when(j == 0)
        def _():
            for c in range(2):
                z_copy(i, c).wait()

        @pl.when(step >= 2)
        def _():
            grad_copy(i, j).wait()

        own_st[j % 2, :bn] = dot_tn(lhs[0, :, :, cols(i)].reshape(2 * rows, bn), wa[:2 * rows, cols(j)])
        grad_copy(i, j).start()
        return carry

    lax.fori_loop(0, steps * steps, grad_tile, 0)
    for j in range(2):
        grad_copy(0, j).wait()
    for j in range(steps):
        core_copy(0, j).wait_send()
        for k in range(2):
            diag_copy(1, k, j).wait_send()
            final_copy(1, k, j).wait_send()
            for phase in (0, 1):
                final_copy(phase, k, j).wait_recv()


def back_layer(act, d_gate, d_up, z_all, diag_in, w_gate, w_up, w_down, tp, bn=512):
    total, width = act.shape
    dim = w_gate.shape[0]
    rows = total // tp
    steps = dim // bn
    anyspace = pl.BlockSpec(memory_space=pl.ANY)
    dma = pltpu.SemaphoreType.DMA
    came = jax.ShapeDtypeStruct((2, rows, dim), BF16)
    return pl.pallas_call(
        functools.partial(back_kernel, rows=rows, bn=bn),
        out_shape=(jax.ShapeDtypeStruct((2, rows, dim), F32), came, came, jax.ShapeDtypeStruct((dim, width), F32)),
        in_specs=[anyspace] * 8,
        out_specs=(anyspace,) * 4,
        scratch_shapes=[pltpu.VMEM((width, dim), BF16), pltpu.VMEM((dim, width), BF16), pltpu.VMEM((2, 2, rows, width), BF16),
                        pltpu.VMEM((4, steps, rows, bn), BF16), pltpu.VMEM((4, steps, rows, bn), BF16),
                        pltpu.VMEM((2, 2, steps, rows // 2, bn), BF16), pltpu.VMEM((2, rows, bn), F32),
                        dma((2, steps)), dma((steps, 2)), dma((3, steps)), dma((2, 2)), dma((2,)), dma((steps,)), dma((4, steps)),
                        dma((2, steps)), dma((2, 2, steps)), dma((2, steps)), dma((2, 2, steps))],
        compiler_params=pltpu.CompilerParams(vmem_limit_bytes=67043328, collective_id=1, has_side_effects=True),
        cost_estimate=pl.CostEstimate(flops=6 * total * dim * width, bytes_accessed=200 << 20, transcendentals=0),
        name="back",
    )(act, d_gate, d_up, z_all, diag_in, w_gate, w_up, w_down)


def norm_back(x, gain, d_out):
    inv_rms = lax.rsqrt(jnp.mean(x * x, axis=-1, keepdims=True) + NORM_EPS)
    unit = x * inv_rms
    scaled = d_out * (1.0 + gain.astype(F32))
    return inv_rms * (scaled - unit * jnp.mean(unit * scaled, axis=-1, keepdims=True)), d_out * unit


def join_kernel(own_ref, x_ref, y_ref, resid_ref, grad_ref, gain_ref, wo_ref, mixed_ref,
                out_ref, d_resid_ref, g_gain_ref, d_mixed_ref, g_out_ref, keep, *, joins):
    step = pl.program_id(0)
    bm = resid_ref.shape[0]

    @pl.when(step == 0)
    def _():
        g_gain_ref[...] = jnp.zeros_like(g_gain_ref)

    @pl.when(step < joins)
    def _():
        mlp_sum, d_gated = [own_ref[k] + x_ref[k].astype(F32) + y_ref[k].astype(F32) for k in range(2)]
        resid = resid_ref[...].astype(F32)
        out_ref[...] = (resid + mlp_sum).astype(BF16)
        d_norm, terms = norm_back(resid, gain_ref[...], d_gated.astype(BF16).astype(F32))
        d_resid = (grad_ref[...].astype(F32) + d_norm).astype(BF16)
        d_resid_ref[...] = d_resid
        keep[pl.ds(pl.multiple_of(step * bm, 16), bm), :] = d_resid
        g_gain_ref[...] += jnp.sum(terms, axis=0, keepdims=True)

    @pl.when(step >= joins)
    def _():
        d_mixed_ref[...] = dot_nt(keep[...], wo_ref[...]).astype(BF16)
        g_out_ref[...] = dot_tn(mixed_ref[...], keep[...])


def join_layer(own_part, x_part, y_part, resid, grad_out, gain, wo_all, mixed, bm=96, bn=512):
    rows, dim = resid.shape
    width = mixed.shape[1]
    joins = rows // bm
    pair = pl.BlockSpec((2, bm, dim), lambda i: (0, jnp.minimum(i, joins - 1), 0))
    row = pl.BlockSpec((bm, dim), lambda i: (jnp.minimum(i, joins - 1), 0))
    one = pl.BlockSpec((1, dim), lambda i: (0, 0))
    col = pl.BlockSpec((rows, bn), lambda i: (0, jnp.maximum(i - joins, 0)))
    block = pl.BlockSpec((bn, dim), lambda i: (jnp.maximum(i - joins, 0), 0))
    act = jax.ShapeDtypeStruct((rows, dim), BF16)
    return pl.pallas_call(
        functools.partial(join_kernel, joins=joins),
        out_shape=(act, act, jax.ShapeDtypeStruct((1, dim), F32), jax.ShapeDtypeStruct((rows, width), BF16),
                   jax.ShapeDtypeStruct((width, dim), F32)),
        grid=(joins + width // bn,),
        in_specs=[pair, pair, pair, row, row, one, block, col],
        out_specs=(row, row, one, col, block),
        scratch_shapes=[pltpu.VMEM((rows, dim), BF16)],
        compiler_params=pltpu.CompilerParams(dimension_semantics=("arbitrary",), vmem_limit_bytes=62 << 20),
        cost_estimate=pl.CostEstimate(flops=4 * rows * dim * width, bytes_accessed=60 << 20, transcendentals=rows),
        name="join",
    )(own_part, x_part, y_part, resid, grad_out, gain.reshape(1, dim), wo_all, mixed)


def finish_kernel(kv_ref, side_ref, back_ref, cos_ref, sin_ref, normed_ref, wk_ref, wv_ref, part_ref, hidden_ref, d_resid_ref, gain_ref,
                  g_key_ref, g_value_ref, out_ref, g_gain_ref):
    head_dim = wk_ref.shape[1]
    half_dim = head_dim // 2
    d_kv = (kv_ref[...] + side_ref[...].astype(F32) + back_ref[...].astype(F32)).astype(BF16)
    first, second = d_kv[:, :half_dim].astype(F32), d_kv[:, half_dim:head_dim].astype(F32)
    cos_t, sin_t = cos_ref[...], sin_ref[...]
    d_key = jnp.concatenate([first * cos_t + second * sin_t, second * cos_t - first * sin_t], axis=1).astype(BF16)
    d_value = d_kv[:, head_dim:]
    d_normed = (part_ref[...] + dot_nt(d_key, wk_ref[...]) + dot_nt(d_value, wv_ref[...])).astype(BF16).astype(F32)
    d_norm, terms = norm_back(hidden_ref[...].astype(F32), gain_ref[...], d_normed)
    out_ref[...] = (d_resid_ref[...].astype(F32) + d_norm).astype(BF16)
    g_key = dot_tn(normed_ref[...], d_key)
    g_value = dot_tn(normed_ref[...], d_value)
    g_gain = jnp.sum(terms, axis=0, keepdims=True)

    @pl.when(pl.program_id(0) == 0)
    def _():
        g_key_ref[...] = g_key
        g_value_ref[...] = g_value
        g_gain_ref[...] = g_gain

    @pl.when(pl.program_id(0) > 0)
    def _():
        g_key_ref[...] += g_key
        g_value_ref[...] += g_value
        g_gain_ref[...] += g_gain


def finish_layer(kv_own, kv_side, kv_back, cos_t, sin_t, normed, w_key, w_value, part, hidden, d_resid, gain):
    rows, dim = hidden.shape
    shard, half_dim = cos_t.shape
    head_dim = w_key.shape[1]

    def row(width):
        return pl.BlockSpec((shard, width), lambda i: (i, 0))

    def whole(*shape):
        return pl.BlockSpec(shape, lambda i: (0, 0))

    kv, act, table, weight, one = row(2 * head_dim), row(dim), whole(shard, half_dim), whole(dim, head_dim), whole(1, dim)
    grad = jax.ShapeDtypeStruct((dim, head_dim), F32)
    return pl.pallas_call(
        finish_kernel,
        out_shape=(grad, grad, jax.ShapeDtypeStruct((rows, dim), BF16), jax.ShapeDtypeStruct((1, dim), F32)),
        grid=(rows // shard,),
        in_specs=[kv, kv, kv, table, table, act, weight, weight, act, act, act, one],
        out_specs=(weight, weight, act, one),
        compiler_params=pltpu.CompilerParams(dimension_semantics=("arbitrary",), vmem_limit_bytes=62 << 20),
        cost_estimate=pl.CostEstimate(flops=8 * rows * dim * head_dim, bytes_accessed=24 << 20, transcendentals=rows),
        name="finish",
    )(kv_own, kv_side, kv_back, cos_t, sin_t, normed, w_key, w_value, part, hidden, d_resid, gain.reshape(1, dim))


def product_kernel(a_ref, b_ref, o_ref):
    o_ref[...] = dot_tn(a_ref[...], b_ref[...])


def weight_grad(a, b, bm=1024, bn=512):
    rows, m = a.shape
    n = b.shape[1]
    return pl.pallas_call(
        product_kernel,
        out_shape=jax.ShapeDtypeStruct((m, n), F32),
        grid=(m // bm, n // bn),
        in_specs=[pl.BlockSpec((rows, bm), lambda i, j: (0, i)), pl.BlockSpec((rows, bn), lambda i, j: (0, j))],
        out_specs=pl.BlockSpec((bm, bn), lambda i, j: (i, j)),
        compiler_params=pltpu.CompilerParams(dimension_semantics=("arbitrary", "arbitrary"), vmem_limit_bytes=62 << 20),
        cost_estimate=pl.CostEstimate(flops=2 * rows * m * n, bytes_accessed=110 << 20, transcendentals=0),
        name="weight_grad",
    )(a, b)


def rest_kernel(a_ref, b_ref, part_ref, o_ref):
    o_ref[...] = part_ref[...] + dot_tn(a_ref[...], b_ref[...])


def weight_grad_rest(a, b, part, count, bm=1024, bn=512):
    m, n = part.shape
    out = pl.BlockSpec((bm, bn), lambda i, j: (i, j))
    return pl.pallas_call(
        rest_kernel,
        out_shape=jax.ShapeDtypeStruct((m, n), F32),
        grid=(m // bm, n // bn),
        in_specs=[pl.BlockSpec((count, bm), lambda i, j: (0, i)), pl.BlockSpec((count, bn), lambda i, j: (0, j)), out],
        out_specs=out,
        compiler_params=pltpu.CompilerParams(dimension_semantics=("arbitrary", "arbitrary"), vmem_limit_bytes=62 << 20),
        cost_estimate=pl.CostEstimate(flops=2 * count * m * n, bytes_accessed=80 << 20, transcendentals=0),
        name="weight_grad_rest",
    )(a, b, part)


def hop_diagonal(diag):
    half = diag.shape[0] // 2
    return swap(diag[:half], 2), swap(diag[half:], 4)


def hop_near(side, back, came_side, came_back):
    half = side.shape[0] // 2
    kind = came_side.dtype
    side = jnp.concatenate([side[:half], side[half:] + came_back.astype(F32)], axis=0).astype(kind)
    back = jnp.concatenate([back[:half] + came_side.astype(F32), back[half:]], axis=0).astype(kind)
    return side, back


def solution(mesh):
    tp_size = mesh.shape["tp"]
    act_spec = P("dp", "tp", None)
    in_specs = (act_spec, act_spec, P("dp"), P("dp"), P(None), P(None, "tp"), P(None, None), P(None, None), P("tp", None), P(None), P(None, "tp"), P(None, "tp"), P("tp", None))
    out_specs = (act_spec, act_spec, P("dp"), P("dp", "tp"), P("dp", None), P("dp", None), P(("dp", "tp"), None), P("dp"), P("dp", "tp"), P("dp", "tp"), P(("dp", "tp"), None))

    def layer(hidden, grad_out, prefix_len, valid_len, attn_norm, w_query, w_key, w_value, w_out, mlp_norm, w_gate, w_up, w_down):
        batch, shard, dim = hidden.shape
        head_dim = w_key.shape[1]
        rows = batch * shard
        me = lax.axis_index("tp")
        starts = (me ^ jnp.array([0, 2, 4, 6, 1, 3, 5, 7], jnp.int32)) * shard
        k_pos = (starts[:, None] + jnp.arange(shard, dtype=jnp.int32)).reshape(1, tp_size * shard)
        cos_own, sin_own = rope_tables(me * shard + jnp.arange(shard), head_dim)
        hidden = hidden.reshape(rows, dim)
        grad_out = grad_out.reshape(rows, dim)
        normed, wq_all, wo_all, kv_all, query, mixed, resid, gated_in, grad_early = front_layer(
            prefix_len, valid_len, k_pos, cos_own, sin_own, attn_norm, mlp_norm, hidden, grad_out, w_query, w_key, w_value, w_out, batch, tp_size)
        wo_all = wo_all.reshape(tp_size * head_dim, dim)

        gated_all, grad_all, act, d_gate, d_upper, diag_in = gated_layer(gated_in, grad_out, grad_early, w_gate, w_up, w_down, tp_size)
        own_part, x_part, y_part, g_gate_part = back_layer(act, d_gate, d_upper, gated_all, diag_in, w_gate, w_up, w_down, tp_size)
        hidden_out, d_resid, g_mlp_norm_part, d_mixed, g_out_part = join_layer(
            own_part, x_part, y_part, resid, grad_out, mlp_norm, wo_all, mixed)
        g_out = lax.psum_scatter(g_out_part, "tp", scatter_dimension=0, tiled=True)
        lens_back = jnp.concatenate([jnp.stack([prefix_len, valid_len, jnp.full((batch,), me, jnp.int32)]),
                                     jnp.broadcast_to(starts[:, None], (tp_size, batch))])
        d_q_raw, dkv_near, dkv_far = attention_backward(lens_back, cos_own, sin_own, query, kv_all, d_mixed, batch)
        near = tp_size // 2
        came_kv = swap(dkv_far, 1)
        g_far = jnp.einsum("kte,td->ked", d_q_raw[near:], normed, preferred_element_type=F32)
        came_kv, g_far = lax.optimization_barrier((came_kv, g_far))
        came_q = swap(g_far, 1)
        kv_own, kv_side, kv_back, kv_diag = [dkv_near[k].astype(F32) + came_kv[k].astype(F32) for k in range(4)]
        kv_came = hop_diagonal(kv_diag.astype(BF16))
        d_normed_q = jnp.einsum("hte,hde->td", d_q_raw, wq_all, preferred_element_type=F32)
        kv_came, d_normed_q = lax.optimization_barrier((kv_came, d_normed_q))
        kv_next = hop_near(kv_side, kv_back, *kv_came)
        kv_last = (swap(kv_next[0], 2), swap(kv_next[1], 4))
        came_q, dq_near = lax.optimization_barrier((came_q, d_q_raw[:near]))
        g_query_sum = jnp.einsum("kte,td->ked", dq_near, normed, preferred_element_type=F32) + came_q
        g_query_sum, act = lax.optimization_barrier((g_query_sum, act))
        q_came = hop_diagonal(g_query_sum[3])
        g_down = weight_grad(act, grad_all)
        kv_last, q_came, g_down = lax.optimization_barrier((kv_last, q_came, g_down))
        q_next = hop_near(g_query_sum[1], g_query_sum[2], *q_came)
        g_key_part, g_value_part, grad_hidden, g_attn_norm_part = finish_layer(
            kv_own, kv_last[0], kv_last[1], cos_own, sin_own, normed, w_key, w_value, d_normed_q, hidden, d_resid, attn_norm)
        norms = jnp.concatenate([g_attn_norm_part, g_mlp_norm_part])
        q_next, g_key_part, g_value_part, norms, d_gate = lax.optimization_barrier((q_next, g_key_part, g_value_part, norms, d_gate))
        g_key, g_value = lax.psum((g_key_part, g_value_part), "tp")
        last_side = swap(q_next[0], 2)
        q_last = (last_side, swap(q_next[1], 4))
        norms_near = [swap(norms, bit) for bit in (2, 4, 6)]
        g_gate = weight_grad_rest(gated_all, d_gate, g_gate_part, 6 * rows)
        norms_near, g_gate, d_upper = lax.optimization_barrier((norms_near, g_gate, d_upper))
        norms = norms + norms_near[0] + norms_near[1] + norms_near[2]
        norms, d_upper = lax.optimization_barrier((norms, d_upper))
        norms_core = swap(norms, 1)
        g_up = weight_grad(gated_all, d_upper)
        norms_core, q_last, g_up = lax.optimization_barrier((norms_core, q_last, g_up))
        g_norms = norms + norms_core
        g_query = (g_query_sum[0] + q_last[0] + q_last[1]).T
        full = (batch, shard, dim)
        return (hidden_out.reshape(full), grad_hidden.reshape(full), g_norms[0], g_query, g_key, g_value, g_out, g_norms[1], g_gate, g_up, g_down)

    return jax.shard_map(layer, mesh=mesh, in_specs=in_specs, out_specs=out_specs, check_vma=False)
```

```python
import functools
import math
import jax
import jax.numpy as jnp
from jax import lax
from jax.experimental import pallas as pl
from jax.experimental.pallas import tpu as pltpu
from jax.sharding import PartitionSpec as P

NORM_EPS = 1e-6
BF16 = jnp.bfloat16
F32 = jnp.float32
GELU_C = math.sqrt(2.0 / math.pi)
GELU_K = 0.044715
MASKED = -1e30
NT = (((1,), (1,)), ((), ()))
TN = (((0,), (0,)), ((), ()))


def rope_tables(positions, head_dim):
    half_dim = head_dim // 2
    exponent = jnp.arange(half_dim, dtype=F32) * (2.0 / head_dim)
    inv_freq = jnp.exp(exponent * (-math.log(10000.0)))
    angles = positions.astype(F32)[:, None] * inv_freq[None, :]
    return jnp.cos(angles), jnp.sin(angles)


def dot_nn(a, b):
    return jnp.dot(a, b, preferred_element_type=F32)


def dot_nt(a, b):
    return lax.dot_general(a, b, NT, preferred_element_type=F32)


def dot_tn(a, b):
    return lax.dot_general(a, b, TN, preferred_element_type=F32)


def swap(x, bit):
    return lax.ppermute(x, "tp", [(t, t ^ bit) for t in range(8)])


def flip(index, bit):
    return index + bit - 2 * bit * ((index // bit) % 2)


def neighbours():
    me = lax.axis_index("tp")
    return me, flip(me, 1), flip(me, 2), flip(me, 4)


def enter(peers):
    barrier = pltpu.get_barrier_semaphore()
    for peer in peers:
        pl.semaphore_signal(barrier, inc=1, device_id={"tp": peer}, device_id_type=pl.DeviceIdType.MESH)
    pl.semaphore_wait(barrier, len(peers))


def attn_bwd_kernel(lens_ref, cos_ref, sin_ref, q_ref, kv_ref, do_ref, dq_ref, dkv0_ref, dkv1_ref, dkv_acc):
    heads, shard, head_dim = q_ref.shape
    tp = kv_ref.shape[0]
    total = tp * shard
    rows = heads * shard
    s_id = pl.program_id(0)
    g_id = pl.program_id(1)
    prefix = lens_ref[0, s_id]
    valid = lens_ref[1, s_id]
    first = lens_ref[2, 0] * shard
    keys = kv_ref[:, :, :head_dim].reshape(total, head_dim)
    values = kv_ref[:, :, head_dim:].reshape(total, head_dim)
    query = q_ref[...].reshape(rows, head_dim) * BF16(head_dim ** -0.5)
    d_out = jnp.concatenate([do_ref[:, h * head_dim:(h + 1) * head_dim] for h in range(heads)], axis=0)
    step = lax.broadcasted_iota(jnp.int32, (shard, 1), 0)
    k_pos = jnp.concatenate([step + lens_ref[3 + r, 0] for r in range(tp)], axis=0)
    q_pos = first + lax.rem(lax.broadcasted_iota(jnp.int32, (1, rows), 1), shard)
    limit = jnp.minimum(valid, jnp.maximum(prefix, q_pos + 1))
    cos_t, sin_t = cos_ref[...][None], sin_ref[...][None]
    d_k = d_v = None
    count = heads // 2
    width = count * shard
    for c in range(2):
        cols = slice(c * width, (c + 1) * width)
        q_c, do_c = query[cols], d_out[cols]
        s = jnp.where(k_pos < limit[:, cols], dot_nt(keys, q_c), MASKED)
        e = jnp.exp(s - jnp.max(s, axis=0, keepdims=True))
        p = e * (1.0 / jnp.sum(e, axis=0, keepdims=True))
        d_p = dot_nt(values, do_c)
        delta = jnp.sum(p * d_p, axis=0, keepdims=True)
        d_s = (p * (d_p - delta)).astype(BF16)
        d_v_c = dot_nn(p.astype(BF16), do_c)
        d_k_c = dot_nn(d_s, q_c)
        d_k, d_v = (d_k_c, d_v_c) if d_k is None else (d_k + d_k_c, d_v + d_v_c)
        d_q = (dot_tn(d_s, keys) * (head_dim ** -0.5)).reshape(count, shard, head_dim)
        first, second = d_q[:, :, :head_dim // 2], d_q[:, :, head_dim // 2:]
        some = slice(c * count, (c + 1) * count)
        dq_ref[some, :, :head_dim // 2] = (first * cos_t + second * sin_t).astype(BF16)
        dq_ref[some, :, head_dim // 2:] = (second * cos_t - first * sin_t).astype(BF16)
    d_kv = jnp.concatenate([d_k, d_v], axis=1)

    @pl.when(g_id == 0)
    def _():
        dkv_acc[...] = d_kv

    @pl.when(g_id > 0)
    def _():
        dkv_acc[...] += d_kv

    @pl.when(g_id == pl.num_programs(1) - 1)
    def _():
        near = (tp // 2, shard, 2 * head_dim)
        dkv0_ref[...] = dkv_acc[:total // 2].astype(BF16).reshape(near)
        dkv1_ref[...] = dkv_acc[total // 2:].astype(BF16).reshape(near)


def remote(src, dst, send, recv, peer):
    return pltpu.make_async_remote_copy(src_ref=src, dst_ref=dst, send_sem=send, recv_sem=recv,
                                        device_id={"tp": peer}, device_id_type=pl.DeviceIdType.MESH)


def front_kernel(prefix_ref, valid_ref, kpos_ref, cos_ref, sin_ref, gain1_ref, gain2_ref, hidden, w_query, w_key, w_value, w_out,
                 normed_out, wq_all, wo_all, kv_all, query_out, mixed_out, resid_out, gated_out,
                 x_buf, n_buf, wkv, wq, wo, kv, q, probs, mix, acc, load, store, send, recv, *, batch):
    rows, dim = x_buf.shape
    shard = rows // batch
    head_dim = w_key.shape[1]
    tp = wq.shape[0]
    near = tp // 2
    total = tp * shard
    half_dim = head_dim // 2
    me, core, side, back = neighbours()
    bufs = (wq, kv, wo)

    def to_side(a):
        return remote(bufs[a].at[0], bufs[a].at[1], send.at[a, 0], recv.at[a, 0], side)

    def to_back(a):
        return remote(bufs[a].at[0], bufs[a].at[2], send.at[a, 1], recv.at[a, 1], back)

    def onward(a, k):
        half = bufs[a].shape[1] // 2
        part = pl.ds(k * half, half)
        return remote(bufs[a].at[1 + k, part], bufs[a].at[3, part], send.at[a, 2 + k], recv.at[a, 2 + k], (back, side)[k])

    def to_core(a, k):
        return remote(bufs[a].at[k], bufs[a].at[near + k], send.at[a, 4 + k], recv.at[a, 4 + k], core)

    loads = [pltpu.make_async_copy(src, dst, load.at[i]) for i, (src, dst) in enumerate((
        (w_query, wq.at[0]), (hidden, x_buf), (w_key, wkv.at[:, :head_dim]), (w_value, wkv.at[:, head_dim:]), (w_out, wo.at[0])))]
    mixed_at = [me, side, back, flip(side, 4)]
    mixed_at = mixed_at + [flip(dev, 1) for dev in mixed_at]
    stores = {name: pltpu.make_async_copy(src, dst, store.at[i]) for i, (name, src, dst) in enumerate((
        ("normed", n_buf, normed_out), ("wq", wq, wq_all), ("wo", wo, wo_all), ("kv", kv, kv_all), ("query", q, query_out),
        ("resid", x_buf, resid_out), ("gated", n_buf, gated_out)))}
    mixed_stores = [pltpu.make_async_copy(mix.at[:, pl.ds(k * head_dim, head_dim)],
                                          mixed_out.at[:, pl.ds(pl.multiple_of(dev * head_dim, 128), head_dim)], store.at[7 + k])
                    for k, dev in enumerate(mixed_at)]

    for cp in loads:
        cp.start()
    enter((core, side, back))
    loads[0].wait()
    to_side(0).start()
    to_back(0).start()
    to_core(0, 0).start()

    def norm_rows(src, gain_ref):
        x_f = src.astype(F32)
        inv_rms = lax.rsqrt(jnp.mean(x_f * x_f, axis=-1, keepdims=True) + NORM_EPS)
        return (x_f * inv_rms * (1.0 + gain_ref[...].astype(F32))).astype(BF16)

    def seq_rows(i):
        return pl.ds(pl.multiple_of(i * shard, 16), shard)

    def rotate(x_f):
        first, second = x_f[:, :half_dim], x_f[:, half_dim:]
        cos_t, sin_t = cos_ref[...], sin_ref[...]
        return first * cos_t - second * sin_t, second * cos_t + first * sin_t

    def norm1(i, carry):
        n_buf[seq_rows(i), :] = norm_rows(x_buf[seq_rows(i), :], gain1_ref)
        return carry

    loads[1].wait()
    lax.fori_loop(0, batch, norm1, 0)
    stores["normed"].start()
    loads[2].wait()
    loads[3].wait()

    def own_kv(i, carry):
        raw = dot_nn(n_buf[seq_rows(i), :], wkv[...])
        first, second = rotate(raw[:, :head_dim])
        kv[0, seq_rows(i), :half_dim] = first.astype(BF16)
        kv[0, seq_rows(i), half_dim:head_dim] = second.astype(BF16)
        kv[0, seq_rows(i), head_dim:] = raw[:, head_dim:].astype(BF16)
        return carry

    lax.fori_loop(0, batch, own_kv, 0)
    to_side(1).start()
    to_back(1).start()
    to_core(1, 0).start()

    def own_query(k):
        def step(i, carry):
            for h in (k, near + k):
                first, second = rotate(dot_nn(n_buf[seq_rows(i), :], wq[h]))
                q[h, seq_rows(i), :half_dim] = first.astype(BF16)
                q[h, seq_rows(i), half_dim:] = second.astype(BF16)
            return carry

        to_core(0, k).wait_recv()
        lax.fori_loop(0, batch, step, 0)

    def pass_on(a):
        to_side(a).wait_recv()
        onward(a, 0).start()
        to_core(a, 1).start()
        to_back(a).wait_recv()
        onward(a, 1).start()
        to_core(a, 2).start()

    def pass_last(a):
        onward(a, 0).wait_recv()
        onward(a, 1).wait_recv()
        to_core(a, 3).start()

    own_query(0)
    pass_on(0)
    own_query(1)
    own_query(2)
    pass_on(1)
    loads[4].wait()
    to_side(2).start()
    to_back(2).start()
    to_core(2, 0).start()
    pass_last(0)
    own_query(3)
    stores["query"].start()
    stores["wq"].start()
    pass_last(1)
    for k in range(near):
        to_core(1, k).wait_recv()
    stores["kv"].start()

    q_pos = me * shard + lax.broadcasted_iota(jnp.int32, (shard, 1), 0)

    def attend(i, carry):
        keys = kv[:, seq_rows(i), :head_dim].reshape(total, head_dim)
        values = kv[:, seq_rows(i), head_dim:].reshape(total, head_dim)
        visible = kpos_ref[...] < jnp.minimum(valid_ref[i], jnp.maximum(prefix_ref[i], q_pos + 1))
        for g in range(2):
            query = q[g * near:(g + 1) * near, seq_rows(i), :].reshape(near * shard, head_dim) * BF16(head_dim ** -0.5)
            scores = dot_nt(query, keys)
            for h in range(near):
                part = slice(h * shard, (h + 1) * shard)
                s = jnp.where(visible, scores[part], MASKED)
                e = jnp.exp(s - jnp.max(s, axis=-1, keepdims=True))
                probs[g, part, :] = (e * (1.0 / jnp.sum(e, axis=-1, keepdims=True))).astype(BF16)
            mixed = dot_nn(probs[g], values).astype(BF16)
            for h in range(near):
                head = g * near + h
                mix[seq_rows(i), head * head_dim:(head + 1) * head_dim] = mixed[h * shard:(h + 1) * shard]
        return carry

    lax.fori_loop(0, batch, attend, 0)
    for cp in mixed_stores:
        cp.start()
    pass_on(2)

    def project(k, first):
        def step(n, carry):
            cols = pl.ds(pl.multiple_of(n * 512, 128), 512)
            part = (dot_nn(mix[:, k * head_dim:(k + 1) * head_dim], wo[k, :, cols])
                    + dot_nn(mix[:, (near + k) * head_dim:(near + k + 1) * head_dim], wo[near + k, :, cols]))
            acc[:, cols] = part if first else acc[:, cols] + part
            return carry

        to_core(2, k).wait_recv()
        lax.fori_loop(0, dim // 512, step, 0)

    project(0, True)
    project(1, False)
    project(2, False)
    pass_last(2)
    project(3, False)
    stores["wo"].start()
    stores["normed"].wait()

    def norm2(i, carry):
        resid = (x_buf[seq_rows(i), :].astype(F32) + acc[seq_rows(i), :]).astype(BF16)
        x_buf[seq_rows(i), :] = resid
        n_buf[seq_rows(i), :] = norm_rows(resid, gain2_ref)
        return carry

    lax.fori_loop(0, batch, norm2, 0)
    stores["resid"].start()
    stores["gated"].start()
    for cp in mixed_stores:
        cp.wait()
    for name in ("wq", "wo", "kv", "query", "resid", "gated"):
        stores[name].wait()
    for a in range(3):
        to_side(a).wait_send()
        to_back(a).wait_send()
        for k in range(2):
            onward(a, k).wait_send()
        for k in range(near):
            to_core(a, k).wait_send()


def front_layer(prefix_len, valid_len, k_pos, cos_t, sin_t, attn_norm, mlp_norm, hidden, w_query, w_key, w_value, w_out, batch, tp):
    rows, dim = hidden.shape
    head_dim = w_key.shape[1]
    shard = rows // batch
    total = tp * shard
    anyspace = pl.BlockSpec(memory_space=pl.ANY)
    vmem = pl.BlockSpec(memory_space=pltpu.VMEM)
    dma = pltpu.SemaphoreType.DMA

    def shape(*dims):
        return jax.ShapeDtypeStruct(dims, BF16)

    return pl.pallas_call(
        functools.partial(front_kernel, batch=batch),
        out_shape=(shape(rows, dim), shape(tp, dim, head_dim), shape(tp, head_dim, dim), shape(tp, rows, 2 * head_dim),
                   shape(tp, rows, head_dim), shape(rows, tp * head_dim), shape(rows, dim), shape(rows, dim)),
        in_specs=[pl.BlockSpec(memory_space=pltpu.SMEM)] * 2 + [vmem] * 5 + [anyspace] * 5,
        out_specs=(anyspace,) * 8,
        scratch_shapes=[pltpu.VMEM((rows, dim), BF16), pltpu.VMEM((rows, dim), BF16), pltpu.VMEM((dim, 2 * head_dim), BF16),
                        pltpu.VMEM((tp, dim, head_dim), BF16), pltpu.VMEM((tp, head_dim, dim), BF16),
                        pltpu.VMEM((tp, rows, 2 * head_dim), BF16), pltpu.VMEM((tp, rows, head_dim), BF16),
                        pltpu.VMEM((2, tp // 2 * shard, total), BF16), pltpu.VMEM((rows, tp * head_dim), BF16), pltpu.VMEM((rows, dim), F32),
                        dma((5,)), dma((15,)), dma((3, 8)), dma((3, 8))],
        compiler_params=pltpu.CompilerParams(vmem_limit_bytes=62 << 20, collective_id=2, has_side_effects=True),
        cost_estimate=pl.CostEstimate(flops=8 * rows * dim * tp * head_dim, bytes_accessed=60 << 20, transcendentals=tp * rows * total),
        name="front",
    )(prefix_len, valid_len, k_pos, cos_t, sin_t, attn_norm.reshape(1, dim), mlp_norm.reshape(1, dim), hidden, w_query, w_key, w_value, w_out)


def attention_backward(lens, cos_t, sin_t, query, kv_all, d_mixed, batch, group=8):
    heads, rows, head_dim = query.shape
    near = kv_all.shape[0] // 2
    shard = rows // batch
    total = 2 * near * shard
    q_spec = pl.BlockSpec((group, shard, head_dim), lambda s, g, *_: (g, s, 0))
    kv_spec = pl.BlockSpec((near, shard, 2 * head_dim), lambda s, g, *_: (0, s, 0))
    table = pl.BlockSpec((shard, head_dim // 2), lambda s, g, *_: (0, 0))
    kv_shape = jax.ShapeDtypeStruct((near, rows, 2 * head_dim), BF16)
    return pl.pallas_call(
        attn_bwd_kernel,
        out_shape=(jax.ShapeDtypeStruct((heads, rows, head_dim), BF16), kv_shape, kv_shape),
        grid_spec=pltpu.PrefetchScalarGridSpec(
            num_scalar_prefetch=1, grid=(batch, heads // group),
            in_specs=[table, table, q_spec, pl.BlockSpec((2 * near, shard, 2 * head_dim), lambda s, g, *_: (0, s, 0)), pl.BlockSpec((shard, group * head_dim), lambda s, g, *_: (s, g))],
            out_specs=(q_spec, kv_spec, kv_spec),
            scratch_shapes=[pltpu.VMEM((total, 2 * head_dim), F32)]),
        compiler_params=pltpu.CompilerParams(dimension_semantics=("arbitrary", "arbitrary"), vmem_limit_bytes=62 << 20),
        cost_estimate=pl.CostEstimate(flops=10 * heads * rows * total * head_dim, bytes_accessed=20 << 20, transcendentals=heads * rows * total),
        name="attn_bwd",
    )(lens, cos_t, sin_t, query, kv_all, d_mixed)


def gated_tile(z, g, w_g, w_u, w_d):
    gate = dot_nn(z, w_g)
    upper = dot_nn(z, w_u)
    d_act = dot_nt(g, w_d).astype(BF16).astype(F32)
    sq = gate * gate
    th = jnp.tanh(gate * (GELU_C + (GELU_C * GELU_K) * sq))
    half = 0.5 + 0.5 * th
    gelu = gate * half
    slope = half + gate * (0.5 - 0.5 * (th * th)) * (GELU_C + (3.0 * GELU_C * GELU_K) * sq)
    return (gelu * upper).astype(BF16), (d_act * upper * slope).astype(BF16), (d_act * gelu).astype(BF16)


def gated_kernel(z_own, g_own, wg_hbm, wu_hbm, wd_hbm, z_all, g_all, act, d_gate, d_up, diag_in,
                 wg, wu, wd, z_buf, g_buf, outs, st, from_core, far_send, far_recv, diag_send, diag_recv, w_sem, in_sem, own_sem, out_sem, send, recv, send0, recv0, *, bn):
    rows, dim = z_own.shape
    width = wg_hbm.shape[1]
    steps = width // bn
    piece = rows // 4
    me, core, side, back = neighbours()
    corner = flip(side, 4)
    own = (z_own, g_own)
    full = (z_all, g_all)

    def part(slot, q):
        return pl.ds(pl.multiple_of(slot * rows + q * piece, 16), piece)

    def link_rows(u, path):
        turn = u // 2
        diag = turn % 2
        if path == 0:
            return side + (corner - side) * diag, (u % 2) + 2 * (turn // 2) + diag * 2
        return back + (corner - back) * diag, (u % 2) + 2 - 2 * (turn // 2) - diag * 2

    def link_copy(u, path, a):
        turn = u // 2
        peer = side if path == 0 else back
        sems = (send.at[path, u, a], recv.at[path, u, a])
        if turn == 1:
            slot = back if path == 0 else side
            q = (2 if path == 0 else 0) + u % 2
            return remote(full[a].at[part(slot, q)], full[a].at[part(slot, q)], *sems, peer)
        q = u % 2 + (2 * (turn // 2) if path == 0 else 2 - 2 * (turn // 2))
        return remote(own[a].at[pl.ds(q * piece, piece)], full[a].at[part(me, q)], *sems, peer)

    def core_copy(u, path, a):
        slot, q = link_rows(u, path)
        return remote(full[a].at[part(slot, q)], full[a].at[part(slot, q)], send.at[2 + path, u, a], recv.at[2 + path, u, a], core)

    def own_copy(a):
        return remote(own[a], full[a].at[pl.ds(pl.multiple_of(me * rows, 16), rows)], send0.at[a], recv0.at[a], core)

    def weight_copies(n):
        cols = pl.ds(pl.multiple_of(n * bn, 128), bn)
        return [pltpu.make_async_copy(wg_hbm.at[:, cols], wg.at[:, cols], w_sem.at[0, n]),
                pltpu.make_async_copy(wu_hbm.at[:, cols], wu.at[:, cols], w_sem.at[1, n]),
                pltpu.make_async_copy(wd_hbm.at[cols], wd.at[cols], w_sem.at[2, n])]

    bufs = (z_buf, g_buf)
    own_in = [pltpu.make_async_copy(own[a], bufs[a], own_sem.at[a]) for a in range(2)]
    own_out = [pltpu.make_async_copy(bufs[a], full[a].at[pl.ds(pl.multiple_of(me * rows, 16), rows)], own_sem.at[2 + a]) for a in range(2)]
    for cp in own_in:
        cp.start()
    for n in range(steps):
        for cp in weight_copies(n):
            cp.start()
    enter((core, side, back))
    for u in range(2):
        for path in range(2):
            for a in range(2):
                link_copy(u, path, a).start()
        if u == 0:
            for a in range(2):
                own_copy(a).start()

    def out_copies(slot, s_rows, n):
        cols = pl.ds(pl.multiple_of(n * bn, 128), bn)
        return [pltpu.make_async_copy(outs.at[slot, k, pl.ds(i * piece, piece)], ref.at[s_rows[i], cols], out_sem.at[slot, k, i])
                for k, ref in enumerate((act, d_gate, d_up)) for i in range(4)]

    def stage_rows(s):
        late = (s + 6) // 8
        u = (s - 2) * late
        first = me + (core - me) * s * (1 - late)
        (slot_x, q_x), (slot_y, q_y) = link_rows(u, 0), link_rows(u, 1)
        base_x, base_y = slot_x * rows + q_x * piece, slot_y * rows + q_y * piece
        pair_x, pair_y = flip(slot_x, 1) * rows + q_x * piece, flip(slot_y, 1) * rows + q_y * piece
        starts = [(1 - late) * (first * rows + i * piece) + late * base for i, base in enumerate((base_x, base_y, pair_x, pair_y))]
        return [pl.ds(pl.multiple_of(st, 16), piece) for st in starts]

    def pass_on(u):
        for path in range(2):
            for a in range(2):
                link_copy(u, path, a).wait_recv()
                core_copy(u, path, a).start()
        later = (2,) if u == 0 else (3, 4, 5) if u == 1 else ()
        for v in later:
            for path in range(2):
                for a in range(2):
                    link_copy(v, path, a).start()

    def far_copy(j):
        return remote(st.at[0, j], from_core.at[j], far_send.at[j], far_recv.at[j], core)

    def diag_copy(k, j):
        half = rows // 2
        return remote(st.at[1, j, pl.ds(k * half, half)], diag_in.at[k, :, pl.ds(pl.multiple_of(j * bn, 128), bn)],
                      diag_send.at[k, j], diag_recv.at[k, j], (side, back)[k])

    def down_diagonal():
        for slot in range(2):
            for cp in out_copies(slot, stage_rows(5), 0):
                cp.wait()
        loads = [pltpu.make_async_copy(act.at[pl.ds(pl.multiple_of(dev * rows, 16), rows)], bufs[a], in_sem.at[a, 0])
                 for a, dev in enumerate((flip(corner, 1), corner))]
        for cp in loads:
            cp.start()

        def theirs(j, carry):
            st[0, j] = dot_nn(z_buf[...], wd[:, pl.ds(pl.multiple_of(j * bn, 128), bn)]).astype(BF16)
            far_copy(j).start()
            return carry

        def mine(j, carry):
            far_copy(j).wait_recv()
            total = dot_nn(g_buf[...], wd[:, pl.ds(pl.multiple_of(j * bn, 128), bn)]) + from_core[j].astype(F32)
            st[1, j] = total.astype(BF16)
            for k in range(2):
                diag_copy(k, j).start()
            return carry

        loads[0].wait()
        lax.fori_loop(0, dim // bn, theirs, 0)
        loads[1].wait()
        lax.fori_loop(0, dim // bn, mine, 0)

    def compute(s):
        s_rows = stage_rows(s)

        def block(n, carry):
            step = s * steps + n
            slot = step % 2

            @pl.when((step >= 2) & (step // 2 != 6 * steps // 2))
            def _():
                for cp in out_copies(slot, s_rows, n):
                    cp.wait()

            @pl.when(s == 0)
            def _():
                for cp in weight_copies(n):
                    cp.wait()

            for u in range(6):
                @pl.when((s == u + 1) & (n == steps - 1))
                def _(u=u):
                    pass_on(u)

            cols = pl.ds(pl.multiple_of(n * bn, 128), bn)
            res = gated_tile(z_buf[...], g_buf[...], wg[:, cols], wu[:, cols], wd[cols, :])
            for k in range(3):
                outs[slot, k] = res[k]
            for cp in out_copies(slot, s_rows, n):
                cp.start()
            return carry

        lax.fori_loop(0, steps, block, 0)

    def stage(s, carry):
        @pl.when(s == 0)
        def _():
            for cp in own_in:
                cp.wait()
            for cp in own_out:
                cp.start()

        @pl.when(s == 1)
        def _():
            for cp in own_out:
                cp.wait()
            for a in range(2):
                own_copy(a).wait_recv()

        for u in range(6):
            @pl.when(s == u + 2)
            def _(u=u):
                if u == 4:
                    down_diagonal()
                for path in range(2):
                    for a in range(2):
                        core_copy(u, path, a).wait_recv()

        @pl.when(s >= 1)
        def _():
            s_rows = stage_rows(s)
            copies = [pltpu.make_async_copy(full[a].at[s_rows[i]], bufs[a].at[pl.ds(i * piece, piece)], in_sem.at[a, i])
                      for a in range(2) for i in range(4)]
            for cp in copies:
                cp.start()
            for cp in copies:
                cp.wait()

        compute(s)
        return carry

    lax.fori_loop(0, 8, stage, 0)
    last = stage_rows(7)
    for slot in range(2):
        for cp in out_copies(slot, last, 0):
            cp.wait()
    for j in range(dim // bn):
        far_copy(j).wait_send()
        for k in range(2):
            diag_copy(k, j).wait_send()
            diag_copy(k, j).wait_recv()
    for a in range(2):
        own_copy(a).wait_send()
        for path in range(2):
            for u in range(6):
                link_copy(u, path, a).wait_send()
                core_copy(u, path, a).wait_send()


def gated_layer(z_own, g_own, w_gate, w_up, w_down, tp, bn=512):
    rows, dim = z_own.shape
    width = w_gate.shape[1]
    total = rows * tp
    anyspace = pl.BlockSpec(memory_space=pl.ANY)
    gathered = jax.ShapeDtypeStruct((total, dim), BF16)
    made = jax.ShapeDtypeStruct((total, width), BF16)
    dma = pltpu.SemaphoreType.DMA
    return pl.pallas_call(
        functools.partial(gated_kernel, bn=bn),
        out_shape=(gathered, gathered, made, made, made, jax.ShapeDtypeStruct((2, rows // 2, dim), BF16)),
        in_specs=[anyspace] * 5,
        out_specs=(anyspace,) * 6,
        scratch_shapes=[pltpu.VMEM((dim, width), BF16), pltpu.VMEM((dim, width), BF16), pltpu.VMEM((width, dim), BF16),
                        pltpu.VMEM((rows, dim), BF16), pltpu.VMEM((rows, dim), BF16), pltpu.VMEM((2, 3, rows, bn), BF16),
                        pltpu.VMEM((2, dim // bn, rows, bn), BF16), pltpu.VMEM((dim // bn, rows, bn), BF16),
                        dma((dim // bn,)), dma((dim // bn,)), dma((2, dim // bn)), dma((2, dim // bn)), dma((3, width // bn)), dma((2, 4)), dma((4,)), dma((2, 3, 4)), dma((4, 6, 2)), dma((4, 6, 2)), dma((2,)), dma((2,))],
        compiler_params=pltpu.CompilerParams(vmem_limit_bytes=67043328, collective_id=0, has_side_effects=True),
        cost_estimate=pl.CostEstimate(flops=6 * total * dim * width, bytes_accessed=200 << 20, transcendentals=total * width),
        name="gated",
    )(z_own, g_own, w_gate, w_up, w_down)


def back_kernel(act, d_gate, d_up, z_all, diag_in, wg_hbm, wu_hbm, wd_hbm, own_out, x_in, y_in, g_gate,
                wa, wb, lhs, st, from_core, from_diag, own_st, in_sem, z_sem, w_sem, l_sem, o_sem, c_send, c_recv, d_send, d_recv, f_send, f_recv, *, rows, bn):
    dim, width = wg_hbm.shape
    steps = dim // bn
    half = rows // 2
    me, core, side, back = neighbours()

    def cols(j):
        return pl.ds(pl.multiple_of(j * bn, 128), bn)

    def shard_of(phase, t):
        if phase == 0:
            return 1 + t // 2, 1 - t % 2
        ge = [(t + 8 - k) // 8 for k in range(8)]
        return ge[2] + ge[3] - ge[5] + 2 * ge[6], 1 - ge[1] + ge[2] - ge[4] + ge[6] - ge[7]

    def lhs_copies(phase, t):
        pair, theirs = shard_of(phase, t)
        dev = me + (1 - pair // 2) * (side - me) + (1 - pair % 2) * (back - me)
        dev = dev + theirs * (flip(dev, 1) - dev)
        src = pl.ds(pl.multiple_of(dev * rows, 16), rows)
        refs = (act,) if phase == 0 else (d_gate, d_up)
        return [pltpu.make_async_copy(ref.at[src], lhs.at[t % 2, k], l_sem.at[t % 2, k]) for k, ref in enumerate(refs)]

    def weight_copy(k, j):
        if k == 0:
            return pltpu.make_async_copy(wd_hbm.at[:, cols(j)], wa.at[pl.ds(0, width), cols(j)], w_sem.at[0, j])
        src, dst = (wg_hbm, wb) if k == 1 else (wu_hbm, wa)
        return pltpu.make_async_copy(src.at[cols(j)], dst.at[cols(j)], w_sem.at[k, j])

    def core_copy(pair, j):
        return remote(st.at[0, j], from_core.at[pair, j], c_send.at[j], c_recv.at[pair, j], core)

    def diag_copy(phase, k, j):
        return remote(st.at[1, j, pl.ds(k * half, half)], from_diag.at[phase, k, j], d_send.at[k, j], d_recv.at[phase, k, j], (side, back)[k])

    def final_copy(phase, k, j):
        return remote(st.at[2 + k, j], (x_in, y_in)[k].at[phase, :, cols(j)], f_send.at[k, j], f_recv.at[phase, k, j], (side, back)[k])

    def own_copy(phase, j):
        return pltpu.make_async_copy(own_st.at[j % 2], own_out.at[phase, :, cols(j)], o_sem.at[j % 2])

    def product(phase, slot, j):
        if phase == 0:
            return dot_nn(lhs[slot, 0], wa[:width, cols(j)])
        return dot_nt(lhs[slot, 0], wb[cols(j), :]) + dot_nt(lhs[slot, 1], wa[cols(j), :])

    def diag_load(k, j):
        return pltpu.make_async_copy(diag_in.at[k, :, cols(j)], from_diag.at[0, k, j], in_sem.at[k, j])

    for cp in lhs_copies(0, 0):
        cp.start()
    for j in range(steps):
        weight_copy(0, j).start()
    for k in range(2):
        for j in range(steps):
            diag_load(k, j).start()
    enter((core, side, back))

    def tiles(body):
        def step(j, carry):
            body(j)
            return carry

        lax.fori_loop(0, steps, step, 0)

    for phase in (0, 1):
        def step(t, carry, phase=phase):
            for cp in lhs_copies(phase, t):
                cp.wait()

            last = 5 if phase == 0 else 7

            @pl.when(t < last)
            def _():
                for cp in lhs_copies(phase, t + 1):
                    cp.start()

            if phase == 0:
                @pl.when(t == 1)
                def _():
                    for j in range(steps):
                        weight_copy(1, j).start()

                @pl.when(t == last)
                def _():
                    for cp in lhs_copies(1, 0):
                        cp.start()

            theirs = (t % 2 == 0) if phase == 0 else ((t % 6 == 0) | (t // 2 == 1))

            @pl.when(theirs)
            def _():
                pair = shard_of(phase, t)[0]

                def body(j):
                    @pl.when(t == 0)
                    def _():
                        for k in ((0,) if phase == 0 else (1, 2)):
                            weight_copy(k, j).wait()

                    if phase == 0:
                        @pl.when(t > 0)
                        def _():
                            core_copy(0, j).wait_send()
                    else:
                        core_copy(0, j).wait_send()
                    st[0, j] = product(phase, t % 2, j).astype(BF16)
                    core_copy(pair, j).start()

                tiles(body)

            if phase == 1:
                @pl.when(t == 1)
                def _():
                    def body(j):
                        core_copy(0, j).wait_recv()
                        st[1, j] = (product(phase, 1, j) + from_core[0, j].astype(F32)).astype(BF16)
                        for k in range(2):
                            diag_copy(phase, k, j).start()

                    tiles(body)

            for k in range(2):
                @pl.when(t == (1 + 2 * k if phase == 0 else 5 - k))
                def _(k=k):
                    def body(j):
                        core_copy(1 + k, j).wait_recv()
                        if phase == 0:
                            diag_load(1 - k, j).wait()
                        else:
                            diag_copy(phase, 1 - k, j).wait_recv()
                            final_copy(0, k, j).wait_send()
                        total = product(phase, 1 if phase == 0 else 1 - k, j) + from_core[1 + k, j].astype(F32)
                        came = from_diag[phase, 1 - k, j].astype(F32)
                        split = slice(half, rows) if k == 0 else slice(0, half)
                        rest = slice(0, half) if k == 0 else slice(half, rows)
                        st[2 + k, j, split, :] = (total[split] + came).astype(BF16)
                        st[2 + k, j, rest, :] = total[rest].astype(BF16)
                        final_copy(phase, k, j).start()

                    tiles(body)

            @pl.when(t == last)
            def _():
                def body(j):
                    core_copy(3, j).wait_recv()

                    @pl.when(j >= 2)
                    def _():
                        own_copy(phase, j).wait()

                    own_st[j % 2] = product(phase, 1, j) + from_core[3, j].astype(F32)
                    own_copy(phase, j).start()

                tiles(body)
                for j in (0, 1):
                    own_copy(phase, j).wait()
                if phase == 0:
                    for j in range(steps):
                        weight_copy(2, j).start()

            return carry

        lax.fori_loop(0, 6 if phase == 0 else 8, step, 0)

    first = z_all.shape[0] - 2 * rows

    def z_copy(j, c):
        return pltpu.make_async_copy(z_all.at[pl.ds(first + c * rows, rows), cols(j)], lhs.at[0, c, :, cols(j)], z_sem.at[j, c])

    def gate_copy(j):
        return pltpu.make_async_copy(d_gate.at[pl.ds(first, 2 * rows), cols(j)], wa.at[pl.ds(0, 2 * rows), cols(j)], w_sem.at[0, j])

    def grad_copy(i, j):
        slot = j % 2
        return pltpu.make_async_copy(own_st.at[slot, pl.ds(0, bn)], g_gate.at[cols(i), cols(j)], o_sem.at[slot])

    for j in range(steps):
        for c in range(2):
            z_copy(j, c).start()
        gate_copy(j).start()

    def grad_tile(step, carry):
        i, j = step // steps, step % steps

        @pl.when(i == 0)
        def _():
            gate_copy(j).wait()

        @pl.when(j == 0)
        def _():
            for c in range(2):
                z_copy(i, c).wait()

        @pl.when(step >= 2)
        def _():
            grad_copy(i, j).wait()

        own_st[j % 2, :bn] = dot_tn(lhs[0, :, :, cols(i)].reshape(2 * rows, bn), wa[:2 * rows, cols(j)])
        grad_copy(i, j).start()
        return carry

    lax.fori_loop(0, steps * steps, grad_tile, 0)
    for j in range(2):
        grad_copy(0, j).wait()
    for j in range(steps):
        core_copy(0, j).wait_send()
        for k in range(2):
            diag_copy(1, k, j).wait_send()
            final_copy(1, k, j).wait_send()
            for phase in (0, 1):
                final_copy(phase, k, j).wait_recv()


def back_layer(act, d_gate, d_up, z_all, diag_in, w_gate, w_up, w_down, tp, bn=512):
    total, width = act.shape
    dim = w_gate.shape[0]
    rows = total // tp
    steps = dim // bn
    anyspace = pl.BlockSpec(memory_space=pl.ANY)
    dma = pltpu.SemaphoreType.DMA
    came = jax.ShapeDtypeStruct((2, rows, dim), BF16)
    return pl.pallas_call(
        functools.partial(back_kernel, rows=rows, bn=bn),
        out_shape=(jax.ShapeDtypeStruct((2, rows, dim), F32), came, came, jax.ShapeDtypeStruct((dim, width), F32)),
        in_specs=[anyspace] * 8,
        out_specs=(anyspace,) * 4,
        scratch_shapes=[pltpu.VMEM((width, dim), BF16), pltpu.VMEM((dim, width), BF16), pltpu.VMEM((2, 2, rows, width), BF16),
                        pltpu.VMEM((4, steps, rows, bn), BF16), pltpu.VMEM((4, steps, rows, bn), BF16),
                        pltpu.VMEM((2, 2, steps, rows // 2, bn), BF16), pltpu.VMEM((2, rows, bn), F32),
                        dma((2, steps)), dma((steps, 2)), dma((3, steps)), dma((2, 2)), dma((2,)), dma((steps,)), dma((4, steps)),
                        dma((2, steps)), dma((2, 2, steps)), dma((2, steps)), dma((2, 2, steps))],
        compiler_params=pltpu.CompilerParams(vmem_limit_bytes=67043328, collective_id=1, has_side_effects=True),
        cost_estimate=pl.CostEstimate(flops=6 * total * dim * width, bytes_accessed=200 << 20, transcendentals=0),
        name="back",
    )(act, d_gate, d_up, z_all, diag_in, w_gate, w_up, w_down)


def norm_back(x, gain, d_out):
    inv_rms = lax.rsqrt(jnp.mean(x * x, axis=-1, keepdims=True) + NORM_EPS)
    unit = x * inv_rms
    scaled = d_out * (1.0 + gain.astype(F32))
    return inv_rms * (scaled - unit * jnp.mean(unit * scaled, axis=-1, keepdims=True)), d_out * unit


def join_kernel(own_ref, x_ref, y_ref, resid_ref, grad_ref, gain_ref, wo_ref, mixed_ref,
                out_ref, d_resid_ref, g_gain_ref, d_mixed_ref, g_out_ref, keep, *, joins):
    step = pl.program_id(0)
    bm = resid_ref.shape[0]

    @pl.when(step == 0)
    def _():
        g_gain_ref[...] = jnp.zeros_like(g_gain_ref)

    @pl.when(step < joins)
    def _():
        mlp_sum, d_gated = [own_ref[k] + x_ref[k].astype(F32) + y_ref[k].astype(F32) for k in range(2)]
        resid = resid_ref[...].astype(F32)
        out_ref[...] = (resid + mlp_sum).astype(BF16)
        d_norm, terms = norm_back(resid, gain_ref[...], d_gated.astype(BF16).astype(F32))
        d_resid = (grad_ref[...].astype(F32) + d_norm).astype(BF16)
        d_resid_ref[...] = d_resid
        keep[pl.ds(pl.multiple_of(step * bm, 16), bm), :] = d_resid
        g_gain_ref[...] += jnp.sum(terms, axis=0, keepdims=True)

    @pl.when(step >= joins)
    def _():
        d_mixed_ref[...] = dot_nt(keep[...], wo_ref[...]).astype(BF16)
        g_out_ref[...] = dot_tn(mixed_ref[...], keep[...])


def join_layer(own_part, x_part, y_part, resid, grad_out, gain, wo_all, mixed, bm=96, bn=512):
    rows, dim = resid.shape
    width = mixed.shape[1]
    joins = rows // bm
    pair = pl.BlockSpec((2, bm, dim), lambda i: (0, jnp.minimum(i, joins - 1), 0))
    row = pl.BlockSpec((bm, dim), lambda i: (jnp.minimum(i, joins - 1), 0))
    one = pl.BlockSpec((1, dim), lambda i: (0, 0))
    col = pl.BlockSpec((rows, bn), lambda i: (0, jnp.maximum(i - joins, 0)))
    block = pl.BlockSpec((bn, dim), lambda i: (jnp.maximum(i - joins, 0), 0))
    act = jax.ShapeDtypeStruct((rows, dim), BF16)
    return pl.pallas_call(
        functools.partial(join_kernel, joins=joins),
        out_shape=(act, act, jax.ShapeDtypeStruct((1, dim), F32), jax.ShapeDtypeStruct((rows, width), BF16),
                   jax.ShapeDtypeStruct((width, dim), F32)),
        grid=(joins + width // bn,),
        in_specs=[pair, pair, pair, row, row, one, block, col],
        out_specs=(row, row, one, col, block),
        scratch_shapes=[pltpu.VMEM((rows, dim), BF16)],
        compiler_params=pltpu.CompilerParams(dimension_semantics=("arbitrary",), vmem_limit_bytes=62 << 20),
        cost_estimate=pl.CostEstimate(flops=4 * rows * dim * width, bytes_accessed=60 << 20, transcendentals=rows),
        name="join",
    )(own_part, x_part, y_part, resid, grad_out, gain.reshape(1, dim), wo_all, mixed)


def finish_kernel(kv_ref, side_ref, back_ref, cos_ref, sin_ref, normed_ref, wk_ref, wv_ref, part_ref, hidden_ref, d_resid_ref, gain_ref,
                  g_key_ref, g_value_ref, out_ref, g_gain_ref):
    head_dim = wk_ref.shape[1]
    half_dim = head_dim // 2
    d_kv = (kv_ref[...] + side_ref[...].astype(F32) + back_ref[...].astype(F32)).astype(BF16)
    first, second = d_kv[:, :half_dim].astype(F32), d_kv[:, half_dim:head_dim].astype(F32)
    cos_t, sin_t = cos_ref[...], sin_ref[...]
    d_key = jnp.concatenate([first * cos_t + second * sin_t, second * cos_t - first * sin_t], axis=1).astype(BF16)
    d_value = d_kv[:, head_dim:]
    d_normed = (part_ref[...] + dot_nt(d_key, wk_ref[...]) + dot_nt(d_value, wv_ref[...])).astype(BF16).astype(F32)
    d_norm, terms = norm_back(hidden_ref[...].astype(F32), gain_ref[...], d_normed)
    out_ref[...] = (d_resid_ref[...].astype(F32) + d_norm).astype(BF16)
    g_key = dot_tn(normed_ref[...], d_key)
    g_value = dot_tn(normed_ref[...], d_value)
    g_gain = jnp.sum(terms, axis=0, keepdims=True)

    @pl.when(pl.program_id(0) == 0)
    def _():
        g_key_ref[...] = g_key
        g_value_ref[...] = g_value
        g_gain_ref[...] = g_gain

    @pl.when(pl.program_id(0) > 0)
    def _():
        g_key_ref[...] += g_key
        g_value_ref[...] += g_value
        g_gain_ref[...] += g_gain


def finish_layer(kv_own, kv_side, kv_back, cos_t, sin_t, normed, w_key, w_value, part, hidden, d_resid, gain):
    rows, dim = hidden.shape
    shard, half_dim = cos_t.shape
    head_dim = w_key.shape[1]

    def row(width):
        return pl.BlockSpec((shard, width), lambda i: (i, 0))

    def whole(*shape):
        return pl.BlockSpec(shape, lambda i: (0, 0))

    kv, act, table, weight, one = row(2 * head_dim), row(dim), whole(shard, half_dim), whole(dim, head_dim), whole(1, dim)
    grad = jax.ShapeDtypeStruct((dim, head_dim), F32)
    return pl.pallas_call(
        finish_kernel,
        out_shape=(grad, grad, jax.ShapeDtypeStruct((rows, dim), BF16), jax.ShapeDtypeStruct((1, dim), F32)),
        grid=(rows // shard,),
        in_specs=[kv, kv, kv, table, table, act, weight, weight, act, act, act, one],
        out_specs=(weight, weight, act, one),
        compiler_params=pltpu.CompilerParams(dimension_semantics=("arbitrary",), vmem_limit_bytes=62 << 20),
        cost_estimate=pl.CostEstimate(flops=8 * rows * dim * head_dim, bytes_accessed=24 << 20, transcendentals=rows),
        name="finish",
    )(kv_own, kv_side, kv_back, cos_t, sin_t, normed, w_key, w_value, part, hidden, d_resid, gain.reshape(1, dim))


def product_kernel(a_ref, b_ref, o_ref):
    o_ref[...] = dot_tn(a_ref[...], b_ref[...])


def weight_grad(a, b, bm=1024, bn=512):
    rows, m = a.shape
    n = b.shape[1]
    return pl.pallas_call(
        product_kernel,
        out_shape=jax.ShapeDtypeStruct((m, n), F32),
        grid=(m // bm, n // bn),
        in_specs=[pl.BlockSpec((rows, bm), lambda i, j: (0, i)), pl.BlockSpec((rows, bn), lambda i, j: (0, j))],
        out_specs=pl.BlockSpec((bm, bn), lambda i, j: (i, j)),
        compiler_params=pltpu.CompilerParams(dimension_semantics=("arbitrary", "arbitrary"), vmem_limit_bytes=62 << 20),
        cost_estimate=pl.CostEstimate(flops=2 * rows * m * n, bytes_accessed=110 << 20, transcendentals=0),
        name="weight_grad",
    )(a, b)


def rest_kernel(a_ref, b_ref, part_ref, o_ref):
    o_ref[...] = part_ref[...] + dot_tn(a_ref[...], b_ref[...])


def weight_grad_rest(a, b, part, count, bm=1024, bn=512):
    m, n = part.shape
    out = pl.BlockSpec((bm, bn), lambda i, j: (i, j))
    return pl.pallas_call(
        rest_kernel,
        out_shape=jax.ShapeDtypeStruct((m, n), F32),
        grid=(m // bm, n // bn),
        in_specs=[pl.BlockSpec((count, bm), lambda i, j: (0, i)), pl.BlockSpec((count, bn), lambda i, j: (0, j)), out],
        out_specs=out,
        compiler_params=pltpu.CompilerParams(dimension_semantics=("arbitrary", "arbitrary"), vmem_limit_bytes=62 << 20),
        cost_estimate=pl.CostEstimate(flops=2 * count * m * n, bytes_accessed=80 << 20, transcendentals=0),
        name="weight_grad_rest",
    )(a, b, part)


def hop_diagonal(diag):
    half = diag.shape[0] // 2
    return swap(diag[:half], 2), swap(diag[half:], 4)


def hop_near(side, back, came_side, came_back):
    half = side.shape[0] // 2
    kind = came_side.dtype
    side = jnp.concatenate([side[:half], side[half:] + came_back.astype(F32)], axis=0).astype(kind)
    back = jnp.concatenate([back[:half] + came_side.astype(F32), back[half:]], axis=0).astype(kind)
    return side, back


def solution(mesh):
    tp_size = mesh.shape["tp"]
    act_spec = P("dp", "tp", None)
    in_specs = (act_spec, act_spec, P("dp"), P("dp"), P(None), P(None, "tp"), P(None, None), P(None, None), P("tp", None), P(None), P(None, "tp"), P(None, "tp"), P("tp", None))
    out_specs = (act_spec, act_spec, P("dp"), P("dp", "tp"), P("dp", None), P("dp", None), P(("dp", "tp"), None), P("dp"), P("dp", "tp"), P("dp", "tp"), P(("dp", "tp"), None))

    def layer(hidden, grad_out, prefix_len, valid_len, attn_norm, w_query, w_key, w_value, w_out, mlp_norm, w_gate, w_up, w_down):
        batch, shard, dim = hidden.shape
        head_dim = w_key.shape[1]
        rows = batch * shard
        me = lax.axis_index("tp")
        starts = (me ^ jnp.array([0, 2, 4, 6, 1, 3, 5, 7], jnp.int32)) * shard
        k_pos = (starts[:, None] + jnp.arange(shard, dtype=jnp.int32)).reshape(1, tp_size * shard)
        cos_own, sin_own = rope_tables(me * shard + jnp.arange(shard), head_dim)
        hidden = hidden.reshape(rows, dim)
        grad_out = grad_out.reshape(rows, dim)
        normed, wq_all, wo_all, kv_all, query, mixed, resid, gated_in = front_layer(
            prefix_len, valid_len, k_pos, cos_own, sin_own, attn_norm, mlp_norm, hidden, w_query, w_key, w_value, w_out, batch, tp_size)
        wo_all = wo_all.reshape(tp_size * head_dim, dim)

        gated_all, grad_all, act, d_gate, d_upper, diag_in = gated_layer(gated_in, grad_out, w_gate, w_up, w_down, tp_size)
        own_part, x_part, y_part, g_gate_part = back_layer(act, d_gate, d_upper, gated_all, diag_in, w_gate, w_up, w_down, tp_size)
        hidden_out, d_resid, g_mlp_norm_part, d_mixed, g_out_part = join_layer(
            own_part, x_part, y_part, resid, grad_out, mlp_norm, wo_all, mixed)
        g_out = lax.psum_scatter(g_out_part, "tp", scatter_dimension=0, tiled=True)
        lens_back = jnp.concatenate([jnp.stack([prefix_len, valid_len, jnp.full((batch,), me, jnp.int32)]),
                                     jnp.broadcast_to(starts[:, None], (tp_size, batch))])
        d_q_raw, dkv_near, dkv_far = attention_backward(lens_back, cos_own, sin_own, query, kv_all, d_mixed, batch)
        near = tp_size // 2
        came_kv = swap(dkv_far, 1)
        g_far = jnp.einsum("kte,td->ked", d_q_raw[near:], normed, preferred_element_type=F32)
        came_kv, g_far = lax.optimization_barrier((came_kv, g_far))
        came_q = swap(g_far, 1)
        kv_own, kv_side, kv_back, kv_diag = [dkv_near[k].astype(F32) + came_kv[k].astype(F32) for k in range(4)]
        kv_came = hop_diagonal(kv_diag.astype(BF16))
        d_normed_q = jnp.einsum("hte,hde->td", d_q_raw, wq_all, preferred_element_type=F32)
        kv_came, d_normed_q = lax.optimization_barrier((kv_came, d_normed_q))
        kv_next = hop_near(kv_side, kv_back, *kv_came)
        kv_last = (swap(kv_next[0], 2), swap(kv_next[1], 4))
        came_q, dq_near = lax.optimization_barrier((came_q, d_q_raw[:near]))
        g_query_sum = jnp.einsum("kte,td->ked", dq_near, normed, preferred_element_type=F32) + came_q
        g_query_sum, act = lax.optimization_barrier((g_query_sum, act))
        q_came = hop_diagonal(g_query_sum[3])
        g_down = weight_grad(act, grad_all)
        kv_last, q_came, g_down = lax.optimization_barrier((kv_last, q_came, g_down))
        q_next = hop_near(g_query_sum[1], g_query_sum[2], *q_came)
        g_key_part, g_value_part, grad_hidden, g_attn_norm_part = finish_layer(
            kv_own, kv_last[0], kv_last[1], cos_own, sin_own, normed, w_key, w_value, d_normed_q, hidden, d_resid, attn_norm)
        norms = jnp.concatenate([g_attn_norm_part, g_mlp_norm_part])
        q_next, g_key_part, g_value_part, norms, d_gate = lax.optimization_barrier((q_next, g_key_part, g_value_part, norms, d_gate))
        g_key, g_value = lax.psum((g_key_part, g_value_part), "tp")
        last_side = swap(q_next[0], 2)
        q_last = (last_side, swap(q_next[1], 4))
        norms_near = [swap(norms, bit) for bit in (2, 4, 6)]
        g_gate = weight_grad_rest(gated_all, d_gate, g_gate_part, 6 * rows)
        norms_near, g_gate, d_upper = lax.optimization_barrier((norms_near, g_gate, d_upper))
        norms = norms + norms_near[0] + norms_near[1] + norms_near[2]
        norms, d_upper = lax.optimization_barrier((norms, d_upper))
        norms_core = swap(norms, 1)
        g_up = weight_grad(gated_all, d_upper)
        norms_core, q_last, g_up = lax.optimization_barrier((norms_core, q_last, g_up))
        g_norms = norms + norms_core
        g_query = (g_query_sum[0] + q_last[0] + q_last[1]).T
        full = (batch, shard, dim)
        return (hidden_out.reshape(full), grad_hidden.reshape(full), g_norms[0], g_query, g_key, g_value, g_out, g_norms[1], g_gate, g_up, g_down)

    return jax.shard_map(layer, mesh=mesh, in_specs=in_specs, out_specs=out_specs, check_vma=False)
```

```python
import functools
import math
import jax
import jax.numpy as jnp
from jax import lax
from jax.experimental import pallas as pl
from jax.experimental.pallas import tpu as pltpu
from jax.sharding import PartitionSpec as P

NORM_EPS = 1e-6
BF16 = jnp.bfloat16
F32 = jnp.float32
GELU_C = math.sqrt(2.0 / math.pi)
GELU_K = 0.044715
MASKED = -1e30
NT = (((1,), (1,)), ((), ()))
TN = (((0,), (0,)), ((), ()))


def rope_tables(positions, head_dim):
    half_dim = head_dim // 2
    exponent = jnp.arange(half_dim, dtype=F32) * (2.0 / head_dim)
    inv_freq = jnp.exp(exponent * (-math.log(10000.0)))
    angles = positions.astype(F32)[:, None] * inv_freq[None, :]
    return jnp.cos(angles), jnp.sin(angles)


def dot_nn(a, b):
    return jnp.dot(a, b, preferred_element_type=F32)


def dot_nt(a, b):
    return lax.dot_general(a, b, NT, preferred_element_type=F32)


def dot_tn(a, b):
    return lax.dot_general(a, b, TN, preferred_element_type=F32)


def swap(x, bit):
    return lax.ppermute(x, "tp", [(t, t ^ bit) for t in range(8)])


def flip(index, bit):
    return index + bit - 2 * bit * ((index // bit) % 2)


def neighbours():
    me = lax.axis_index("tp")
    return me, flip(me, 1), flip(me, 2), flip(me, 4)


def enter(peers):
    barrier = pltpu.get_barrier_semaphore()
    for peer in peers:
        pl.semaphore_signal(barrier, inc=1, device_id={"tp": peer}, device_id_type=pl.DeviceIdType.MESH)
    pl.semaphore_wait(barrier, len(peers))


def attn_bwd_kernel(lens_ref, cos_ref, sin_ref, q_ref, kv_ref, do_ref, dq_ref, dkv0_ref, dkv1_ref, dkv_acc):
    heads, shard, head_dim = q_ref.shape
    tp = kv_ref.shape[0]
    total = tp * shard
    rows = heads * shard
    s_id = pl.program_id(0)
    g_id = pl.program_id(1)
    prefix = lens_ref[0, s_id]
    valid = lens_ref[1, s_id]
    first = lens_ref[2, 0] * shard
    keys = kv_ref[:, :, :head_dim].reshape(total, head_dim)
    values = kv_ref[:, :, head_dim:].reshape(total, head_dim)
    query = q_ref[...].reshape(rows, head_dim) * BF16(head_dim ** -0.5)
    d_out = jnp.concatenate([do_ref[:, h * head_dim:(h + 1) * head_dim] for h in range(heads)], axis=0)
    step = lax.broadcasted_iota(jnp.int32, (shard, 1), 0)
    k_pos = jnp.concatenate([step + lens_ref[3 + r, 0] for r in range(tp)], axis=0)
    q_pos = first + lax.rem(lax.broadcasted_iota(jnp.int32, (1, rows), 1), shard)
    limit = jnp.minimum(valid, jnp.maximum(prefix, q_pos + 1))
    cos_t, sin_t = cos_ref[...][None], sin_ref[...][None]
    d_k = d_v = None
    count = heads // 2
    width = count * shard
    for c in range(2):
        cols = slice(c * width, (c + 1) * width)
        q_c, do_c = query[cols], d_out[cols]
        s = jnp.where(k_pos < limit[:, cols], dot_nt(keys, q_c), MASKED)
        e = jnp.exp(s - jnp.max(s, axis=0, keepdims=True))
        p = e * (1.0 / jnp.sum(e, axis=0, keepdims=True))
        d_p = dot_nt(values, do_c)
        delta = jnp.sum(p * d_p, axis=0, keepdims=True)
        d_s = (p * (d_p - delta)).astype(BF16)
        d_v_c = dot_nn(p.astype(BF16), do_c)
        d_k_c = dot_nn(d_s, q_c)
        d_k, d_v = (d_k_c, d_v_c) if d_k is None else (d_k + d_k_c, d_v + d_v_c)
        d_q = (dot_tn(d_s, keys) * (head_dim ** -0.5)).reshape(count, shard, head_dim)
        first, second = d_q[:, :, :head_dim // 2], d_q[:, :, head_dim // 2:]
        some = slice(c * count, (c + 1) * count)
        dq_ref[some, :, :head_dim // 2] = (first * cos_t + second * sin_t).astype(BF16)
        dq_ref[some, :, head_dim // 2:] = (second * cos_t - first * sin_t).astype(BF16)
    d_kv = jnp.concatenate([d_k, d_v], axis=1)

    @pl.when(g_id == 0)
    def _():
        dkv_acc[...] = d_kv

    @pl.when(g_id > 0)
    def _():
        dkv_acc[...] += d_kv

    @pl.when(g_id == pl.num_programs(1) - 1)
    def _():
        near = (tp // 2, shard, 2 * head_dim)
        dkv0_ref[...] = dkv_acc[:total // 2].astype(BF16).reshape(near)
        dkv1_ref[...] = dkv_acc[total // 2:].astype(BF16).reshape(near)


def remote(src, dst, send, recv, peer):
    return pltpu.make_async_remote_copy(src_ref=src, dst_ref=dst, send_sem=send, recv_sem=recv,
                                        device_id={"tp": peer}, device_id_type=pl.DeviceIdType.MESH)


def front_kernel(prefix_ref, valid_ref, kpos_ref, cos_ref, sin_ref, gain1_ref, gain2_ref, hidden, w_query, w_key, w_value, w_out,
                 normed_out, wq_all, wo_all, kv_all, query_out, mixed_out, resid_out, gated_out,
                 x_buf, n_buf, wkv, wq, wo, kv, q, probs, mix, acc, load, store, send, recv, *, batch):
    rows, dim = x_buf.shape
    shard = rows // batch
    head_dim = w_key.shape[1]
    tp = wq.shape[0]
    near = tp // 2
    total = tp * shard
    half_dim = head_dim // 2
    me, core, side, back = neighbours()
    bufs = (wq, kv, wo)

    def to_side(a):
        return remote(bufs[a].at[0], bufs[a].at[1], send.at[a, 0], recv.at[a, 0], side)

    def to_back(a):
        return remote(bufs[a].at[0], bufs[a].at[2], send.at[a, 1], recv.at[a, 1], back)

    def onward(a, k):
        half = bufs[a].shape[1] // 2
        part = pl.ds(k * half, half)
        return remote(bufs[a].at[1 + k, part], bufs[a].at[3, part], send.at[a, 2 + k], recv.at[a, 2 + k], (back, side)[k])

    def to_core(a, k):
        return remote(bufs[a].at[k], bufs[a].at[near + k], send.at[a, 4 + k], recv.at[a, 4 + k], core)

    loads = [pltpu.make_async_copy(src, dst, load.at[i]) for i, (src, dst) in enumerate((
        (w_query, wq.at[0]), (hidden, x_buf), (w_key, wkv.at[:, :head_dim]), (w_value, wkv.at[:, head_dim:]), (w_out, wo.at[0])))]
    mixed_at = [me, side, back, flip(side, 4)]
    mixed_at = mixed_at + [flip(dev, 1) for dev in mixed_at]
    stores = {name: pltpu.make_async_copy(src, dst, store.at[i]) for i, (name, src, dst) in enumerate((
        ("normed", n_buf, normed_out), ("wq", wq, wq_all), ("wo", wo, wo_all), ("kv", kv, kv_all), ("query", q, query_out),
        ("resid", x_buf, resid_out), ("gated", n_buf, gated_out)))}
    mixed_stores = [pltpu.make_async_copy(mix.at[:, pl.ds(k * head_dim, head_dim)],
                                          mixed_out.at[:, pl.ds(pl.multiple_of(dev * head_dim, 128), head_dim)], store.at[7 + k])
                    for k, dev in enumerate(mixed_at)]

    for cp in loads:
        cp.start()
    enter((core, side, back))
    loads[0].wait()
    to_side(0).start()
    to_back(0).start()
    to_core(0, 0).start()

    def norm_rows(src, gain_ref):
        x_f = src.astype(F32)
        inv_rms = lax.rsqrt(jnp.mean(x_f * x_f, axis=-1, keepdims=True) + NORM_EPS)
        return (x_f * inv_rms * (1.0 + gain_ref[...].astype(F32))).astype(BF16)

    def seq_rows(i):
        return pl.ds(pl.multiple_of(i * shard, 16), shard)

    def rotate(x_f):
        first, second = x_f[:, :half_dim], x_f[:, half_dim:]
        cos_t, sin_t = cos_ref[...], sin_ref[...]
        return first * cos_t - second * sin_t, second * cos_t + first * sin_t

    def norm1(i, carry):
        n_buf[seq_rows(i), :] = norm_rows(x_buf[seq_rows(i), :], gain1_ref)
        return carry

    loads[1].wait()
    lax.fori_loop(0, batch, norm1, 0)
    stores["normed"].start()
    loads[2].wait()
    loads[3].wait()

    def own_kv(i, carry):
        raw = dot_nn(n_buf[seq_rows(i), :], wkv[...])
        first, second = rotate(raw[:, :head_dim])
        kv[0, seq_rows(i), :half_dim] = first.astype(BF16)
        kv[0, seq_rows(i), half_dim:head_dim] = second.astype(BF16)
        kv[0, seq_rows(i), head_dim:] = raw[:, head_dim:].astype(BF16)
        return carry

    lax.fori_loop(0, batch, own_kv, 0)
    to_side(1).start()
    to_back(1).start()
    to_core(1, 0).start()

    def own_query(k):
        def step(i, carry):
            for h in (k, near + k):
                first, second = rotate(dot_nn(n_buf[seq_rows(i), :], wq[h]))
                q[h, seq_rows(i), :half_dim] = first.astype(BF16)
                q[h, seq_rows(i), half_dim:] = second.astype(BF16)
            return carry

        to_core(0, k).wait_recv()
        lax.fori_loop(0, batch, step, 0)

    def pass_on(a):
        to_side(a).wait_recv()
        onward(a, 0).start()
        to_core(a, 1).start()
        to_back(a).wait_recv()
        onward(a, 1).start()
        to_core(a, 2).start()

    def pass_last(a):
        onward(a, 0).wait_recv()
        onward(a, 1).wait_recv()
        to_core(a, 3).start()

    own_query(0)
    pass_on(0)
    own_query(1)
    own_query(2)
    pass_on(1)
    loads[4].wait()
    to_side(2).start()
    to_back(2).start()
    to_core(2, 0).start()
    pass_last(0)
    own_query(3)
    stores["query"].start()
    stores["wq"].start()
    pass_last(1)
    for k in range(near):
        to_core(1, k).wait_recv()
    stores["kv"].start()

    q_pos = me * shard + lax.broadcasted_iota(jnp.int32, (shard, 1), 0)

    def attend(i, carry):
        keys = kv[:, seq_rows(i), :head_dim].reshape(total, head_dim)
        values = kv[:, seq_rows(i), head_dim:].reshape(total, head_dim)
        visible = kpos_ref[...] < jnp.minimum(valid_ref[i], jnp.maximum(prefix_ref[i], q_pos + 1))
        for g in range(2):
            query = q[g * near:(g + 1) * near, seq_rows(i), :].reshape(near * shard, head_dim) * BF16(head_dim ** -0.5)
            scores = dot_nt(query, keys)
            for h in range(near):
                part = slice(h * shard, (h + 1) * shard)
                s = jnp.where(visible, scores[part], MASKED)
                e = jnp.exp(s - jnp.max(s, axis=-1, keepdims=True))
                probs[g, part, :] = (e * (1.0 / jnp.sum(e, axis=-1, keepdims=True))).astype(BF16)
            mixed = dot_nn(probs[g], values).astype(BF16)
            for h in range(near):
                head = g * near + h
                mix[seq_rows(i), head * head_dim:(head + 1) * head_dim] = mixed[h * shard:(h + 1) * shard]
        return carry

    lax.fori_loop(0, batch, attend, 0)
    for cp in mixed_stores:
        cp.start()
    pass_on(2)

    def project(k, first):
        def step(n, carry):
            cols = pl.ds(pl.multiple_of(n * 512, 128), 512)
            part = (dot_nn(mix[:, k * head_dim:(k + 1) * head_dim], wo[k, :, cols])
                    + dot_nn(mix[:, (near + k) * head_dim:(near + k + 1) * head_dim], wo[near + k, :, cols]))
            acc[:, cols] = part if first else acc[:, cols] + part
            return carry

        to_core(2, k).wait_recv()
        lax.fori_loop(0, dim // 512, step, 0)

    project(0, True)
    project(1, False)
    project(2, False)
    pass_last(2)
    project(3, False)
    stores["wo"].start()
    stores["normed"].wait()

    def norm2(i, carry):
        resid = (x_buf[seq_rows(i), :].astype(F32) + acc[seq_rows(i), :]).astype(BF16)
        x_buf[seq_rows(i), :] = resid
        n_buf[seq_rows(i), :] = norm_rows(resid, gain2_ref)
        return carry

    lax.fori_loop(0, batch, norm2, 0)
    stores["resid"].start()
    stores["gated"].start()
    for cp in mixed_stores:
        cp.wait()
    for name in ("wq", "wo", "kv", "query", "resid", "gated"):
        stores[name].wait()
    for a in range(3):
        to_side(a).wait_send()
        to_back(a).wait_send()
        for k in range(2):
            onward(a, k).wait_send()
        for k in range(near):
            to_core(a, k).wait_send()


def front_layer(prefix_len, valid_len, k_pos, cos_t, sin_t, attn_norm, mlp_norm, hidden, w_query, w_key, w_value, w_out, batch, tp):
    rows, dim = hidden.shape
    head_dim = w_key.shape[1]
    shard = rows // batch
    total = tp * shard
    anyspace = pl.BlockSpec(memory_space=pl.ANY)
    vmem = pl.BlockSpec(memory_space=pltpu.VMEM)
    dma = pltpu.SemaphoreType.DMA

    def shape(*dims):
        return jax.ShapeDtypeStruct(dims, BF16)

    return pl.pallas_call(
        functools.partial(front_kernel, batch=batch),
        out_shape=(shape(rows, dim), shape(tp, dim, head_dim), shape(tp, head_dim, dim), shape(tp, rows, 2 * head_dim),
                   shape(tp, rows, head_dim), shape(rows, tp * head_dim), shape(rows, dim), shape(rows, dim)),
        in_specs=[pl.BlockSpec(memory_space=pltpu.SMEM)] * 2 + [vmem] * 5 + [anyspace] * 5,
        out_specs=(anyspace,) * 8,
        scratch_shapes=[pltpu.VMEM((rows, dim), BF16), pltpu.VMEM((rows, dim), BF16), pltpu.VMEM((dim, 2 * head_dim), BF16),
                        pltpu.VMEM((tp, dim, head_dim), BF16), pltpu.VMEM((tp, head_dim, dim), BF16),
                        pltpu.VMEM((tp, rows, 2 * head_dim), BF16), pltpu.VMEM((tp, rows, head_dim), BF16),
                        pltpu.VMEM((2, tp // 2 * shard, total), BF16), pltpu.VMEM((rows, tp * head_dim), BF16), pltpu.VMEM((rows, dim), F32),
                        dma((5,)), dma((15,)), dma((3, 8)), dma((3, 8))],
        compiler_params=pltpu.CompilerParams(vmem_limit_bytes=62 << 20, collective_id=2, has_side_effects=True),
        cost_estimate=pl.CostEstimate(flops=8 * rows * dim * tp * head_dim, bytes_accessed=60 << 20, transcendentals=tp * rows * total),
        name="front",
    )(prefix_len, valid_len, k_pos, cos_t, sin_t, attn_norm.reshape(1, dim), mlp_norm.reshape(1, dim), hidden, w_query, w_key, w_value, w_out)


def attention_backward(lens, cos_t, sin_t, query, kv_all, d_mixed, batch, group=8):
    heads, rows, head_dim = query.shape
    near = kv_all.shape[0] // 2
    shard = rows // batch
    total = 2 * near * shard
    q_spec = pl.BlockSpec((group, shard, head_dim), lambda s, g, *_: (g, s, 0))
    kv_spec = pl.BlockSpec((near, shard, 2 * head_dim), lambda s, g, *_: (0, s, 0))
    table = pl.BlockSpec((shard, head_dim // 2), lambda s, g, *_: (0, 0))
    kv_shape = jax.ShapeDtypeStruct((near, rows, 2 * head_dim), BF16)
    return pl.pallas_call(
        attn_bwd_kernel,
        out_shape=(jax.ShapeDtypeStruct((heads, rows, head_dim), BF16), kv_shape, kv_shape),
        grid_spec=pltpu.PrefetchScalarGridSpec(
            num_scalar_prefetch=1, grid=(batch, heads // group),
            in_specs=[table, table, q_spec, pl.BlockSpec((2 * near, shard, 2 * head_dim), lambda s, g, *_: (0, s, 0)), pl.BlockSpec((shard, group * head_dim), lambda s, g, *_: (s, g))],
            out_specs=(q_spec, kv_spec, kv_spec),
            scratch_shapes=[pltpu.VMEM((total, 2 * head_dim), F32)]),
        compiler_params=pltpu.CompilerParams(dimension_semantics=("arbitrary", "arbitrary"), vmem_limit_bytes=62 << 20),
        cost_estimate=pl.CostEstimate(flops=10 * heads * rows * total * head_dim, bytes_accessed=20 << 20, transcendentals=heads * rows * total),
        name="attn_bwd",
    )(lens, cos_t, sin_t, query, kv_all, d_mixed)


def gated_tile(z, g, w_g, w_u, w_d):
    gate = dot_nn(z, w_g)
    upper = dot_nn(z, w_u)
    d_act = dot_nt(g, w_d).astype(BF16).astype(F32)
    sq = gate * gate
    th = jnp.tanh(gate * (GELU_C + (GELU_C * GELU_K) * sq))
    half = 0.5 + 0.5 * th
    gelu = gate * half
    slope = half + gate * (0.5 - 0.5 * (th * th)) * (GELU_C + (3.0 * GELU_C * GELU_K) * sq)
    return (gelu * upper).astype(BF16), (d_act * upper * slope).astype(BF16), (d_act * gelu).astype(BF16)


def gated_kernel(z_own, g_own, wg_hbm, wu_hbm, wd_hbm, z_all, g_all, act, d_gate, d_up, diag_in,
                 wg, wu, wd, z_buf, g_buf, outs, st, from_core, far_send, far_recv, diag_send, diag_recv, w_sem, in_sem, own_sem, out_sem, send, recv, send0, recv0, *, bn):
    rows, dim = z_own.shape
    width = wg_hbm.shape[1]
    steps = width // bn
    piece = rows // 4
    me, core, side, back = neighbours()
    corner = flip(side, 4)
    own = (z_own, g_own)
    full = (z_all, g_all)

    def part(slot, q):
        return pl.ds(pl.multiple_of(slot * rows + q * piece, 16), piece)

    def link_rows(u, path):
        turn = u // 2
        diag = turn % 2
        if path == 0:
            return side + (corner - side) * diag, (u % 2) + 2 * (turn // 2) + diag * 2
        return back + (corner - back) * diag, (u % 2) + 2 - 2 * (turn // 2) - diag * 2

    def link_copy(u, path, a):
        turn = u // 2
        peer = side if path == 0 else back
        sems = (send.at[path, u, a], recv.at[path, u, a])
        if turn == 1:
            slot = back if path == 0 else side
            q = (2 if path == 0 else 0) + u % 2
            return remote(full[a].at[part(slot, q)], full[a].at[part(slot, q)], *sems, peer)
        q = u % 2 + (2 * (turn // 2) if path == 0 else 2 - 2 * (turn // 2))
        return remote(own[a].at[pl.ds(q * piece, piece)], full[a].at[part(me, q)], *sems, peer)

    def core_copy(u, path, a):
        slot, q = link_rows(u, path)
        return remote(full[a].at[part(slot, q)], full[a].at[part(slot, q)], send.at[2 + path, u, a], recv.at[2 + path, u, a], core)

    def own_copy(a):
        return remote(own[a], full[a].at[pl.ds(pl.multiple_of(me * rows, 16), rows)], send0.at[a], recv0.at[a], core)

    def weight_copies(n):
        cols = pl.ds(pl.multiple_of(n * bn, 128), bn)
        return [pltpu.make_async_copy(wg_hbm.at[:, cols], wg.at[:, cols], w_sem.at[0, n]),
                pltpu.make_async_copy(wu_hbm.at[:, cols], wu.at[:, cols], w_sem.at[1, n]),
                pltpu.make_async_copy(wd_hbm.at[cols], wd.at[cols], w_sem.at[2, n])]

    bufs = (z_buf, g_buf)
    own_in = [pltpu.make_async_copy(own[a], bufs[a], own_sem.at[a]) for a in range(2)]
    own_out = [pltpu.make_async_copy(bufs[a], full[a].at[pl.ds(pl.multiple_of(me * rows, 16), rows)], own_sem.at[2 + a]) for a in range(2)]
    for cp in own_in:
        cp.start()
    for n in range(steps):
        for cp in weight_copies(n):
            cp.start()
    enter((core, side, back))
    for u in range(2):
        for path in range(2):
            for a in range(2):
                link_copy(u, path, a).start()
        if u == 0:
            for a in range(2):
                own_copy(a).start()

    def out_copies(slot, s_rows, n):
        cols = pl.ds(pl.multiple_of(n * bn, 128), bn)
        return [pltpu.make_async_copy(outs.at[slot, k, pl.ds(i * piece, piece)], ref.at[s_rows[i], cols], out_sem.at[slot, k, i])
                for k, ref in enumerate((act, d_gate, d_up)) for i in range(4)]

    def stage_rows(s):
        late = (s + 6) // 8
        u = (s - 2) * late
        first = me + (core - me) * s * (1 - late)
        (slot_x, q_x), (slot_y, q_y) = link_rows(u, 0), link_rows(u, 1)
        base_x, base_y = slot_x * rows + q_x * piece, slot_y * rows + q_y * piece
        pair_x, pair_y = flip(slot_x, 1) * rows + q_x * piece, flip(slot_y, 1) * rows + q_y * piece
        starts = [(1 - late) * (first * rows + i * piece) + late * base for i, base in enumerate((base_x, base_y, pair_x, pair_y))]
        return [pl.ds(pl.multiple_of(st, 16), piece) for st in starts]

    def pass_on(u):
        for path in range(2):
            for a in range(2):
                link_copy(u, path, a).wait_recv()
                core_copy(u, path, a).start()
        later = (2,) if u == 0 else (3, 4, 5) if u == 1 else ()
        for v in later:
            for path in range(2):
                for a in range(2):
                    link_copy(v, path, a).start()

    def far_copy(j):
        return remote(st.at[0, j], from_core.at[j], far_send.at[j], far_recv.at[j], core)

    def diag_copy(k, j):
        half = rows // 2
        return remote(st.at[1, j, pl.ds(k * half, half)], diag_in.at[k, :, pl.ds(pl.multiple_of(j * bn, 128), bn)],
                      diag_send.at[k, j], diag_recv.at[k, j], (side, back)[k])

    def down_diagonal():
        for slot in range(2):
            for cp in out_copies(slot, stage_rows(5), 0):
                cp.wait()
        loads = [pltpu.make_async_copy(act.at[pl.ds(pl.multiple_of(dev * rows, 16), rows)], bufs[a], in_sem.at[a, 0])
                 for a, dev in enumerate((flip(corner, 1), corner))]
        for cp in loads:
            cp.start()

        def theirs(j, carry):
            st[0, j] = dot_nn(z_buf[...], wd[:, pl.ds(pl.multiple_of(j * bn, 128), bn)]).astype(BF16)
            far_copy(j).start()
            return carry

        def mine(j, carry):
            far_copy(j).wait_recv()
            total = dot_nn(g_buf[...], wd[:, pl.ds(pl.multiple_of(j * bn, 128), bn)]) + from_core[j].astype(F32)
            st[1, j] = total.astype(BF16)
            for k in range(2):
                diag_copy(k, j).start()
            return carry

        loads[0].wait()
        lax.fori_loop(0, dim // bn, theirs, 0)
        loads[1].wait()
        lax.fori_loop(0, dim // bn, mine, 0)

    def compute(s):
        s_rows = stage_rows(s)

        def block(n, carry):
            step = s * steps + n
            slot = step % 2

            @pl.when((step >= 2) & (step // 2 != 6 * steps // 2))
            def _():
                for cp in out_copies(slot, s_rows, n):
                    cp.wait()

            @pl.when(s == 0)
            def _():
                for cp in weight_copies(n):
                    cp.wait()

            for u in range(6):
                @pl.when((s == u + 1) & (n == steps - 1))
                def _(u=u):
                    pass_on(u)

            cols = pl.ds(pl.multiple_of(n * bn, 128), bn)
            res = gated_tile(z_buf[...], g_buf[...], wg[:, cols], wu[:, cols], wd[cols, :])
            for k in range(3):
                outs[slot, k] = res[k]
            for cp in out_copies(slot, s_rows, n):
                cp.start()
            return carry

        lax.fori_loop(0, steps, block, 0)

    def stage(s, carry):
        @pl.when(s == 0)
        def _():
            for cp in own_in:
                cp.wait()
            for cp in own_out:
                cp.start()

        @pl.when(s == 1)
        def _():
            for cp in own_out:
                cp.wait()
            for a in range(2):
                own_copy(a).wait_recv()

        for u in range(6):
            @pl.when(s == u + 2)
            def _(u=u):
                if u == 4:
                    down_diagonal()
                for path in range(2):
                    for a in range(2):
                        core_copy(u, path, a).wait_recv()

        @pl.when(s >= 1)
        def _():
            s_rows = stage_rows(s)
            copies = [pltpu.make_async_copy(full[a].at[s_rows[i]], bufs[a].at[pl.ds(i * piece, piece)], in_sem.at[a, i])
                      for a in range(2) for i in range(4)]
            for cp in copies:
                cp.start()
            for cp in copies:
                cp.wait()

        compute(s)
        return carry

    lax.fori_loop(0, 8, stage, 0)
    last = stage_rows(7)
    for slot in range(2):
        for cp in out_copies(slot, last, 0):
            cp.wait()
    for j in range(dim // bn):
        far_copy(j).wait_send()
        for k in range(2):
            diag_copy(k, j).wait_send()
            diag_copy(k, j).wait_recv()
    for a in range(2):
        own_copy(a).wait_send()
        for path in range(2):
            for u in range(6):
                link_copy(u, path, a).wait_send()
                core_copy(u, path, a).wait_send()


def gated_layer(z_own, g_own, w_gate, w_up, w_down, tp, bn=512):
    rows, dim = z_own.shape
    width = w_gate.shape[1]
    total = rows * tp
    anyspace = pl.BlockSpec(memory_space=pl.ANY)
    gathered = jax.ShapeDtypeStruct((total, dim), BF16)
    made = jax.ShapeDtypeStruct((total, width), BF16)
    dma = pltpu.SemaphoreType.DMA
    return pl.pallas_call(
        functools.partial(gated_kernel, bn=bn),
        out_shape=(gathered, gathered, made, made, made, jax.ShapeDtypeStruct((2, rows // 2, dim), BF16)),
        in_specs=[anyspace] * 5,
        out_specs=(anyspace,) * 6,
        scratch_shapes=[pltpu.VMEM((dim, width), BF16), pltpu.VMEM((dim, width), BF16), pltpu.VMEM((width, dim), BF16),
                        pltpu.VMEM((rows, dim), BF16), pltpu.VMEM((rows, dim), BF16), pltpu.VMEM((2, 3, rows, bn), BF16),
                        pltpu.VMEM((2, dim // bn, rows, bn), BF16), pltpu.VMEM((dim // bn, rows, bn), BF16),
                        dma((dim // bn,)), dma((dim // bn,)), dma((2, dim // bn)), dma((2, dim // bn)), dma((3, width // bn)), dma((2, 4)), dma((4,)), dma((2, 3, 4)), dma((4, 6, 2)), dma((4, 6, 2)), dma((2,)), dma((2,))],
        compiler_params=pltpu.CompilerParams(vmem_limit_bytes=67043328, collective_id=0, has_side_effects=True),
        cost_estimate=pl.CostEstimate(flops=6 * total * dim * width, bytes_accessed=200 << 20, transcendentals=total * width),
        name="gated",
    )(z_own, g_own, w_gate, w_up, w_down)


def back_kernel(act, d_gate, d_up, z_all, diag_in, wg_hbm, wu_hbm, wd_hbm, own_out, x_in, y_in, g_gate,
                wa, wb, lhs, st, from_core, from_diag, own_st, in_sem, z_sem, w_sem, l_sem, o_sem, c_send, c_recv, d_send, d_recv, f_send, f_recv, *, rows, bn):
    dim, width = wg_hbm.shape
    steps = dim // bn
    half = rows // 2
    me, core, side, back = neighbours()

    def cols(j):
        return pl.ds(pl.multiple_of(j * bn, 128), bn)

    def shard_of(phase, t):
        if phase == 0:
            return 1 + t // 2, 1 - t % 2
        ge = [(t + 8 - k) // 8 for k in range(8)]
        return ge[2] + ge[3] - ge[5] + 2 * ge[6], 1 - ge[1] + ge[2] - ge[4] + ge[6] - ge[7]

    def lhs_copies(phase, t):
        pair, theirs = shard_of(phase, t)
        dev = me + (1 - pair // 2) * (side - me) + (1 - pair % 2) * (back - me)
        dev = dev + theirs * (flip(dev, 1) - dev)
        src = pl.ds(pl.multiple_of(dev * rows, 16), rows)
        refs = (act,) if phase == 0 else (d_gate, d_up)
        return [pltpu.make_async_copy(ref.at[src], lhs.at[t % 2, k], l_sem.at[t % 2, k]) for k, ref in enumerate(refs)]

    def weight_copy(k, j):
        if k == 0:
            return pltpu.make_async_copy(wd_hbm.at[:, cols(j)], wa.at[pl.ds(0, width), cols(j)], w_sem.at[0, j])
        src, dst = (wg_hbm, wb) if k == 1 else (wu_hbm, wa)
        return pltpu.make_async_copy(src.at[cols(j)], dst.at[cols(j)], w_sem.at[k, j])

    def core_copy(pair, j):
        return remote(st.at[0, j], from_core.at[pair, j], c_send.at[j], c_recv.at[pair, j], core)

    def diag_copy(phase, k, j):
        return remote(st.at[1, j, pl.ds(k * half, half)], from_diag.at[phase, k, j], d_send.at[k, j], d_recv.at[phase, k, j], (side, back)[k])

    def final_copy(phase, k, j):
        return remote(st.at[2 + k, j], (x_in, y_in)[k].at[phase, :, cols(j)], f_send.at[k, j], f_recv.at[phase, k, j], (side, back)[k])

    def own_copy(phase, j):
        return pltpu.make_async_copy(own_st.at[j % 2], own_out.at[phase, :, cols(j)], o_sem.at[j % 2])

    def product(phase, slot, j):
        if phase == 0:
            return dot_nn(lhs[slot, 0], wa[:width, cols(j)])
        return dot_nt(lhs[slot, 0], wb[cols(j), :]) + dot_nt(lhs[slot, 1], wa[cols(j), :])

    def diag_load(k, j):
        return pltpu.make_async_copy(diag_in.at[k, :, cols(j)], from_diag.at[0, k, j], in_sem.at[k, j])

    for cp in lhs_copies(0, 0):
        cp.start()
    for j in range(steps):
        weight_copy(0, j).start()
    for k in range(2):
        for j in range(steps):
            diag_load(k, j).start()
    enter((core, side, back))

    def tiles(body):
        def step(j, carry):
            body(j)
            return carry

        lax.fori_loop(0, steps, step, 0)

    for phase in (0, 1):
        def step(t, carry, phase=phase):
            for cp in lhs_copies(phase, t):
                cp.wait()

            last = 5 if phase == 0 else 7

            @pl.when(t < last)
            def _():
                for cp in lhs_copies(phase, t + 1):
                    cp.start()

            if phase == 0:
                @pl.when(t == 1)
                def _():
                    for j in range(steps):
                        weight_copy(1, j).start()

                @pl.when(t == last)
                def _():
                    for cp in lhs_copies(1, 0):
                        cp.start()

            theirs = (t % 2 == 0) if phase == 0 else ((t % 6 == 0) | (t // 2 == 1))

            @pl.when(theirs)
            def _():
                pair = shard_of(phase, t)[0]

                def body(j):
                    @pl.when(t == 0)
                    def _():
                        for k in ((0,) if phase == 0 else (1, 2)):
                            weight_copy(k, j).wait()

                    if phase == 0:
                        @pl.when(t > 0)
                        def _():
                            core_copy(0, j).wait_send()
                    else:
                        core_copy(0, j).wait_send()
                    st[0, j] = product(phase, t % 2, j).astype(BF16)
                    core_copy(pair, j).start()

                tiles(body)

            if phase == 1:
                @pl.when(t == 1)
                def _():
                    def body(j):
                        core_copy(0, j).wait_recv()
                        st[1, j] = (product(phase, 1, j) + from_core[0, j].astype(F32)).astype(BF16)
                        for k in range(2):
                            diag_copy(phase, k, j).start()

                    tiles(body)

            for k in range(2):
                @pl.when(t == (1 + 2 * k if phase == 0 else 5 - k))
                def _(k=k):
                    def body(j):
                        core_copy(1 + k, j).wait_recv()
                        if phase == 0:
                            diag_load(1 - k, j).wait()
                        else:
                            diag_copy(phase, 1 - k, j).wait_recv()
                            final_copy(0, k, j).wait_send()
                        total = product(phase, 1 if phase == 0 else 1 - k, j) + from_core[1 + k, j].astype(F32)
                        came = from_diag[phase, 1 - k, j].astype(F32)
                        split = slice(half, rows) if k == 0 else slice(0, half)
                        rest = slice(0, half) if k == 0 else slice(half, rows)
                        st[2 + k, j, split, :] = (total[split] + came).astype(BF16)
                        st[2 + k, j, rest, :] = total[rest].astype(BF16)
                        final_copy(phase, k, j).start()

                    tiles(body)

            @pl.when(t == last)
            def _():
                def body(j):
                    core_copy(3, j).wait_recv()

                    @pl.when(j >= 2)
                    def _():
                        own_copy(phase, j).wait()

                    own_st[j % 2] = product(phase, 1, j) + from_core[3, j].astype(F32)
                    own_copy(phase, j).start()

                tiles(body)
                for j in (0, 1):
                    own_copy(phase, j).wait()
                if phase == 0:
                    for j in range(steps):
                        weight_copy(2, j).start()

            return carry

        lax.fori_loop(0, 6 if phase == 0 else 8, step, 0)

    first = z_all.shape[0] - 2 * rows

    def z_copy(j, c):
        return pltpu.make_async_copy(z_all.at[pl.ds(first + c * rows, rows), cols(j)], lhs.at[0, c, :, cols(j)], z_sem.at[j, c])

    def gate_copy(j):
        return pltpu.make_async_copy(d_gate.at[pl.ds(first, 2 * rows), cols(j)], wa.at[pl.ds(0, 2 * rows), cols(j)], w_sem.at[0, j])

    def grad_copy(i, j):
        slot = j % 2
        return pltpu.make_async_copy(own_st.at[slot, pl.ds(0, bn)], g_gate.at[cols(i), cols(j)], o_sem.at[slot])

    for j in range(steps):
        for c in range(2):
            z_copy(j, c).start()
        gate_copy(j).start()

    def grad_tile(step, carry):
        i, j = step // steps, step % steps

        @pl.when(i == 0)
        def _():
            gate_copy(j).wait()

        @pl.when(j == 0)
        def _():
            for c in range(2):
                z_copy(i, c).wait()

        @pl.when(step >= 2)
        def _():
            grad_copy(i, j).wait()

        own_st[j % 2, :bn] = dot_tn(lhs[0, :, :, cols(i)].reshape(2 * rows, bn), wa[:2 * rows, cols(j)])
        grad_copy(i, j).start()
        return carry

    lax.fori_loop(0, steps * steps, grad_tile, 0)
    for j in range(2):
        grad_copy(0, j).wait()
    for j in range(steps):
        core_copy(0, j).wait_send()
        for k in range(2):
            diag_copy(1, k, j).wait_send()
            final_copy(1, k, j).wait_send()
            for phase in (0, 1):
                final_copy(phase, k, j).wait_recv()


def back_layer(act, d_gate, d_up, z_all, diag_in, w_gate, w_up, w_down, tp, bn=512):
    total, width = act.shape
    dim = w_gate.shape[0]
    rows = total // tp
    steps = dim // bn
    anyspace = pl.BlockSpec(memory_space=pl.ANY)
    dma = pltpu.SemaphoreType.DMA
    came = jax.ShapeDtypeStruct((2, rows, dim), BF16)
    return pl.pallas_call(
        functools.partial(back_kernel, rows=rows, bn=bn),
        out_shape=(jax.ShapeDtypeStruct((2, rows, dim), F32), came, came, jax.ShapeDtypeStruct((dim, width), F32)),
        in_specs=[anyspace] * 8,
        out_specs=(anyspace,) * 4,
        scratch_shapes=[pltpu.VMEM((width, dim), BF16), pltpu.VMEM((dim, width), BF16), pltpu.VMEM((2, 2, rows, width), BF16),
                        pltpu.VMEM((4, steps, rows, bn), BF16), pltpu.VMEM((4, steps, rows, bn), BF16),
                        pltpu.VMEM((2, 2, steps, rows // 2, bn), BF16), pltpu.VMEM((2, rows, bn), F32),
                        dma((2, steps)), dma((steps, 2)), dma((3, steps)), dma((2, 2)), dma((2,)), dma((steps,)), dma((4, steps)),
                        dma((2, steps)), dma((2, 2, steps)), dma((2, steps)), dma((2, 2, steps))],
        compiler_params=pltpu.CompilerParams(vmem_limit_bytes=67043328, collective_id=1, has_side_effects=True),
        cost_estimate=pl.CostEstimate(flops=6 * total * dim * width, bytes_accessed=200 << 20, transcendentals=0),
        name="back",
    )(act, d_gate, d_up, z_all, diag_in, w_gate, w_up, w_down)


def norm_back(x, gain, d_out):
    inv_rms = lax.rsqrt(jnp.mean(x * x, axis=-1, keepdims=True) + NORM_EPS)
    unit = x * inv_rms
    scaled = d_out * (1.0 + gain.astype(F32))
    return inv_rms * (scaled - unit * jnp.mean(unit * scaled, axis=-1, keepdims=True)), d_out * unit


def join_kernel(own_ref, x_ref, y_ref, resid_ref, grad_ref, gain_ref, wo_ref, mixed_ref,
                out_ref, d_resid_ref, g_gain_ref, d_mixed_ref, g_out_ref, keep, *, joins):
    step = pl.program_id(0)
    bm = resid_ref.shape[0]

    @pl.when(step == 0)
    def _():
        g_gain_ref[...] = jnp.zeros_like(g_gain_ref)

    @pl.when(step < joins)
    def _():
        mlp_sum, d_gated = [own_ref[k] + x_ref[k].astype(F32) + y_ref[k].astype(F32) for k in range(2)]
        resid = resid_ref[...].astype(F32)
        out_ref[...] = (resid + mlp_sum).astype(BF16)
        d_norm, terms = norm_back(resid, gain_ref[...], d_gated.astype(BF16).astype(F32))
        d_resid = (grad_ref[...].astype(F32) + d_norm).astype(BF16)
        d_resid_ref[...] = d_resid
        keep[pl.ds(pl.multiple_of(step * bm, 16), bm), :] = d_resid
        g_gain_ref[...] += jnp.sum(terms, axis=0, keepdims=True)

    @pl.when(step >= joins)
    def _():
        d_mixed_ref[...] = dot_nt(keep[...], wo_ref[...]).astype(BF16)
        g_out_ref[...] = dot_tn(mixed_ref[...], keep[...])


def join_layer(own_part, x_part, y_part, resid, grad_out, gain, wo_all, mixed, bm=96, bn=512):
    rows, dim = resid.shape
    width = mixed.shape[1]
    joins = rows // bm
    pair = pl.BlockSpec((2, bm, dim), lambda i: (0, jnp.minimum(i, joins - 1), 0))
    row = pl.BlockSpec((bm, dim), lambda i: (jnp.minimum(i, joins - 1), 0))
    one = pl.BlockSpec((1, dim), lambda i: (0, 0))
    col = pl.BlockSpec((rows, bn), lambda i: (0, jnp.maximum(i - joins, 0)))
    block = pl.BlockSpec((bn, dim), lambda i: (jnp.maximum(i - joins, 0), 0))
    act = jax.ShapeDtypeStruct((rows, dim), BF16)
    return pl.pallas_call(
        functools.partial(join_kernel, joins=joins),
        out_shape=(act, act, jax.ShapeDtypeStruct((1, dim), F32), jax.ShapeDtypeStruct((rows, width), BF16),
                   jax.ShapeDtypeStruct((width, dim), F32)),
        grid=(joins + width // bn,),
        in_specs=[pair, pair, pair, row, row, one, block, col],
        out_specs=(row, row, one, col, block),
        scratch_shapes=[pltpu.VMEM((rows, dim), BF16)],
        compiler_params=pltpu.CompilerParams(dimension_semantics=("arbitrary",), vmem_limit_bytes=62 << 20),
        cost_estimate=pl.CostEstimate(flops=4 * rows * dim * width, bytes_accessed=60 << 20, transcendentals=rows),
        name="join",
    )(own_part, x_part, y_part, resid, grad_out, gain.reshape(1, dim), wo_all, mixed)


def finish_kernel(kv_ref, side_ref, back_ref, cos_ref, sin_ref, normed_ref, wk_ref, wv_ref, part_ref, hidden_ref, d_resid_ref, gain_ref, mlp_ref,
                  g_key_ref, g_value_ref, out_ref):
    head_dim = wk_ref.shape[1]
    half_dim = head_dim // 2
    d_kv = (kv_ref[...] + side_ref[...].astype(F32) + back_ref[...].astype(F32)).astype(BF16)
    first, second = d_kv[:, :half_dim].astype(F32), d_kv[:, half_dim:head_dim].astype(F32)
    cos_t, sin_t = cos_ref[...], sin_ref[...]
    d_key = jnp.concatenate([first * cos_t + second * sin_t, second * cos_t - first * sin_t], axis=1).astype(BF16)
    d_value = d_kv[:, head_dim:]
    d_normed = (part_ref[...] + dot_nt(d_key, wk_ref[...]) + dot_nt(d_value, wv_ref[...])).astype(BF16).astype(F32)
    d_norm, terms = norm_back(hidden_ref[...].astype(F32), gain_ref[...], d_normed)
    out_ref[...] = (d_resid_ref[...].astype(F32) + d_norm).astype(BF16)
    g_key = dot_tn(normed_ref[...], d_key)
    g_value = dot_tn(normed_ref[...], d_value)
    g_gain = jnp.sum(terms, axis=0, keepdims=True)
    dim = g_key.shape[0]
    lines = dim // head_dim

    @pl.when(pl.program_id(0) == 0)
    def _():
        g_key_ref[...] = g_key
        g_value_ref[:dim] = g_value
        for r in range(lines):
            part = slice(r * head_dim, (r + 1) * head_dim)
            g_value_ref[dim + r:dim + r + 1] = g_gain[:, part]
            g_value_ref[dim + lines + r:dim + lines + r + 1] = mlp_ref[:, part]

    @pl.when(pl.program_id(0) > 0)
    def _():
        g_key_ref[...] += g_key
        g_value_ref[:dim] += g_value
        for r in range(lines):
            g_value_ref[dim + r:dim + r + 1] += g_gain[:, r * head_dim:(r + 1) * head_dim]


def finish_layer(kv_own, kv_side, kv_back, cos_t, sin_t, normed, w_key, w_value, part, hidden, d_resid, gain, g_mlp_norm):
    rows, dim = hidden.shape
    shard, half_dim = cos_t.shape
    head_dim = w_key.shape[1]

    def row(width):
        return pl.BlockSpec((shard, width), lambda i: (i, 0))

    def whole(*shape):
        return pl.BlockSpec(shape, lambda i: (0, 0))

    kv, act, table, weight, one = row(2 * head_dim), row(dim), whole(shard, half_dim), whole(dim, head_dim), whole(1, dim)
    grad = jax.ShapeDtypeStruct((dim, head_dim), F32)
    return pl.pallas_call(
        finish_kernel,
        out_shape=(grad, jax.ShapeDtypeStruct((dim + 2 * dim // head_dim, head_dim), F32), jax.ShapeDtypeStruct((rows, dim), BF16)),
        grid=(rows // shard,),
        in_specs=[kv, kv, kv, table, table, act, weight, weight, act, act, act, one, one],
        out_specs=(weight, whole(dim + 2 * dim // head_dim, head_dim), act),
        compiler_params=pltpu.CompilerParams(dimension_semantics=("arbitrary",), vmem_limit_bytes=62 << 20),
        cost_estimate=pl.CostEstimate(flops=8 * rows * dim * head_dim, bytes_accessed=24 << 20, transcendentals=rows),
        name="finish",
    )(kv_own, kv_side, kv_back, cos_t, sin_t, normed, w_key, w_value, part, hidden, d_resid, gain.reshape(1, dim), g_mlp_norm)


def product_kernel(a_ref, b_ref, o_ref):
    o_ref[...] = dot_tn(a_ref[...], b_ref[...])


def weight_grad(a, b, bm=1024, bn=512):
    rows, m = a.shape
    n = b.shape[1]
    return pl.pallas_call(
        product_kernel,
        out_shape=jax.ShapeDtypeStruct((m, n), F32),
        grid=(m // bm, n // bn),
        in_specs=[pl.BlockSpec((rows, bm), lambda i, j: (0, i)), pl.BlockSpec((rows, bn), lambda i, j: (0, j))],
        out_specs=pl.BlockSpec((bm, bn), lambda i, j: (i, j)),
        compiler_params=pltpu.CompilerParams(dimension_semantics=("arbitrary", "arbitrary"), vmem_limit_bytes=62 << 20),
        cost_estimate=pl.CostEstimate(flops=2 * rows * m * n, bytes_accessed=110 << 20, transcendentals=0),
        name="weight_grad",
    )(a, b)


def rest_kernel(a_ref, b_ref, part_ref, o_ref):
    o_ref[...] = part_ref[...] + dot_tn(a_ref[...], b_ref[...])


def weight_grad_rest(a, b, part, count, bm=1024, bn=512):
    m, n = part.shape
    out = pl.BlockSpec((bm, bn), lambda i, j: (i, j))
    return pl.pallas_call(
        rest_kernel,
        out_shape=jax.ShapeDtypeStruct((m, n), F32),
        grid=(m // bm, n // bn),
        in_specs=[pl.BlockSpec((count, bm), lambda i, j: (0, i)), pl.BlockSpec((count, bn), lambda i, j: (0, j)), out],
        out_specs=out,
        compiler_params=pltpu.CompilerParams(dimension_semantics=("arbitrary", "arbitrary"), vmem_limit_bytes=62 << 20),
        cost_estimate=pl.CostEstimate(flops=2 * count * m * n, bytes_accessed=80 << 20, transcendentals=0),
        name="weight_grad_rest",
    )(a, b, part)


def hop_diagonal(diag):
    half = diag.shape[0] // 2
    return swap(diag[:half], 2), swap(diag[half:], 4)


def hop_near(side, back, came_side, came_back):
    half = side.shape[0] // 2
    kind = came_side.dtype
    side = jnp.concatenate([side[:half], side[half:] + came_back.astype(F32)], axis=0).astype(kind)
    back = jnp.concatenate([back[:half] + came_side.astype(F32), back[half:]], axis=0).astype(kind)
    return side, back


def solution(mesh):
    tp_size = mesh.shape["tp"]
    act_spec = P("dp", "tp", None)
    in_specs = (act_spec, act_spec, P("dp"), P("dp"), P(None), P(None, "tp"), P(None, None), P(None, None), P("tp", None), P(None), P(None, "tp"), P(None, "tp"), P("tp", None))
    out_specs = (act_spec, act_spec, P("dp"), P("dp", "tp"), P("dp", None), P("dp", None), P(("dp", "tp"), None), P("dp"), P("dp", "tp"), P("dp", "tp"), P(("dp", "tp"), None))

    def layer(hidden, grad_out, prefix_len, valid_len, attn_norm, w_query, w_key, w_value, w_out, mlp_norm, w_gate, w_up, w_down):
        batch, shard, dim = hidden.shape
        head_dim = w_key.shape[1]
        rows = batch * shard
        me = lax.axis_index("tp")
        starts = (me ^ jnp.array([0, 2, 4, 6, 1, 3, 5, 7], jnp.int32)) * shard
        k_pos = (starts[:, None] + jnp.arange(shard, dtype=jnp.int32)).reshape(1, tp_size * shard)
        cos_own, sin_own = rope_tables(me * shard + jnp.arange(shard), head_dim)
        hidden = hidden.reshape(rows, dim)
        grad_out = grad_out.reshape(rows, dim)
        normed, wq_all, wo_all, kv_all, query, mixed, resid, gated_in = front_layer(
            prefix_len, valid_len, k_pos, cos_own, sin_own, attn_norm, mlp_norm, hidden, w_query, w_key, w_value, w_out, batch, tp_size)
        wo_all = wo_all.reshape(tp_size * head_dim, dim)

        gated_all, grad_all, act, d_gate, d_upper, diag_in = gated_layer(gated_in, grad_out, w_gate, w_up, w_down, tp_size)
        own_part, x_part, y_part, g_gate_part = back_layer(act, d_gate, d_upper, gated_all, diag_in, w_gate, w_up, w_down, tp_size)
        hidden_out, d_resid, g_mlp_norm_part, d_mixed, g_out_part = join_layer(
            own_part, x_part, y_part, resid, grad_out, mlp_norm, wo_all, mixed)
        g_out = lax.psum_scatter(g_out_part, "tp", scatter_dimension=0, tiled=True)
        lens_back = jnp.concatenate([jnp.stack([prefix_len, valid_len, jnp.full((batch,), me, jnp.int32)]),
                                     jnp.broadcast_to(starts[:, None], (tp_size, batch))])
        d_q_raw, dkv_near, dkv_far = attention_backward(lens_back, cos_own, sin_own, query, kv_all, d_mixed, batch)
        near = tp_size // 2
        came_kv = swap(dkv_far, 1)
        g_far = jnp.einsum("kte,td->ked", d_q_raw[near:], normed, preferred_element_type=F32)
        came_kv, g_far = lax.optimization_barrier((came_kv, g_far))
        came_q = swap(g_far, 1)
        kv_own, kv_side, kv_back, kv_diag = [dkv_near[k].astype(F32) + came_kv[k].astype(F32) for k in range(4)]
        kv_came = hop_diagonal(kv_diag.astype(BF16))
        d_normed_q = jnp.einsum("hte,hde->td", d_q_raw, wq_all, preferred_element_type=F32)
        kv_came, d_normed_q = lax.optimization_barrier((kv_came, d_normed_q))
        kv_next = hop_near(kv_side, kv_back, *kv_came)
        kv_last = (swap(kv_next[0], 2), swap(kv_next[1], 4))
        came_q, dq_near = lax.optimization_barrier((came_q, d_q_raw[:near]))
        g_query_sum = jnp.einsum("kte,td->ked", dq_near, normed, preferred_element_type=F32) + came_q
        g_query_sum, act = lax.optimization_barrier((g_query_sum, act))
        q_came = hop_diagonal(g_query_sum[3])
        g_down = weight_grad(act, grad_all)
        kv_last, q_came, g_down = lax.optimization_barrier((kv_last, q_came, g_down))
        q_next = hop_near(g_query_sum[1], g_query_sum[2], *q_came)
        g_key_part, g_value_part, grad_hidden = finish_layer(
            kv_own, kv_last[0], kv_last[1], cos_own, sin_own, normed, w_key, w_value, d_normed_q, hidden, d_resid, attn_norm, g_mlp_norm_part)
        parts = (g_key_part, g_value_part)
        q_next, parts, d_gate = lax.optimization_barrier((q_next, parts, d_gate))
        g_key, g_value = lax.psum(parts, "tp")
        last_side = swap(q_next[0], 2)
        q_last = (last_side, swap(q_next[1], 4))
        g_gate = weight_grad_rest(gated_all, d_gate, g_gate_part, 6 * rows)
        d_upper, g_gate = lax.optimization_barrier((d_upper, g_gate))
        g_up = weight_grad(gated_all, d_upper)
        q_last, g_up = lax.optimization_barrier((q_last, g_up))
        g_query = (g_query_sum[0] + q_last[0] + q_last[1]).T
        g_attn_norm, g_mlp_norm = g_value[dim:].reshape(2, dim)
        g_value = g_value[:dim]
        full = (batch, shard, dim)
        return (hidden_out.reshape(full), grad_hidden.reshape(full), g_attn_norm, g_query, g_key, g_value, g_out, g_mlp_norm, g_gate, g_up, g_down)

    return jax.shard_map(layer, mesh=mesh, in_specs=in_specs, out_specs=out_specs, check_vma=False)
```
